32 devices in a mesh: dp: 4 (over z), expert: 8 (over y, x, core).
Axes of the slice: x: 2, y: 2, z: 4, core: 2. Of those that a mesh axis runs over, the one named last changes fastest.
Arguments:
- hidden_in: bfloat16 [8192, 2048], P(('dp', 'expert')), may hold values from -8 to 8
- segment_ids: int32 [8192], P(('dp', 'expert')), may hold values from 0 to 127, never falling along the last dimension, each value on 1 to 256 neighbouring positions
- expert_ids: int32 [8192, 8], P(('dp', 'expert')), may hold values from 0 to 31, as said below
- attn_gain: bfloat16 [2048], P(('dp', 'expert')), may hold values from 0.5 to 1.5
- query_gain: bfloat16 [128], P(('dp', 'expert')), may hold values from 0.5 to 1.5
- key_gain: bfloat16 [128], P(('dp', 'expert')), may hold values from 0.5 to 1.5
- w_query: bfloat16 [2048, 4096], P(('dp', 'expert')), may hold values from -0.125 to 0.125
- w_key: bfloat16 [2048, 512], P(('dp', 'expert')), may hold values from -0.125 to 0.125
- w_value: bfloat16 [2048, 512], P(('dp', 'expert')), may hold values from -0.125 to 0.125
- w_output: bfloat16 [4096, 2048], P(('dp', 'expert')), may hold values from -0.375 to 0.375
- mlp_gain: bfloat16 [2048], P(('dp', 'expert')), may hold values from 0.5 to 1.5
- w_router: bfloat16 [2048, 32], P(('dp', 'expert')), may hold values from -0.019897461 to 0.019897461
- w_gate: bfloat16 [32, 2048, 768], P(('dp', 'expert')), may hold values from -0.125 to 0.125
- w_up: bfloat16 [32, 2048, 768], P(('dp', 'expert')), may hold values from -0.125 to 0.125
- w_down: bfloat16 [32, 768, 2048], P(('dp', 'expert')), may hold values from -0.875 to 0.875
- out_grad: bfloat16 [8192, 2048], P(('dp', 'expert')), may hold values from -6 to 6
Outputs:
- block_out: float32 [8192, 2048], P(('dp', 'expert'))
- grad_in: float32 [8192, 2048], P(('dp', 'expert'))
- grad_attn_gain: float32 [2048], P(('dp', 'expert'))
- grad_query_gain: float32 [128], P(('dp', 'expert'))
- grad_key_gain: float32 [128], P(('dp', 'expert'))
- grad_w_query: float32 [2048, 4096], P(('dp', 'expert'))
- grad_w_key: float32 [2048, 512], P(('dp', 'expert'))
- grad_w_value: float32 [2048, 512], P(('dp', 'expert'))
- grad_w_output: float32 [4096, 2048], P(('dp', 'expert'))
- grad_mlp_gain: float32 [2048], P(('dp', 'expert'))
- grad_w_router: float32 [2048, 32], P(('dp', 'expert'))
- grad_w_gate: float32 [32, 2048, 768], P(('dp', 'expert'))
- grad_w_up: float32 [32, 2048, 768], P(('dp', 'expert'))
- grad_w_down: float32 [32, 768, 2048], P(('dp', 'expert'))
The draws below stay inside these ranges and needn't reach their ends.
Inputs may be any that keep to these rules, and one draw needn't show every extreme that they name: `expert_ids`: each row names 8 different experts. On one device the experts fall into 4 groups of 8, and each row names all experts of one group. The rows of one device name each expert at least 26 and at most 80 times; one expert is named exactly 80 times by the rows of every device.
All inputs are finite; a program needn't handle non-finite values.
Results may differ from the reference program's by a relative error of at most 0.02.
Values may be sent and summed in bfloat16 or wider, within the bound.
A program may use at most 384 MiB of HBM per device.

```python
import math
from functools import partial
import jax
import jax.numpy as jnp
import numpy as np
from jax import lax

D = 2048
HEADS = 32
KV_HEADS = 4
HEAD_DIM = 128
FF = 768
TOP = 8
TOK_DEV = 256
EXPERTS = 32
TOKENS = 8192
CAP = 80
N_DP = 4
N_EXPERT = 8


def draw_hidden_in(key, part):
    key_rows, key_cols, key_base = jax.random.split(key, 3)
    row_scale = jnp.exp(jax.random.uniform(key_rows, (TOKENS, 1), jnp.float32, math.log(0.3), math.log(3.0)))
    column_scale = jnp.exp(jax.random.uniform(key_cols, (1, D), jnp.float32, math.log(0.3), math.log(3.0)))
    base_draw = jax.random.normal(key_base, (TOKENS, D), jnp.float32)
    return jnp.clip(base_draw * row_scale * column_scale, -8.0, 8.0).astype(jnp.bfloat16)


def draw_expert_ids(key, part):
    block_count = TOKENS // TOK_DEV
    group_count = EXPERTS // TOP
    mean_load = TOK_DEV // group_count
    spread = CAP - mean_load
    key_hot, key_pair, key_rest = jax.random.split(jax.random.fold_in(key, 17), 3)
    hot_pair = jax.random.randint(key_pair, (), 0, group_count // 2)
    hot_expert = jax.random.randint(key_hot, (), 0, EXPERTS)
    pair_index = jnp.arange(group_count // 2)
    position = jnp.arange(TOK_DEV)

    def one_block(block_key):
        key_delta, key_order, key_place = jax.random.split(block_key, 3)
        load_delta = jax.random.randint(key_delta, (group_count // 2,), 0, spread + 1)
        load_delta = jnp.where(pair_index == hot_pair, spread, load_delta)
        class_loads = jnp.stack([mean_load + load_delta, mean_load - load_delta], 1).reshape(group_count)
        bounds = jnp.cumsum(class_loads)
        class_label = jnp.sum((position[:, None] >= bounds[None, :]).astype(jnp.int32), 1)
        class_label = class_label[jax.random.permutation(key_place, TOK_DEV)]
        expert_order = jax.random.permutation(key_order, EXPERTS)
        hot_class = 2 * hot_pair
        expert_order = jnp.where(expert_order == hot_expert, expert_order[hot_class], expert_order)
        expert_order = expert_order.at[hot_class].set(hot_expert)
        slot_index = class_label[:, None] + group_count * jnp.arange(TOP)[None, :]
        return expert_order[slot_index]
    block_keys = jax.random.split(key_rest, block_count)
    return jax.vmap(one_block)(block_keys).reshape(TOKENS, TOP).astype(jnp.int32)


def steps_of(key, extent, shards, low, high):
    def one(dim, blocks):
        steps = jax.random.uniform(jax.random.fold_in(jax.random.fold_in(key, 6), dim), (blocks,), jnp.float32, low / len(shards), high / len(shards))
        return jnp.repeat(jnp.exp(steps), extent[dim] // blocks).reshape((-1,) + (1,) * (len(extent) - dim - 1))

    gain = one(*shards[0])
    for cut in shards[1:]:
        gain = gain * one(*cut)
    return gain


def length_profile(number_of, total, most, skew):
    portions = [(1 << 20) // math.isqrt(standing ** skew) + 1 for standing in range(2, number_of + 1)]
    surplus, given = total - most - (number_of - 1), [1] * (number_of - 1)
    while surplus > 0:
        movable = [i for i in range(number_of - 1) if given[i] < most]
        mass, left = sum([portions[i] for i in movable]), surplus
        for i in movable:
            addition = min(most - given[i], max(1, left * portions[i] // mass), surplus)
            given[i] = given[i] + addition
            surplus = surplus - addition
    return np.array([most] + given)


def uneven_parts(key, count, total, reach, skew):
    if count == 2:
        one = jax.random.randint(key, (), max(1, total - reach), min(reach, total - 1) + 1)
        return jnp.stack([one, total - one])
    tallies = jnp.asarray(length_profile(count, total, reach, skew), jnp.int32)
    couples = (count - 1) // 2
    source_of, sink = tallies[1:1 + 2 * couples:2], tallies[2:2 + 2 * couples:2]
    room = jnp.minimum(source_of - 1, reach - sink)
    shifted = jax.random.randint(jax.random.fold_in(key, 1), (couples,), 0, 1 << 20) % (room + 1)
    tallies = tallies.at[1:1 + 2 * couples:2].set(source_of - shifted).at[2:2 + 2 * couples:2].set(sink + shifted)
    return tallies[jax.random.permutation(jax.random.fold_in(key, 2), count)]


def bell_draw(own_key, extent, scale, reach, pieces=(), held_as=jnp.bfloat16):
    values = scale * jax.random.normal(own_key, extent, jnp.float32)
    if pieces:
        values = values * steps_of(own_key, extent, pieces, -0.22, 0.18)
    return jnp.clip(values, -reach, reach).astype(held_as)


def setup_inputs(seed: int = 0) -> dict:
    arg_keys = jax.random.split(jax.random.key(seed), 17)
    hidden_in = draw_hidden_in(jax.random.fold_in(arg_keys[16], 71), 0)
    segment_ids = jnp.searchsorted(jnp.cumsum(uneven_parts(arg_keys[1], 4 * TOKENS // TOK_DEV, TOKENS, TOK_DEV, 2)), jnp.arange(TOKENS), side="right").astype(jnp.int32)
    expert_ids = draw_expert_ids(jax.random.fold_in(arg_keys[16], 71), 0)
    attn_gain = jnp.clip(1.0 + 0.1 * jax.random.normal(arg_keys[3], (D,), jnp.float32), 0.5, 1.5).astype(jnp.bfloat16)
    query_gain = jnp.clip(1.0 + 0.1 * jax.random.normal(arg_keys[4], (HEAD_DIM,), jnp.float32), 0.5, 1.5).astype(jnp.bfloat16)
    key_gain = jnp.clip(1.0 + 0.1 * jax.random.normal(arg_keys[5], (HEAD_DIM,), jnp.float32), 0.5, 1.5).astype(jnp.bfloat16)
    w_query = bell_draw(arg_keys[6], (D, HEADS * HEAD_DIM), D ** -0.5, 0.125, ((0, 32),))
    w_key = bell_draw(arg_keys[7], (D, KV_HEADS * HEAD_DIM), D ** -0.5, 0.125, ((0, 32),))
    w_value = bell_draw(arg_keys[8], (D, KV_HEADS * HEAD_DIM), D ** -0.5, 0.125, ((0, 32),))
    w_output = bell_draw(arg_keys[9], (HEADS * HEAD_DIM, D), (HEADS * HEAD_DIM // 16) ** -0.5, 0.375, ((0, 32),))
    mlp_gain = jnp.clip(1.0 + 0.1 * jax.random.normal(arg_keys[10], (D,), jnp.float32), 0.5, 1.5).astype(jnp.bfloat16)
    w_router = jnp.clip(jax.random.uniform(arg_keys[11], (D, EXPERTS), jnp.float32, -0.019897461, 0.019897461) * steps_of(arg_keys[11], (D, EXPERTS), ((0, 32),), -0.4, 0.0), -0.019897461, 0.019897461).astype(jnp.bfloat16)
    w_gate = bell_draw(arg_keys[12], (EXPERTS, D, FF), D ** -0.5, 0.125, ((0, 32),))
    w_up = bell_draw(arg_keys[13], (EXPERTS, D, FF), D ** -0.5, 0.125, ((0, 32),))
    w_down = bell_draw(arg_keys[14], (EXPERTS, FF, D), (FF // 16) ** -0.5, 0.875, ((0, 32),))
    out_grad = bell_draw(arg_keys[15], (TOKENS, D), 1.0, 6.0, ((0, 32),))
    return dict(hidden_in=hidden_in, segment_ids=segment_ids, expert_ids=expert_ids, attn_gain=attn_gain, query_gain=query_gain, key_gain=key_gain, w_query=w_query, w_key=w_key, w_value=w_value, w_output=w_output, mlp_gain=mlp_gain, w_router=w_router, w_gate=w_gate, w_up=w_up, w_down=w_down, out_grad=out_grad)


EPS = 1e-06
ROPE_BASE = 1000000.0

def to_wide(low_values):
    return lax.optimization_barrier(low_values).astype(jnp.float32)

def rms_scale(values):
    return lax.rsqrt(lax.optimization_barrier(jnp.mean(values * values, -1, keepdims=True)) + EPS)

def norm_grad(upstream, values, inverse, gain_vec):
    weighted = upstream * gain_vec
    return inverse * weighted - values * inverse ** 3 * lax.optimization_barrier(jnp.mean(weighted * values, -1, keepdims=True))

def rope_tables(positions, head_dim):
    half_dim = head_dim // 2
    frequency = ROPE_BASE ** (-(jnp.arange(half_dim).astype(jnp.float32) * 2.0 / head_dim))
    angles = positions.astype(jnp.float32)[:, None] * frequency[None, :]
    return (jnp.cos(angles)[:, None, :], jnp.sin(angles)[:, None, :])

def rotate(values, cosine_table, sine_table):
    half_dim = values.shape[-1] // 2
    first_half = values[..., :half_dim]
    second_half = values[..., half_dim:]
    return jnp.concatenate([first_half * cosine_table - second_half * sine_table, second_half * cosine_table + first_half * sine_table], -1)

def unrotate(values, cosine_table, sine_table):
    half_dim = values.shape[-1] // 2
    first_half = values[..., :half_dim]
    second_half = values[..., half_dim:]
    return jnp.concatenate([first_half * cosine_table + second_half * sine_table, second_half * cosine_table - first_half * sine_table], -1)

def attend(query_rot, key_rot, value_rows, allowed):
    score_scale = 1.0 / math.sqrt(HEAD_DIM)
    scores = jnp.einsum('qkgd,tkd->kgqt', to_wide(query_rot), to_wide(key_rot)) * score_scale
    exp_scores = jnp.where(allowed, jnp.exp(scores), 0.0)
    totals = lax.optimization_barrier(jnp.sum(exp_scores, -1, keepdims=True))
    probs_low = (exp_scores / totals).astype(jnp.bfloat16)
    attended = jnp.einsum('kgqt,tkd->qkgd', to_wide(probs_low), to_wide(value_rows)).astype(jnp.bfloat16)
    return (attended, jnp.log(totals))

def attend_grad(query_rot, key_rot, value_rows, allowed, log_totals, attended_grad):
    score_scale = 1.0 / math.sqrt(HEAD_DIM)
    scores = jnp.einsum('qkgd,tkd->kgqt', to_wide(query_rot), to_wide(key_rot)) * score_scale
    probs_back = jnp.where(allowed, jnp.exp(scores - log_totals), 0.0)
    probs_wide = to_wide(probs_back.astype(jnp.bfloat16))
    grad_wide = to_wide(attended_grad)
    value_sum_grad = jnp.einsum('kgqt,qkgd->tkd', probs_wide, grad_wide)
    prob_grad = jnp.einsum('qkgd,tkd->kgqt', grad_wide, to_wide(value_rows))
    score_grad = probs_back * (prob_grad - lax.optimization_barrier(jnp.sum(probs_back * prob_grad, -1, keepdims=True)))
    score_wide = to_wide(score_grad.astype(jnp.bfloat16))
    query_rot_grad = jnp.einsum('kgqt,tkd->qkgd', score_wide, to_wide(key_rot)) * score_scale
    key_rot_grad = jnp.einsum('kgqt,qkgd->tkd', score_wide, to_wide(query_rot)) * score_scale
    return (query_rot_grad, key_rot_grad, value_sum_grad)

def mixer_forward(block_in, block_segments, weights):
    w_query, w_key, w_value, w_output, w_router, attn_gain, mlp_gain, query_gain, key_gain = weights
    row_count = block_in.shape[0]
    seq_count = row_count // TOK_DEV
    group_size = HEADS // KV_HEADS
    plain_in = block_in.astype(jnp.float32)
    inv_attn = rms_scale(plain_in)
    normed_attn = (plain_in * inv_attn * attn_gain).astype(jnp.bfloat16)
    query_raw = jnp.dot(normed_attn, w_query, preferred_element_type=jnp.float32).reshape(row_count, HEADS, HEAD_DIM)
    key_raw = jnp.dot(normed_attn, w_key, preferred_element_type=jnp.float32).reshape(row_count, KV_HEADS, HEAD_DIM)
    value_rows = jnp.dot(normed_attn, w_value, preferred_element_type=jnp.float32).astype(jnp.bfloat16)
    value_rows = value_rows.reshape(seq_count, TOK_DEV, KV_HEADS, HEAD_DIM)
    query_scale = rms_scale(query_raw)
    key_scale = rms_scale(key_raw)
    cosine_table, sine_table = rope_tables(jnp.arange(row_count) % TOK_DEV, HEAD_DIM)
    query_rot = rotate(query_raw * query_scale * query_gain, cosine_table, sine_table).astype(jnp.bfloat16)
    query_rot = query_rot.reshape(seq_count, TOK_DEV, KV_HEADS, group_size, HEAD_DIM)
    key_rot = rotate(key_raw * key_scale * key_gain, cosine_table, sine_table).astype(jnp.bfloat16)
    key_rot = key_rot.reshape(seq_count, TOK_DEV, KV_HEADS, HEAD_DIM)
    segments = block_segments.reshape(seq_count, TOK_DEV)
    position = jnp.arange(TOK_DEV)
    allowed = (segments[:, :, None] == segments[:, None, :]) & (position[None, None, :] <= position[None, :, None])
    attended, log_totals = jax.vmap(attend)(query_rot, key_rot, value_rows, allowed)
    attended = attended.reshape(row_count, HEADS * HEAD_DIM)
    residual = plain_in + jnp.dot(attended, w_output, preferred_element_type=jnp.float32)
    saved_state = (plain_in, inv_attn, normed_attn, query_raw, key_raw, value_rows, query_scale, key_scale, query_rot, key_rot, allowed, log_totals, attended, cosine_table, sine_table)
    return (residual, saved_state)

def mixer_backward(residual_grad, saved_state, weights):
    w_query, w_key, w_value, w_output, w_router, attn_gain, mlp_gain, query_gain, key_gain = weights
    plain_in, inv_attn, normed_attn, query_raw, key_raw, value_rows, query_scale, key_scale, query_rot, key_rot, allowed, log_totals, attended, cosine_table, sine_table = saved_state
    row_count = residual_grad.shape[0]
    seq_count = row_count // TOK_DEV
    group_size = HEADS // KV_HEADS
    branch_grad = residual_grad.astype(jnp.bfloat16)
    grad_w_output = jnp.dot(attended.T, branch_grad, preferred_element_type=jnp.float32)
    attended_grad = jnp.dot(branch_grad, w_output.T, preferred_element_type=jnp.float32).astype(jnp.bfloat16)
    attended_grad = attended_grad.reshape(seq_count, TOK_DEV, KV_HEADS, group_size, HEAD_DIM)
    query_rot_grad, key_rot_grad, value_sum_grad = jax.vmap(attend_grad)(query_rot, key_rot, value_rows, allowed, log_totals, attended_grad)
    query_normed_grad = unrotate(query_rot_grad.reshape(row_count, HEADS, HEAD_DIM), cosine_table, sine_table)
    key_normed_grad = unrotate(key_rot_grad.reshape(row_count, KV_HEADS, HEAD_DIM), cosine_table, sine_table)
    grad_query_gain = lax.optimization_barrier(jnp.sum(query_normed_grad * query_raw * query_scale, (0, 1)))
    grad_key_gain = lax.optimization_barrier(jnp.sum(key_normed_grad * key_raw * key_scale, (0, 1)))
    query_grad = norm_grad(query_normed_grad, query_raw, query_scale, query_gain).astype(jnp.bfloat16)
    query_grad = query_grad.reshape(row_count, HEADS * HEAD_DIM)
    key_grad = norm_grad(key_normed_grad, key_raw, key_scale, key_gain).astype(jnp.bfloat16)
    key_grad = key_grad.reshape(row_count, KV_HEADS * HEAD_DIM)
    value_grad = value_sum_grad.astype(jnp.bfloat16).reshape(row_count, KV_HEADS * HEAD_DIM)
    grad_w_query = jnp.dot(normed_attn.T, query_grad, preferred_element_type=jnp.float32)
    grad_w_key = jnp.dot(normed_attn.T, key_grad, preferred_element_type=jnp.float32)
    grad_w_value = jnp.dot(normed_attn.T, value_grad, preferred_element_type=jnp.float32)
    normed_attn_grad = jnp.dot(query_grad, w_query.T, preferred_element_type=jnp.float32) + jnp.dot(key_grad, w_key.T, preferred_element_type=jnp.float32) + jnp.dot(value_grad, w_value.T, preferred_element_type=jnp.float32)
    grad_attn_gain = lax.optimization_barrier(jnp.sum(normed_attn_grad * plain_in * inv_attn, 0))
    grad_in = residual_grad + norm_grad(normed_attn_grad, plain_in, inv_attn, attn_gain)
    return (grad_in, (grad_attn_gain, grad_query_gain, grad_key_gain, grad_w_query, grad_w_key, grad_w_value, grad_w_output))

def dispatch_table(expert_rows, experts, capacity):
    length, choices = expert_rows.shape
    flat_ids = expert_rows.reshape(length * choices)
    marks = (flat_ids[:, None] == jnp.arange(experts)[None, :]).astype(jnp.int32)
    earlier = jnp.cumsum(marks, 0) - marks
    destination = flat_ids * capacity + lax.optimization_barrier(jnp.sum(earlier * marks, -1))
    pair_ids = jnp.zeros((experts * capacity,), jnp.int32).at[destination].set(jnp.arange(length * choices).astype(jnp.int32))
    filled = jnp.zeros((experts * capacity,), jnp.float32).at[destination].set(1.0)
    return (destination, pair_ids, filled)

def reference(hidden_in, segment_ids, expert_ids, attn_gain, query_gain, key_gain, w_query, w_key, w_value, w_output, mlp_gain, w_router, w_gate, w_up, w_down, out_grad):
    weights = (w_query, w_key, w_value, w_output, w_router, attn_gain, mlp_gain, query_gain, key_gain)
    devices = N_DP * N_EXPERT
    seq_total = TOKENS // TOK_DEV
    per_block = math.gcd(seq_total, max(1, 4096 // TOK_DEV))
    blocks = seq_total // per_block
    block_rows = per_block * TOK_DEV
    inputs_blocked = hidden_in.reshape(blocks, block_rows, D)
    segments_blocked = segment_ids.reshape(blocks, block_rows)

    def forward_block(running, scan_item):
        block_in, block_segments = scan_item
        return (running, mixer_forward(block_in, block_segments, weights)[0])
    _unused, residual = lax.scan(forward_block, 0, (inputs_blocked, segments_blocked))
    residual = residual.reshape(TOKENS, D)
    inv_mlp = rms_scale(residual)
    normed_mlp = (residual * inv_mlp * mlp_gain).astype(jnp.bfloat16)
    logits = jnp.dot(normed_mlp, w_router, preferred_element_type=jnp.float32)
    chosen = jnp.take_along_axis(logits, expert_ids, 1)
    raised = jnp.exp(chosen)
    gate_weights = raised / lax.optimization_barrier(jnp.sum(raised, -1, keepdims=True))
    cotangent = out_grad.astype(jnp.float32)
    per_device = expert_ids.reshape(devices, TOK_DEV, TOP)
    destination, pair_local, filled = jax.vmap(partial(dispatch_table, experts=EXPERTS, capacity=CAP))(per_device)
    offset = (jnp.arange(devices) * (TOK_DEV * TOP)).astype(jnp.int32)
    pair_table = (pair_local + offset[:, None]).reshape(devices, EXPERTS, CAP)
    pair_table = jnp.transpose(pair_table, (1, 0, 2)).reshape(EXPERTS, devices * CAP)
    live_slots = jnp.transpose(filled.reshape(devices, EXPERTS, CAP), (1, 0, 2)).reshape(EXPERTS, devices * CAP)
    gate_flat = gate_weights.reshape(TOKENS * TOP)

    def per_expert(running, scan_item):
        mixed_out, back_sum, pair_grad = running
        pair_ids, live_rows, gate_proj, up_proj, down_proj = scan_item
        tokens = pair_ids // TOP
        rows_in = normed_mlp[tokens] * live_rows.astype(jnp.bfloat16)[:, None]
        pre_gate = jnp.dot(rows_in, gate_proj, preferred_element_type=jnp.float32)
        pre_up = jnp.dot(rows_in, up_proj, preferred_element_type=jnp.float32)
        gate_sigmoid = jax.nn.sigmoid(pre_gate)
        silu_gate = pre_gate * gate_sigmoid
        activation = (silu_gate * pre_up).astype(jnp.bfloat16)
        out_rows = jnp.dot(activation, down_proj, preferred_element_type=jnp.float32).astype(jnp.bfloat16)
        pair_weight = gate_flat[pair_ids] * live_rows
        mixed_out = mixed_out.at[tokens].add(pair_weight[:, None] * out_rows.astype(jnp.float32))
        token_cot = cotangent[tokens]
        pair_grad = pair_grad.at[pair_ids].add(live_rows * lax.optimization_barrier(jnp.sum(token_cot * out_rows.astype(jnp.float32), -1)))
        down_in = (pair_weight[:, None] * token_cot).astype(jnp.bfloat16)
        act_grad = jnp.dot(down_in, down_proj.T, preferred_element_type=jnp.float32)
        grad_down = jnp.dot(activation.T, down_in, preferred_element_type=jnp.float32)
        gate_pre_grad = (act_grad * pre_up * gate_sigmoid * (1.0 + pre_gate * (1.0 - gate_sigmoid))).astype(jnp.bfloat16)
        up_pre_grad = (act_grad * silu_gate).astype(jnp.bfloat16)
        grad_gate = jnp.dot(rows_in.T, gate_pre_grad, preferred_element_type=jnp.float32)
        grad_up = jnp.dot(rows_in.T, up_pre_grad, preferred_element_type=jnp.float32)
        row_grad = (jnp.dot(gate_pre_grad, gate_proj.T, preferred_element_type=jnp.float32) + jnp.dot(up_pre_grad, up_proj.T, preferred_element_type=jnp.float32)).astype(jnp.bfloat16)
        back_sum = back_sum.at[tokens].add(live_rows[:, None] * row_grad.astype(jnp.float32))
        return ((mixed_out, back_sum, pair_grad), (grad_gate, grad_up, grad_down))
    start_state = (jnp.zeros((TOKENS, D), jnp.float32), jnp.zeros((TOKENS, D), jnp.float32), jnp.zeros((TOKENS * TOP,), jnp.float32))
    (mixed_out, back_sum, pair_grad), (grad_w_gate, grad_w_up, grad_w_down) = lax.scan(per_expert, start_state, (pair_table, live_slots, w_gate, w_up, w_down))
    block_out = residual + mixed_out
    gate_grad = pair_grad.reshape(TOKENS, TOP)
    sel_grad = gate_weights * (gate_grad - lax.optimization_barrier(jnp.sum(gate_weights * gate_grad, -1, keepdims=True)))
    one_hot = expert_ids[:, :, None] == jnp.arange(EXPERTS)[None, None, :]
    logit_grad = lax.optimization_barrier(jnp.sum(jnp.where(one_hot, sel_grad[:, :, None], 0.0), 1)).astype(jnp.bfloat16)
    grad_w_router = jnp.dot(normed_mlp.T, logit_grad, preferred_element_type=jnp.float32)
    normed_mlp_grad = back_sum + jnp.dot(logit_grad, w_router.T, preferred_element_type=jnp.float32)
    grad_mlp_gain = lax.optimization_barrier(jnp.sum(normed_mlp_grad * residual * inv_mlp, 0))
    residual_grad = cotangent + norm_grad(normed_mlp_grad, residual, inv_mlp, mlp_gain)

    def backward_block(running, scan_item):
        block_in, block_segments, block_grad = scan_item
        saved_state = mixer_forward(block_in, block_segments, weights)[1]
        grad_block, grads = mixer_backward(block_grad, saved_state, weights)
        running = jax.tree.map(lambda total_sum, addend: total_sum + addend, running, grads)
        return (running, grad_block)
    zero_grads = (jnp.zeros((D,), jnp.float32), jnp.zeros((HEAD_DIM,), jnp.float32), jnp.zeros((HEAD_DIM,), jnp.float32), jnp.zeros((D, HEADS * HEAD_DIM), jnp.float32), jnp.zeros((D, KV_HEADS * HEAD_DIM), jnp.float32), jnp.zeros((D, KV_HEADS * HEAD_DIM), jnp.float32), jnp.zeros((HEADS * HEAD_DIM, D), jnp.float32))
    mixer_sums, grad_in = lax.scan(backward_block, zero_grads, (inputs_blocked, segments_blocked, residual_grad.reshape(blocks, block_rows, D)))
    grad_attn_gain, grad_query_gain, grad_key_gain, grad_w_query, grad_w_key, grad_w_value, grad_w_output = mixer_sums
    return (block_out, grad_in.reshape(TOKENS, D), grad_attn_gain, grad_query_gain, grad_key_gain, grad_w_query, grad_w_key, grad_w_value, grad_w_output, grad_mlp_gain, grad_w_router, grad_w_gate, grad_w_up, grad_w_down)
```

```python
import functools
import math

import jax
import jax.numpy as jnp
from jax import lax
from jax.experimental import pallas as pl
from jax.experimental.pallas import tpu as pltpu
from jax.sharding import PartitionSpec as P

F32, BF16 = jnp.float32, jnp.bfloat16
MESH = pl.DeviceIdType.MESH
VMEM_LIMIT = 63 * 1024 * 1024


HEADS = 32
KV_HEADS = 4
HEAD_DIM = 128
TOK_DEV = 256


EPS = 1e-06
ROPE_BASE = 1000000.0


def rms_scale(values):
    return lax.rsqrt(jnp.mean(values * values, -1, keepdims=True) + EPS)


def norm_grad(upstream, values, inverse, gain_vec):
    weighted = upstream * gain_vec
    return inverse * weighted - values * inverse**3 * jnp.mean(weighted * values, -1, keepdims=True)


def rope_tables(positions, head_dim):
    half_dim = head_dim // 2
    frequency = ROPE_BASE ** (-(jnp.arange(half_dim).astype(jnp.float32) * 2.0 / head_dim))
    angles = positions.astype(jnp.float32)[:, None] * frequency[None, :]
    return (jnp.cos(angles)[:, None, :], jnp.sin(angles)[:, None, :])


def rotate(values, cosine_table, sine_table):
    half_dim = values.shape[-1] // 2
    first_half = values[..., :half_dim]
    second_half = values[..., half_dim:]
    return jnp.concatenate(
        [
            first_half * cosine_table - second_half * sine_table,
            second_half * cosine_table + first_half * sine_table,
        ],
        -1,
    )


def unrotate(values, cosine_table, sine_table):
    half_dim = values.shape[-1] // 2
    first_half = values[..., :half_dim]
    second_half = values[..., half_dim:]
    return jnp.concatenate(
        [
            first_half * cosine_table + second_half * sine_table,
            second_half * cosine_table - first_half * sine_table,
        ],
        -1,
    )


def attend(query_rot, key_rot, value_rows, allowed):
    score_scale = 1.0 / math.sqrt(HEAD_DIM)
    scores = (
        jnp.einsum("qkgd,tkd->kgqt", query_rot, key_rot, preferred_element_type=jnp.float32)
        * score_scale
    )
    exp_scores = jnp.where(allowed, jnp.exp(scores), 0.0)
    totals = jnp.sum(exp_scores, -1, keepdims=True)
    probs_low = (exp_scores / totals).astype(jnp.bfloat16)
    attended = jnp.einsum(
        "kgqt,tkd->qkgd", probs_low, value_rows, preferred_element_type=jnp.float32
    ).astype(jnp.bfloat16)
    return (attended, jnp.log(totals))


def attend_grad(query_rot, key_rot, value_rows, allowed, log_totals, attended_grad):
    score_scale = 1.0 / math.sqrt(HEAD_DIM)
    scores = (
        jnp.einsum("qkgd,tkd->kgqt", query_rot, key_rot, preferred_element_type=jnp.float32)
        * score_scale
    )
    probs_back = jnp.where(allowed, jnp.exp(scores - log_totals), 0.0)
    probs_low = probs_back.astype(jnp.bfloat16)
    value_sum_grad = jnp.einsum(
        "kgqt,qkgd->tkd", probs_low, attended_grad, preferred_element_type=jnp.float32
    )
    prob_grad = jnp.einsum(
        "qkgd,tkd->kgqt", attended_grad, value_rows, preferred_element_type=jnp.float32
    )
    score_grad = (
        probs_back * (prob_grad - jnp.sum(probs_back * prob_grad, -1, keepdims=True))
    ).astype(jnp.bfloat16)
    query_rot_grad = (
        jnp.einsum("kgqt,tkd->qkgd", score_grad, key_rot, preferred_element_type=jnp.float32)
        * score_scale
    )
    key_rot_grad = (
        jnp.einsum("kgqt,qkgd->tkd", score_grad, query_rot, preferred_element_type=jnp.float32)
        * score_scale
    )
    return (query_rot_grad, key_rot_grad, value_sum_grad)


def mixer_forward(block_in, block_segments, weights):
    w_query, w_key, w_value, w_output, w_router, attn_gain, mlp_gain, query_gain, key_gain = weights
    row_count = block_in.shape[0]
    seq_count = row_count // TOK_DEV
    group_size = HEADS // KV_HEADS
    plain_in = block_in.astype(jnp.float32)
    inv_attn = rms_scale(plain_in)
    normed_attn = (plain_in * inv_attn * attn_gain).astype(jnp.bfloat16)
    query_raw = jnp.dot(normed_attn, w_query, preferred_element_type=jnp.float32).reshape(
        row_count, HEADS, HEAD_DIM
    )
    key_raw = jnp.dot(normed_attn, w_key, preferred_element_type=jnp.float32).reshape(
        row_count, KV_HEADS, HEAD_DIM
    )
    value_rows = jnp.dot(normed_attn, w_value, preferred_element_type=jnp.float32).astype(
        jnp.bfloat16
    )
    value_rows = value_rows.reshape(seq_count, TOK_DEV, KV_HEADS, HEAD_DIM)
    query_scale = rms_scale(query_raw)
    key_scale = rms_scale(key_raw)
    cosine_table, sine_table = rope_tables(jnp.arange(row_count) % TOK_DEV, HEAD_DIM)
    query_rot = rotate(query_raw * query_scale * query_gain, cosine_table, sine_table).astype(
        jnp.bfloat16
    )
    query_rot = query_rot.reshape(seq_count, TOK_DEV, KV_HEADS, group_size, HEAD_DIM)
    key_rot = rotate(key_raw * key_scale * key_gain, cosine_table, sine_table).astype(jnp.bfloat16)
    key_rot = key_rot.reshape(seq_count, TOK_DEV, KV_HEADS, HEAD_DIM)
    segments = block_segments.reshape(seq_count, TOK_DEV)
    position = jnp.arange(TOK_DEV)
    allowed = (segments[:, :, None] == segments[:, None, :]) & (
        position[None, None, :] <= position[None, :, None]
    )
    attended, log_totals = jax.vmap(attend)(query_rot, key_rot, value_rows, allowed)
    attended = attended.reshape(row_count, HEADS * HEAD_DIM)
    residual = plain_in + jnp.dot(attended, w_output, preferred_element_type=jnp.float32)
    saved_state = (
        plain_in,
        inv_attn,
        normed_attn,
        query_raw,
        key_raw,
        value_rows,
        query_scale,
        key_scale,
        query_rot,
        key_rot,
        allowed,
        log_totals,
        attended,
        cosine_table,
        sine_table,
    )
    return (residual, saved_state)


def mixer_backward(residual_grad, saved_state, weights):
    w_query, w_key, w_value, w_output, w_router, attn_gain, mlp_gain, query_gain, key_gain = weights
    (
        plain_in,
        inv_attn,
        normed_attn,
        query_raw,
        key_raw,
        value_rows,
        query_scale,
        key_scale,
        query_rot,
        key_rot,
        allowed,
        log_totals,
        attended,
        cosine_table,
        sine_table,
    ) = saved_state
    row_count = residual_grad.shape[0]
    seq_count = row_count // TOK_DEV
    group_size = HEADS // KV_HEADS
    branch_grad = residual_grad.astype(jnp.bfloat16)
    grad_w_output = jnp.dot(attended.T, branch_grad, preferred_element_type=jnp.float32)
    attended_grad = jnp.dot(branch_grad, w_output.T, preferred_element_type=jnp.float32).astype(
        jnp.bfloat16
    )
    attended_grad = attended_grad.reshape(seq_count, TOK_DEV, KV_HEADS, group_size, HEAD_DIM)
    query_rot_grad, key_rot_grad, value_sum_grad = jax.vmap(attend_grad)(
        query_rot, key_rot, value_rows, allowed, log_totals, attended_grad
    )
    query_normed_grad = unrotate(
        query_rot_grad.reshape(row_count, HEADS, HEAD_DIM), cosine_table, sine_table
    )
    key_normed_grad = unrotate(
        key_rot_grad.reshape(row_count, KV_HEADS, HEAD_DIM), cosine_table, sine_table
    )
    grad_query_gain = jnp.sum(query_normed_grad * query_raw * query_scale, (0, 1))
    grad_key_gain = jnp.sum(key_normed_grad * key_raw * key_scale, (0, 1))
    query_grad = norm_grad(query_normed_grad, query_raw, query_scale, query_gain).astype(
        jnp.bfloat16
    )
    query_grad = query_grad.reshape(row_count, HEADS * HEAD_DIM)
    key_grad = norm_grad(key_normed_grad, key_raw, key_scale, key_gain).astype(jnp.bfloat16)
    key_grad = key_grad.reshape(row_count, KV_HEADS * HEAD_DIM)
    value_grad = value_sum_grad.astype(jnp.bfloat16).reshape(row_count, KV_HEADS * HEAD_DIM)
    grad_w_query = jnp.dot(normed_attn.T, query_grad, preferred_element_type=jnp.float32)
    grad_w_key = jnp.dot(normed_attn.T, key_grad, preferred_element_type=jnp.float32)
    grad_w_value = jnp.dot(normed_attn.T, value_grad, preferred_element_type=jnp.float32)
    normed_attn_grad = (
        jnp.dot(query_grad, w_query.T, preferred_element_type=jnp.float32)
        + jnp.dot(key_grad, w_key.T, preferred_element_type=jnp.float32)
        + jnp.dot(value_grad, w_value.T, preferred_element_type=jnp.float32)
    )
    grad_attn_gain = jnp.sum(normed_attn_grad * plain_in * inv_attn, 0)
    grad_in = residual_grad + norm_grad(normed_attn_grad, plain_in, inv_attn, attn_gain)
    return (
        grad_in,
        (
            grad_attn_gain,
            grad_query_gain,
            grad_key_gain,
            grad_w_query,
            grad_w_key,
            grad_w_value,
            grad_w_output,
        ),
    )


def dispatch_table(expert_rows, experts, capacity):
    length, choices = expert_rows.shape
    flat_ids = expert_rows.reshape(length * choices)
    marks = (flat_ids[:, None] == jnp.arange(experts)[None, :]).astype(jnp.int32)
    earlier = jnp.cumsum(marks, 0) - marks
    destination = flat_ids * capacity + jnp.sum(earlier * marks, -1)
    pair_ids = (
        jnp.zeros((experts * capacity,), jnp.int32)
        .at[destination]
        .set(jnp.arange(length * choices, dtype=jnp.int32))
    )
    filled = jnp.zeros((experts * capacity,), jnp.bfloat16).at[destination].set(1.0)
    return (destination, pair_ids, filled)


def move_rows(row_block, section_name):
    if section_name == "dispatch":
        return lax.all_to_all(row_block, ("dp", "expert"), split_axis=0, concat_axis=0, tiled=True)
    if section_name == "combine":
        return lax.all_to_all(row_block, ("dp", "expert"), split_axis=0, concat_axis=0, tiled=True)
    if section_name == "grad_dispatch":
        return lax.all_to_all(row_block, ("dp", "expert"), split_axis=0, concat_axis=0, tiled=True)
    return lax.all_to_all(row_block, ("dp", "expert"), split_axis=0, concat_axis=0, tiled=True)


def per_device_exchange(
    hidden_in,
    segment_ids,
    expert_ids,
    attn_gain,
    query_gain,
    key_gain,
    w_query,
    w_key,
    w_value,
    w_output,
    mlp_gain,
    w_router,
    w_gate,
    w_up,
    w_down,
    out_grad,
):
    weights = (
        lax.all_gather(w_query, ("dp", "expert"), axis=0, tiled=True),
        lax.all_gather(w_key, ("dp", "expert"), axis=0, tiled=True),
        lax.all_gather(w_value, ("dp", "expert"), axis=0, tiled=True),
        lax.all_gather(w_output, ("dp", "expert"), axis=0, tiled=True),
        lax.all_gather(w_router, ("dp", "expert"), axis=0, tiled=True),
        lax.all_gather(attn_gain, ("dp", "expert"), axis=0, tiled=True),
        lax.all_gather(mlp_gain, ("dp", "expert"), axis=0, tiled=True),
        lax.all_gather(query_gain, ("dp", "expert"), axis=0, tiled=True),
        lax.all_gather(key_gain, ("dp", "expert"), axis=0, tiled=True),
    )
    residual, saved_state = mixer_forward(hidden_in, segment_ids, weights)
    full_router = weights[4]
    full_mlp_gain = weights[6]
    inv_mlp = rms_scale(residual)
    normed_mlp = (residual * inv_mlp * full_mlp_gain).astype(jnp.bfloat16)
    logits = jnp.dot(normed_mlp, full_router, preferred_element_type=jnp.float32)
    device_count = lax.axis_size(("dp", "expert"))
    local_experts = w_gate.shape[0]
    experts = local_experts * device_count
    length, choices = expert_ids.shape
    model_width = hidden_in.shape[1]
    capacity = 5 * length * choices // (4 * experts)
    one_hot = expert_ids[:, :, None] == jnp.arange(experts)[None, None, :]
    chosen = jnp.sum(jnp.where(one_hot, logits[:, None, :], 0.0), -1)
    raised = jnp.exp(chosen)
    gate_weights = raised / jnp.sum(raised, -1, keepdims=True)
    destination, pair_ids, filled = dispatch_table(expert_ids, experts, capacity)
    send_rows = normed_mlp[pair_ids // choices] * filled[:, None]
    received = move_rows(
        send_rows.reshape(device_count, local_experts * capacity, model_width), "dispatch"
    )
    received = received.reshape(device_count, local_experts, capacity, model_width)
    pre_gate = jnp.einsum("secd,edf->secf", received, w_gate, preferred_element_type=jnp.float32)
    pre_up = jnp.einsum("secd,edf->secf", received, w_up, preferred_element_type=jnp.float32)
    gate_sigmoid = jax.nn.sigmoid(pre_gate)
    silu_gate = pre_gate * gate_sigmoid
    activation = (silu_gate * pre_up).astype(jnp.bfloat16)
    expert_out = jnp.einsum(
        "secf,efd->secd", activation, w_down, preferred_element_type=jnp.float32
    ).astype(jnp.bfloat16)
    returned = move_rows(
        expert_out.reshape(device_count, local_experts * capacity, model_width), "combine"
    )
    picked = returned.reshape(experts * capacity, model_width)[destination].reshape(
        length, choices, model_width
    )
    block_out = residual + jnp.sum(gate_weights[:, :, None] * picked.astype(jnp.float32), 1)
    weights = (
        lax.all_gather(w_query, ("dp", "expert"), axis=0, tiled=True),
        lax.all_gather(w_key, ("dp", "expert"), axis=0, tiled=True),
        lax.all_gather(w_value, ("dp", "expert"), axis=0, tiled=True),
        lax.all_gather(w_output, ("dp", "expert"), axis=0, tiled=True),
        lax.all_gather(w_router, ("dp", "expert"), axis=0, tiled=True),
        lax.all_gather(attn_gain, ("dp", "expert"), axis=0, tiled=True),
        lax.all_gather(mlp_gain, ("dp", "expert"), axis=0, tiled=True),
        lax.all_gather(query_gain, ("dp", "expert"), axis=0, tiled=True),
        lax.all_gather(key_gain, ("dp", "expert"), axis=0, tiled=True),
    )
    full_router = weights[4]
    full_mlp_gain = weights[6]
    cotangent = out_grad.astype(jnp.float32)
    gate_grad = jnp.sum(cotangent[:, None, :] * picked.astype(jnp.float32), -1)
    down_in = (
        (gate_weights[:, :, None] * cotangent[:, None, :])
        .astype(jnp.bfloat16)
        .reshape(length * choices, model_width)
    )
    send_grad = down_in[pair_ids] * filled[:, None]
    recv_grad = move_rows(
        send_grad.reshape(device_count, local_experts * capacity, model_width), "grad_dispatch"
    )
    recv_grad = recv_grad.reshape(device_count, local_experts, capacity, model_width)
    act_grad = jnp.einsum("secd,efd->secf", recv_grad, w_down, preferred_element_type=jnp.float32)
    grad_w_down = jnp.einsum(
        "secf,secd->efd", activation, recv_grad, preferred_element_type=jnp.float32
    )
    gate_pre_grad = (
        act_grad * pre_up * gate_sigmoid * (1.0 + pre_gate * (1.0 - gate_sigmoid))
    ).astype(jnp.bfloat16)
    up_pre_grad = (act_grad * silu_gate).astype(jnp.bfloat16)
    grad_w_gate = jnp.einsum(
        "secd,secf->edf", received, gate_pre_grad, preferred_element_type=jnp.float32
    )
    grad_w_up = jnp.einsum(
        "secd,secf->edf", received, up_pre_grad, preferred_element_type=jnp.float32
    )
    row_grad = (
        jnp.einsum("secf,edf->secd", gate_pre_grad, w_gate, preferred_element_type=jnp.float32)
        + jnp.einsum("secf,edf->secd", up_pre_grad, w_up, preferred_element_type=jnp.float32)
    ).astype(jnp.bfloat16)
    row_back = move_rows(
        row_grad.reshape(device_count, local_experts * capacity, model_width), "grad_return"
    )
    row_back = row_back.reshape(experts * capacity, model_width)[destination].reshape(
        length, choices, model_width
    )
    sel_grad = gate_weights * (gate_grad - jnp.sum(gate_weights * gate_grad, -1, keepdims=True))
    logit_grad = jnp.sum(jnp.where(one_hot, sel_grad[:, :, None], 0.0), 1).astype(jnp.bfloat16)
    grad_w_router = jnp.dot(normed_mlp.T, logit_grad, preferred_element_type=jnp.float32)
    normed_mlp_grad = jnp.sum(row_back.astype(jnp.float32), 1) + jnp.dot(
        logit_grad, full_router.T, preferred_element_type=jnp.float32
    )
    grad_mlp_gain = jnp.sum(normed_mlp_grad * residual * inv_mlp, 0)
    residual_grad = cotangent + norm_grad(normed_mlp_grad, residual, inv_mlp, full_mlp_gain)
    grad_in, mixer_terms = mixer_backward(residual_grad, saved_state, weights)
    (
        grad_attn_gain,
        grad_query_gain,
        grad_key_gain,
        grad_w_query,
        grad_w_key,
        grad_w_value,
        grad_w_output,
    ) = mixer_terms
    summed = (
        lax.psum_scatter(grad_w_query, ("dp", "expert"), scatter_dimension=0, tiled=True),
        lax.psum_scatter(grad_w_key, ("dp", "expert"), scatter_dimension=0, tiled=True),
        lax.psum_scatter(grad_w_value, ("dp", "expert"), scatter_dimension=0, tiled=True),
        lax.psum_scatter(grad_w_output, ("dp", "expert"), scatter_dimension=0, tiled=True),
        lax.psum_scatter(grad_w_router, ("dp", "expert"), scatter_dimension=0, tiled=True),
        lax.psum_scatter(grad_attn_gain, ("dp", "expert"), scatter_dimension=0, tiled=True),
        lax.psum_scatter(grad_mlp_gain, ("dp", "expert"), scatter_dimension=0, tiled=True),
        lax.psum_scatter(grad_query_gain, ("dp", "expert"), scatter_dimension=0, tiled=True),
        lax.psum_scatter(grad_key_gain, ("dp", "expert"), scatter_dimension=0, tiled=True),
    )
    (
        share_w_query,
        share_w_key,
        share_w_value,
        share_w_output,
        share_w_router,
        share_attn_gain,
        share_mlp_gain,
        share_query_gain,
        share_key_gain,
    ) = summed
    return (
        block_out,
        grad_in,
        share_attn_gain,
        share_query_gain,
        share_key_gain,
        share_w_query,
        share_w_key,
        share_w_value,
        share_w_output,
        share_mlp_gain,
        share_w_router,
        grad_w_gate,
        grad_w_up,
        grad_w_down,
    )


def place():
    z = lax.axis_index("dp")
    e = lax.axis_index("expert")
    return z, e


def line_order(z, nz, j):
    near = jnp.minimum(z, nz - 1 - z)
    step = (j + 1) // 2
    zigzag = z + (step if j % 2 == 0 else -step)
    tail = jnp.where(z < nz - 1 - z, j, nz - 1 - j)
    return jnp.where(j <= 2 * near, zigzag, tail)


def greet(z, e, nz):
    barrier = pltpu.get_barrier_semaphore()
    for mate in (e ^ 1, e ^ 2, e ^ 4):
        pl.semaphore_signal(barrier, inc=1, device_id=(z, mate), device_id_type=MESH)

    @pl.when(z > 0)
    def _():
        pl.semaphore_signal(barrier, inc=1, device_id=(z - 1, e), device_id_type=MESH)

    @pl.when(z < nz - 1)
    def _():
        pl.semaphore_signal(barrier, inc=1, device_id=(z + 1, e), device_id_type=MESH)

    ends = (z > 0).astype(jnp.int32) + (z < nz - 1).astype(jnp.int32)
    pl.semaphore_wait(barrier, 3 + ends)


class Gather:
    Z, XA, XB, XF, YB, YA, YF, P0, PXA, PXB, PYB, PYA, PDB, PDA = range(14)

    def __init__(self, nz, shards, outs, send, recv, local):
        self.nz, self.shards, self.outs = nz, shards, outs
        self.send, self.recv, self.local = send, recv, local
        self.z, self.e = place()
        self.x, self.y, self.p = self.e ^ 2, self.e ^ 4, self.e ^ 1
        self.d = self.e ^ 6

    def at(self, i, zz, ee, half):
        ref = self.outs[i].at[zz, ee]
        return ref if half is None else ref.at[half]

    def own(self, i, half):
        ref = self.shards[i]
        return ref if half is None else ref.at[half]

    def copy(self, i, kind, zz, ee, half, dev, mine=False):
        dst = self.at(i, zz, ee, half)
        return pltpu.make_async_remote_copy(
            src_ref=self.own(i, half) if mine else dst,
            dst_ref=dst,
            send_sem=self.send.at[i, zz, kind],
            recv_sem=self.recv.at[i, zz, kind],
            device_id=dev,
            device_id_type=MESH,
        )

    def start(self, kind, zz, ee, half, dev, mine=False):
        for i in range(len(self.outs)):
            self.copy(i, kind, zz, ee, half, dev, mine).start()

    def arrived(self, kind, zz, ee, half):
        for i in range(len(self.outs)):
            self.copy(i, kind, zz, ee, half, (self.z, self.e)).wait_recv()

    def sent(self, kind, zz, ee, half, mine=False):
        for i in range(len(self.outs)):
            self.copy(i, kind, zz, ee, half, (self.z, self.e), mine).wait_send()

    def zz(self, j):
        return line_order(self.z, self.nz, j)

    def launch(self, j):
        z, e, nz = self.z, self.e, self.nz
        zz = self.zz(j)
        mine = j == 0
        if mine:
            for i in range(len(self.outs)):
                pltpu.make_async_copy(self.shards[i], self.at(i, z, e, None), self.local.at[i]).start()
        else:
            self.arrived(self.Z, zz, e, None)

        @pl.when(jnp.logical_and(zz <= z, z < nz - 1))
        def _():
            self.start(self.Z, zz, e, None, (z + 1, e), mine)

        if mine:
            @pl.when(z > 0)
            def _():
                for i in range(len(self.outs)):
                    pltpu.make_async_remote_copy(
                        src_ref=self.own(i, None), dst_ref=self.at(i, z, e, None),
                        send_sem=self.local.at[len(self.outs) + i],
                        recv_sem=self.recv.at[i, z, self.Z],
                        device_id=(z - 1, e), device_id_type=MESH).start()
        else:
            @pl.when(jnp.logical_and(zz > z, z > 0))
            def _():
                self.start(self.Z, zz, e, None, (z - 1, e))

        self.start(self.XA, zz, e, 0, (z, self.x), mine)
        self.start(self.YB, zz, e, 1, (z, self.y), mine)
        self.start(self.XB, zz, e, 1, (z, self.x), mine)
        self.start(self.YA, zz, e, 0, (z, self.y), mine)
        self.start(self.P0, zz, e, None, (z, self.p), mine)

    def relay(self, j):
        z = self.z
        zz = self.zz(j)
        self.arrived(self.XA, zz, self.x, 0)
        self.start(self.YF, zz, self.x, 0, (z, self.y))
        self.start(self.PXA, zz, self.x, 0, (z, self.p))
        self.arrived(self.YB, zz, self.y, 1)
        self.start(self.XF, zz, self.y, 1, (z, self.x))
        self.start(self.PYB, zz, self.y, 1, (z, self.p))

    def finish(self, j):
        z = self.z
        zz = self.zz(j)
        self.arrived(self.XB, zz, self.x, 1)
        self.start(self.PXB, zz, self.x, 1, (z, self.p))
        self.arrived(self.YA, zz, self.y, 0)
        self.start(self.PYA, zz, self.y, 0, (z, self.p))
        self.arrived(self.XF, zz, self.d, 1)
        self.start(self.PDB, zz, self.d, 1, (z, self.p))
        self.arrived(self.YF, zz, self.d, 0)
        self.start(self.PDA, zz, self.d, 0, (z, self.p))

    def shared(self, j):
        zz = self.zz(j)
        p = self.p
        self.arrived(self.P0, zz, p, None)
        self.arrived(self.PXA, zz, p ^ 2, 0)
        self.arrived(self.PXB, zz, p ^ 2, 1)
        self.arrived(self.PYA, zz, p ^ 4, 0)
        self.arrived(self.PYB, zz, p ^ 4, 1)
        self.arrived(self.PDA, zz, p ^ 6, 0)
        self.arrived(self.PDB, zz, p ^ 6, 1)

    def drain(self, j):
        z, e, nz = self.z, self.e, self.nz
        zz = self.zz(j)
        mine = j == 0

        @pl.when(jnp.logical_and(zz <= z, z < nz - 1))
        def _():
            self.sent(self.Z, zz, e, None, mine)

        if mine:
            for i in range(len(self.outs)):
                pltpu.make_async_copy(self.shards[i], self.at(i, z, e, None), self.local.at[i]).wait()

            @pl.when(z > 0)
            def _():
                for i in range(len(self.outs)):
                    pltpu.make_async_remote_copy(
                        src_ref=self.own(i, None), dst_ref=self.at(i, z, e, None),
                        send_sem=self.local.at[len(self.outs) + i],
                        recv_sem=self.recv.at[i, z, self.Z],
                        device_id=(z, e), device_id_type=MESH).wait_send()
        else:
            @pl.when(jnp.logical_and(zz > z, z > 0))
            def _():
                self.sent(self.Z, zz, e, None)

        self.sent(self.XA, zz, e, 0, mine)
        self.sent(self.XB, zz, e, 1, mine)
        self.sent(self.YA, zz, e, 0, mine)
        self.sent(self.YB, zz, e, 1, mine)
        self.sent(self.P0, zz, e, None, mine)
        self.sent(self.YF, zz, self.x, 0)
        self.sent(self.XF, zz, self.y, 1)
        self.sent(self.PXA, zz, self.x, 0)
        self.sent(self.PXB, zz, self.x, 1)
        self.sent(self.PYA, zz, self.y, 0)
        self.sent(self.PYB, zz, self.y, 1)
        self.sent(self.PDA, zz, self.d, 0)
        self.sent(self.PDB, zz, self.d, 1)


def gather_kernel(nz, count, *refs):
    shards, outs = refs[:count], refs[count : 2 * count]
    send, recv, local = refs[2 * count :]
    z, e = place()
    greet(z, e, nz)
    g = Gather(nz, shards, outs, send, recv, local)
    for j in range(nz):
        g.launch(j)
        g.relay(j)
        if j > 0:
            g.finish(j - 1)
    g.finish(nz - 1)
    for j in range(nz):
        g.shared(j)
    for j in range(nz):
        g.drain(j)


def gather_scratch(nz, count):
    return [
        pltpu.SemaphoreType.DMA((count, nz, 14)),
        pltpu.SemaphoreType.DMA((count, nz, 14)),
        pltpu.SemaphoreType.DMA((2 * count,)),
    ]


def gather_all(arrays, collective_id):
    nz, width = lax.axis_size("dp"), lax.axis_size("expert")
    count = len(arrays)
    halves = [a.reshape((2, a.shape[0] // 2) + a.shape[1:]) for a in arrays]
    outs = pl.pallas_call(
        functools.partial(gather_kernel, nz, count),
        out_shape=[jax.ShapeDtypeStruct((nz, width) + h.shape, h.dtype) for h in halves],
        in_specs=[pl.BlockSpec(memory_space=pltpu.VMEM)] * count,
        out_specs=[pl.BlockSpec(memory_space=pl.ANY)] * count,
        scratch_shapes=gather_scratch(nz, count),
        compiler_params=pltpu.CompilerParams(
            collective_id=collective_id, has_side_effects=True, vmem_limit_bytes=VMEM_LIMIT
        ),
        name="gather_all",
    )(*halves)
    return [
        o.reshape((nz * width * a.shape[0],) + a.shape[1:]) for o, a in zip(outs, arrays)
    ]


def accumulate(dst, src):
    rows = dst.shape[0]
    block = 32 if rows % 32 == 0 else rows

    def body(r, _):
        at = pl.ds(pl.multiple_of(r * block, block), block)
        dst[at, :] = dst[at, :] + src[at, :]
        return 0

    lax.fori_loop(0, rows // block, body, 0)


class Scatter:
    YD, YO, XD, XO, XA, YB, Z, ZB = range(4, 12)

    def __init__(self, nz, terms, outs, sums, temps, from_y, from_x, last_x, last_y, from_z, send, recv, local):
        self.nz, self.terms, self.outs = nz, terms, outs
        self.sums, self.temps = sums, temps
        self.from_y, self.from_x, self.last_x, self.last_y, self.from_z = from_y, from_x, last_x, last_y, from_z
        self.send, self.recv, self.local = send, recv, local
        self.count = len(terms)
        self.z, self.e = place()
        self.core = self.e % 2
        self.chip = self.e // 2
        self.x, self.y, self.p = self.e ^ 2, self.e ^ 4, self.e ^ 1
        self.chips = (self.chip ^ 3, self.chip ^ 1, self.chip ^ 2, self.chip)

    def zz(self, j):
        return line_order(self.z, self.nz, self.nz - 1 - j)

    def remote(self, i, kind, zz, src, dst, dev):
        return pltpu.make_async_remote_copy(
            src_ref=src, dst_ref=dst, send_sem=self.send.at[i, zz, kind], recv_sem=self.recv.at[i, zz, kind],
            device_id=dev, device_id_type=MESH)

    def pair(self, i, j, q):
        zz, chip = self.zz(j), self.chips[q]
        return self.remote(i, q, zz, self.terms[i].at[zz, chip * 2 + (1 - self.core)], self.sums[i].at[zz, q],
                           (self.z, self.p))

    def load(self, i, j, q):
        slot = q % 2
        return pltpu.make_async_copy(
            self.terms[i].at[self.zz(j), self.chips[q] * 2 + self.core], self.temps[i].at[slot], self.local.at[i, slot])

    def begin(self):
        for j in range(self.nz):
            for q in range(4):
                for i in range(self.count):
                    self.pair(i, j, q).start()
        for i in range(self.count):
            self.load(i, 0, 0).start()

    def yd(self, i, zz):
        return self.remote(i, self.YD, zz, self.sums[i].at[zz, 0, 0], self.from_y[i].at[zz, 0], (self.z, self.y))

    def yo(self, i, zz):
        return self.remote(i, self.YO, zz, self.sums[i].at[zz, 2, 0], self.from_y[i].at[zz, 1], (self.z, self.y))

    def xd(self, i, zz):
        return self.remote(i, self.XD, zz, self.sums[i].at[zz, 0, 1], self.from_x[i].at[zz, 0], (self.z, self.x))

    def xo(self, i, zz):
        return self.remote(i, self.XO, zz, self.sums[i].at[zz, 1, 1], self.from_x[i].at[zz, 1], (self.z, self.x))

    def xa(self, i, zz):
        return self.remote(i, self.XA, zz, self.sums[i].at[zz, 1, 0], self.last_x[i].at[zz], (self.z, self.x))

    def yb(self, i, zz):
        return self.remote(i, self.YB, zz, self.sums[i].at[zz, 2, 1], self.last_y[i].at[zz], (self.z, self.y))

    def up(self, i, zz):
        return self.remote(i, self.Z, zz, self.sums[i].at[zz, 3], self.from_z[i].at[zz], (self.z + 1, self.e))

    def down(self, i, zz):
        return self.remote(i, self.Z, zz, self.sums[i].at[zz, 3], self.from_z[i].at[zz], (self.z - 1, self.e))

    def down_last(self, i, zz):
        return self.remote(i, self.ZB, zz, self.sums[i].at[zz, 3], self.from_z[i].at[self.nz], (self.z - 1, self.e))

    def first(self, j):
        zz = self.zz(j)
        for q in range(4):
            for i in range(self.count):
                if q < 3:
                    self.load(i, j, q + 1).start()
                elif j < self.nz - 1:
                    self.load(i, j + 1, 0).start()
                self.pair(i, j, q).wait_recv()
                self.load(i, j, q).wait()
                for h in range(2):
                    accumulate(self.sums[i].at[zz, q, h], self.temps[i].at[q % 2, h])
                if q == 0:
                    self.yd(i, zz).start()
                    self.xd(i, zz).start()
                if q == 1:
                    self.xo(i, zz).start()
                if q == 2:
                    self.yo(i, zz).start()

    def second(self, j):
        zz = self.zz(j)
        for i in range(self.count):
            self.yd(i, zz).wait_recv()
            accumulate(self.sums[i].at[zz, 1, 0], self.from_y[i].at[zz, 0])
            self.xa(i, zz).start()
            self.xd(i, zz).wait_recv()
            accumulate(self.sums[i].at[zz, 2, 1], self.from_x[i].at[zz, 0])
            self.yb(i, zz).start()

    def third(self, j):
        z, nz = self.z, self.nz
        zz = self.zz(j)
        for i in range(self.count):
            self.yo(i, zz).wait_recv()
            accumulate(self.sums[i].at[zz, 3, 0], self.from_y[i].at[zz, 1])
            self.xo(i, zz).wait_recv()
            accumulate(self.sums[i].at[zz, 3, 1], self.from_x[i].at[zz, 1])
            self.xa(i, zz).wait_recv()
            accumulate(self.sums[i].at[zz, 3, 0], self.last_x[i].at[zz])
            self.yb(i, zz).wait_recv()
            accumulate(self.sums[i].at[zz, 3, 1], self.last_y[i].at[zz])
            if j < nz - 1:
                @pl.when(jnp.logical_or(jnp.logical_and(zz > z, z > 0), jnp.logical_and(zz < z, z < nz - 1)))
                def _():
                    self.up(i, zz).wait_recv()
                    for h in range(2):
                        accumulate(self.sums[i].at[zz, 3, h], self.from_z[i].at[zz, h])

                @pl.when(zz > z)
                def _():
                    self.up(i, zz).start()

                @pl.when(zz < z - 1)
                def _():
                    self.down(i, zz).start()

                @pl.when(zz == z - 1)
                def _():
                    self.down_last(i, zz).start()
            else:
                @pl.when(z > 0)
                def _():
                    self.up(i, z).wait_recv()
                    for h in range(2):
                        accumulate(self.sums[i].at[z, 3, h], self.from_z[i].at[z, h])

                @pl.when(z < nz - 1)
                def _():
                    self.down_last(i, z).wait_recv()
                    for h in range(2):
                        accumulate(self.sums[i].at[z, 3, h], self.from_z[i].at[nz, h])

                self.outs[i][...] = self.sums[i][z, 3].astype(self.outs[i].dtype)

    def drain(self, j):
        z, nz = self.z, self.nz
        zz = self.zz(j)
        for i in range(self.count):
            for q in range(4):
                self.pair(i, j, q).wait_send()
            for c in (self.yd, self.yo, self.xd, self.xo, self.xa, self.yb):
                c(i, zz).wait_send()
            if j < nz - 1:
                @pl.when(zz > z)
                def _():
                    self.up(i, zz).wait_send()

                @pl.when(zz < z - 1)
                def _():
                    self.down(i, zz).wait_send()

                @pl.when(zz == z - 1)
                def _():
                    self.down_last(i, zz).wait_send()


def scatter_kernel(nz, count, *refs):
    groups = [refs[k * count : (k + 1) * count] for k in range(9)]
    send, recv, local = refs[9 * count :]
    z, e = place()
    greet(z, e, nz)
    s = Scatter(nz, *groups, send, recv, local)
    s.begin()
    for j in range(nz):
        s.first(j)
        if j > 0:
            s.second(j - 1)
        if j > 1:
            s.third(j - 2)
    s.second(nz - 1)
    if nz > 1:
        s.third(nz - 2)
    s.third(nz - 1)
    for j in range(nz):
        s.drain(j)


def scatter_sum(arrays, collective_id):
    nz, width = lax.axis_size("dp"), lax.axis_size("expert")
    count = len(arrays)
    devices = nz * width
    terms = [a.reshape(nz, width, 2, a.shape[0] // (2 * devices), a.shape[1]) for a in arrays]
    chips = width // 2
    scratch = []
    shapes = [t.shape[3:] for t in terms]
    kinds = [a.dtype for a in arrays]
    for lead in ((nz, chips, 2), (2, 2), (nz, 2), (nz, 2), (nz,), (nz,), (nz + 1, 2)):
        scratch += [pltpu.VMEM(lead + s, k) for s, k in zip(shapes, kinds)]
    outs = pl.pallas_call(
        functools.partial(scatter_kernel, nz, count),
        out_shape=[jax.ShapeDtypeStruct((2,) + s, jnp.float32) for s in shapes],
        in_specs=[pl.BlockSpec(memory_space=pl.ANY)] * count,
        out_specs=[pl.BlockSpec(memory_space=pltpu.VMEM)] * count,
        scratch_shapes=scratch
        + [
            pltpu.SemaphoreType.DMA((count, nz, 12)),
            pltpu.SemaphoreType.DMA((count, nz, 12)),
            pltpu.SemaphoreType.DMA((count, 2)),
        ],
        compiler_params=pltpu.CompilerParams(
            collective_id=collective_id, has_side_effects=True, vmem_limit_bytes=VMEM_LIMIT
        ),
        name="scatter_sum",
    )(*terms)
    return [o.reshape(2 * s[0], s[1]) for o, s in zip(outs, shapes)]


def mm(a, b, da=1, db=0):
    return lax.dot_general(a, b, (((da,), (db,)), ((), ())), preferred_element_type=F32)


def expert_kernel(group, cap, x_ref, g_ref, gate_ref, rank_ref, wg_ref, wu_ref, wd_ref,
                  y_ref, r_ref, gg_ref, rows_ref, down_ref, act_ref, gp_ref, up_ref, cot_ref):
    length, width = x_ref.shape[1:]
    slot = lax.broadcasted_iota(jnp.int32, (cap, length), 0).astype(F32)
    picks, gates = [], []
    for s in range(group):
        hit = slot == rank_ref[s]
        pick = hit.astype(BF16)
        picks.append(pick)
        gate = jnp.sum(jnp.where(hit, gate_ref[s], 0.0), 1, keepdims=True)
        gates.append(gate)
        at = pl.ds(s * cap, cap)
        rows_ref[at, :] = mm(pick, x_ref[s]).astype(BF16)
        cot = mm(pick, g_ref[s])
        cot_ref[at, :] = cot.astype(BF16)
        down_ref[at, :] = (gate * cot).astype(BF16)
    gate_all = jnp.concatenate(gates, 0)
    rows = rows_ref[...]
    pre_gate = mm(rows, wg_ref[...])
    pre_up = mm(rows, wu_ref[...])
    sig = jax.nn.sigmoid(pre_gate)
    silu = pre_gate * sig
    act_ref[...] = (silu * pre_up).astype(BF16)
    act_grad = mm(down_ref[...], wd_ref[...], 1, 1)
    gp_ref[...] = (act_grad * pre_up * sig * (1.0 + pre_gate * (1.0 - sig))).astype(BF16)
    up_ref[...] = (act_grad * silu).astype(BF16)
    tile = 512
    gg = jnp.zeros((group * cap, 1), F32)
    for n in range(width // tile):
        cols = pl.ds(n * tile, tile)
        out = mm(act_ref[...], wd_ref[:, cols]).astype(BF16).astype(F32)
        gg = gg + jnp.sum(out * cot_ref[:, cols].astype(F32), 1, keepdims=True)
        out = (out * gate_all).astype(BF16)
        back = (mm(gp_ref[...], wg_ref[cols, :], 1, 1) + mm(up_ref[...], wu_ref[cols, :], 1, 1)).astype(BF16)
        for s in range(group):
            part = slice(s * cap, (s + 1) * cap)
            y_ref[s, :, cols] = mm(picks[s], out[part], 0, 0).astype(BF16)
            r_ref[s, :, cols] = mm(picks[s], back[part], 0, 0).astype(BF16)
    for s in range(group):
        gg_ref[s] = jnp.sum(picks[s].astype(F32) * gg[s * cap : (s + 1) * cap], 0, keepdims=True)


def experts(x, g, gate, rank, wg, wu, wd, cap, group):
    devices, length, width = x.shape
    ff = wg.shape[1]
    rows = devices * cap
    step = group * cap
    block = lambda *tail: pl.BlockSpec((group,) + tail, lambda i: (i,) + (0,) * len(tail))
    flat = lambda n: pl.BlockSpec((step, n), lambda i: (i, 0))
    whole = lambda a: pl.BlockSpec(a.shape, lambda i: (0, 0), pipeline_mode=pl.Buffered(1))
    return pl.pallas_call(
        functools.partial(expert_kernel, group, cap),
        grid=(devices // group,),
        in_specs=[block(length, width), block(length, width), block(1, length), block(1, length),
                  whole(wg), whole(wu), whole(wd)],
        out_specs=[block(length, width), block(length, width), block(1, length),
                   flat(width), flat(width), flat(ff), flat(ff), flat(ff)],
        out_shape=[
            jax.ShapeDtypeStruct((devices, length, width), BF16),
            jax.ShapeDtypeStruct((devices, length, width), BF16),
            jax.ShapeDtypeStruct((devices, 1, length), F32),
            jax.ShapeDtypeStruct((rows, width), BF16),
            jax.ShapeDtypeStruct((rows, width), BF16),
            jax.ShapeDtypeStruct((rows, ff), BF16),
            jax.ShapeDtypeStruct((rows, ff), BF16),
            jax.ShapeDtypeStruct((rows, ff), BF16),
        ],
        scratch_shapes=[pltpu.VMEM((step, width), BF16)],
        compiler_params=pltpu.CompilerParams(vmem_limit_bytes=VMEM_LIMIT, dimension_semantics=("arbitrary",)),
        name="experts",
    )(x, g, gate, rank, wg, wu, wd)


def pack_columns(columns, rows, lanes, dtype):
    parts = [c.astype(dtype) for c in columns]
    used = sum(c.shape[1] for c in parts)
    return jnp.concatenate(parts + [jnp.zeros((rows, lanes - used), dtype)], 1)


def spread(vector, devices, rows):
    blocks = vector.reshape(devices, -1)
    return jnp.pad(blocks, ((0, 0), (0, rows - blocks.shape[1]))).reshape(devices * rows, 1)


def per_device_gather(
    hidden_in,
    segment_ids,
    expert_ids,
    attn_gain,
    query_gain,
    key_gain,
    w_query,
    w_key,
    w_value,
    w_output,
    mlp_gain,
    w_router,
    w_gate,
    w_up,
    w_down,
    out_grad,
):
    devices = lax.axis_size(("dp", "expert"))
    me = lax.axis_index(("dp", "expert"))
    length, choices = expert_ids.shape
    width = hidden_in.shape[1]
    experts_total = devices
    capacity = 5 * length * choices // (4 * experts_total)
    query_cols, key_cols = w_query.shape[1], w_key.shape[1]
    rows = w_query.shape[0]
    head_rows = query_gain.shape[0]

    column = lambda v: jnp.pad(v, (0, rows - v.shape[0]))[:, None]
    lanes = 128 * pl.cdiv(experts_total + 4, 128)
    small = pack_columns(
        [w_router, column(attn_gain), column(mlp_gain), column(query_gain), column(key_gain)], rows, lanes, BF16
    )
    w_mixed = jnp.concatenate([w_query, w_key, w_value], 1)
    w_mixed, w_out, small = gather_all([w_mixed, w_output, small], 1)
    router = small[:, :experts_total]
    attn_gain, mlp_gain = small[:, experts_total], small[:, experts_total + 1]
    heads_of = small.reshape(devices, rows, lanes)[:, :head_rows]
    query_gain = heads_of[:, :, experts_total + 2].reshape(-1)
    key_gain = heads_of[:, :, experts_total + 3].reshape(-1)

    group_size = HEADS // KV_HEADS
    plain_in = hidden_in.astype(F32)
    inv_attn = rms_scale(plain_in)
    normed_attn = (plain_in * inv_attn * attn_gain).astype(BF16)
    mixed = jnp.dot(normed_attn, w_mixed, preferred_element_type=F32)
    query_raw = mixed[:, :query_cols].reshape(length, HEADS, HEAD_DIM)
    key_raw = mixed[:, query_cols : query_cols + key_cols].reshape(length, KV_HEADS, HEAD_DIM)
    value_rows = mixed[:, query_cols + key_cols :].astype(BF16).reshape(length, KV_HEADS, HEAD_DIM)
    query_scale = rms_scale(query_raw)
    key_scale = rms_scale(key_raw)
    cosine_table, sine_table = rope_tables(jnp.arange(length) % TOK_DEV, HEAD_DIM)
    query_rot = rotate(query_raw * query_scale * query_gain, cosine_table, sine_table).astype(BF16)
    query_rot = query_rot.reshape(length, KV_HEADS, group_size, HEAD_DIM)
    key_rot = rotate(key_raw * key_scale * key_gain, cosine_table, sine_table).astype(BF16)
    position = jnp.arange(length)
    allowed = (segment_ids[:, None] == segment_ids[None, :]) & (position[None, :] <= position[:, None])
    attended, log_totals = attend(query_rot, key_rot, value_rows, allowed)
    attended = attended.reshape(length, HEADS * HEAD_DIM)
    residual = plain_in + jnp.dot(attended, w_out, preferred_element_type=F32)

    inv_mlp = rms_scale(residual)
    normed_mlp = (residual * inv_mlp * mlp_gain).astype(BF16)
    logits = jnp.dot(normed_mlp, router, preferred_element_type=F32)
    chosen = jnp.any(expert_ids[:, :, None] == jnp.arange(experts_total)[None, None, :], 1)
    raised = jnp.where(chosen, jnp.exp(logits), 0.0)
    gate = raised / jnp.sum(raised, -1, keepdims=True)
    not_after = (position[None, :] <= position[:, None]).astype(BF16)
    rank = jnp.dot(not_after, chosen.astype(BF16), preferred_element_type=F32) - 1.0
    rank = jnp.where(chosen, rank, -1.0)
    gate_high = lax.reduce_precision(gate, 8, 7)
    table = jnp.concatenate([gate_high, gate - gate_high, rank], 1).T.astype(BF16)

    all_rows, all_tables = gather_all([normed_mlp, table], 2)
    (all_grads,) = gather_all([out_grad], 3)
    mine = lax.dynamic_index_in_dim(
        all_tables.reshape(devices, 3, experts_total, length), me, 2, keepdims=False
    ).astype(F32)
    cube = (devices, length, width)
    y_terms, r_terms, gate_terms, rows_in, down_in, act, gate_pre_grad, up_pre_grad = experts(
        all_rows.reshape(cube), all_grads.reshape(cube), mine[:, :1] + mine[:, 1:2], mine[:, 2:],
        w_gate[0], w_up[0], w_down[0], capacity, 4,
    )
    is_me = (jnp.arange(experts_total) == me).astype(F32)
    gate_terms = (gate_terms * is_me[None, :, None]).reshape(devices * experts_total, length)
    row_grad_sum, gate_grad = scatter_sum([r_terms.reshape(devices * length, width), gate_terms], 4)
    (mixed_out,) = scatter_sum([y_terms.reshape(devices * length, width)], 5)
    block_out = residual + mixed_out
    grad_w_down = jnp.dot(act.T, down_in, preferred_element_type=F32)[None]
    grad_w_gate = jnp.dot(rows_in.T, gate_pre_grad, preferred_element_type=F32)[None]
    grad_w_up = jnp.dot(rows_in.T, up_pre_grad, preferred_element_type=F32)[None]

    gate_grad = gate_grad.T
    sel_grad = gate * (gate_grad - jnp.sum(gate * gate_grad, -1, keepdims=True))
    logit_grad = jnp.where(chosen, sel_grad, 0.0).astype(BF16)
    grad_w_router = jnp.dot(normed_mlp.T, logit_grad, preferred_element_type=F32)
    normed_mlp_grad = row_grad_sum + jnp.dot(logit_grad, router.T, preferred_element_type=F32)
    grad_mlp_gain = jnp.sum(normed_mlp_grad * residual * inv_mlp, 0)
    residual_grad = out_grad.astype(F32) + norm_grad(normed_mlp_grad, residual, inv_mlp, mlp_gain)

    branch_grad = residual_grad.astype(BF16)
    grad_w_output = jnp.dot(attended.T, branch_grad, preferred_element_type=F32).astype(BF16)
    attended_grad = jnp.dot(branch_grad, w_out.T, preferred_element_type=F32).astype(BF16)
    attended_grad = attended_grad.reshape(length, KV_HEADS, group_size, HEAD_DIM)
    query_rot_grad, key_rot_grad, value_sum_grad = attend_grad(
        query_rot, key_rot, value_rows, allowed, log_totals, attended_grad
    )
    query_normed_grad = unrotate(query_rot_grad.reshape(length, HEADS, HEAD_DIM), cosine_table, sine_table)
    key_normed_grad = unrotate(key_rot_grad, cosine_table, sine_table)
    grad_query_gain = jnp.sum(query_normed_grad * query_raw * query_scale, (0, 1))
    grad_key_gain = jnp.sum(key_normed_grad * key_raw * key_scale, (0, 1))
    query_grad = norm_grad(query_normed_grad, query_raw, query_scale, query_gain).astype(BF16)
    key_grad = norm_grad(key_normed_grad, key_raw, key_scale, key_gain).astype(BF16)
    mixed_grad = jnp.concatenate(
        [
            query_grad.reshape(length, query_cols),
            key_grad.reshape(length, key_cols),
            value_sum_grad.astype(BF16).reshape(length, key_cols),
        ],
        1,
    )
    grad_w_mixed = jnp.dot(normed_attn.T, mixed_grad, preferred_element_type=F32).astype(BF16)
    normed_attn_grad = jnp.dot(mixed_grad, w_mixed.T, preferred_element_type=F32)
    grad_attn_gain = jnp.sum(normed_attn_grad * plain_in * inv_attn, 0)
    grad_in = residual_grad + norm_grad(normed_attn_grad, plain_in, inv_attn, attn_gain)

    small_grads = pack_columns(
        [
            grad_w_router,
            grad_attn_gain[:, None],
            grad_mlp_gain[:, None],
            spread(grad_query_gain, devices, rows),
            spread(grad_key_gain, devices, rows),
        ],
        width,
        lanes,
        F32,
    )
    share_mixed, share_w_output, share_small = scatter_sum([grad_w_mixed, grad_w_output, small_grads], 6)
    return (
        block_out,
        grad_in,
        share_small[:, experts_total],
        share_small[:head_rows, experts_total + 2],
        share_small[:head_rows, experts_total + 3],
        share_mixed[:, :query_cols],
        share_mixed[:, query_cols : query_cols + key_cols],
        share_mixed[:, query_cols + key_cols :],
        share_w_output,
        share_small[:, experts_total + 1],
        share_small[:, :experts_total],
        grad_w_gate,
        grad_w_up,
        grad_w_down,
    )


def per_device(*arguments):
    expert_ids, w_gate = arguments[2], arguments[12]
    devices, width = lax.axis_size(("dp", "expert")), lax.axis_size("expert")
    length, choices = expert_ids.shape
    capacity = 5 * length * choices // (4 * devices)
    dense = devices <= 4 * choices and w_gate.shape[0] == 1 and width == 8
    if dense and capacity % 16 == 0 and devices % 4 == 0:
        return per_device_gather(*arguments)
    return per_device_exchange(*arguments)


def solution(mesh):
    in_specs = (
        P(("dp", "expert"), None),
        P(("dp", "expert")),
        P(("dp", "expert"), None),
        P(("dp", "expert")),
        P(("dp", "expert")),
        P(("dp", "expert")),
        P(("dp", "expert"), None),
        P(("dp", "expert"), None),
        P(("dp", "expert"), None),
        P(("dp", "expert"), None),
        P(("dp", "expert")),
        P(("dp", "expert"), None),
        P(("dp", "expert"), None, None),
        P(("dp", "expert"), None, None),
        P(("dp", "expert"), None, None),
        P(("dp", "expert"), None),
    )
    out_specs = (
        P(("dp", "expert"), None),
        P(("dp", "expert"), None),
        P(("dp", "expert")),
        P(("dp", "expert")),
        P(("dp", "expert")),
        P(("dp", "expert"), None),
        P(("dp", "expert"), None),
        P(("dp", "expert"), None),
        P(("dp", "expert"), None),
        P(("dp", "expert")),
        P(("dp", "expert"), None),
        P(("dp", "expert"), None, None),
        P(("dp", "expert"), None, None),
        P(("dp", "expert"), None, None),
    )
    return jax.shard_map(
        per_device, mesh=mesh, in_specs=in_specs, out_specs=out_specs, check_vma=False
    )
```

```python
import functools
import math

import jax
import jax.numpy as jnp
from jax import lax
from jax.experimental import pallas as pl
from jax.experimental.pallas import tpu as pltpu
from jax.sharding import PartitionSpec as P

F32, BF16 = jnp.float32, jnp.bfloat16
MESH = pl.DeviceIdType.MESH
VMEM_LIMIT = 63 * 1024 * 1024


HEADS = 32
KV_HEADS = 4
HEAD_DIM = 128
TOK_DEV = 256


EPS = 1e-06
ROPE_BASE = 1000000.0


def rms_scale(values):
    return lax.rsqrt(jnp.mean(values * values, -1, keepdims=True) + EPS)


def norm_grad(upstream, values, inverse, gain_vec):
    weighted = upstream * gain_vec
    return inverse * weighted - values * inverse**3 * jnp.mean(weighted * values, -1, keepdims=True)


def rope_tables(positions, head_dim):
    half_dim = head_dim // 2
    frequency = ROPE_BASE ** (-(jnp.arange(half_dim).astype(jnp.float32) * 2.0 / head_dim))
    angles = positions.astype(jnp.float32)[:, None] * frequency[None, :]
    return (jnp.cos(angles)[:, None, :], jnp.sin(angles)[:, None, :])


def rotate(values, cosine_table, sine_table):
    half_dim = values.shape[-1] // 2
    first_half = values[..., :half_dim]
    second_half = values[..., half_dim:]
    return jnp.concatenate(
        [
            first_half * cosine_table - second_half * sine_table,
            second_half * cosine_table + first_half * sine_table,
        ],
        -1,
    )


def unrotate(values, cosine_table, sine_table):
    half_dim = values.shape[-1] // 2
    first_half = values[..., :half_dim]
    second_half = values[..., half_dim:]
    return jnp.concatenate(
        [
            first_half * cosine_table + second_half * sine_table,
            second_half * cosine_table - first_half * sine_table,
        ],
        -1,
    )


def attend(query_rot, key_rot, value_rows, allowed):
    score_scale = 1.0 / math.sqrt(HEAD_DIM)
    scores = (
        jnp.einsum("qkgd,tkd->kgqt", query_rot, key_rot, preferred_element_type=jnp.float32)
        * score_scale
    )
    exp_scores = jnp.where(allowed, jnp.exp(scores), 0.0)
    totals = jnp.sum(exp_scores, -1, keepdims=True)
    probs_low = (exp_scores / totals).astype(jnp.bfloat16)
    attended = jnp.einsum(
        "kgqt,tkd->qkgd", probs_low, value_rows, preferred_element_type=jnp.float32
    ).astype(jnp.bfloat16)
    return (attended, jnp.log(totals))


def attend_grad(query_rot, key_rot, value_rows, allowed, log_totals, attended_grad):
    score_scale = 1.0 / math.sqrt(HEAD_DIM)
    scores = (
        jnp.einsum("qkgd,tkd->kgqt", query_rot, key_rot, preferred_element_type=jnp.float32)
        * score_scale
    )
    probs_back = jnp.where(allowed, jnp.exp(scores - log_totals), 0.0)
    probs_low = probs_back.astype(jnp.bfloat16)
    value_sum_grad = jnp.einsum(
        "kgqt,qkgd->tkd", probs_low, attended_grad, preferred_element_type=jnp.float32
    )
    prob_grad = jnp.einsum(
        "qkgd,tkd->kgqt", attended_grad, value_rows, preferred_element_type=jnp.float32
    )
    score_grad = (
        probs_back * (prob_grad - jnp.sum(probs_back * prob_grad, -1, keepdims=True))
    ).astype(jnp.bfloat16)
    query_rot_grad = (
        jnp.einsum("kgqt,tkd->qkgd", score_grad, key_rot, preferred_element_type=jnp.float32)
        * score_scale
    )
    key_rot_grad = (
        jnp.einsum("kgqt,qkgd->tkd", score_grad, query_rot, preferred_element_type=jnp.float32)
        * score_scale
    )
    return (query_rot_grad, key_rot_grad, value_sum_grad)


def mixer_forward(block_in, block_segments, weights):
    w_query, w_key, w_value, w_output, w_router, attn_gain, mlp_gain, query_gain, key_gain = weights
    row_count = block_in.shape[0]
    seq_count = row_count // TOK_DEV
    group_size = HEADS // KV_HEADS
    plain_in = block_in.astype(jnp.float32)
    inv_attn = rms_scale(plain_in)
    normed_attn = (plain_in * inv_attn * attn_gain).astype(jnp.bfloat16)
    query_raw = jnp.dot(normed_attn, w_query, preferred_element_type=jnp.float32).reshape(
        row_count, HEADS, HEAD_DIM
    )
    key_raw = jnp.dot(normed_attn, w_key, preferred_element_type=jnp.float32).reshape(
        row_count, KV_HEADS, HEAD_DIM
    )
    value_rows = jnp.dot(normed_attn, w_value, preferred_element_type=jnp.float32).astype(
        jnp.bfloat16
    )
    value_rows = value_rows.reshape(seq_count, TOK_DEV, KV_HEADS, HEAD_DIM)
    query_scale = rms_scale(query_raw)
    key_scale = rms_scale(key_raw)
    cosine_table, sine_table = rope_tables(jnp.arange(row_count) % TOK_DEV, HEAD_DIM)
    query_rot = rotate(query_raw * query_scale * query_gain, cosine_table, sine_table).astype(
        jnp.bfloat16
    )
    query_rot = query_rot.reshape(seq_count, TOK_DEV, KV_HEADS, group_size, HEAD_DIM)
    key_rot = rotate(key_raw * key_scale * key_gain, cosine_table, sine_table).astype(jnp.bfloat16)
    key_rot = key_rot.reshape(seq_count, TOK_DEV, KV_HEADS, HEAD_DIM)
    segments = block_segments.reshape(seq_count, TOK_DEV)
    position = jnp.arange(TOK_DEV)
    allowed = (segments[:, :, None] == segments[:, None, :]) & (
        position[None, None, :] <= position[None, :, None]
    )
    attended, log_totals = jax.vmap(attend)(query_rot, key_rot, value_rows, allowed)
    attended = attended.reshape(row_count, HEADS * HEAD_DIM)
    residual = plain_in + jnp.dot(attended, w_output, preferred_element_type=jnp.float32)
    saved_state = (
        plain_in,
        inv_attn,
        normed_attn,
        query_raw,
        key_raw,
        value_rows,
        query_scale,
        key_scale,
        query_rot,
        key_rot,
        allowed,
        log_totals,
        attended,
        cosine_table,
        sine_table,
    )
    return (residual, saved_state)


def mixer_backward(residual_grad, saved_state, weights):
    w_query, w_key, w_value, w_output, w_router, attn_gain, mlp_gain, query_gain, key_gain = weights
    (
        plain_in,
        inv_attn,
        normed_attn,
        query_raw,
        key_raw,
        value_rows,
        query_scale,
        key_scale,
        query_rot,
        key_rot,
        allowed,
        log_totals,
        attended,
        cosine_table,
        sine_table,
    ) = saved_state
    row_count = residual_grad.shape[0]
    seq_count = row_count // TOK_DEV
    group_size = HEADS // KV_HEADS
    branch_grad = residual_grad.astype(jnp.bfloat16)
    grad_w_output = jnp.dot(attended.T, branch_grad, preferred_element_type=jnp.float32)
    attended_grad = jnp.dot(branch_grad, w_output.T, preferred_element_type=jnp.float32).astype(
        jnp.bfloat16
    )
    attended_grad = attended_grad.reshape(seq_count, TOK_DEV, KV_HEADS, group_size, HEAD_DIM)
    query_rot_grad, key_rot_grad, value_sum_grad = jax.vmap(attend_grad)(
        query_rot, key_rot, value_rows, allowed, log_totals, attended_grad
    )
    query_normed_grad = unrotate(
        query_rot_grad.reshape(row_count, HEADS, HEAD_DIM), cosine_table, sine_table
    )
    key_normed_grad = unrotate(
        key_rot_grad.reshape(row_count, KV_HEADS, HEAD_DIM), cosine_table, sine_table
    )
    grad_query_gain = jnp.sum(query_normed_grad * query_raw * query_scale, (0, 1))
    grad_key_gain = jnp.sum(key_normed_grad * key_raw * key_scale, (0, 1))
    query_grad = norm_grad(query_normed_grad, query_raw, query_scale, query_gain).astype(
        jnp.bfloat16
    )
    query_grad = query_grad.reshape(row_count, HEADS * HEAD_DIM)
    key_grad = norm_grad(key_normed_grad, key_raw, key_scale, key_gain).astype(jnp.bfloat16)
    key_grad = key_grad.reshape(row_count, KV_HEADS * HEAD_DIM)
    value_grad = value_sum_grad.astype(jnp.bfloat16).reshape(row_count, KV_HEADS * HEAD_DIM)
    grad_w_query = jnp.dot(normed_attn.T, query_grad, preferred_element_type=jnp.float32)
    grad_w_key = jnp.dot(normed_attn.T, key_grad, preferred_element_type=jnp.float32)
    grad_w_value = jnp.dot(normed_attn.T, value_grad, preferred_element_type=jnp.float32)
    normed_attn_grad = (
        jnp.dot(query_grad, w_query.T, preferred_element_type=jnp.float32)
        + jnp.dot(key_grad, w_key.T, preferred_element_type=jnp.float32)
        + jnp.dot(value_grad, w_value.T, preferred_element_type=jnp.float32)
    )
    grad_attn_gain = jnp.sum(normed_attn_grad * plain_in * inv_attn, 0)
    grad_in = residual_grad + norm_grad(normed_attn_grad, plain_in, inv_attn, attn_gain)
    return (
        grad_in,
        (
            grad_attn_gain,
            grad_query_gain,
            grad_key_gain,
            grad_w_query,
            grad_w_key,
            grad_w_value,
            grad_w_output,
        ),
    )


def dispatch_table(expert_rows, experts, capacity):
    length, choices = expert_rows.shape
    flat_ids = expert_rows.reshape(length * choices)
    marks = (flat_ids[:, None] == jnp.arange(experts)[None, :]).astype(jnp.int32)
    earlier = jnp.cumsum(marks, 0) - marks
    destination = flat_ids * capacity + jnp.sum(earlier * marks, -1)
    pair_ids = (
        jnp.zeros((experts * capacity,), jnp.int32)
        .at[destination]
        .set(jnp.arange(length * choices, dtype=jnp.int32))
    )
    filled = jnp.zeros((experts * capacity,), jnp.bfloat16).at[destination].set(1.0)
    return (destination, pair_ids, filled)


def move_rows(row_block, section_name):
    if section_name == "dispatch":
        return lax.all_to_all(row_block, ("dp", "expert"), split_axis=0, concat_axis=0, tiled=True)
    if section_name == "combine":
        return lax.all_to_all(row_block, ("dp", "expert"), split_axis=0, concat_axis=0, tiled=True)
    if section_name == "grad_dispatch":
        return lax.all_to_all(row_block, ("dp", "expert"), split_axis=0, concat_axis=0, tiled=True)
    return lax.all_to_all(row_block, ("dp", "expert"), split_axis=0, concat_axis=0, tiled=True)


def per_device_exchange(
    hidden_in,
    segment_ids,
    expert_ids,
    attn_gain,
    query_gain,
    key_gain,
    w_query,
    w_key,
    w_value,
    w_output,
    mlp_gain,
    w_router,
    w_gate,
    w_up,
    w_down,
    out_grad,
):
    weights = (
        lax.all_gather(w_query, ("dp", "expert"), axis=0, tiled=True),
        lax.all_gather(w_key, ("dp", "expert"), axis=0, tiled=True),
        lax.all_gather(w_value, ("dp", "expert"), axis=0, tiled=True),
        lax.all_gather(w_output, ("dp", "expert"), axis=0, tiled=True),
        lax.all_gather(w_router, ("dp", "expert"), axis=0, tiled=True),
        lax.all_gather(attn_gain, ("dp", "expert"), axis=0, tiled=True),
        lax.all_gather(mlp_gain, ("dp", "expert"), axis=0, tiled=True),
        lax.all_gather(query_gain, ("dp", "expert"), axis=0, tiled=True),
        lax.all_gather(key_gain, ("dp", "expert"), axis=0, tiled=True),
    )
    residual, saved_state = mixer_forward(hidden_in, segment_ids, weights)
    full_router = weights[4]
    full_mlp_gain = weights[6]
    inv_mlp = rms_scale(residual)
    normed_mlp = (residual * inv_mlp * full_mlp_gain).astype(jnp.bfloat16)
    logits = jnp.dot(normed_mlp, full_router, preferred_element_type=jnp.float32)
    device_count = lax.axis_size(("dp", "expert"))
    local_experts = w_gate.shape[0]
    experts = local_experts * device_count
    length, choices = expert_ids.shape
    model_width = hidden_in.shape[1]
    capacity = 5 * length * choices // (4 * experts)
    one_hot = expert_ids[:, :, None] == jnp.arange(experts)[None, None, :]
    chosen = jnp.sum(jnp.where(one_hot, logits[:, None, :], 0.0), -1)
    raised = jnp.exp(chosen)
    gate_weights = raised / jnp.sum(raised, -1, keepdims=True)
    destination, pair_ids, filled = dispatch_table(expert_ids, experts, capacity)
    send_rows = normed_mlp[pair_ids // choices] * filled[:, None]
    received = move_rows(
        send_rows.reshape(device_count, local_experts * capacity, model_width), "dispatch"
    )
    received = received.reshape(device_count, local_experts, capacity, model_width)
    pre_gate = jnp.einsum("secd,edf->secf", received, w_gate, preferred_element_type=jnp.float32)
    pre_up = jnp.einsum("secd,edf->secf", received, w_up, preferred_element_type=jnp.float32)
    gate_sigmoid = jax.nn.sigmoid(pre_gate)
    silu_gate = pre_gate * gate_sigmoid
    activation = (silu_gate * pre_up).astype(jnp.bfloat16)
    expert_out = jnp.einsum(
        "secf,efd->secd", activation, w_down, preferred_element_type=jnp.float32
    ).astype(jnp.bfloat16)
    returned = move_rows(
        expert_out.reshape(device_count, local_experts * capacity, model_width), "combine"
    )
    picked = returned.reshape(experts * capacity, model_width)[destination].reshape(
        length, choices, model_width
    )
    block_out = residual + jnp.sum(gate_weights[:, :, None] * picked.astype(jnp.float32), 1)
    weights = (
        lax.all_gather(w_query, ("dp", "expert"), axis=0, tiled=True),
        lax.all_gather(w_key, ("dp", "expert"), axis=0, tiled=True),
        lax.all_gather(w_value, ("dp", "expert"), axis=0, tiled=True),
        lax.all_gather(w_output, ("dp", "expert"), axis=0, tiled=True),
        lax.all_gather(w_router, ("dp", "expert"), axis=0, tiled=True),
        lax.all_gather(attn_gain, ("dp", "expert"), axis=0, tiled=True),
        lax.all_gather(mlp_gain, ("dp", "expert"), axis=0, tiled=True),
        lax.all_gather(query_gain, ("dp", "expert"), axis=0, tiled=True),
        lax.all_gather(key_gain, ("dp", "expert"), axis=0, tiled=True),
    )
    full_router = weights[4]
    full_mlp_gain = weights[6]
    cotangent = out_grad.astype(jnp.float32)
    gate_grad = jnp.sum(cotangent[:, None, :] * picked.astype(jnp.float32), -1)
    down_in = (
        (gate_weights[:, :, None] * cotangent[:, None, :])
        .astype(jnp.bfloat16)
        .reshape(length * choices, model_width)
    )
    send_grad = down_in[pair_ids] * filled[:, None]
    recv_grad = move_rows(
        send_grad.reshape(device_count, local_experts * capacity, model_width), "grad_dispatch"
    )
    recv_grad = recv_grad.reshape(device_count, local_experts, capacity, model_width)
    act_grad = jnp.einsum("secd,efd->secf", recv_grad, w_down, preferred_element_type=jnp.float32)
    grad_w_down = jnp.einsum(
        "secf,secd->efd", activation, recv_grad, preferred_element_type=jnp.float32
    )
    gate_pre_grad = (
        act_grad * pre_up * gate_sigmoid * (1.0 + pre_gate * (1.0 - gate_sigmoid))
    ).astype(jnp.bfloat16)
    up_pre_grad = (act_grad * silu_gate).astype(jnp.bfloat16)
    grad_w_gate = jnp.einsum(
        "secd,secf->edf", received, gate_pre_grad, preferred_element_type=jnp.float32
    )
    grad_w_up = jnp.einsum(
        "secd,secf->edf", received, up_pre_grad, preferred_element_type=jnp.float32
    )
    row_grad = (
        jnp.einsum("secf,edf->secd", gate_pre_grad, w_gate, preferred_element_type=jnp.float32)
        + jnp.einsum("secf,edf->secd", up_pre_grad, w_up, preferred_element_type=jnp.float32)
    ).astype(jnp.bfloat16)
    row_back = move_rows(
        row_grad.reshape(device_count, local_experts * capacity, model_width), "grad_return"
    )
    row_back = row_back.reshape(experts * capacity, model_width)[destination].reshape(
        length, choices, model_width
    )
    sel_grad = gate_weights * (gate_grad - jnp.sum(gate_weights * gate_grad, -1, keepdims=True))
    logit_grad = jnp.sum(jnp.where(one_hot, sel_grad[:, :, None], 0.0), 1).astype(jnp.bfloat16)
    grad_w_router = jnp.dot(normed_mlp.T, logit_grad, preferred_element_type=jnp.float32)
    normed_mlp_grad = jnp.sum(row_back.astype(jnp.float32), 1) + jnp.dot(
        logit_grad, full_router.T, preferred_element_type=jnp.float32
    )
    grad_mlp_gain = jnp.sum(normed_mlp_grad * residual * inv_mlp, 0)
    residual_grad = cotangent + norm_grad(normed_mlp_grad, residual, inv_mlp, full_mlp_gain)
    grad_in, mixer_terms = mixer_backward(residual_grad, saved_state, weights)
    (
        grad_attn_gain,
        grad_query_gain,
        grad_key_gain,
        grad_w_query,
        grad_w_key,
        grad_w_value,
        grad_w_output,
    ) = mixer_terms
    summed = (
        lax.psum_scatter(grad_w_query, ("dp", "expert"), scatter_dimension=0, tiled=True),
        lax.psum_scatter(grad_w_key, ("dp", "expert"), scatter_dimension=0, tiled=True),
        lax.psum_scatter(grad_w_value, ("dp", "expert"), scatter_dimension=0, tiled=True),
        lax.psum_scatter(grad_w_output, ("dp", "expert"), scatter_dimension=0, tiled=True),
        lax.psum_scatter(grad_w_router, ("dp", "expert"), scatter_dimension=0, tiled=True),
        lax.psum_scatter(grad_attn_gain, ("dp", "expert"), scatter_dimension=0, tiled=True),
        lax.psum_scatter(grad_mlp_gain, ("dp", "expert"), scatter_dimension=0, tiled=True),
        lax.psum_scatter(grad_query_gain, ("dp", "expert"), scatter_dimension=0, tiled=True),
        lax.psum_scatter(grad_key_gain, ("dp", "expert"), scatter_dimension=0, tiled=True),
    )
    (
        share_w_query,
        share_w_key,
        share_w_value,
        share_w_output,
        share_w_router,
        share_attn_gain,
        share_mlp_gain,
        share_query_gain,
        share_key_gain,
    ) = summed
    return (
        block_out,
        grad_in,
        share_attn_gain,
        share_query_gain,
        share_key_gain,
        share_w_query,
        share_w_key,
        share_w_value,
        share_w_output,
        share_mlp_gain,
        share_w_router,
        grad_w_gate,
        grad_w_up,
        grad_w_down,
    )


def place():
    z = lax.axis_index("dp")
    e = lax.axis_index("expert")
    return z, e


def line_order(z, nz, j):
    near = jnp.minimum(z, nz - 1 - z)
    step = (j + 1) // 2
    zigzag = z + (step if j % 2 == 0 else -step)
    tail = jnp.where(z < nz - 1 - z, j, nz - 1 - j)
    return jnp.where(j <= 2 * near, zigzag, tail)


def greet(z, e, nz):
    barrier = pltpu.get_barrier_semaphore()
    for mate in (e ^ 1, e ^ 2, e ^ 4):
        pl.semaphore_signal(barrier, inc=1, device_id=(z, mate), device_id_type=MESH)

    @pl.when(z > 0)
    def _():
        pl.semaphore_signal(barrier, inc=1, device_id=(z - 1, e), device_id_type=MESH)

    @pl.when(z < nz - 1)
    def _():
        pl.semaphore_signal(barrier, inc=1, device_id=(z + 1, e), device_id_type=MESH)

    ends = (z > 0).astype(jnp.int32) + (z < nz - 1).astype(jnp.int32)
    pl.semaphore_wait(barrier, 3 + ends)


class Gather:
    Z, ZX, ZY, X3, X2, XQ, Y3, Y2, YQ, P0, PX3, PXQ, PY3, PYQ, PDX, PDY = range(16)
    KINDS = 16
    WHOLE, LOW, HIGH, LOW3, HIGH3, Q0, Q3 = (0, 4), (0, 2), (2, 2), (0, 3), (1, 3), (0, 1), (3, 1)

    def __init__(self, nz, shards, outs, send, recv, local):
        self.nz, self.shards, self.outs = nz, shards, outs
        self.send, self.recv, self.local = send, recv, local
        self.z, self.e = place()
        self.p, self.x, self.y, self.d = self.e ^ 1, self.e ^ 2, self.e ^ 4, self.e ^ 6

    def zz(self, j):
        return line_order(self.z, self.nz, j)

    def part(self, ref, piece):
        return ref.at[pl.ds(piece[0], piece[1])]

    def copy(self, i, kind, zz, ee, piece, dev, mine=False, sem=None):
        dst = self.part(self.outs[i].at[zz, ee], piece)
        return pltpu.make_async_remote_copy(
            src_ref=self.part(self.shards[i], piece) if mine else dst,
            dst_ref=dst,
            send_sem=self.send.at[i, zz, kind] if sem is None else sem,
            recv_sem=self.recv.at[i, zz, kind],
            device_id=dev,
            device_id_type=MESH,
        )

    def start(self, kind, zz, ee, piece, dev, mine=False):
        for i in range(len(self.outs)):
            self.copy(i, kind, zz, ee, piece, dev, mine).start()

    def arrived(self, kind, zz, ee, piece):
        for i in range(len(self.outs)):
            self.copy(i, kind, zz, ee, piece, (self.z, self.e)).wait_recv()

    def sent(self, kind, zz, ee, piece, mine=False):
        for i in range(len(self.outs)):
            self.copy(i, kind, zz, ee, piece, (self.z, self.e), mine).wait_send()

    def along(self, j, kind, ee, piece, act):
        z, e, nz = self.z, self.e, self.nz
        zz, mine = self.zz(j), j == 0 and kind == self.Z
        for i in range(len(self.outs)):
            @pl.when(jnp.logical_and(zz <= z, z < nz - 1))
            def _():
                act(self.copy(i, kind, zz, ee, piece, (z + 1, e), mine))

            @pl.when(jnp.logical_and(zz >= z, z > 0))
            def _():
                sem = self.local.at[1 + kind, i] if j == 0 else None
                act(self.copy(i, kind, zz, ee, piece, (z - 1, e), mine, sem))

    def keep(self, i):
        return pltpu.make_async_copy(self.shards[i], self.outs[i].at[self.z, self.e], self.local.at[0, i])

    def launch(self, j):
        z, e, zz, mine = self.z, self.e, self.zz(j), j == 0
        if not mine:
            self.arrived(self.Z, zz, e, self.WHOLE)
        else:
            self.start(self.XQ, zz, e, self.Q3, (z, self.x), mine)
            self.start(self.YQ, zz, e, self.Q0, (z, self.y), mine)
        self.along(j, self.Z, e, self.WHOLE, lambda c: c.start())
        self.start(self.X3, zz, e, self.LOW3, (z, self.x), mine)
        self.start(self.Y3, zz, e, self.HIGH3, (z, self.y), mine)
        self.start(self.P0, zz, e, self.WHOLE, (z, self.p), mine)
        if mine:
            for i in range(len(self.outs)):
                self.keep(i).start()

    def mates(self, j):
        zz, mine = self.zz(j), j == 0
        self.arrived(self.XQ if mine else self.ZX, zz, self.x, self.Q3)
        self.along(j, self.ZX, self.x, self.Q3, lambda c: c.start())
        self.start(self.PXQ, zz, self.x, self.Q3, (self.z, self.p))
        self.arrived(self.YQ if mine else self.ZY, zz, self.y, self.Q0)
        self.along(j, self.ZY, self.y, self.Q0, lambda c: c.start())
        self.start(self.PYQ, zz, self.y, self.Q0, (self.z, self.p))

    def relay(self, j):
        zz = self.zz(j)
        self.arrived(self.X3, zz, self.x, self.LOW3)
        self.start(self.Y2, zz, self.x, self.HIGH, (self.z, self.y))
        self.start(self.PX3, zz, self.x, self.LOW3, (self.z, self.p))
        self.arrived(self.Y3, zz, self.y, self.HIGH3)
        self.start(self.X2, zz, self.y, self.LOW, (self.z, self.x))
        self.start(self.PY3, zz, self.y, self.HIGH3, (self.z, self.p))

    def finish(self, j):
        zz = self.zz(j)
        self.arrived(self.X2, zz, self.d, self.LOW)
        self.start(self.PDX, zz, self.d, self.LOW, (self.z, self.p))
        self.arrived(self.Y2, zz, self.d, self.HIGH)
        self.start(self.PDY, zz, self.d, self.HIGH, (self.z, self.p))

    def shared(self, j):
        zz, p = self.zz(j), self.p
        self.arrived(self.P0, zz, p, self.WHOLE)
        self.arrived(self.PXQ, zz, p ^ 2, self.Q3)
        self.arrived(self.PYQ, zz, p ^ 4, self.Q0)
        self.arrived(self.PX3, zz, p ^ 2, self.LOW3)
        self.arrived(self.PY3, zz, p ^ 4, self.HIGH3)
        self.arrived(self.PDX, zz, p ^ 6, self.LOW)
        self.arrived(self.PDY, zz, p ^ 6, self.HIGH)

    def drain(self, j):
        zz, e, mine = self.zz(j), self.e, j == 0
        if mine:
            self.sent(self.XQ, zz, e, self.Q3, mine)
            self.sent(self.YQ, zz, e, self.Q0, mine)
            for i in range(len(self.outs)):
                self.keep(i).wait()
        for kind, ee, piece in ((self.Z, e, self.WHOLE), (self.ZX, self.x, self.Q3), (self.ZY, self.y, self.Q0)):
            self.along(j, kind, ee, piece, lambda c: c.wait_send())
        self.sent(self.X3, zz, e, self.LOW3, mine)
        self.sent(self.Y3, zz, e, self.HIGH3, mine)
        self.sent(self.P0, zz, e, self.WHOLE, mine)
        self.sent(self.PXQ, zz, self.x, self.Q3)
        self.sent(self.PYQ, zz, self.y, self.Q0)
        self.sent(self.Y2, zz, self.x, self.HIGH)
        self.sent(self.X2, zz, self.y, self.LOW)
        self.sent(self.PX3, zz, self.x, self.LOW3)
        self.sent(self.PY3, zz, self.y, self.HIGH3)
        self.sent(self.PDX, zz, self.d, self.LOW)
        self.sent(self.PDY, zz, self.d, self.HIGH)

    def steps(self):
        n = self.nz
        todo = [(self.launch, 0), (self.mates, 0)]
        for j in range(1, n + 2):
            todo += [(self.launch, j), (self.mates, j - 1) if j > 1 else None, (self.relay, j - 1), (self.finish, j - 2)]
        return [functools.partial(f, j) for f, j in filter(None, todo) if 0 <= j < n]


def gather_kernel(nz, count, *refs):
    shards, outs = refs[:count], refs[count : 2 * count]
    send, recv, local = refs[2 * count :]
    z, e = place()
    greet(z, e, nz)
    g = Gather(nz, shards, outs, send, recv, local)
    for step in g.steps():
        step()
    for j in range(nz):
        g.shared(j)
    for j in range(nz):
        g.drain(j)


def gather_scratch(nz, count):
    return [
        pltpu.SemaphoreType.DMA((count, nz, Gather.KINDS)),
        pltpu.SemaphoreType.DMA((count, nz, Gather.KINDS)),
        pltpu.SemaphoreType.DMA((4, count)),
    ]


def gather_all(arrays, collective_id):
    nz, width = lax.axis_size("dp"), lax.axis_size("expert")
    count = len(arrays)
    parts = [a.reshape((4, a.shape[0] // 4) + a.shape[1:]) for a in arrays]
    outs = pl.pallas_call(
        functools.partial(gather_kernel, nz, count),
        out_shape=[jax.ShapeDtypeStruct((nz, width) + h.shape, h.dtype) for h in parts],
        in_specs=[pl.BlockSpec(memory_space=pltpu.VMEM)] * count,
        out_specs=[pl.BlockSpec(memory_space=pl.ANY)] * count,
        scratch_shapes=gather_scratch(nz, count),
        compiler_params=pltpu.CompilerParams(
            collective_id=collective_id, has_side_effects=True, vmem_limit_bytes=VMEM_LIMIT
        ),
        name="gather_all",
    )(*parts)
    return [o.reshape((nz * width * a.shape[0],) + a.shape[1:]) for o, a in zip(outs, arrays)]


def accumulate(dst, src):
    rows = dst.shape[0]
    block = 32 if rows % 32 == 0 else rows

    def body(r, _):
        at = pl.ds(pl.multiple_of(r * block, block), block)
        dst[at, :] = dst[at, :] + src[at, :]
        return 0

    lax.fori_loop(0, rows // block, body, 0)


class Scatter:
    X2, Y2, X3, Y3, Z, ZB, ZX, ZXB, ZY, ZYB, XQ, YQ = range(4, 16)
    KINDS = 16
    BUFFERS = 9

    def __init__(self, nz, terms, outs, sums, temps, from_x2, from_y2, from_x3, from_y3, from_z, from_zm, from_q, send, recv, local):
        self.nz, self.terms, self.outs = nz, terms, outs
        self.sums, self.temps = sums, temps
        self.from_x2, self.from_y2, self.from_x3, self.from_y3 = from_x2, from_y2, from_x3, from_y3
        self.from_z, self.from_zm, self.from_q = from_z, from_zm, from_q
        self.send, self.recv, self.local = send, recv, local
        self.count = len(terms)
        self.z, self.e = place()
        self.core, self.chip = self.e % 2, self.e // 2
        self.p, self.x, self.y = self.e ^ 1, self.e ^ 2, self.e ^ 4
        self.chips = (self.chip ^ 3, self.chip ^ 1, self.chip ^ 2, self.chip)

    def zz(self, j):
        return line_order(self.z, self.nz, self.nz - 1 - j)

    def remote(self, i, kind, zz, src, dst, dev):
        return pltpu.make_async_remote_copy(
            src_ref=src, dst_ref=dst, send_sem=self.send.at[i, zz, kind], recv_sem=self.recv.at[i, zz, kind],
            device_id=dev, device_id_type=MESH)

    def quarters(self, i, zz, q, first, n):
        return self.sums[i].at[zz, q, pl.ds(first, n)]

    def pair(self, i, j, q):
        zz, chip = self.zz(j), self.chips[q]
        return self.remote(i, q, zz, self.terms[i].at[zz, chip * 2 + (1 - self.core)], self.sums[i].at[zz, q],
                           (self.z, self.p))

    def load(self, i, j, q):
        slot = q % 2
        return pltpu.make_async_copy(
            self.terms[i].at[self.zz(j), self.chips[q] * 2 + self.core], self.temps[i].at[slot], self.local.at[i, slot])

    def x2(self, i, zz):
        return self.remote(i, self.X2, zz, self.quarters(i, zz, 0, 0, 2), self.from_x2[i].at[zz], (self.z, self.x))

    def y2(self, i, zz):
        return self.remote(i, self.Y2, zz, self.quarters(i, zz, 0, 2, 2), self.from_y2[i].at[zz], (self.z, self.y))

    def x3(self, i, zz):
        return self.remote(i, self.X3, zz, self.quarters(i, zz, 1, 0, 3), self.from_x3[i].at[zz], (self.z, self.x))

    def y3(self, i, zz):
        return self.remote(i, self.Y3, zz, self.quarters(i, zz, 2, 1, 3), self.from_y3[i].at[zz], (self.z, self.y))

    def xq(self, i):
        return self.remote(i, self.XQ, self.z, self.quarters(i, self.z, 1, 3, 1), self.from_q[i].at[pl.ds(0, 1)], (self.z, self.x))

    def yq(self, i):
        return self.remote(i, self.YQ, self.z, self.quarters(i, self.z, 2, 0, 1), self.from_q[i].at[pl.ds(1, 1)], (self.z, self.y))

    def line(self, i, zz, which, dz, last=False):
        slot = self.nz if last else zz
        kind = (self.Z, self.ZX, self.ZY)[which] + int(last)
        src = (self.sums[i].at[zz, 3], self.quarters(i, zz, 1, 3, 1), self.quarters(i, zz, 2, 0, 1))[which]
        dst = self.from_z[i].at[slot] if which == 0 else self.from_zm[i].at[slot, pl.ds(which - 1, 1)]
        return self.remote(i, kind, zz, src, dst, (self.z + dz, self.e))

    def add(self, i, zz, q, first, n, src):
        for k in range(n):
            accumulate(self.sums[i].at[zz, q, first + k], src.at[k])

    def begin(self):
        for j in range(self.nz):
            for q in range(4):
                for i in range(self.count):
                    self.pair(i, j, q).start()
        for i in range(self.count):
            self.load(i, 0, 0).start()

    def first(self, j):
        zz = self.zz(j)
        for q in range(4):
            for i in range(self.count):
                if q < 3:
                    self.load(i, j, q + 1).start()
                elif j < self.nz - 1:
                    self.load(i, j + 1, 0).start()
                self.pair(i, j, q).wait_recv()
                self.load(i, j, q).wait()
                self.add(i, zz, q, 0, 4, self.temps[i].at[q % 2])
                if q == 0:
                    self.x2(i, zz).start()
                    self.y2(i, zz).start()

    def second(self, j):
        zz = self.zz(j)
        for i in range(self.count):
            self.y2(i, zz).wait_recv()
            self.add(i, zz, 1, 2, 2, self.from_y2[i].at[zz])
            self.x3(i, zz).start()
            self.x2(i, zz).wait_recv()
            self.add(i, zz, 2, 0, 2, self.from_x2[i].at[zz])
            self.y3(i, zz).start()
            for which in (1, 2):
                self.flow(i, j, which)

    def flow(self, i, j, which):
        z, nz, zz = self.z, self.nz, self.zz(j)
        q, first, n = ((3, 0, 4), (1, 3, 1), (2, 0, 1))[which]

        def came(slot):
            ref = self.from_z[i].at[slot] if which == 0 else self.from_zm[i].at[slot, pl.ds(which - 1, 1)]
            self.add(i, zz, q, first, n, ref)

        if j < nz - 1:
            @pl.when(jnp.logical_or(jnp.logical_and(zz > z, z > 0), jnp.logical_and(zz < z, z < nz - 1)))
            def _():
                self.line(i, zz, which, 1).wait_recv()
                came(zz)

            @pl.when(zz > z)
            def _():
                self.line(i, zz, which, 1).start()

            @pl.when(zz < z - 1)
            def _():
                self.line(i, zz, which, -1).start()

            @pl.when(zz == z - 1)
            def _():
                self.line(i, zz, which, -1, True).start()
        else:
            @pl.when(z > 0)
            def _():
                self.line(i, zz, which, 1).wait_recv()
                came(zz)

            @pl.when(z < nz - 1)
            def _():
                self.line(i, zz, which, -1, True).wait_recv()
                came(nz)

            if which == 1:
                self.xq(i).start()
            if which == 2:
                self.yq(i).start()

    def third(self, j):
        zz = self.zz(j)
        for i in range(self.count):
            self.x3(i, zz).wait_recv()
            self.add(i, zz, 3, 0, 3, self.from_x3[i].at[zz])
            self.y3(i, zz).wait_recv()
            self.add(i, zz, 3, 1, 3, self.from_y3[i].at[zz])
            self.flow(i, j, 0)

    def result(self):
        for i in range(self.count):
            self.xq(i).wait_recv()
            self.add(i, self.z, 3, 3, 1, self.from_q[i].at[pl.ds(0, 1)])
            self.yq(i).wait_recv()
            self.add(i, self.z, 3, 0, 1, self.from_q[i].at[pl.ds(1, 1)])
            self.outs[i][...] = self.sums[i][self.z, 3].astype(self.outs[i].dtype)

    def drain(self, j):
        z, nz = self.z, self.nz
        zz = self.zz(j)
        for i in range(self.count):
            for q in range(4):
                self.pair(i, j, q).wait_send()
            for c in (self.x2, self.y2, self.x3, self.y3):
                c(i, zz).wait_send()
            if j < nz - 1:
                for which in range(3):
                    @pl.when(zz > z)
                    def _():
                        self.line(i, zz, which, 1).wait_send()

                    @pl.when(zz < z - 1)
                    def _():
                        self.line(i, zz, which, -1).wait_send()

                    @pl.when(zz == z - 1)
                    def _():
                        self.line(i, zz, which, -1, True).wait_send()
            else:
                self.xq(i).wait_send()
                self.yq(i).wait_send()

    def steps(self):
        todo = []
        for j in range(self.nz + 2):
            todo += [(self.first, j), (self.second, j - 1), (self.third, j - 2)]
        return [functools.partial(f, j) for f, j in todo if 0 <= j < self.nz] + [self.result]


def scatter_kernel(nz, count, *refs):
    groups = [refs[k * count : (k + 1) * count] for k in range(2 + Scatter.BUFFERS)]
    send, recv, local = refs[(2 + Scatter.BUFFERS) * count :]
    z, e = place()
    greet(z, e, nz)
    s = Scatter(nz, *groups, send, recv, local)
    s.begin()
    for step in s.steps():
        step()
    for j in range(nz):
        s.drain(j)


def scatter_sum(arrays, collective_id):
    nz, width = lax.axis_size("dp"), lax.axis_size("expert")
    count = len(arrays)
    devices = nz * width
    terms = [a.reshape(nz, width, 4, a.shape[0] // (4 * devices), a.shape[1]) for a in arrays]
    scratch = []
    shapes = [t.shape[3:] for t in terms]
    leads = ((nz, width // 2, 4), (2, 4), (nz, 2), (nz, 2), (nz, 3), (nz, 3), (nz + 1, 4), (nz + 1, 2), (2,))
    for lead in leads:
        scratch += [pltpu.VMEM(lead + s, a.dtype) for s, a in zip(shapes, arrays)]
    outs = pl.pallas_call(
        functools.partial(scatter_kernel, nz, count),
        out_shape=[jax.ShapeDtypeStruct((4,) + s, jnp.float32) for s in shapes],
        in_specs=[pl.BlockSpec(memory_space=pl.ANY)] * count,
        out_specs=[pl.BlockSpec(memory_space=pltpu.VMEM)] * count,
        scratch_shapes=scratch
        + [
            pltpu.SemaphoreType.DMA((count, nz, Scatter.KINDS)),
            pltpu.SemaphoreType.DMA((count, nz, Scatter.KINDS)),
            pltpu.SemaphoreType.DMA((count, 2)),
        ],
        compiler_params=pltpu.CompilerParams(
            collective_id=collective_id, has_side_effects=True, vmem_limit_bytes=VMEM_LIMIT
        ),
        name="scatter_sum",
    )(*terms)
    return [o.reshape(4 * s[0], s[1]) for o, s in zip(outs, shapes)]


def mm(a, b, da=1, db=0):
    return lax.dot_general(a, b, (((da,), (db,)), ((), ())), preferred_element_type=F32)


def expert_kernel(group, cap, x_ref, g_ref, gate_ref, rank_ref, wg_ref, wu_ref, wd_ref,
                  y_ref, r_ref, gg_ref, rows_ref, down_ref, act_ref, gp_ref, up_ref, cot_ref):
    length, width = x_ref.shape[1:]
    slot = lax.broadcasted_iota(jnp.int32, (cap, length), 0).astype(F32)
    picks, gates = [], []
    for s in range(group):
        hit = slot == rank_ref[s]
        pick = hit.astype(BF16)
        picks.append(pick)
        gate = jnp.sum(jnp.where(hit, gate_ref[s], 0.0), 1, keepdims=True)
        gates.append(gate)
        at = pl.ds(s * cap, cap)
        rows_ref[at, :] = mm(pick, x_ref[s]).astype(BF16)
        cot = mm(pick, g_ref[s])
        cot_ref[at, :] = cot.astype(BF16)
        down_ref[at, :] = (gate * cot).astype(BF16)
    gate_all = jnp.concatenate(gates, 0)
    rows = rows_ref[...]
    pre_gate = mm(rows, wg_ref[...])
    pre_up = mm(rows, wu_ref[...])
    sig = jax.nn.sigmoid(pre_gate)
    silu = pre_gate * sig
    act_ref[...] = (silu * pre_up).astype(BF16)
    act_grad = mm(down_ref[...], wd_ref[...], 1, 1)
    gp_ref[...] = (act_grad * pre_up * sig * (1.0 + pre_gate * (1.0 - sig))).astype(BF16)
    up_ref[...] = (act_grad * silu).astype(BF16)
    tile = 512
    gg = jnp.zeros((group * cap, 1), F32)
    for n in range(width // tile):
        cols = pl.ds(n * tile, tile)
        out = mm(act_ref[...], wd_ref[:, cols]).astype(BF16).astype(F32)
        gg = gg + jnp.sum(out * cot_ref[:, cols].astype(F32), 1, keepdims=True)
        out = (out * gate_all).astype(BF16)
        back = (mm(gp_ref[...], wg_ref[cols, :], 1, 1) + mm(up_ref[...], wu_ref[cols, :], 1, 1)).astype(BF16)
        for s in range(group):
            part = slice(s * cap, (s + 1) * cap)
            y_ref[s, :, cols] = mm(picks[s], out[part], 0, 0).astype(BF16)
            r_ref[s, :, cols] = mm(picks[s], back[part], 0, 0).astype(BF16)
    for s in range(group):
        gg_ref[s] = jnp.sum(picks[s].astype(F32) * gg[s * cap : (s + 1) * cap], 0, keepdims=True)


def experts(x, g, gate, rank, wg, wu, wd, cap, group):
    devices, length, width = x.shape
    ff = wg.shape[1]
    rows = devices * cap
    step = group * cap
    block = lambda *tail: pl.BlockSpec((group,) + tail, lambda i: (i,) + (0,) * len(tail))
    flat = lambda n: pl.BlockSpec((step, n), lambda i: (i, 0))
    whole = lambda a: pl.BlockSpec(a.shape, lambda i: (0, 0), pipeline_mode=pl.Buffered(1))
    return pl.pallas_call(
        functools.partial(expert_kernel, group, cap),
        grid=(devices // group,),
        in_specs=[block(length, width), block(length, width), block(1, length), block(1, length),
                  whole(wg), whole(wu), whole(wd)],
        out_specs=[block(length, width), block(length, width), block(1, length),
                   flat(width), flat(width), flat(ff), flat(ff), flat(ff)],
        out_shape=[
            jax.ShapeDtypeStruct((devices, length, width), BF16),
            jax.ShapeDtypeStruct((devices, length, width), BF16),
            jax.ShapeDtypeStruct((devices, 1, length), F32),
            jax.ShapeDtypeStruct((rows, width), BF16),
            jax.ShapeDtypeStruct((rows, width), BF16),
            jax.ShapeDtypeStruct((rows, ff), BF16),
            jax.ShapeDtypeStruct((rows, ff), BF16),
            jax.ShapeDtypeStruct((rows, ff), BF16),
        ],
        scratch_shapes=[pltpu.VMEM((step, width), BF16)],
        compiler_params=pltpu.CompilerParams(vmem_limit_bytes=VMEM_LIMIT, dimension_semantics=("arbitrary",)),
        name="experts",
    )(x, g, gate, rank, wg, wu, wd)


def pack_columns(columns, rows, lanes, dtype):
    parts = [c.astype(dtype) for c in columns]
    used = sum(c.shape[1] for c in parts)
    return jnp.concatenate(parts + [jnp.zeros((rows, lanes - used), dtype)], 1)


def spread(vector, devices, rows):
    blocks = vector.reshape(devices, -1)
    return jnp.pad(blocks, ((0, 0), (0, rows - blocks.shape[1]))).reshape(devices * rows, 1)


def per_device_gather(
    hidden_in,
    segment_ids,
    expert_ids,
    attn_gain,
    query_gain,
    key_gain,
    w_query,
    w_key,
    w_value,
    w_output,
    mlp_gain,
    w_router,
    w_gate,
    w_up,
    w_down,
    out_grad,
):
    devices = lax.axis_size(("dp", "expert"))
    me = lax.axis_index(("dp", "expert"))
    length, choices = expert_ids.shape
    width = hidden_in.shape[1]
    experts_total = devices
    capacity = 5 * length * choices // (4 * experts_total)
    query_cols, key_cols = w_query.shape[1], w_key.shape[1]
    rows = w_query.shape[0]
    head_rows = query_gain.shape[0]

    column = lambda v: jnp.pad(v, (0, rows - v.shape[0]))[:, None]
    lanes = 128 * pl.cdiv(experts_total + 4, 128)
    small = pack_columns(
        [w_router, column(attn_gain), column(mlp_gain), column(query_gain), column(key_gain)], rows, lanes, BF16
    )
    w_mixed = jnp.concatenate([w_query, w_key, w_value], 1)
    w_mixed, w_out, small = gather_all([w_mixed, w_output, small], 1)
    router = small[:, :experts_total]
    attn_gain, mlp_gain = small[:, experts_total], small[:, experts_total + 1]
    heads_of = small.reshape(devices, rows, lanes)[:, :head_rows]
    query_gain = heads_of[:, :, experts_total + 2].reshape(-1)
    key_gain = heads_of[:, :, experts_total + 3].reshape(-1)

    group_size = HEADS // KV_HEADS
    plain_in = hidden_in.astype(F32)
    inv_attn = rms_scale(plain_in)
    normed_attn = (plain_in * inv_attn * attn_gain).astype(BF16)
    mixed = jnp.dot(normed_attn, w_mixed, preferred_element_type=F32)
    query_raw = mixed[:, :query_cols].reshape(length, HEADS, HEAD_DIM)
    key_raw = mixed[:, query_cols : query_cols + key_cols].reshape(length, KV_HEADS, HEAD_DIM)
    value_rows = mixed[:, query_cols + key_cols :].astype(BF16).reshape(length, KV_HEADS, HEAD_DIM)
    query_scale = rms_scale(query_raw)
    key_scale = rms_scale(key_raw)
    cosine_table, sine_table = rope_tables(jnp.arange(length) % TOK_DEV, HEAD_DIM)
    query_rot = rotate(query_raw * query_scale * query_gain, cosine_table, sine_table).astype(BF16)
    query_rot = query_rot.reshape(length, KV_HEADS, group_size, HEAD_DIM)
    key_rot = rotate(key_raw * key_scale * key_gain, cosine_table, sine_table).astype(BF16)
    position = jnp.arange(length)
    allowed = (segment_ids[:, None] == segment_ids[None, :]) & (position[None, :] <= position[:, None])
    attended, log_totals = attend(query_rot, key_rot, value_rows, allowed)
    attended = attended.reshape(length, HEADS * HEAD_DIM)
    residual = plain_in + jnp.dot(attended, w_out, preferred_element_type=F32)

    inv_mlp = rms_scale(residual)
    normed_mlp = (residual * inv_mlp * mlp_gain).astype(BF16)
    logits = jnp.dot(normed_mlp, router, preferred_element_type=F32)
    chosen = jnp.any(expert_ids[:, :, None] == jnp.arange(experts_total)[None, None, :], 1)
    raised = jnp.where(chosen, jnp.exp(logits), 0.0)
    gate = raised / jnp.sum(raised, -1, keepdims=True)
    not_after = (position[None, :] <= position[:, None]).astype(BF16)
    rank = jnp.dot(not_after, chosen.astype(BF16), preferred_element_type=F32) - 1.0
    rank = jnp.where(chosen, rank, -1.0)
    gate_high = lax.reduce_precision(gate, 8, 7)
    table = jnp.concatenate([gate_high, gate - gate_high, rank], 1).T.astype(BF16)

    all_rows, all_tables = gather_all([normed_mlp, table], 2)
    (all_grads,) = gather_all([out_grad], 3)
    mine = lax.dynamic_index_in_dim(
        all_tables.reshape(devices, 3, experts_total, length), me, 2, keepdims=False
    ).astype(F32)
    cube = (devices, length, width)
    y_terms, r_terms, gate_terms, rows_in, down_in, act, gate_pre_grad, up_pre_grad = experts(
        all_rows.reshape(cube), all_grads.reshape(cube), mine[:, :1] + mine[:, 1:2], mine[:, 2:],
        w_gate[0], w_up[0], w_down[0], capacity, 4,
    )
    is_me = (jnp.arange(experts_total) == me).astype(F32)
    gate_terms = (gate_terms * is_me[None, :, None]).reshape(devices * experts_total, length)
    row_grad_sum, gate_grad = scatter_sum([r_terms.reshape(devices * length, width), gate_terms], 4)
    (mixed_out,) = scatter_sum([y_terms.reshape(devices * length, width)], 5)
    block_out = residual + mixed_out
    grad_w_down = jnp.dot(act.T, down_in, preferred_element_type=F32)[None]
    grad_w_gate = jnp.dot(rows_in.T, gate_pre_grad, preferred_element_type=F32)[None]
    grad_w_up = jnp.dot(rows_in.T, up_pre_grad, preferred_element_type=F32)[None]

    gate_grad = gate_grad.T
    sel_grad = gate * (gate_grad - jnp.sum(gate * gate_grad, -1, keepdims=True))
    logit_grad = jnp.where(chosen, sel_grad, 0.0).astype(BF16)
    grad_w_router = jnp.dot(normed_mlp.T, logit_grad, preferred_element_type=F32)
    normed_mlp_grad = row_grad_sum + jnp.dot(logit_grad, router.T, preferred_element_type=F32)
    grad_mlp_gain = jnp.sum(normed_mlp_grad * residual * inv_mlp, 0)
    residual_grad = out_grad.astype(F32) + norm_grad(normed_mlp_grad, residual, inv_mlp, mlp_gain)

    branch_grad = residual_grad.astype(BF16)
    grad_w_output = jnp.dot(attended.T, branch_grad, preferred_element_type=F32).astype(BF16)
    attended_grad = jnp.dot(branch_grad, w_out.T, preferred_element_type=F32).astype(BF16)
    attended_grad = attended_grad.reshape(length, KV_HEADS, group_size, HEAD_DIM)
    query_rot_grad, key_rot_grad, value_sum_grad = attend_grad(
        query_rot, key_rot, value_rows, allowed, log_totals, attended_grad
    )
    query_normed_grad = unrotate(query_rot_grad.reshape(length, HEADS, HEAD_DIM), cosine_table, sine_table)
    key_normed_grad = unrotate(key_rot_grad, cosine_table, sine_table)
    grad_query_gain = jnp.sum(query_normed_grad * query_raw * query_scale, (0, 1))
    grad_key_gain = jnp.sum(key_normed_grad * key_raw * key_scale, (0, 1))
    query_grad = norm_grad(query_normed_grad, query_raw, query_scale, query_gain).astype(BF16)
    key_grad = norm_grad(key_normed_grad, key_raw, key_scale, key_gain).astype(BF16)
    mixed_grad = jnp.concatenate(
        [
            query_grad.reshape(length, query_cols),
            key_grad.reshape(length, key_cols),
            value_sum_grad.astype(BF16).reshape(length, key_cols),
        ],
        1,
    )
    grad_w_mixed = jnp.dot(normed_attn.T, mixed_grad, preferred_element_type=F32).astype(BF16)
    normed_attn_grad = jnp.dot(mixed_grad, w_mixed.T, preferred_element_type=F32)
    grad_attn_gain = jnp.sum(normed_attn_grad * plain_in * inv_attn, 0)
    grad_in = residual_grad + norm_grad(normed_attn_grad, plain_in, inv_attn, attn_gain)

    small_grads = pack_columns(
        [
            grad_w_router,
            grad_attn_gain[:, None],
            grad_mlp_gain[:, None],
            spread(grad_query_gain, devices, rows),
            spread(grad_key_gain, devices, rows),
        ],
        width,
        lanes,
        F32,
    )
    share_mixed, share_w_output, share_small = scatter_sum([grad_w_mixed, grad_w_output, small_grads], 6)
    return (
        block_out,
        grad_in,
        share_small[:, experts_total],
        share_small[:head_rows, experts_total + 2],
        share_small[:head_rows, experts_total + 3],
        share_mixed[:, :query_cols],
        share_mixed[:, query_cols : query_cols + key_cols],
        share_mixed[:, query_cols + key_cols :],
        share_w_output,
        share_small[:, experts_total + 1],
        share_small[:, :experts_total],
        grad_w_gate,
        grad_w_up,
        grad_w_down,
    )


def per_device(*arguments):
    expert_ids, w_gate = arguments[2], arguments[12]
    devices, width = lax.axis_size(("dp", "expert")), lax.axis_size("expert")
    length, choices = expert_ids.shape
    capacity = 5 * length * choices // (4 * devices)
    dense = devices <= 4 * choices and w_gate.shape[0] == 1 and width == 8
    if dense and capacity % 16 == 0 and devices % 4 == 0:
        return per_device_gather(*arguments)
    return per_device_exchange(*arguments)


def solution(mesh):
    in_specs = (
        P(("dp", "expert"), None),
        P(("dp", "expert")),
        P(("dp", "expert"), None),
        P(("dp", "expert")),
        P(("dp", "expert")),
        P(("dp", "expert")),
        P(("dp", "expert"), None),
        P(("dp", "expert"), None),
        P(("dp", "expert"), None),
        P(("dp", "expert"), None),
        P(("dp", "expert")),
        P(("dp", "expert"), None),
        P(("dp", "expert"), None, None),
        P(("dp", "expert"), None, None),
        P(("dp", "expert"), None, None),
        P(("dp", "expert"), None),
    )
    out_specs = (
        P(("dp", "expert"), None),
        P(("dp", "expert"), None),
        P(("dp", "expert")),
        P(("dp", "expert")),
        P(("dp", "expert")),
        P(("dp", "expert"), None),
        P(("dp", "expert"), None),
        P(("dp", "expert"), None),
        P(("dp", "expert"), None),
        P(("dp", "expert")),
        P(("dp", "expert"), None),
        P(("dp", "expert"), None, None),
        P(("dp", "expert"), None, None),
        P(("dp", "expert"), None, None),
    )
    return jax.shard_map(
        per_device, mesh=mesh, in_specs=in_specs, out_specs=out_specs, check_vma=False
    )
```

```python
import functools
import math

import jax
import jax.numpy as jnp
from jax import lax
from jax.experimental import pallas as pl
from jax.experimental.pallas import tpu as pltpu
from jax.sharding import PartitionSpec as P

F32, BF16 = jnp.float32, jnp.bfloat16
MESH = pl.DeviceIdType.MESH
VMEM_LIMIT = 63 * 1024 * 1024


HEADS = 32
KV_HEADS = 4
HEAD_DIM = 128
TOK_DEV = 256


EPS = 1e-06
ROPE_BASE = 1000000.0


def rms_scale(values):
    return lax.rsqrt(jnp.mean(values * values, -1, keepdims=True) + EPS)


def norm_grad(upstream, values, inverse, gain_vec):
    weighted = upstream * gain_vec
    return inverse * weighted - values * inverse**3 * jnp.mean(weighted * values, -1, keepdims=True)


def rope_tables(positions, head_dim):
    half_dim = head_dim // 2
    frequency = ROPE_BASE ** (-(jnp.arange(half_dim).astype(jnp.float32) * 2.0 / head_dim))
    angles = positions.astype(jnp.float32)[:, None] * frequency[None, :]
    return (jnp.cos(angles)[:, None, :], jnp.sin(angles)[:, None, :])


def rotate(values, cosine_table, sine_table):
    half_dim = values.shape[-1] // 2
    first_half = values[..., :half_dim]
    second_half = values[..., half_dim:]
    return jnp.concatenate(
        [
            first_half * cosine_table - second_half * sine_table,
            second_half * cosine_table + first_half * sine_table,
        ],
        -1,
    )


def unrotate(values, cosine_table, sine_table):
    half_dim = values.shape[-1] // 2
    first_half = values[..., :half_dim]
    second_half = values[..., half_dim:]
    return jnp.concatenate(
        [
            first_half * cosine_table + second_half * sine_table,
            second_half * cosine_table - first_half * sine_table,
        ],
        -1,
    )


def attend(query_rot, key_rot, value_rows, allowed):
    score_scale = 1.0 / math.sqrt(HEAD_DIM)
    scores = (
        jnp.einsum("qkgd,tkd->kgqt", query_rot, key_rot, preferred_element_type=jnp.float32)
        * score_scale
    )
    exp_scores = jnp.where(allowed, jnp.exp(scores), 0.0)
    totals = jnp.sum(exp_scores, -1, keepdims=True)
    probs_low = (exp_scores / totals).astype(jnp.bfloat16)
    attended = jnp.einsum(
        "kgqt,tkd->qkgd", probs_low, value_rows, preferred_element_type=jnp.float32
    ).astype(jnp.bfloat16)
    return (attended, jnp.log(totals))


def attend_grad(query_rot, key_rot, value_rows, allowed, log_totals, attended_grad):
    score_scale = 1.0 / math.sqrt(HEAD_DIM)
    scores = (
        jnp.einsum("qkgd,tkd->kgqt", query_rot, key_rot, preferred_element_type=jnp.float32)
        * score_scale
    )
    probs_back = jnp.where(allowed, jnp.exp(scores - log_totals), 0.0)
    probs_low = probs_back.astype(jnp.bfloat16)
    value_sum_grad = jnp.einsum(
        "kgqt,qkgd->tkd", probs_low, attended_grad, preferred_element_type=jnp.float32
    )
    prob_grad = jnp.einsum(
        "qkgd,tkd->kgqt", attended_grad, value_rows, preferred_element_type=jnp.float32
    )
    score_grad = (
        probs_back * (prob_grad - jnp.sum(probs_back * prob_grad, -1, keepdims=True))
    ).astype(jnp.bfloat16)
    query_rot_grad = (
        jnp.einsum("kgqt,tkd->qkgd", score_grad, key_rot, preferred_element_type=jnp.float32)
        * score_scale
    )
    key_rot_grad = (
        jnp.einsum("kgqt,qkgd->tkd", score_grad, query_rot, preferred_element_type=jnp.float32)
        * score_scale
    )
    return (query_rot_grad, key_rot_grad, value_sum_grad)


def mixer_forward(block_in, block_segments, weights):
    w_query, w_key, w_value, w_output, w_router, attn_gain, mlp_gain, query_gain, key_gain = weights
    row_count = block_in.shape[0]
    seq_count = row_count // TOK_DEV
    group_size = HEADS // KV_HEADS
    plain_in = block_in.astype(jnp.float32)
    inv_attn = rms_scale(plain_in)
    normed_attn = (plain_in * inv_attn * attn_gain).astype(jnp.bfloat16)
    query_raw = jnp.dot(normed_attn, w_query, preferred_element_type=jnp.float32).reshape(
        row_count, HEADS, HEAD_DIM
    )
    key_raw = jnp.dot(normed_attn, w_key, preferred_element_type=jnp.float32).reshape(
        row_count, KV_HEADS, HEAD_DIM
    )
    value_rows = jnp.dot(normed_attn, w_value, preferred_element_type=jnp.float32).astype(
        jnp.bfloat16
    )
    value_rows = value_rows.reshape(seq_count, TOK_DEV, KV_HEADS, HEAD_DIM)
    query_scale = rms_scale(query_raw)
    key_scale = rms_scale(key_raw)
    cosine_table, sine_table = rope_tables(jnp.arange(row_count) % TOK_DEV, HEAD_DIM)
    query_rot = rotate(query_raw * query_scale * query_gain, cosine_table, sine_table).astype(
        jnp.bfloat16
    )
    query_rot = query_rot.reshape(seq_count, TOK_DEV, KV_HEADS, group_size, HEAD_DIM)
    key_rot = rotate(key_raw * key_scale * key_gain, cosine_table, sine_table).astype(jnp.bfloat16)
    key_rot = key_rot.reshape(seq_count, TOK_DEV, KV_HEADS, HEAD_DIM)
    segments = block_segments.reshape(seq_count, TOK_DEV)
    position = jnp.arange(TOK_DEV)
    allowed = (segments[:, :, None] == segments[:, None, :]) & (
        position[None, None, :] <= position[None, :, None]
    )
    attended, log_totals = jax.vmap(attend)(query_rot, key_rot, value_rows, allowed)
    attended = attended.reshape(row_count, HEADS * HEAD_DIM)
    residual = plain_in + jnp.dot(attended, w_output, preferred_element_type=jnp.float32)
    saved_state = (
        plain_in,
        inv_attn,
        normed_attn,
        query_raw,
        key_raw,
        value_rows,
        query_scale,
        key_scale,
        query_rot,
        key_rot,
        allowed,
        log_totals,
        attended,
        cosine_table,
        sine_table,
    )
    return (residual, saved_state)


def mixer_backward(residual_grad, saved_state, weights):
    w_query, w_key, w_value, w_output, w_router, attn_gain, mlp_gain, query_gain, key_gain = weights
    (
        plain_in,
        inv_attn,
        normed_attn,
        query_raw,
        key_raw,
        value_rows,
        query_scale,
        key_scale,
        query_rot,
        key_rot,
        allowed,
        log_totals,
        attended,
        cosine_table,
        sine_table,
    ) = saved_state
    row_count = residual_grad.shape[0]
    seq_count = row_count // TOK_DEV
    group_size = HEADS // KV_HEADS
    branch_grad = residual_grad.astype(jnp.bfloat16)
    grad_w_output = jnp.dot(attended.T, branch_grad, preferred_element_type=jnp.float32)
    attended_grad = jnp.dot(branch_grad, w_output.T, preferred_element_type=jnp.float32).astype(
        jnp.bfloat16
    )
    attended_grad = attended_grad.reshape(seq_count, TOK_DEV, KV_HEADS, group_size, HEAD_DIM)
    query_rot_grad, key_rot_grad, value_sum_grad = jax.vmap(attend_grad)(
        query_rot, key_rot, value_rows, allowed, log_totals, attended_grad
    )
    query_normed_grad = unrotate(
        query_rot_grad.reshape(row_count, HEADS, HEAD_DIM), cosine_table, sine_table
    )
    key_normed_grad = unrotate(
        key_rot_grad.reshape(row_count, KV_HEADS, HEAD_DIM), cosine_table, sine_table
    )
    grad_query_gain = jnp.sum(query_normed_grad * query_raw * query_scale, (0, 1))
    grad_key_gain = jnp.sum(key_normed_grad * key_raw * key_scale, (0, 1))
    query_grad = norm_grad(query_normed_grad, query_raw, query_scale, query_gain).astype(
        jnp.bfloat16
    )
    query_grad = query_grad.reshape(row_count, HEADS * HEAD_DIM)
    key_grad = norm_grad(key_normed_grad, key_raw, key_scale, key_gain).astype(jnp.bfloat16)
    key_grad = key_grad.reshape(row_count, KV_HEADS * HEAD_DIM)
    value_grad = value_sum_grad.astype(jnp.bfloat16).reshape(row_count, KV_HEADS * HEAD_DIM)
    grad_w_query = jnp.dot(normed_attn.T, query_grad, preferred_element_type=jnp.float32)
    grad_w_key = jnp.dot(normed_attn.T, key_grad, preferred_element_type=jnp.float32)
    grad_w_value = jnp.dot(normed_attn.T, value_grad, preferred_element_type=jnp.float32)
    normed_attn_grad = (
        jnp.dot(query_grad, w_query.T, preferred_element_type=jnp.float32)
        + jnp.dot(key_grad, w_key.T, preferred_element_type=jnp.float32)
        + jnp.dot(value_grad, w_value.T, preferred_element_type=jnp.float32)
    )
    grad_attn_gain = jnp.sum(normed_attn_grad * plain_in * inv_attn, 0)
    grad_in = residual_grad + norm_grad(normed_attn_grad, plain_in, inv_attn, attn_gain)
    return (
        grad_in,
        (
            grad_attn_gain,
            grad_query_gain,
            grad_key_gain,
            grad_w_query,
            grad_w_key,
            grad_w_value,
            grad_w_output,
        ),
    )


def dispatch_table(expert_rows, experts, capacity):
    length, choices = expert_rows.shape
    flat_ids = expert_rows.reshape(length * choices)
    marks = (flat_ids[:, None] == jnp.arange(experts)[None, :]).astype(jnp.int32)
    earlier = jnp.cumsum(marks, 0) - marks
    destination = flat_ids * capacity + jnp.sum(earlier * marks, -1)
    pair_ids = (
        jnp.zeros((experts * capacity,), jnp.int32)
        .at[destination]
        .set(jnp.arange(length * choices, dtype=jnp.int32))
    )
    filled = jnp.zeros((experts * capacity,), jnp.bfloat16).at[destination].set(1.0)
    return (destination, pair_ids, filled)


def move_rows(row_block, section_name):
    if section_name == "dispatch":
        return lax.all_to_all(row_block, ("dp", "expert"), split_axis=0, concat_axis=0, tiled=True)
    if section_name == "combine":
        return lax.all_to_all(row_block, ("dp", "expert"), split_axis=0, concat_axis=0, tiled=True)
    if section_name == "grad_dispatch":
        return lax.all_to_all(row_block, ("dp", "expert"), split_axis=0, concat_axis=0, tiled=True)
    return lax.all_to_all(row_block, ("dp", "expert"), split_axis=0, concat_axis=0, tiled=True)


def per_device_exchange(
    hidden_in,
    segment_ids,
    expert_ids,
    attn_gain,
    query_gain,
    key_gain,
    w_query,
    w_key,
    w_value,
    w_output,
    mlp_gain,
    w_router,
    w_gate,
    w_up,
    w_down,
    out_grad,
):
    weights = (
        lax.all_gather(w_query, ("dp", "expert"), axis=0, tiled=True),
        lax.all_gather(w_key, ("dp", "expert"), axis=0, tiled=True),
        lax.all_gather(w_value, ("dp", "expert"), axis=0, tiled=True),
        lax.all_gather(w_output, ("dp", "expert"), axis=0, tiled=True),
        lax.all_gather(w_router, ("dp", "expert"), axis=0, tiled=True),
        lax.all_gather(attn_gain, ("dp", "expert"), axis=0, tiled=True),
        lax.all_gather(mlp_gain, ("dp", "expert"), axis=0, tiled=True),
        lax.all_gather(query_gain, ("dp", "expert"), axis=0, tiled=True),
        lax.all_gather(key_gain, ("dp", "expert"), axis=0, tiled=True),
    )
    residual, saved_state = mixer_forward(hidden_in, segment_ids, weights)
    full_router = weights[4]
    full_mlp_gain = weights[6]
    inv_mlp = rms_scale(residual)
    normed_mlp = (residual * inv_mlp * full_mlp_gain).astype(jnp.bfloat16)
    logits = jnp.dot(normed_mlp, full_router, preferred_element_type=jnp.float32)
    device_count = lax.axis_size(("dp", "expert"))
    local_experts = w_gate.shape[0]
    experts = local_experts * device_count
    length, choices = expert_ids.shape
    model_width = hidden_in.shape[1]
    capacity = 5 * length * choices // (4 * experts)
    one_hot = expert_ids[:, :, None] == jnp.arange(experts)[None, None, :]
    chosen = jnp.sum(jnp.where(one_hot, logits[:, None, :], 0.0), -1)
    raised = jnp.exp(chosen)
    gate_weights = raised / jnp.sum(raised, -1, keepdims=True)
    destination, pair_ids, filled = dispatch_table(expert_ids, experts, capacity)
    send_rows = normed_mlp[pair_ids // choices] * filled[:, None]
    received = move_rows(
        send_rows.reshape(device_count, local_experts * capacity, model_width), "dispatch"
    )
    received = received.reshape(device_count, local_experts, capacity, model_width)
    pre_gate = jnp.einsum("secd,edf->secf", received, w_gate, preferred_element_type=jnp.float32)
    pre_up = jnp.einsum("secd,edf->secf", received, w_up, preferred_element_type=jnp.float32)
    gate_sigmoid = jax.nn.sigmoid(pre_gate)
    silu_gate = pre_gate * gate_sigmoid
    activation = (silu_gate * pre_up).astype(jnp.bfloat16)
    expert_out = jnp.einsum(
        "secf,efd->secd", activation, w_down, preferred_element_type=jnp.float32
    ).astype(jnp.bfloat16)
    returned = move_rows(
        expert_out.reshape(device_count, local_experts * capacity, model_width), "combine"
    )
    picked = returned.reshape(experts * capacity, model_width)[destination].reshape(
        length, choices, model_width
    )
    block_out = residual + jnp.sum(gate_weights[:, :, None] * picked.astype(jnp.float32), 1)
    weights = (
        lax.all_gather(w_query, ("dp", "expert"), axis=0, tiled=True),
        lax.all_gather(w_key, ("dp", "expert"), axis=0, tiled=True),
        lax.all_gather(w_value, ("dp", "expert"), axis=0, tiled=True),
        lax.all_gather(w_output, ("dp", "expert"), axis=0, tiled=True),
        lax.all_gather(w_router, ("dp", "expert"), axis=0, tiled=True),
        lax.all_gather(attn_gain, ("dp", "expert"), axis=0, tiled=True),
        lax.all_gather(mlp_gain, ("dp", "expert"), axis=0, tiled=True),
        lax.all_gather(query_gain, ("dp", "expert"), axis=0, tiled=True),
        lax.all_gather(key_gain, ("dp", "expert"), axis=0, tiled=True),
    )
    full_router = weights[4]
    full_mlp_gain = weights[6]
    cotangent = out_grad.astype(jnp.float32)
    gate_grad = jnp.sum(cotangent[:, None, :] * picked.astype(jnp.float32), -1)
    down_in = (
        (gate_weights[:, :, None] * cotangent[:, None, :])
        .astype(jnp.bfloat16)
        .reshape(length * choices, model_width)
    )
    send_grad = down_in[pair_ids] * filled[:, None]
    recv_grad = move_rows(
        send_grad.reshape(device_count, local_experts * capacity, model_width), "grad_dispatch"
    )
    recv_grad = recv_grad.reshape(device_count, local_experts, capacity, model_width)
    act_grad = jnp.einsum("secd,efd->secf", recv_grad, w_down, preferred_element_type=jnp.float32)
    grad_w_down = jnp.einsum(
        "secf,secd->efd", activation, recv_grad, preferred_element_type=jnp.float32
    )
    gate_pre_grad = (
        act_grad * pre_up * gate_sigmoid * (1.0 + pre_gate * (1.0 - gate_sigmoid))
    ).astype(jnp.bfloat16)
    up_pre_grad = (act_grad * silu_gate).astype(jnp.bfloat16)
    grad_w_gate = jnp.einsum(
        "secd,secf->edf", received, gate_pre_grad, preferred_element_type=jnp.float32
    )
    grad_w_up = jnp.einsum(
        "secd,secf->edf", received, up_pre_grad, preferred_element_type=jnp.float32
    )
    row_grad = (
        jnp.einsum("secf,edf->secd", gate_pre_grad, w_gate, preferred_element_type=jnp.float32)
        + jnp.einsum("secf,edf->secd", up_pre_grad, w_up, preferred_element_type=jnp.float32)
    ).astype(jnp.bfloat16)
    row_back = move_rows(
        row_grad.reshape(device_count, local_experts * capacity, model_width), "grad_return"
    )
    row_back = row_back.reshape(experts * capacity, model_width)[destination].reshape(
        length, choices, model_width
    )
    sel_grad = gate_weights * (gate_grad - jnp.sum(gate_weights * gate_grad, -1, keepdims=True))
    logit_grad = jnp.sum(jnp.where(one_hot, sel_grad[:, :, None], 0.0), 1).astype(jnp.bfloat16)
    grad_w_router = jnp.dot(normed_mlp.T, logit_grad, preferred_element_type=jnp.float32)
    normed_mlp_grad = jnp.sum(row_back.astype(jnp.float32), 1) + jnp.dot(
        logit_grad, full_router.T, preferred_element_type=jnp.float32
    )
    grad_mlp_gain = jnp.sum(normed_mlp_grad * residual * inv_mlp, 0)
    residual_grad = cotangent + norm_grad(normed_mlp_grad, residual, inv_mlp, full_mlp_gain)
    grad_in, mixer_terms = mixer_backward(residual_grad, saved_state, weights)
    (
        grad_attn_gain,
        grad_query_gain,
        grad_key_gain,
        grad_w_query,
        grad_w_key,
        grad_w_value,
        grad_w_output,
    ) = mixer_terms
    summed = (
        lax.psum_scatter(grad_w_query, ("dp", "expert"), scatter_dimension=0, tiled=True),
        lax.psum_scatter(grad_w_key, ("dp", "expert"), scatter_dimension=0, tiled=True),
        lax.psum_scatter(grad_w_value, ("dp", "expert"), scatter_dimension=0, tiled=True),
        lax.psum_scatter(grad_w_output, ("dp", "expert"), scatter_dimension=0, tiled=True),
        lax.psum_scatter(grad_w_router, ("dp", "expert"), scatter_dimension=0, tiled=True),
        lax.psum_scatter(grad_attn_gain, ("dp", "expert"), scatter_dimension=0, tiled=True),
        lax.psum_scatter(grad_mlp_gain, ("dp", "expert"), scatter_dimension=0, tiled=True),
        lax.psum_scatter(grad_query_gain, ("dp", "expert"), scatter_dimension=0, tiled=True),
        lax.psum_scatter(grad_key_gain, ("dp", "expert"), scatter_dimension=0, tiled=True),
    )
    (
        share_w_query,
        share_w_key,
        share_w_value,
        share_w_output,
        share_w_router,
        share_attn_gain,
        share_mlp_gain,
        share_query_gain,
        share_key_gain,
    ) = summed
    return (
        block_out,
        grad_in,
        share_attn_gain,
        share_query_gain,
        share_key_gain,
        share_w_query,
        share_w_key,
        share_w_value,
        share_w_output,
        share_mlp_gain,
        share_w_router,
        grad_w_gate,
        grad_w_up,
        grad_w_down,
    )


def place():
    z = lax.axis_index("dp")
    e = lax.axis_index("expert")
    return z, e


def line_order(z, nz, j):
    near = jnp.minimum(z, nz - 1 - z)
    step = (j + 1) // 2
    zigzag = z + (step if j % 2 == 0 else -step)
    tail = jnp.where(z < nz - 1 - z, j, nz - 1 - j)
    return jnp.where(j <= 2 * near, zigzag, tail)


def greet(z, e, nz):
    barrier = pltpu.get_barrier_semaphore()
    for mate in (e ^ 1, e ^ 2, e ^ 4):
        pl.semaphore_signal(barrier, inc=1, device_id=(z, mate), device_id_type=MESH)

    @pl.when(z > 0)
    def _():
        pl.semaphore_signal(barrier, inc=1, device_id=(z - 1, e), device_id_type=MESH)

    @pl.when(z < nz - 1)
    def _():
        pl.semaphore_signal(barrier, inc=1, device_id=(z + 1, e), device_id_type=MESH)

    ends = (z > 0).astype(jnp.int32) + (z < nz - 1).astype(jnp.int32)
    pl.semaphore_wait(barrier, 3 + ends)


class Gather:
    Z, ZX, ZY, X3, X2, XQ, Y3, Y2, YQ, P0, PX3, PXQ, PY3, PYQ, PDX, PDY = range(16)
    KINDS = 16
    WHOLE, LOW, HIGH, LOW3, HIGH3, Q0, Q3 = (0, 4), (0, 2), (2, 2), (0, 3), (1, 3), (0, 1), (3, 1)

    def __init__(self, nz, shards, outs, send, recv, local):
        self.nz, self.shards, self.outs = nz, shards, outs
        self.send, self.recv, self.local = send, recv, local
        self.z, self.e = place()
        self.p, self.x, self.y, self.d = self.e ^ 1, self.e ^ 2, self.e ^ 4, self.e ^ 6

    def zz(self, j):
        return line_order(self.z, self.nz, j)

    def part(self, ref, piece):
        return ref.at[pl.ds(piece[0], piece[1])]

    def copy(self, i, kind, zz, ee, piece, dev, mine=False, sem=None):
        dst = self.part(self.outs[i].at[zz, ee], piece)
        return pltpu.make_async_remote_copy(
            src_ref=self.part(self.shards[i], piece) if mine else dst,
            dst_ref=dst,
            send_sem=self.send.at[i, zz, kind] if sem is None else sem,
            recv_sem=self.recv.at[i, zz, kind],
            device_id=dev,
            device_id_type=MESH,
        )

    def start(self, kind, zz, ee, piece, dev, mine=False):
        for i in range(len(self.outs)):
            self.copy(i, kind, zz, ee, piece, dev, mine).start()

    def arrived(self, kind, zz, ee, piece):
        for i in range(len(self.outs)):
            self.copy(i, kind, zz, ee, piece, (self.z, self.e)).wait_recv()

    def sent(self, kind, zz, ee, piece, mine=False):
        for i in range(len(self.outs)):
            self.copy(i, kind, zz, ee, piece, (self.z, self.e), mine).wait_send()

    def along(self, j, kind, ee, piece, act):
        z, e, nz = self.z, self.e, self.nz
        zz, mine = self.zz(j), j == 0 and kind == self.Z
        for i in range(len(self.outs)):
            @pl.when(jnp.logical_and(zz <= z, z < nz - 1))
            def _():
                act(self.copy(i, kind, zz, ee, piece, (z + 1, e), mine))

            @pl.when(jnp.logical_and(zz >= z, z > 0))
            def _():
                sem = self.local.at[1 + kind, i] if j == 0 else None
                act(self.copy(i, kind, zz, ee, piece, (z - 1, e), mine, sem))

    def keep(self, i):
        return pltpu.make_async_copy(self.shards[i], self.outs[i].at[self.z, self.e], self.local.at[0, i])

    def launch(self, j):
        z, e, zz, mine = self.z, self.e, self.zz(j), j == 0
        if not mine:
            self.arrived(self.Z, zz, e, self.WHOLE)
        else:
            self.start(self.XQ, zz, e, self.Q3, (z, self.x), mine)
            self.start(self.YQ, zz, e, self.Q0, (z, self.y), mine)
        self.along(j, self.Z, e, self.WHOLE, lambda c: c.start())
        self.start(self.X3, zz, e, self.LOW3, (z, self.x), mine)
        self.start(self.Y3, zz, e, self.HIGH3, (z, self.y), mine)
        self.start(self.P0, zz, e, self.WHOLE, (z, self.p), mine)
        if mine:
            for i in range(len(self.outs)):
                self.keep(i).start()

    def mates(self, j):
        zz, mine = self.zz(j), j == 0
        self.arrived(self.XQ if mine else self.ZX, zz, self.x, self.Q3)
        self.along(j, self.ZX, self.x, self.Q3, lambda c: c.start())
        self.start(self.PXQ, zz, self.x, self.Q3, (self.z, self.p))
        self.arrived(self.YQ if mine else self.ZY, zz, self.y, self.Q0)
        self.along(j, self.ZY, self.y, self.Q0, lambda c: c.start())
        self.start(self.PYQ, zz, self.y, self.Q0, (self.z, self.p))

    def relay(self, j):
        zz = self.zz(j)
        self.arrived(self.X3, zz, self.x, self.LOW3)
        self.start(self.Y2, zz, self.x, self.HIGH, (self.z, self.y))
        self.start(self.PX3, zz, self.x, self.LOW3, (self.z, self.p))
        self.arrived(self.Y3, zz, self.y, self.HIGH3)
        self.start(self.X2, zz, self.y, self.LOW, (self.z, self.x))
        self.start(self.PY3, zz, self.y, self.HIGH3, (self.z, self.p))

    def finish(self, j):
        zz = self.zz(j)
        self.arrived(self.X2, zz, self.d, self.LOW)
        self.start(self.PDX, zz, self.d, self.LOW, (self.z, self.p))
        self.arrived(self.Y2, zz, self.d, self.HIGH)
        self.start(self.PDY, zz, self.d, self.HIGH, (self.z, self.p))

    def shared(self, j):
        zz, p = self.zz(j), self.p
        self.arrived(self.P0, zz, p, self.WHOLE)
        self.arrived(self.PXQ, zz, p ^ 2, self.Q3)
        self.arrived(self.PYQ, zz, p ^ 4, self.Q0)
        self.arrived(self.PX3, zz, p ^ 2, self.LOW3)
        self.arrived(self.PY3, zz, p ^ 4, self.HIGH3)
        self.arrived(self.PDX, zz, p ^ 6, self.LOW)
        self.arrived(self.PDY, zz, p ^ 6, self.HIGH)

    def drain(self, j):
        zz, e, mine = self.zz(j), self.e, j == 0
        if mine:
            self.sent(self.XQ, zz, e, self.Q3, mine)
            self.sent(self.YQ, zz, e, self.Q0, mine)
            for i in range(len(self.outs)):
                self.keep(i).wait()
        for kind, ee, piece in ((self.Z, e, self.WHOLE), (self.ZX, self.x, self.Q3), (self.ZY, self.y, self.Q0)):
            self.along(j, kind, ee, piece, lambda c: c.wait_send())
        self.sent(self.X3, zz, e, self.LOW3, mine)
        self.sent(self.Y3, zz, e, self.HIGH3, mine)
        self.sent(self.P0, zz, e, self.WHOLE, mine)
        self.sent(self.PXQ, zz, self.x, self.Q3)
        self.sent(self.PYQ, zz, self.y, self.Q0)
        self.sent(self.Y2, zz, self.x, self.HIGH)
        self.sent(self.X2, zz, self.y, self.LOW)
        self.sent(self.PX3, zz, self.x, self.LOW3)
        self.sent(self.PY3, zz, self.y, self.HIGH3)
        self.sent(self.PDX, zz, self.d, self.LOW)
        self.sent(self.PDY, zz, self.d, self.HIGH)

    def steps(self):
        n = self.nz
        todo = [(self.launch, 0), (self.mates, 0)]
        for j in range(1, n + 2):
            todo += [(self.launch, j), (self.mates, j - 1) if j > 1 else None, (self.relay, j - 1), (self.finish, j - 2)]
        return [functools.partial(f, j) for f, j in filter(None, todo) if 0 <= j < n]


def gather_kernel(nz, count, *refs):
    shards, outs = refs[:count], refs[count : 2 * count]
    send, recv, local = refs[2 * count :]
    z, e = place()
    greet(z, e, nz)
    g = Gather(nz, shards, outs, send, recv, local)
    for step in g.steps():
        step()
    for j in range(nz):
        g.shared(j)
    for j in range(nz):
        g.drain(j)


def gather_scratch(nz, count):
    return [
        pltpu.SemaphoreType.DMA((count, nz, Gather.KINDS)),
        pltpu.SemaphoreType.DMA((count, nz, Gather.KINDS)),
        pltpu.SemaphoreType.DMA((4, count)),
    ]


def gather_all(arrays, collective_id):
    nz, width = lax.axis_size("dp"), lax.axis_size("expert")
    count = len(arrays)
    parts = [a.reshape((4, a.shape[0] // 4) + a.shape[1:]) for a in arrays]
    outs = pl.pallas_call(
        functools.partial(gather_kernel, nz, count),
        out_shape=[jax.ShapeDtypeStruct((nz, width) + h.shape, h.dtype) for h in parts],
        in_specs=[pl.BlockSpec(memory_space=pltpu.VMEM)] * count,
        out_specs=[pl.BlockSpec(memory_space=pl.ANY)] * count,
        scratch_shapes=gather_scratch(nz, count),
        compiler_params=pltpu.CompilerParams(
            collective_id=collective_id, has_side_effects=True, vmem_limit_bytes=VMEM_LIMIT
        ),
        name="gather_all",
    )(*parts)
    return [o.reshape((nz * width * a.shape[0],) + a.shape[1:]) for o, a in zip(outs, arrays)]


def accumulate(dst, src):
    rows = dst.shape[0]
    block = 32 if rows % 32 == 0 else rows

    def body(r, _):
        at = pl.ds(pl.multiple_of(r * block, block), block)
        dst[at, :] = dst[at, :] + src[at, :]
        return 0

    lax.fori_loop(0, rows // block, body, 0)


class Scatter:
    X2, Y2, X3, Y3, Z, ZB, ZX, ZXB, ZY, ZYB, XQ, YQ = range(4, 16)
    KINDS = 16
    BUFFERS = 9

    def __init__(self, nz, terms, outs, sums, temps, from_x2, from_y2, from_x3, from_y3, from_z, from_zm, from_q, send, recv, local):
        self.nz, self.terms, self.outs = nz, terms, outs
        self.sums, self.temps = sums, temps
        self.from_x2, self.from_y2, self.from_x3, self.from_y3 = from_x2, from_y2, from_x3, from_y3
        self.from_z, self.from_zm, self.from_q = from_z, from_zm, from_q
        self.send, self.recv, self.local = send, recv, local
        self.count = len(terms)
        self.z, self.e = place()
        self.core, self.chip = self.e % 2, self.e // 2
        self.p, self.x, self.y = self.e ^ 1, self.e ^ 2, self.e ^ 4
        self.chips = (self.chip ^ 3, self.chip ^ 1, self.chip ^ 2, self.chip)

    def zz(self, j):
        return line_order(self.z, self.nz, self.nz - 1 - j)

    def remote(self, i, kind, zz, src, dst, dev):
        return pltpu.make_async_remote_copy(
            src_ref=src, dst_ref=dst, send_sem=self.send.at[i, zz, kind], recv_sem=self.recv.at[i, zz, kind],
            device_id=dev, device_id_type=MESH)

    def quarters(self, i, zz, q, first, n):
        return self.sums[i].at[zz, q, pl.ds(first, n)]

    def pair(self, i, j, q):
        zz, chip = self.zz(j), self.chips[q]
        return self.remote(i, q, zz, self.terms[i].at[zz, chip * 2 + (1 - self.core)], self.sums[i].at[zz, q],
                           (self.z, self.p))

    def load(self, i, j, q):
        slot = q % 2
        return pltpu.make_async_copy(
            self.terms[i].at[self.zz(j), self.chips[q] * 2 + self.core], self.temps[i].at[slot], self.local.at[i, slot])

    def x2(self, i, zz):
        return self.remote(i, self.X2, zz, self.quarters(i, zz, 0, 0, 2), self.from_x2[i].at[zz], (self.z, self.x))

    def y2(self, i, zz):
        return self.remote(i, self.Y2, zz, self.quarters(i, zz, 0, 2, 2), self.from_y2[i].at[zz], (self.z, self.y))

    def x3(self, i, zz):
        return self.remote(i, self.X3, zz, self.quarters(i, zz, 1, 0, 3), self.from_x3[i].at[zz], (self.z, self.x))

    def y3(self, i, zz):
        return self.remote(i, self.Y3, zz, self.quarters(i, zz, 2, 1, 3), self.from_y3[i].at[zz], (self.z, self.y))

    def xq(self, i):
        return self.remote(i, self.XQ, self.z, self.quarters(i, self.z, 1, 3, 1), self.from_q[i].at[pl.ds(0, 1)], (self.z, self.x))

    def yq(self, i):
        return self.remote(i, self.YQ, self.z, self.quarters(i, self.z, 2, 0, 1), self.from_q[i].at[pl.ds(1, 1)], (self.z, self.y))

    def line(self, i, zz, which, dz, last=False):
        slot = self.nz if last else zz
        kind = (self.Z, self.ZX, self.ZY)[which] + int(last)
        src = (self.sums[i].at[zz, 3], self.quarters(i, zz, 1, 3, 1), self.quarters(i, zz, 2, 0, 1))[which]
        dst = self.from_z[i].at[slot] if which == 0 else self.from_zm[i].at[slot, pl.ds(which - 1, 1)]
        return self.remote(i, kind, zz, src, dst, (self.z + dz, self.e))

    def add(self, i, zz, q, first, n, src):
        for k in range(n):
            accumulate(self.sums[i].at[zz, q, first + k], src.at[k])

    def begin(self):
        for j in range(self.nz):
            for q in range(4):
                for i in range(self.count):
                    self.pair(i, j, q).start()
        for i in range(self.count):
            self.load(i, 0, 0).start()

    def first(self, j):
        zz = self.zz(j)
        for q in range(4):
            for i in range(self.count):
                if q < 3:
                    self.load(i, j, q + 1).start()
                elif j < self.nz - 1:
                    self.load(i, j + 1, 0).start()
                self.pair(i, j, q).wait_recv()
                self.load(i, j, q).wait()
                self.add(i, zz, q, 0, 4, self.temps[i].at[q % 2])
                if q == 0:
                    self.x2(i, zz).start()
                    self.y2(i, zz).start()

    def second(self, j):
        zz = self.zz(j)
        for i in range(self.count):
            self.y2(i, zz).wait_recv()
            self.add(i, zz, 1, 2, 2, self.from_y2[i].at[zz])
            self.x3(i, zz).start()
            self.x2(i, zz).wait_recv()
            self.add(i, zz, 2, 0, 2, self.from_x2[i].at[zz])
            self.y3(i, zz).start()
            for which in (1, 2):
                self.flow(i, j, which)

    def flow(self, i, j, which):
        z, nz, zz = self.z, self.nz, self.zz(j)
        q, first, n = ((3, 0, 4), (1, 3, 1), (2, 0, 1))[which]

        def came(slot):
            ref = self.from_z[i].at[slot] if which == 0 else self.from_zm[i].at[slot, pl.ds(which - 1, 1)]
            self.add(i, zz, q, first, n, ref)

        if j < nz - 1:
            @pl.when(jnp.logical_or(jnp.logical_and(zz > z, z > 0), jnp.logical_and(zz < z, z < nz - 1)))
            def _():
                self.line(i, zz, which, 1).wait_recv()
                came(zz)

            @pl.when(zz > z)
            def _():
                self.line(i, zz, which, 1).start()

            @pl.when(zz < z - 1)
            def _():
                self.line(i, zz, which, -1).start()

            @pl.when(zz == z - 1)
            def _():
                self.line(i, zz, which, -1, True).start()
        else:
            @pl.when(z > 0)
            def _():
                self.line(i, zz, which, 1).wait_recv()
                came(zz)

            @pl.when(z < nz - 1)
            def _():
                self.line(i, zz, which, -1, True).wait_recv()
                came(nz)

            if which == 1:
                self.xq(i).start()
            if which == 2:
                self.yq(i).start()

    def third(self, j):
        zz = self.zz(j)
        for i in range(self.count):
            self.x3(i, zz).wait_recv()
            self.add(i, zz, 3, 0, 3, self.from_x3[i].at[zz])
            self.y3(i, zz).wait_recv()
            self.add(i, zz, 3, 1, 3, self.from_y3[i].at[zz])
            self.flow(i, j, 0)

    def result(self):
        for i in range(self.count):
            self.xq(i).wait_recv()
            self.add(i, self.z, 3, 3, 1, self.from_q[i].at[pl.ds(0, 1)])
            self.yq(i).wait_recv()
            self.add(i, self.z, 3, 0, 1, self.from_q[i].at[pl.ds(1, 1)])
            self.outs[i][...] = self.sums[i][self.z, 3].astype(self.outs[i].dtype)

    def drain(self, j):
        z, nz = self.z, self.nz
        zz = self.zz(j)
        for i in range(self.count):
            for q in range(4):
                self.pair(i, j, q).wait_send()
            for c in (self.x2, self.y2, self.x3, self.y3):
                c(i, zz).wait_send()
            if j < nz - 1:
                for which in range(3):
                    @pl.when(zz > z)
                    def _():
                        self.line(i, zz, which, 1).wait_send()

                    @pl.when(zz < z - 1)
                    def _():
                        self.line(i, zz, which, -1).wait_send()

                    @pl.when(zz == z - 1)
                    def _():
                        self.line(i, zz, which, -1, True).wait_send()
            else:
                self.xq(i).wait_send()
                self.yq(i).wait_send()

    def steps(self):
        todo = []
        for j in range(self.nz + 2):
            todo += [(self.first, j), (self.second, j - 1), (self.third, j - 2)]
        return [functools.partial(f, j) for f, j in todo if 0 <= j < self.nz] + [self.result]


def scatter_kernel(nz, count, *refs):
    groups = [refs[k * count : (k + 1) * count] for k in range(2 + Scatter.BUFFERS)]
    send, recv, local = refs[(2 + Scatter.BUFFERS) * count :]
    z, e = place()
    greet(z, e, nz)
    s = Scatter(nz, *groups, send, recv, local)
    s.begin()
    for step in s.steps():
        step()
    for j in range(nz):
        s.drain(j)


def scatter_buffers(nz, width, kinds):
    leads = ((nz, width // 2, 4), (2, 4), (nz, 2), (nz, 2), (nz, 3), (nz, 3), (nz + 1, 4), (nz + 1, 2), (2,))
    return [pltpu.VMEM(lead + shape, dtype) for lead in leads for shape, dtype in kinds] + [
        pltpu.SemaphoreType.DMA((len(kinds), nz, Scatter.KINDS)),
        pltpu.SemaphoreType.DMA((len(kinds), nz, Scatter.KINDS)),
        pltpu.SemaphoreType.DMA((len(kinds), 2)),
    ]


def scatter_sum(arrays, collective_id):
    nz, width = lax.axis_size("dp"), lax.axis_size("expert")
    count = len(arrays)
    devices = nz * width
    terms = [a.reshape(nz, width, 4, a.shape[0] // (4 * devices), a.shape[1]) for a in arrays]
    shapes = [t.shape[3:] for t in terms]
    outs = pl.pallas_call(
        functools.partial(scatter_kernel, nz, count),
        out_shape=[jax.ShapeDtypeStruct((4,) + s, jnp.float32) for s in shapes],
        in_specs=[pl.BlockSpec(memory_space=pl.ANY)] * count,
        out_specs=[pl.BlockSpec(memory_space=pltpu.VMEM)] * count,
        scratch_shapes=scatter_buffers(nz, width, [(s, a.dtype) for s, a in zip(shapes, arrays)]),
        compiler_params=pltpu.CompilerParams(
            collective_id=collective_id, has_side_effects=True, vmem_limit_bytes=VMEM_LIMIT
        ),
        name="scatter_sum",
    )(*terms)
    return [o.reshape(4 * s[0], s[1]) for o, s in zip(outs, shapes)]


def mm(a, b, da=1, db=0):
    return lax.dot_general(a, b, (((da,), (db,)), ((), ())), preferred_element_type=F32)


def expert_kernel(group, cap, x_ref, g_ref, gate_ref, rank_ref, wg_ref, wu_ref, wd_ref,
                  y_ref, r_ref, gg_ref, rows_ref, down_ref, act_ref, gp_ref, up_ref, cot_ref):
    length, width = x_ref.shape[1:]
    slot = lax.broadcasted_iota(jnp.int32, (cap, length), 0).astype(F32)
    picks, gates = [], []
    for s in range(group):
        hit = slot == rank_ref[s]
        pick = hit.astype(BF16)
        picks.append(pick)
        gate = jnp.sum(jnp.where(hit, gate_ref[s], 0.0), 1, keepdims=True)
        gates.append(gate)
        at = pl.ds(s * cap, cap)
        rows_ref[at, :] = mm(pick, x_ref[s]).astype(BF16)
        cot = mm(pick, g_ref[s])
        cot_ref[at, :] = cot.astype(BF16)
        down_ref[at, :] = (gate * cot).astype(BF16)
    gate_all = jnp.concatenate(gates, 0)
    rows = rows_ref[...]
    pre_gate = mm(rows, wg_ref[...])
    pre_up = mm(rows, wu_ref[...])
    sig = jax.nn.sigmoid(pre_gate)
    silu = pre_gate * sig
    act_ref[...] = (silu * pre_up).astype(BF16)
    act_grad = mm(down_ref[...], wd_ref[...], 1, 1)
    gp_ref[...] = (act_grad * pre_up * sig * (1.0 + pre_gate * (1.0 - sig))).astype(BF16)
    up_ref[...] = (act_grad * silu).astype(BF16)
    tile = 512
    gg = jnp.zeros((group * cap, 1), F32)
    for n in range(width // tile):
        cols = pl.ds(n * tile, tile)
        out = mm(act_ref[...], wd_ref[:, cols]).astype(BF16).astype(F32)
        gg = gg + jnp.sum(out * cot_ref[:, cols].astype(F32), 1, keepdims=True)
        out = (out * gate_all).astype(BF16)
        back = (mm(gp_ref[...], wg_ref[cols, :], 1, 1) + mm(up_ref[...], wu_ref[cols, :], 1, 1)).astype(BF16)
        for s in range(group):
            part = slice(s * cap, (s + 1) * cap)
            y_ref[s, :, cols] = mm(picks[s], out[part], 0, 0).astype(BF16)
            r_ref[s, :, cols] = mm(picks[s], back[part], 0, 0).astype(BF16)
    for s in range(group):
        gg_ref[s] = jnp.sum(picks[s].astype(F32) * gg[s * cap : (s + 1) * cap], 0, keepdims=True)


def experts(x, g, gate, rank, wg, wu, wd, cap, group):
    devices, length, width = x.shape
    ff = wg.shape[1]
    rows = devices * cap
    step = group * cap
    block = lambda *tail: pl.BlockSpec((group,) + tail, lambda i: (i,) + (0,) * len(tail))
    flat = lambda n: pl.BlockSpec((step, n), lambda i: (i, 0))
    whole = lambda a: pl.BlockSpec(a.shape, lambda i: (0, 0), pipeline_mode=pl.Buffered(1))
    return pl.pallas_call(
        functools.partial(expert_kernel, group, cap),
        grid=(devices // group,),
        in_specs=[block(length, width), block(length, width), block(1, length), block(1, length),
                  whole(wg), whole(wu), whole(wd)],
        out_specs=[block(length, width), block(length, width), block(1, length),
                   flat(width), flat(width), flat(ff), flat(ff), flat(ff)],
        out_shape=[
            jax.ShapeDtypeStruct((devices, length, width), BF16),
            jax.ShapeDtypeStruct((devices, length, width), BF16),
            jax.ShapeDtypeStruct((devices, 1, length), F32),
            jax.ShapeDtypeStruct((rows, width), BF16),
            jax.ShapeDtypeStruct((rows, width), BF16),
            jax.ShapeDtypeStruct((rows, ff), BF16),
            jax.ShapeDtypeStruct((rows, ff), BF16),
            jax.ShapeDtypeStruct((rows, ff), BF16),
        ],
        scratch_shapes=[pltpu.VMEM((step, width), BF16)],
        compiler_params=pltpu.CompilerParams(vmem_limit_bytes=VMEM_LIMIT, dimension_semantics=("arbitrary",)),
        name="experts",
    )(x, g, gate, rank, wg, wu, wd)


def rope(values, cosine, sine):
    return values * cosine + pltpu.roll(values, values.shape[1] // 2, 1) * sine


class AttentionGrad:
    def __init__(self, branch, w_out, raw, tables, gains, seg_col, seg_row, grads, gain_grads,
                 w_buf, q_buf, k_buf, v_buf, mask, k_rot, v_low, dk, dv, sems):
        self.branch, self.w_out, self.raw, self.tables, self.gains = branch, w_out, raw, tables, gains
        self.seg_col, self.seg_row, self.grads, self.gain_grads = seg_col, seg_row, grads, gain_grads
        self.w_buf, self.q_buf, self.k_buf, self.v_buf, self.mask = w_buf, q_buf, k_buf, v_buf, mask
        self.k_rot, self.v_low, self.dk, self.dv, self.sems = k_rot, v_low, dk, dv, sems
        self.cols = w_buf.shape[1]
        self.query_cols = w_out.shape[0]
        self.key_cols = k_buf.shape[1]
        self.count = self.query_cols // self.cols
        self.per_key = self.count // (self.key_cols // HEAD_DIM)

    def fetch(self, t, slot):
        at = pl.ds(pl.multiple_of(t * self.cols, self.cols), self.cols)
        return (
            pltpu.make_async_copy(self.w_out.at[at, :], self.w_buf.at[slot], self.sems.at[0, slot]),
            pltpu.make_async_copy(self.raw.at[:, at], self.q_buf.at[slot], self.sems.at[1, slot]),
        )

    def prepare(self):
        q, k = self.query_cols, self.key_cols
        key = pltpu.make_async_copy(self.raw.at[:, pl.ds(q, k)], self.k_buf, self.sems.at[2, 0])
        value = pltpu.make_async_copy(self.raw.at[:, pl.ds(q + k, k)], self.v_buf, self.sems.at[2, 1])
        key.start()
        value.start()
        for c in self.fetch(0, 0):
            c.start()
        length = self.seg_col.shape[0]
        row = lax.broadcasted_iota(jnp.int32, (length, length), 0)
        col = lax.broadcasted_iota(jnp.int32, (length, length), 1)
        same = self.seg_col[...] == self.seg_row[...]
        self.mask[...] = jnp.where(jnp.logical_and(same, col <= row), 1.0, 0.0)
        self.gain_grads[...] = jnp.zeros_like(self.gain_grads)
        key.wait()
        value.wait()

    def normed(self, raw, which):
        scale = lax.rsqrt(jnp.mean(raw * raw, 1, keepdims=True) + EPS)
        return scale, (raw * scale) * self.gains[which : which + 1, :]

    def back(self, rot_grad, raw, scale, which):
        cosine, sine = self.tables[0], self.tables[1]
        grad = rope(rot_grad, cosine, -sine)
        part = jnp.sum(grad * raw * scale, 0, keepdims=True)
        self.gain_grads[which : which + 1, :] = self.gain_grads[which : which + 1, :] + part
        weighted = grad * self.gains[which : which + 1, :]
        mean = jnp.mean(weighted * raw, 1, keepdims=True)
        return scale * weighted - raw * (scale * scale * scale) * mean

    def step(self, t):
        slot = lax.rem(t, 2)
        last = t + 1 < self.count

        @pl.when(last)
        def _():
            for c in self.fetch(t + 1, 1 - slot):
                c.start()

        for c in self.fetch(t, slot):
            c.wait()
        cosine, sine = self.tables[0], self.tables[1]
        at_key = pl.ds(pl.multiple_of(t // self.per_key * HEAD_DIM, HEAD_DIM), HEAD_DIM)

        @pl.when(lax.rem(t, self.per_key) == 0)
        def _():
            _, key = self.normed(self.k_buf[:, at_key], 1)
            self.k_rot[...] = rope(key, cosine, sine).astype(BF16)
            self.v_low[...] = self.v_buf[:, at_key].astype(BF16)
            self.dk[...] = jnp.zeros_like(self.dk)
            self.dv[...] = jnp.zeros_like(self.dv)

        score_scale = 1.0 / math.sqrt(HEAD_DIM)
        out_grad = mm(self.branch[...], self.w_buf[slot], 1, 1).astype(BF16)
        mask = self.mask[...] > 0.0
        k_rot, v_low = self.k_rot[...], self.v_low[...]
        for h in range(self.cols // HEAD_DIM):
            here = slice(h * HEAD_DIM, (h + 1) * HEAD_DIM)
            raw = self.q_buf[slot, :, here]
            scale, query = self.normed(raw, 0)
            q_rot = rope(query, cosine, sine).astype(BF16)
            d_out = out_grad[:, here]
            scores = mm(q_rot, k_rot, 1, 1) * score_scale
            raised = jnp.where(mask, jnp.exp(scores), 0.0)
            probs = raised / jnp.sum(raised, 1, keepdims=True)
            self.dv[...] += mm(probs.astype(BF16), d_out, 0, 0)
            d_probs = mm(d_out, v_low, 1, 1)
            d_scores = (probs * (d_probs - jnp.sum(probs * d_probs, 1, keepdims=True))).astype(BF16)
            dq = mm(d_scores, k_rot) * score_scale
            self.dk[...] += mm(d_scores, q_rot, 0, 0)
            at = pl.ds(pl.multiple_of(t * self.cols + h * HEAD_DIM, HEAD_DIM), HEAD_DIM)
            self.grads[:, at] = self.back(dq, raw, scale, 0).astype(BF16)

        @pl.when(lax.rem(t, self.per_key) == self.per_key - 1)
        def _():
            raw = self.k_buf[:, at_key]
            scale, _ = self.normed(raw, 1)
            shift = pl.multiple_of(t // self.per_key * HEAD_DIM, HEAD_DIM)
            self.grads[:, pl.ds(self.query_cols + shift, HEAD_DIM)] = self.back(
                self.dk[...] * score_scale, raw, scale, 1
            ).astype(BF16)
            self.grads[:, pl.ds(self.query_cols + self.key_cols + shift, HEAD_DIM)] = self.dv[...].astype(BF16)


def scatter_attention_kernel(nz, plan, term, branch, w_out, raw, tables, gains, seg_col, seg_row,
                             total, grads, gain_grads, *scratch):
    buffers, rest = scratch[: Scatter.BUFFERS], scratch[Scatter.BUFFERS :]
    send, recv, local = rest[:3]
    z, e = place()
    greet(z, e, nz)
    s = Scatter(nz, [term], [total], *[[b] for b in buffers], send, recv, local)
    a = AttentionGrad(branch, w_out, raw, tables, gains, seg_col, seg_row, grads, gain_grads, *rest[3:])
    s.begin()
    a.prepare()
    steps = s.steps()
    run_beside(a.count, a.step, steps, plan)
    for j in range(nz):
        s.drain(j)


def run_beside(count, work, steps, plan):
    bounds = [sum(plan[:t]) for t in range(len(plan) + 1)]

    def body(t, _):
        for k in range(count):
            todo = steps[bounds[k] : bounds[k + 1]]
            if todo:
                @pl.when(t == k)
                def _():
                    for step in todo:
                        step()
        work(t)
        return 0

    lax.fori_loop(0, count, body, 0)
    for step in steps[bounds[count] :]:
        step()


def scatter_with_attention(terms, branch, w_out, raw, tables, gains, segments, collective_id):
    nz, width = lax.axis_size("dp"), lax.axis_size("expert")
    devices = nz * width
    length = branch.shape[0]
    shape = (terms.shape[0] // (4 * devices), terms.shape[1])
    term = terms.reshape((nz, width, 4) + shape)
    heads = 4
    cols = heads * HEAD_DIM
    key_cols = (raw.shape[1] - w_out.shape[0]) // 2
    vmem = pl.BlockSpec(memory_space=pltpu.VMEM)
    hbm = pl.BlockSpec(memory_space=pl.ANY)
    plan = [3, 1, 1, 1, 1, 1, 1, 1]
    total, grads, gain_grads = pl.pallas_call(
        functools.partial(scatter_attention_kernel, nz, plan),
        out_shape=[
            jax.ShapeDtypeStruct((4,) + shape, F32),
            jax.ShapeDtypeStruct(raw.shape, BF16),
            jax.ShapeDtypeStruct((2, HEAD_DIM), F32),
        ],
        in_specs=[hbm, vmem, hbm, hbm, vmem, vmem, vmem, vmem],
        out_specs=[vmem, vmem, vmem],
        scratch_shapes=scatter_buffers(nz, width, [(shape, terms.dtype)])
        + [
            pltpu.VMEM((2, cols, w_out.shape[1]), BF16),
            pltpu.VMEM((2, length, cols), F32),
            pltpu.VMEM((length, key_cols), F32),
            pltpu.VMEM((length, key_cols), F32),
            pltpu.VMEM((length, length), F32),
            pltpu.VMEM((length, HEAD_DIM), BF16),
            pltpu.VMEM((length, HEAD_DIM), BF16),
            pltpu.VMEM((length, HEAD_DIM), F32),
            pltpu.VMEM((length, HEAD_DIM), F32),
            pltpu.SemaphoreType.DMA((3, 2)),
        ],
        compiler_params=pltpu.CompilerParams(
            collective_id=collective_id, has_side_effects=True, vmem_limit_bytes=VMEM_LIMIT
        ),
        name="scatter_attention",
    )(term, branch, w_out, raw, tables, gains, segments[:, None], segments[None, :])
    return total.reshape(4 * shape[0], shape[1]), grads, gain_grads


def pack_columns(columns, rows, lanes, dtype):
    parts = [c.astype(dtype) for c in columns]
    used = sum(c.shape[1] for c in parts)
    return jnp.concatenate(parts + [jnp.zeros((rows, lanes - used), dtype)], 1)


def spread(vector, devices, rows):
    blocks = vector.reshape(devices, -1)
    return jnp.pad(blocks, ((0, 0), (0, rows - blocks.shape[1]))).reshape(devices * rows, 1)


def per_device_gather(
    hidden_in,
    segment_ids,
    expert_ids,
    attn_gain,
    query_gain,
    key_gain,
    w_query,
    w_key,
    w_value,
    w_output,
    mlp_gain,
    w_router,
    w_gate,
    w_up,
    w_down,
    out_grad,
):
    devices = lax.axis_size(("dp", "expert"))
    me = lax.axis_index(("dp", "expert"))
    length, choices = expert_ids.shape
    width = hidden_in.shape[1]
    experts_total = devices
    capacity = 5 * length * choices // (4 * experts_total)
    query_cols, key_cols = w_query.shape[1], w_key.shape[1]
    rows = w_query.shape[0]
    head_rows = query_gain.shape[0]

    column = lambda v: jnp.pad(v, (0, rows - v.shape[0]))[:, None]
    lanes = 128 * pl.cdiv(experts_total + 4, 128)
    small = pack_columns(
        [w_router, column(attn_gain), column(mlp_gain), column(query_gain), column(key_gain)], rows, lanes, BF16
    )
    w_mixed = jnp.concatenate([w_query, w_key, w_value], 1)
    w_mixed, w_out, small = gather_all([w_mixed, w_output, small], 1)
    router = small[:, :experts_total]
    attn_gain, mlp_gain = small[:, experts_total], small[:, experts_total + 1]
    heads_of = small.reshape(devices, rows, lanes)[:, :head_rows]
    query_gain = heads_of[:, :, experts_total + 2].reshape(-1)
    key_gain = heads_of[:, :, experts_total + 3].reshape(-1)

    group_size = HEADS // KV_HEADS
    plain_in = hidden_in.astype(F32)
    inv_attn = rms_scale(plain_in)
    normed_attn = (plain_in * inv_attn * attn_gain).astype(BF16)
    mixed = jnp.dot(normed_attn, w_mixed, preferred_element_type=F32)
    query_raw = mixed[:, :query_cols].reshape(length, HEADS, HEAD_DIM)
    key_raw = mixed[:, query_cols : query_cols + key_cols].reshape(length, KV_HEADS, HEAD_DIM)
    value_rows = mixed[:, query_cols + key_cols :].astype(BF16).reshape(length, KV_HEADS, HEAD_DIM)
    query_scale = rms_scale(query_raw)
    key_scale = rms_scale(key_raw)
    cosine_table, sine_table = rope_tables(jnp.arange(length) % TOK_DEV, HEAD_DIM)
    query_rot = rotate(query_raw * query_scale * query_gain, cosine_table, sine_table).astype(BF16)
    query_rot = query_rot.reshape(length, KV_HEADS, group_size, HEAD_DIM)
    key_rot = rotate(key_raw * key_scale * key_gain, cosine_table, sine_table).astype(BF16)
    position = jnp.arange(length)
    allowed = (segment_ids[:, None] == segment_ids[None, :]) & (position[None, :] <= position[:, None])
    attended, log_totals = attend(query_rot, key_rot, value_rows, allowed)
    attended = attended.reshape(length, HEADS * HEAD_DIM)
    residual = plain_in + jnp.dot(attended, w_out, preferred_element_type=F32)

    inv_mlp = rms_scale(residual)
    normed_mlp = (residual * inv_mlp * mlp_gain).astype(BF16)
    logits = jnp.dot(normed_mlp, router, preferred_element_type=F32)
    chosen = jnp.any(expert_ids[:, :, None] == jnp.arange(experts_total)[None, None, :], 1)
    raised = jnp.where(chosen, jnp.exp(logits), 0.0)
    gate = raised / jnp.sum(raised, -1, keepdims=True)
    not_after = (position[None, :] <= position[:, None]).astype(BF16)
    rank = jnp.dot(not_after, chosen.astype(BF16), preferred_element_type=F32) - 1.0
    rank = jnp.where(chosen, rank, -1.0)
    gate_high = lax.reduce_precision(gate, 8, 7)
    table = jnp.concatenate([gate_high, gate - gate_high, rank], 1).T.astype(BF16)

    all_rows, all_tables = gather_all([normed_mlp, table], 2)
    (all_grads,) = gather_all([out_grad], 3)
    mine = lax.dynamic_index_in_dim(
        all_tables.reshape(devices, 3, experts_total, length), me, 2, keepdims=False
    ).astype(F32)
    cube = (devices, length, width)
    y_terms, r_terms, gate_terms, rows_in, down_in, act, gate_pre_grad, up_pre_grad = experts(
        all_rows.reshape(cube), all_grads.reshape(cube), mine[:, :1] + mine[:, 1:2], mine[:, 2:],
        w_gate[0], w_up[0], w_down[0], capacity, 4,
    )
    is_me = (jnp.arange(experts_total) == me).astype(F32)
    gate_terms = (gate_terms * is_me[None, :, None]).reshape(devices * experts_total, length)
    row_grad_sum, gate_grad = scatter_sum([r_terms.reshape(devices * length, width), gate_terms], 4)
    grad_w_down = jnp.dot(act.T, down_in, preferred_element_type=F32)[None]
    grad_w_gate = jnp.dot(rows_in.T, gate_pre_grad, preferred_element_type=F32)[None]
    grad_w_up = jnp.dot(rows_in.T, up_pre_grad, preferred_element_type=F32)[None]

    gate_grad = gate_grad.T
    sel_grad = gate * (gate_grad - jnp.sum(gate * gate_grad, -1, keepdims=True))
    logit_grad = jnp.where(chosen, sel_grad, 0.0).astype(BF16)
    grad_w_router = jnp.dot(normed_mlp.T, logit_grad, preferred_element_type=F32)
    normed_mlp_grad = row_grad_sum + jnp.dot(logit_grad, router.T, preferred_element_type=F32)
    grad_mlp_gain = jnp.sum(normed_mlp_grad * residual * inv_mlp, 0)
    residual_grad = out_grad.astype(F32) + norm_grad(normed_mlp_grad, residual, inv_mlp, mlp_gain)

    branch_grad = residual_grad.astype(BF16)
    grad_w_output = jnp.dot(attended.T, branch_grad, preferred_element_type=F32).astype(BF16)
    cosine, sine = cosine_table[:, 0], sine_table[:, 0]
    tables = jnp.stack([jnp.concatenate([cosine, cosine], 1), jnp.concatenate([-sine, sine], 1)])
    head_gains = jnp.stack([query_gain, key_gain]).astype(F32)
    mixed_out, mixed_grad, gain_grads = scatter_with_attention(
        y_terms.reshape(devices * length, width), branch_grad, w_out, mixed, tables, head_gains, segment_ids, 5
    )
    block_out = residual + mixed_out
    grad_query_gain, grad_key_gain = gain_grads[0], gain_grads[1]
    grad_w_mixed = jnp.dot(normed_attn.T, mixed_grad, preferred_element_type=F32).astype(BF16)
    normed_attn_grad = jnp.dot(mixed_grad, w_mixed.T, preferred_element_type=F32)
    grad_attn_gain = jnp.sum(normed_attn_grad * plain_in * inv_attn, 0)
    grad_in = residual_grad + norm_grad(normed_attn_grad, plain_in, inv_attn, attn_gain)

    small_grads = pack_columns(
        [
            grad_w_router,
            grad_attn_gain[:, None],
            grad_mlp_gain[:, None],
            spread(grad_query_gain, devices, rows),
            spread(grad_key_gain, devices, rows),
        ],
        width,
        lanes,
        F32,
    )
    share_mixed, share_w_output, share_small = scatter_sum([grad_w_mixed, grad_w_output, small_grads], 6)
    return (
        block_out,
        grad_in,
        share_small[:, experts_total],
        share_small[:head_rows, experts_total + 2],
        share_small[:head_rows, experts_total + 3],
        share_mixed[:, :query_cols],
        share_mixed[:, query_cols : query_cols + key_cols],
        share_mixed[:, query_cols + key_cols :],
        share_w_output,
        share_small[:, experts_total + 1],
        share_small[:, :experts_total],
        grad_w_gate,
        grad_w_up,
        grad_w_down,
    )


def per_device(*arguments):
    expert_ids, w_gate = arguments[2], arguments[12]
    devices, width = lax.axis_size(("dp", "expert")), lax.axis_size("expert")
    length, choices = expert_ids.shape
    capacity = 5 * length * choices // (4 * devices)
    dense = devices <= 4 * choices and w_gate.shape[0] == 1 and width == 8
    if dense and capacity % 16 == 0 and devices % 4 == 0:
        return per_device_gather(*arguments)
    return per_device_exchange(*arguments)


def solution(mesh):
    in_specs = (
        P(("dp", "expert"), None),
        P(("dp", "expert")),
        P(("dp", "expert"), None),
        P(("dp", "expert")),
        P(("dp", "expert")),
        P(("dp", "expert")),
        P(("dp", "expert"), None),
        P(("dp", "expert"), None),
        P(("dp", "expert"), None),
        P(("dp", "expert"), None),
        P(("dp", "expert")),
        P(("dp", "expert"), None),
        P(("dp", "expert"), None, None),
        P(("dp", "expert"), None, None),
        P(("dp", "expert"), None, None),
        P(("dp", "expert"), None),
    )
    out_specs = (
        P(("dp", "expert"), None),
        P(("dp", "expert"), None),
        P(("dp", "expert")),
        P(("dp", "expert")),
        P(("dp", "expert")),
        P(("dp", "expert"), None),
        P(("dp", "expert"), None),
        P(("dp", "expert"), None),
        P(("dp", "expert"), None),
        P(("dp", "expert")),
        P(("dp", "expert"), None),
        P(("dp", "expert"), None, None),
        P(("dp", "expert"), None, None),
        P(("dp", "expert"), None, None),
    )
    return jax.shard_map(
        per_device, mesh=mesh, in_specs=in_specs, out_specs=out_specs, check_vma=False
    )
```

```python
import functools
import math

import jax
import jax.numpy as jnp
from jax import lax
from jax.experimental import pallas as pl
from jax.experimental.pallas import tpu as pltpu
from jax.sharding import PartitionSpec as P

F32, BF16 = jnp.float32, jnp.bfloat16
MESH = pl.DeviceIdType.MESH
VMEM_LIMIT = 63 * 1024 * 1024


HEADS = 32
KV_HEADS = 4
HEAD_DIM = 128
TOK_DEV = 256


EPS = 1e-06
ROPE_BASE = 1000000.0


def rms_scale(values):
    return lax.rsqrt(jnp.mean(values * values, -1, keepdims=True) + EPS)


def norm_grad(upstream, values, inverse, gain_vec):
    weighted = upstream * gain_vec
    return inverse * weighted - values * inverse**3 * jnp.mean(weighted * values, -1, keepdims=True)


def rope_tables(positions, head_dim):
    half_dim = head_dim // 2
    frequency = ROPE_BASE ** (-(jnp.arange(half_dim).astype(jnp.float32) * 2.0 / head_dim))
    angles = positions.astype(jnp.float32)[:, None] * frequency[None, :]
    return (jnp.cos(angles)[:, None, :], jnp.sin(angles)[:, None, :])


def rotate(values, cosine_table, sine_table):
    half_dim = values.shape[-1] // 2
    first_half = values[..., :half_dim]
    second_half = values[..., half_dim:]
    return jnp.concatenate(
        [
            first_half * cosine_table - second_half * sine_table,
            second_half * cosine_table + first_half * sine_table,
        ],
        -1,
    )


def unrotate(values, cosine_table, sine_table):
    half_dim = values.shape[-1] // 2
    first_half = values[..., :half_dim]
    second_half = values[..., half_dim:]
    return jnp.concatenate(
        [
            first_half * cosine_table + second_half * sine_table,
            second_half * cosine_table - first_half * sine_table,
        ],
        -1,
    )


def attend(query_rot, key_rot, value_rows, allowed):
    score_scale = 1.0 / math.sqrt(HEAD_DIM)
    scores = (
        jnp.einsum("qkgd,tkd->kgqt", query_rot, key_rot, preferred_element_type=jnp.float32)
        * score_scale
    )
    exp_scores = jnp.where(allowed, jnp.exp(scores), 0.0)
    totals = jnp.sum(exp_scores, -1, keepdims=True)
    probs_low = (exp_scores / totals).astype(jnp.bfloat16)
    attended = jnp.einsum(
        "kgqt,tkd->qkgd", probs_low, value_rows, preferred_element_type=jnp.float32
    ).astype(jnp.bfloat16)
    return (attended, jnp.log(totals))


def attend_grad(query_rot, key_rot, value_rows, allowed, log_totals, attended_grad):
    score_scale = 1.0 / math.sqrt(HEAD_DIM)
    scores = (
        jnp.einsum("qkgd,tkd->kgqt", query_rot, key_rot, preferred_element_type=jnp.float32)
        * score_scale
    )
    probs_back = jnp.where(allowed, jnp.exp(scores - log_totals), 0.0)
    probs_low = probs_back.astype(jnp.bfloat16)
    value_sum_grad = jnp.einsum(
        "kgqt,qkgd->tkd", probs_low, attended_grad, preferred_element_type=jnp.float32
    )
    prob_grad = jnp.einsum(
        "qkgd,tkd->kgqt", attended_grad, value_rows, preferred_element_type=jnp.float32
    )
    score_grad = (
        probs_back * (prob_grad - jnp.sum(probs_back * prob_grad, -1, keepdims=True))
    ).astype(jnp.bfloat16)
    query_rot_grad = (
        jnp.einsum("kgqt,tkd->qkgd", score_grad, key_rot, preferred_element_type=jnp.float32)
        * score_scale
    )
    key_rot_grad = (
        jnp.einsum("kgqt,qkgd->tkd", score_grad, query_rot, preferred_element_type=jnp.float32)
        * score_scale
    )
    return (query_rot_grad, key_rot_grad, value_sum_grad)


def mixer_forward(block_in, block_segments, weights):
    w_query, w_key, w_value, w_output, w_router, attn_gain, mlp_gain, query_gain, key_gain = weights
    row_count = block_in.shape[0]
    seq_count = row_count // TOK_DEV
    group_size = HEADS // KV_HEADS
    plain_in = block_in.astype(jnp.float32)
    inv_attn = rms_scale(plain_in)
    normed_attn = (plain_in * inv_attn * attn_gain).astype(jnp.bfloat16)
    query_raw = jnp.dot(normed_attn, w_query, preferred_element_type=jnp.float32).reshape(
        row_count, HEADS, HEAD_DIM
    )
    key_raw = jnp.dot(normed_attn, w_key, preferred_element_type=jnp.float32).reshape(
        row_count, KV_HEADS, HEAD_DIM
    )
    value_rows = jnp.dot(normed_attn, w_value, preferred_element_type=jnp.float32).astype(
        jnp.bfloat16
    )
    value_rows = value_rows.reshape(seq_count, TOK_DEV, KV_HEADS, HEAD_DIM)
    query_scale = rms_scale(query_raw)
    key_scale = rms_scale(key_raw)
    cosine_table, sine_table = rope_tables(jnp.arange(row_count) % TOK_DEV, HEAD_DIM)
    query_rot = rotate(query_raw * query_scale * query_gain, cosine_table, sine_table).astype(
        jnp.bfloat16
    )
    query_rot = query_rot.reshape(seq_count, TOK_DEV, KV_HEADS, group_size, HEAD_DIM)
    key_rot = rotate(key_raw * key_scale * key_gain, cosine_table, sine_table).astype(jnp.bfloat16)
    key_rot = key_rot.reshape(seq_count, TOK_DEV, KV_HEADS, HEAD_DIM)
    segments = block_segments.reshape(seq_count, TOK_DEV)
    position = jnp.arange(TOK_DEV)
    allowed = (segments[:, :, None] == segments[:, None, :]) & (
        position[None, None, :] <= position[None, :, None]
    )
    attended, log_totals = jax.vmap(attend)(query_rot, key_rot, value_rows, allowed)
    attended = attended.reshape(row_count, HEADS * HEAD_DIM)
    residual = plain_in + jnp.dot(attended, w_output, preferred_element_type=jnp.float32)
    saved_state = (
        plain_in,
        inv_attn,
        normed_attn,
        query_raw,
        key_raw,
        value_rows,
        query_scale,
        key_scale,
        query_rot,
        key_rot,
        allowed,
        log_totals,
        attended,
        cosine_table,
        sine_table,
    )
    return (residual, saved_state)


def mixer_backward(residual_grad, saved_state, weights):
    w_query, w_key, w_value, w_output, w_router, attn_gain, mlp_gain, query_gain, key_gain = weights
    (
        plain_in,
        inv_attn,
        normed_attn,
        query_raw,
        key_raw,
        value_rows,
        query_scale,
        key_scale,
        query_rot,
        key_rot,
        allowed,
        log_totals,
        attended,
        cosine_table,
        sine_table,
    ) = saved_state
    row_count = residual_grad.shape[0]
    seq_count = row_count // TOK_DEV
    group_size = HEADS // KV_HEADS
    branch_grad = residual_grad.astype(jnp.bfloat16)
    grad_w_output = jnp.dot(attended.T, branch_grad, preferred_element_type=jnp.float32)
    attended_grad = jnp.dot(branch_grad, w_output.T, preferred_element_type=jnp.float32).astype(
        jnp.bfloat16
    )
    attended_grad = attended_grad.reshape(seq_count, TOK_DEV, KV_HEADS, group_size, HEAD_DIM)
    query_rot_grad, key_rot_grad, value_sum_grad = jax.vmap(attend_grad)(
        query_rot, key_rot, value_rows, allowed, log_totals, attended_grad
    )
    query_normed_grad = unrotate(
        query_rot_grad.reshape(row_count, HEADS, HEAD_DIM), cosine_table, sine_table
    )
    key_normed_grad = unrotate(
        key_rot_grad.reshape(row_count, KV_HEADS, HEAD_DIM), cosine_table, sine_table
    )
    grad_query_gain = jnp.sum(query_normed_grad * query_raw * query_scale, (0, 1))
    grad_key_gain = jnp.sum(key_normed_grad * key_raw * key_scale, (0, 1))
    query_grad = norm_grad(query_normed_grad, query_raw, query_scale, query_gain).astype(
        jnp.bfloat16
    )
    query_grad = query_grad.reshape(row_count, HEADS * HEAD_DIM)
    key_grad = norm_grad(key_normed_grad, key_raw, key_scale, key_gain).astype(jnp.bfloat16)
    key_grad = key_grad.reshape(row_count, KV_HEADS * HEAD_DIM)
    value_grad = value_sum_grad.astype(jnp.bfloat16).reshape(row_count, KV_HEADS * HEAD_DIM)
    grad_w_query = jnp.dot(normed_attn.T, query_grad, preferred_element_type=jnp.float32)
    grad_w_key = jnp.dot(normed_attn.T, key_grad, preferred_element_type=jnp.float32)
    grad_w_value = jnp.dot(normed_attn.T, value_grad, preferred_element_type=jnp.float32)
    normed_attn_grad = (
        jnp.dot(query_grad, w_query.T, preferred_element_type=jnp.float32)
        + jnp.dot(key_grad, w_key.T, preferred_element_type=jnp.float32)
        + jnp.dot(value_grad, w_value.T, preferred_element_type=jnp.float32)
    )
    grad_attn_gain = jnp.sum(normed_attn_grad * plain_in * inv_attn, 0)
    grad_in = residual_grad + norm_grad(normed_attn_grad, plain_in, inv_attn, attn_gain)
    return (
        grad_in,
        (
            grad_attn_gain,
            grad_query_gain,
            grad_key_gain,
            grad_w_query,
            grad_w_key,
            grad_w_value,
            grad_w_output,
        ),
    )


def dispatch_table(expert_rows, experts, capacity):
    length, choices = expert_rows.shape
    flat_ids = expert_rows.reshape(length * choices)
    marks = (flat_ids[:, None] == jnp.arange(experts)[None, :]).astype(jnp.int32)
    earlier = jnp.cumsum(marks, 0) - marks
    destination = flat_ids * capacity + jnp.sum(earlier * marks, -1)
    pair_ids = (
        jnp.zeros((experts * capacity,), jnp.int32)
        .at[destination]
        .set(jnp.arange(length * choices, dtype=jnp.int32))
    )
    filled = jnp.zeros((experts * capacity,), jnp.bfloat16).at[destination].set(1.0)
    return (destination, pair_ids, filled)


def move_rows(row_block, section_name):
    if section_name == "dispatch":
        return lax.all_to_all(row_block, ("dp", "expert"), split_axis=0, concat_axis=0, tiled=True)
    if section_name == "combine":
        return lax.all_to_all(row_block, ("dp", "expert"), split_axis=0, concat_axis=0, tiled=True)
    if section_name == "grad_dispatch":
        return lax.all_to_all(row_block, ("dp", "expert"), split_axis=0, concat_axis=0, tiled=True)
    return lax.all_to_all(row_block, ("dp", "expert"), split_axis=0, concat_axis=0, tiled=True)


def per_device_exchange(
    hidden_in,
    segment_ids,
    expert_ids,
    attn_gain,
    query_gain,
    key_gain,
    w_query,
    w_key,
    w_value,
    w_output,
    mlp_gain,
    w_router,
    w_gate,
    w_up,
    w_down,
    out_grad,
):
    weights = (
        lax.all_gather(w_query, ("dp", "expert"), axis=0, tiled=True),
        lax.all_gather(w_key, ("dp", "expert"), axis=0, tiled=True),
        lax.all_gather(w_value, ("dp", "expert"), axis=0, tiled=True),
        lax.all_gather(w_output, ("dp", "expert"), axis=0, tiled=True),
        lax.all_gather(w_router, ("dp", "expert"), axis=0, tiled=True),
        lax.all_gather(attn_gain, ("dp", "expert"), axis=0, tiled=True),
        lax.all_gather(mlp_gain, ("dp", "expert"), axis=0, tiled=True),
        lax.all_gather(query_gain, ("dp", "expert"), axis=0, tiled=True),
        lax.all_gather(key_gain, ("dp", "expert"), axis=0, tiled=True),
    )
    residual, saved_state = mixer_forward(hidden_in, segment_ids, weights)
    full_router = weights[4]
    full_mlp_gain = weights[6]
    inv_mlp = rms_scale(residual)
    normed_mlp = (residual * inv_mlp * full_mlp_gain).astype(jnp.bfloat16)
    logits = jnp.dot(normed_mlp, full_router, preferred_element_type=jnp.float32)
    device_count = lax.axis_size(("dp", "expert"))
    local_experts = w_gate.shape[0]
    experts = local_experts * device_count
    length, choices = expert_ids.shape
    model_width = hidden_in.shape[1]
    capacity = 5 * length * choices // (4 * experts)
    one_hot = expert_ids[:, :, None] == jnp.arange(experts)[None, None, :]
    chosen = jnp.sum(jnp.where(one_hot, logits[:, None, :], 0.0), -1)
    raised = jnp.exp(chosen)
    gate_weights = raised / jnp.sum(raised, -1, keepdims=True)
    destination, pair_ids, filled = dispatch_table(expert_ids, experts, capacity)
    send_rows = normed_mlp[pair_ids // choices] * filled[:, None]
    received = move_rows(
        send_rows.reshape(device_count, local_experts * capacity, model_width), "dispatch"
    )
    received = received.reshape(device_count, local_experts, capacity, model_width)
    pre_gate = jnp.einsum("secd,edf->secf", received, w_gate, preferred_element_type=jnp.float32)
    pre_up = jnp.einsum("secd,edf->secf", received, w_up, preferred_element_type=jnp.float32)
    gate_sigmoid = jax.nn.sigmoid(pre_gate)
    silu_gate = pre_gate * gate_sigmoid
    activation = (silu_gate * pre_up).astype(jnp.bfloat16)
    expert_out = jnp.einsum(
        "secf,efd->secd", activation, w_down, preferred_element_type=jnp.float32
    ).astype(jnp.bfloat16)
    returned = move_rows(
        expert_out.reshape(device_count, local_experts * capacity, model_width), "combine"
    )
    picked = returned.reshape(experts * capacity, model_width)[destination].reshape(
        length, choices, model_width
    )
    block_out = residual + jnp.sum(gate_weights[:, :, None] * picked.astype(jnp.float32), 1)
    weights = (
        lax.all_gather(w_query, ("dp", "expert"), axis=0, tiled=True),
        lax.all_gather(w_key, ("dp", "expert"), axis=0, tiled=True),
        lax.all_gather(w_value, ("dp", "expert"), axis=0, tiled=True),
        lax.all_gather(w_output, ("dp", "expert"), axis=0, tiled=True),
        lax.all_gather(w_router, ("dp", "expert"), axis=0, tiled=True),
        lax.all_gather(attn_gain, ("dp", "expert"), axis=0, tiled=True),
        lax.all_gather(mlp_gain, ("dp", "expert"), axis=0, tiled=True),
        lax.all_gather(query_gain, ("dp", "expert"), axis=0, tiled=True),
        lax.all_gather(key_gain, ("dp", "expert"), axis=0, tiled=True),
    )
    full_router = weights[4]
    full_mlp_gain = weights[6]
    cotangent = out_grad.astype(jnp.float32)
    gate_grad = jnp.sum(cotangent[:, None, :] * picked.astype(jnp.float32), -1)
    down_in = (
        (gate_weights[:, :, None] * cotangent[:, None, :])
        .astype(jnp.bfloat16)
        .reshape(length * choices, model_width)
    )
    send_grad = down_in[pair_ids] * filled[:, None]
    recv_grad = move_rows(
        send_grad.reshape(device_count, local_experts * capacity, model_width), "grad_dispatch"
    )
    recv_grad = recv_grad.reshape(device_count, local_experts, capacity, model_width)
    act_grad = jnp.einsum("secd,efd->secf", recv_grad, w_down, preferred_element_type=jnp.float32)
    grad_w_down = jnp.einsum(
        "secf,secd->efd", activation, recv_grad, preferred_element_type=jnp.float32
    )
    gate_pre_grad = (
        act_grad * pre_up * gate_sigmoid * (1.0 + pre_gate * (1.0 - gate_sigmoid))
    ).astype(jnp.bfloat16)
    up_pre_grad = (act_grad * silu_gate).astype(jnp.bfloat16)
    grad_w_gate = jnp.einsum(
        "secd,secf->edf", received, gate_pre_grad, preferred_element_type=jnp.float32
    )
    grad_w_up = jnp.einsum(
        "secd,secf->edf", received, up_pre_grad, preferred_element_type=jnp.float32
    )
    row_grad = (
        jnp.einsum("secf,edf->secd", gate_pre_grad, w_gate, preferred_element_type=jnp.float32)
        + jnp.einsum("secf,edf->secd", up_pre_grad, w_up, preferred_element_type=jnp.float32)
    ).astype(jnp.bfloat16)
    row_back = move_rows(
        row_grad.reshape(device_count, local_experts * capacity, model_width), "grad_return"
    )
    row_back = row_back.reshape(experts * capacity, model_width)[destination].reshape(
        length, choices, model_width
    )
    sel_grad = gate_weights * (gate_grad - jnp.sum(gate_weights * gate_grad, -1, keepdims=True))
    logit_grad = jnp.sum(jnp.where(one_hot, sel_grad[:, :, None], 0.0), 1).astype(jnp.bfloat16)
    grad_w_router = jnp.dot(normed_mlp.T, logit_grad, preferred_element_type=jnp.float32)
    normed_mlp_grad = jnp.sum(row_back.astype(jnp.float32), 1) + jnp.dot(
        logit_grad, full_router.T, preferred_element_type=jnp.float32
    )
    grad_mlp_gain = jnp.sum(normed_mlp_grad * residual * inv_mlp, 0)
    residual_grad = cotangent + norm_grad(normed_mlp_grad, residual, inv_mlp, full_mlp_gain)
    grad_in, mixer_terms = mixer_backward(residual_grad, saved_state, weights)
    (
        grad_attn_gain,
        grad_query_gain,
        grad_key_gain,
        grad_w_query,
        grad_w_key,
        grad_w_value,
        grad_w_output,
    ) = mixer_terms
    summed = (
        lax.psum_scatter(grad_w_query, ("dp", "expert"), scatter_dimension=0, tiled=True),
        lax.psum_scatter(grad_w_key, ("dp", "expert"), scatter_dimension=0, tiled=True),
        lax.psum_scatter(grad_w_value, ("dp", "expert"), scatter_dimension=0, tiled=True),
        lax.psum_scatter(grad_w_output, ("dp", "expert"), scatter_dimension=0, tiled=True),
        lax.psum_scatter(grad_w_router, ("dp", "expert"), scatter_dimension=0, tiled=True),
        lax.psum_scatter(grad_attn_gain, ("dp", "expert"), scatter_dimension=0, tiled=True),
        lax.psum_scatter(grad_mlp_gain, ("dp", "expert"), scatter_dimension=0, tiled=True),
        lax.psum_scatter(grad_query_gain, ("dp", "expert"), scatter_dimension=0, tiled=True),
        lax.psum_scatter(grad_key_gain, ("dp", "expert"), scatter_dimension=0, tiled=True),
    )
    (
        share_w_query,
        share_w_key,
        share_w_value,
        share_w_output,
        share_w_router,
        share_attn_gain,
        share_mlp_gain,
        share_query_gain,
        share_key_gain,
    ) = summed
    return (
        block_out,
        grad_in,
        share_attn_gain,
        share_query_gain,
        share_key_gain,
        share_w_query,
        share_w_key,
        share_w_value,
        share_w_output,
        share_mlp_gain,
        share_w_router,
        grad_w_gate,
        grad_w_up,
        grad_w_down,
    )


def place():
    z = lax.axis_index("dp")
    e = lax.axis_index("expert")
    return z, e


def line_order(z, nz, j):
    near = jnp.minimum(z, nz - 1 - z)
    step = (j + 1) // 2
    zigzag = z + (step if j % 2 == 0 else -step)
    tail = jnp.where(z < nz - 1 - z, j, nz - 1 - j)
    return jnp.where(j <= 2 * near, zigzag, tail)


def greet(z, e, nz):
    barrier = pltpu.get_barrier_semaphore()
    for mate in (e ^ 1, e ^ 2, e ^ 4):
        pl.semaphore_signal(barrier, inc=1, device_id=(z, mate), device_id_type=MESH)

    @pl.when(z > 0)
    def _():
        pl.semaphore_signal(barrier, inc=1, device_id=(z - 1, e), device_id_type=MESH)

    @pl.when(z < nz - 1)
    def _():
        pl.semaphore_signal(barrier, inc=1, device_id=(z + 1, e), device_id_type=MESH)

    ends = (z > 0).astype(jnp.int32) + (z < nz - 1).astype(jnp.int32)
    pl.semaphore_wait(barrier, 3 + ends)


class Gather:
    Z, ZX, ZY, X3, X2, XQ, Y3, Y2, YQ, P0, PX3, PXQ, PY3, PYQ, PDX, PDY = range(16)
    KINDS = 16
    WHOLE, LOW, HIGH, LOW3, HIGH3, Q0, Q3 = (0, 4), (0, 2), (2, 2), (0, 3), (1, 3), (0, 1), (3, 1)

    def __init__(self, nz, shards, outs, send, recv, local):
        self.nz, self.shards, self.outs = nz, shards, outs
        self.send, self.recv, self.local = send, recv, local
        self.z, self.e = place()
        self.p, self.x, self.y, self.d = self.e ^ 1, self.e ^ 2, self.e ^ 4, self.e ^ 6

    def zz(self, j):
        return line_order(self.z, self.nz, j)

    def part(self, ref, piece):
        return ref.at[pl.ds(piece[0], piece[1])]

    def copy(self, i, kind, zz, ee, piece, dev, mine=False, sem=None):
        dst = self.part(self.outs[i].at[zz, ee], piece)
        return pltpu.make_async_remote_copy(
            src_ref=self.part(self.shards[i], piece) if mine else dst,
            dst_ref=dst,
            send_sem=self.send.at[i, zz, kind] if sem is None else sem,
            recv_sem=self.recv.at[i, zz, kind],
            device_id=dev,
            device_id_type=MESH,
        )

    def start(self, kind, zz, ee, piece, dev, mine=False):
        for i in range(len(self.outs)):
            self.copy(i, kind, zz, ee, piece, dev, mine).start()

    def arrived(self, kind, zz, ee, piece):
        for i in range(len(self.outs)):
            self.copy(i, kind, zz, ee, piece, (self.z, self.e)).wait_recv()

    def sent(self, kind, zz, ee, piece, mine=False):
        for i in range(len(self.outs)):
            self.copy(i, kind, zz, ee, piece, (self.z, self.e), mine).wait_send()

    def along(self, j, kind, ee, piece, act):
        z, e, nz = self.z, self.e, self.nz
        zz, mine = self.zz(j), j == 0 and kind == self.Z
        for i in range(len(self.outs)):
            @pl.when(jnp.logical_and(zz <= z, z < nz - 1))
            def _():
                act(self.copy(i, kind, zz, ee, piece, (z + 1, e), mine))

            @pl.when(jnp.logical_and(zz >= z, z > 0))
            def _():
                sem = self.local.at[1 + kind, i] if j == 0 else None
                act(self.copy(i, kind, zz, ee, piece, (z - 1, e), mine, sem))

    def keep(self, i):
        return pltpu.make_async_copy(self.shards[i], self.outs[i].at[self.z, self.e], self.local.at[0, i])

    def kept(self):
        for i in range(len(self.outs)):
            self.keep(i).wait()

    def launch(self, j):
        z, e, zz, mine = self.z, self.e, self.zz(j), j == 0
        if not mine:
            self.arrived(self.Z, zz, e, self.WHOLE)
        else:
            self.start(self.XQ, zz, e, self.Q3, (z, self.x), mine)
            self.start(self.YQ, zz, e, self.Q0, (z, self.y), mine)
        self.along(j, self.Z, e, self.WHOLE, lambda c: c.start())
        self.start(self.X3, zz, e, self.LOW3, (z, self.x), mine)
        self.start(self.Y3, zz, e, self.HIGH3, (z, self.y), mine)
        self.start(self.P0, zz, e, self.WHOLE, (z, self.p), mine)
        if mine:
            for i in range(len(self.outs)):
                self.keep(i).start()

    def mates(self, j):
        zz, mine = self.zz(j), j == 0
        self.arrived(self.XQ if mine else self.ZX, zz, self.x, self.Q3)
        self.along(j, self.ZX, self.x, self.Q3, lambda c: c.start())
        self.start(self.PXQ, zz, self.x, self.Q3, (self.z, self.p))
        self.arrived(self.YQ if mine else self.ZY, zz, self.y, self.Q0)
        self.along(j, self.ZY, self.y, self.Q0, lambda c: c.start())
        self.start(self.PYQ, zz, self.y, self.Q0, (self.z, self.p))

    def relay(self, j):
        zz = self.zz(j)
        self.arrived(self.X3, zz, self.x, self.LOW3)
        self.start(self.Y2, zz, self.x, self.HIGH, (self.z, self.y))
        self.start(self.PX3, zz, self.x, self.LOW3, (self.z, self.p))
        self.arrived(self.Y3, zz, self.y, self.HIGH3)
        self.start(self.X2, zz, self.y, self.LOW, (self.z, self.x))
        self.start(self.PY3, zz, self.y, self.HIGH3, (self.z, self.p))

    def finish(self, j):
        zz = self.zz(j)
        self.arrived(self.X2, zz, self.d, self.LOW)
        self.start(self.PDX, zz, self.d, self.LOW, (self.z, self.p))
        self.arrived(self.Y2, zz, self.d, self.HIGH)
        self.start(self.PDY, zz, self.d, self.HIGH, (self.z, self.p))

    def shared_near(self, j):
        zz, p = self.zz(j), self.p
        self.arrived(self.P0, zz, p, self.WHOLE)
        self.arrived(self.PXQ, zz, p ^ 2, self.Q3)
        self.arrived(self.PX3, zz, p ^ 2, self.LOW3)

    def shared_far(self, j):
        zz, p = self.zz(j), self.p
        self.arrived(self.PYQ, zz, p ^ 4, self.Q0)
        self.arrived(self.PY3, zz, p ^ 4, self.HIGH3)
        self.arrived(self.PDX, zz, p ^ 6, self.LOW)
        self.arrived(self.PDY, zz, p ^ 6, self.HIGH)

    def drain(self, j, kept=False):
        zz, e, mine = self.zz(j), self.e, j == 0
        if mine:
            self.sent(self.XQ, zz, e, self.Q3, mine)
            self.sent(self.YQ, zz, e, self.Q0, mine)
            if not kept:
                self.kept()
        for kind, ee, piece in ((self.Z, e, self.WHOLE), (self.ZX, self.x, self.Q3), (self.ZY, self.y, self.Q0)):
            self.along(j, kind, ee, piece, lambda c: c.wait_send())
        self.sent(self.X3, zz, e, self.LOW3, mine)
        self.sent(self.Y3, zz, e, self.HIGH3, mine)
        self.sent(self.P0, zz, e, self.WHOLE, mine)
        self.sent(self.PXQ, zz, self.x, self.Q3)
        self.sent(self.PYQ, zz, self.y, self.Q0)
        self.sent(self.Y2, zz, self.x, self.HIGH)
        self.sent(self.X2, zz, self.y, self.LOW)
        self.sent(self.PX3, zz, self.x, self.LOW3)
        self.sent(self.PY3, zz, self.y, self.HIGH3)
        self.sent(self.PDX, zz, self.d, self.LOW)
        self.sent(self.PDY, zz, self.d, self.HIGH)

    def steps(self):
        n = self.nz
        todo = [(self.launch, 0), (self.mates, 0)]
        for j in range(1, n + 2):
            todo += [(self.launch, j), (self.mates, j - 1) if j > 1 else None, (self.relay, j - 1), (self.finish, j - 2)]
        return [functools.partial(f, j) for f, j in filter(None, todo) if 0 <= j < n]


def gather_kernel(nz, count, *refs):
    shards, outs = refs[:count], refs[count : 2 * count]
    send, recv, local = refs[2 * count :]
    z, e = place()
    greet(z, e, nz)
    g = Gather(nz, shards, outs, send, recv, local)
    for step in g.steps():
        step()
    for j in range(nz):
        g.shared_near(j)
        g.shared_far(j)
    for j in range(nz):
        g.drain(j)


def gather_scratch(nz, count):
    return [
        pltpu.SemaphoreType.DMA((count, nz, Gather.KINDS)),
        pltpu.SemaphoreType.DMA((count, nz, Gather.KINDS)),
        pltpu.SemaphoreType.DMA((4, count)),
    ]


def gather_all(arrays, collective_id):
    nz, width = lax.axis_size("dp"), lax.axis_size("expert")
    count = len(arrays)
    parts = [a.reshape((4, a.shape[0] // 4) + a.shape[1:]) for a in arrays]
    outs = pl.pallas_call(
        functools.partial(gather_kernel, nz, count),
        out_shape=[jax.ShapeDtypeStruct((nz, width) + h.shape, h.dtype) for h in parts],
        in_specs=[pl.BlockSpec(memory_space=pltpu.VMEM)] * count,
        out_specs=[pl.BlockSpec(memory_space=pl.ANY)] * count,
        scratch_shapes=gather_scratch(nz, count),
        compiler_params=pltpu.CompilerParams(
            collective_id=collective_id, has_side_effects=True, vmem_limit_bytes=VMEM_LIMIT
        ),
        name="gather_all",
    )(*parts)
    return [o.reshape((nz * width * a.shape[0],) + a.shape[1:]) for o, a in zip(outs, arrays)]


def accumulate(dst, src):
    rows = dst.shape[0]
    block = 32 if rows % 32 == 0 else rows

    def body(r, _):
        at = pl.ds(pl.multiple_of(r * block, block), block)
        dst[at, :] = dst[at, :] + src[at, :]
        return 0

    lax.fori_loop(0, rows // block, body, 0)


class Scatter:
    X2, Y2, X3, Y3, Z, ZB, ZX, ZXB, ZY, ZYB, XQ, YQ = range(4, 16)
    KINDS = 16
    BUFFERS = 9

    def __init__(self, nz, terms, outs, sums, temps, from_x2, from_y2, from_x3, from_y3, from_z, from_zm, from_q, send, recv, local):
        self.nz, self.terms, self.outs = nz, terms, outs
        self.sums, self.temps = sums, temps
        self.from_x2, self.from_y2, self.from_x3, self.from_y3 = from_x2, from_y2, from_x3, from_y3
        self.from_z, self.from_zm, self.from_q = from_z, from_zm, from_q
        self.send, self.recv, self.local = send, recv, local
        self.count = len(terms)
        self.z, self.e = place()
        self.core, self.chip = self.e % 2, self.e // 2
        self.p, self.x, self.y = self.e ^ 1, self.e ^ 2, self.e ^ 4
        self.chips = (self.chip ^ 3, self.chip ^ 1, self.chip ^ 2, self.chip)

    def zz(self, j):
        return line_order(self.z, self.nz, self.nz - 1 - j)

    def remote(self, i, kind, zz, src, dst, dev):
        return pltpu.make_async_remote_copy(
            src_ref=src, dst_ref=dst, send_sem=self.send.at[i, zz, kind], recv_sem=self.recv.at[i, zz, kind],
            device_id=dev, device_id_type=MESH)

    def quarters(self, i, zz, q, first, n):
        return self.sums[i].at[zz, q, pl.ds(first, n)]

    def pair(self, i, j, q):
        zz, chip = self.zz(j), self.chips[q]
        return self.remote(i, q, zz, self.terms[i].at[zz, chip * 2 + (1 - self.core)], self.sums[i].at[zz, q],
                           (self.z, self.p))

    def load(self, i, j, q):
        slot = q % 2
        return pltpu.make_async_copy(
            self.terms[i].at[self.zz(j), self.chips[q] * 2 + self.core], self.temps[i].at[slot], self.local.at[i, slot])

    def x2(self, i, zz):
        return self.remote(i, self.X2, zz, self.quarters(i, zz, 0, 0, 2), self.from_x2[i].at[zz], (self.z, self.x))

    def y2(self, i, zz):
        return self.remote(i, self.Y2, zz, self.quarters(i, zz, 0, 2, 2), self.from_y2[i].at[zz], (self.z, self.y))

    def x3(self, i, zz):
        return self.remote(i, self.X3, zz, self.quarters(i, zz, 1, 0, 3), self.from_x3[i].at[zz], (self.z, self.x))

    def y3(self, i, zz):
        return self.remote(i, self.Y3, zz, self.quarters(i, zz, 2, 1, 3), self.from_y3[i].at[zz], (self.z, self.y))

    def xq(self, i):
        return self.remote(i, self.XQ, self.z, self.quarters(i, self.z, 1, 3, 1), self.from_q[i].at[pl.ds(0, 1)], (self.z, self.x))

    def yq(self, i):
        return self.remote(i, self.YQ, self.z, self.quarters(i, self.z, 2, 0, 1), self.from_q[i].at[pl.ds(1, 1)], (self.z, self.y))

    def line(self, i, zz, which, dz, last=False):
        slot = self.nz if last else zz
        kind = (self.Z, self.ZX, self.ZY)[which] + int(last)
        src = (self.sums[i].at[zz, 3], self.quarters(i, zz, 1, 3, 1), self.quarters(i, zz, 2, 0, 1))[which]
        dst = self.from_z[i].at[slot] if which == 0 else self.from_zm[i].at[slot, pl.ds(which - 1, 1)]
        return self.remote(i, kind, zz, src, dst, (self.z + dz, self.e))

    def add(self, i, zz, q, first, n, src):
        for k in range(n):
            accumulate(self.sums[i].at[zz, q, first + k], src.at[k])

    def begin(self):
        for j in range(self.nz):
            for q in range(4):
                for i in range(self.count):
                    self.pair(i, j, q).start()
        for i in range(self.count):
            self.load(i, 0, 0).start()

    def first(self, j):
        zz = self.zz(j)
        for q in range(4):
            for i in range(self.count):
                if q < 3:
                    self.load(i, j, q + 1).start()
                elif j < self.nz - 1:
                    self.load(i, j + 1, 0).start()
                self.pair(i, j, q).wait_recv()
                self.load(i, j, q).wait()
                self.add(i, zz, q, 0, 4, self.temps[i].at[q % 2])
                if q == 0:
                    self.x2(i, zz).start()
                    self.y2(i, zz).start()

    def second(self, j):
        zz = self.zz(j)
        for i in range(self.count):
            self.y2(i, zz).wait_recv()
            self.add(i, zz, 1, 2, 2, self.from_y2[i].at[zz])
            self.x3(i, zz).start()
            self.x2(i, zz).wait_recv()
            self.add(i, zz, 2, 0, 2, self.from_x2[i].at[zz])
            self.y3(i, zz).start()
            for which in (1, 2):
                self.flow(i, j, which)

    def flow(self, i, j, which):
        z, nz, zz = self.z, self.nz, self.zz(j)
        q, first, n = ((3, 0, 4), (1, 3, 1), (2, 0, 1))[which]

        def came(slot):
            ref = self.from_z[i].at[slot] if which == 0 else self.from_zm[i].at[slot, pl.ds(which - 1, 1)]
            self.add(i, zz, q, first, n, ref)

        if j < nz - 1:
            @pl.when(jnp.logical_or(jnp.logical_and(zz > z, z > 0), jnp.logical_and(zz < z, z < nz - 1)))
            def _():
                self.line(i, zz, which, 1).wait_recv()
                came(zz)

            @pl.when(zz > z)
            def _():
                self.line(i, zz, which, 1).start()

            @pl.when(zz < z - 1)
            def _():
                self.line(i, zz, which, -1).start()

            @pl.when(zz == z - 1)
            def _():
                self.line(i, zz, which, -1, True).start()
        else:
            @pl.when(z > 0)
            def _():
                self.line(i, zz, which, 1).wait_recv()
                came(zz)

            @pl.when(z < nz - 1)
            def _():
                self.line(i, zz, which, -1, True).wait_recv()
                came(nz)

            if which == 1:
                self.xq(i).start()
            if which == 2:
                self.yq(i).start()

    def third(self, j):
        zz = self.zz(j)
        for i in range(self.count):
            self.x3(i, zz).wait_recv()
            self.add(i, zz, 3, 0, 3, self.from_x3[i].at[zz])
            self.y3(i, zz).wait_recv()
            self.add(i, zz, 3, 1, 3, self.from_y3[i].at[zz])
            self.flow(i, j, 0)

    def result(self):
        for i in range(self.count):
            self.xq(i).wait_recv()
            self.add(i, self.z, 3, 3, 1, self.from_q[i].at[pl.ds(0, 1)])
            self.yq(i).wait_recv()
            self.add(i, self.z, 3, 0, 1, self.from_q[i].at[pl.ds(1, 1)])
            self.outs[i][...] = self.sums[i][self.z, 3].astype(self.outs[i].dtype)

    def drain(self, j):
        z, nz = self.z, self.nz
        zz = self.zz(j)
        for i in range(self.count):
            for q in range(4):
                self.pair(i, j, q).wait_send()
            for c in (self.x2, self.y2, self.x3, self.y3):
                c(i, zz).wait_send()
            if j < nz - 1:
                for which in range(3):
                    @pl.when(zz > z)
                    def _():
                        self.line(i, zz, which, 1).wait_send()

                    @pl.when(zz < z - 1)
                    def _():
                        self.line(i, zz, which, -1).wait_send()

                    @pl.when(zz == z - 1)
                    def _():
                        self.line(i, zz, which, -1, True).wait_send()
            else:
                self.xq(i).wait_send()
                self.yq(i).wait_send()

    def steps(self):
        todo = []
        for j in range(self.nz + 2):
            todo += [(self.first, j), (self.second, j - 1), (self.third, j - 2)]
        return [functools.partial(f, j) for f, j in todo if 0 <= j < self.nz] + [self.result]


def scatter_kernel(nz, count, *refs):
    groups = [refs[k * count : (k + 1) * count] for k in range(2 + Scatter.BUFFERS)]
    send, recv, local = refs[(2 + Scatter.BUFFERS) * count :]
    z, e = place()
    greet(z, e, nz)
    s = Scatter(nz, *groups, send, recv, local)
    s.begin()
    for step in s.steps():
        step()
    for j in range(nz):
        s.drain(j)


def scatter_buffers(nz, width, kinds):
    leads = ((nz, width // 2, 4), (2, 4), (nz, 2), (nz, 2), (nz, 3), (nz, 3), (nz + 1, 4), (nz + 1, 2), (2,))
    return [pltpu.VMEM(lead + shape, dtype) for lead in leads for shape, dtype in kinds] + [
        pltpu.SemaphoreType.DMA((len(kinds), nz, Scatter.KINDS)),
        pltpu.SemaphoreType.DMA((len(kinds), nz, Scatter.KINDS)),
        pltpu.SemaphoreType.DMA((len(kinds), 2)),
    ]


def scatter_sum(arrays, collective_id):
    nz, width = lax.axis_size("dp"), lax.axis_size("expert")
    count = len(arrays)
    devices = nz * width
    terms = [a.reshape(nz, width, 4, a.shape[0] // (4 * devices), a.shape[1]) for a in arrays]
    shapes = [t.shape[3:] for t in terms]
    outs = pl.pallas_call(
        functools.partial(scatter_kernel, nz, count),
        out_shape=[jax.ShapeDtypeStruct((4,) + s, jnp.float32) for s in shapes],
        in_specs=[pl.BlockSpec(memory_space=pl.ANY)] * count,
        out_specs=[pl.BlockSpec(memory_space=pltpu.VMEM)] * count,
        scratch_shapes=scatter_buffers(nz, width, [(s, a.dtype) for s, a in zip(shapes, arrays)]),
        compiler_params=pltpu.CompilerParams(
            collective_id=collective_id, has_side_effects=True, vmem_limit_bytes=VMEM_LIMIT
        ),
        name="scatter_sum",
    )(*terms)
    return [o.reshape(4 * s[0], s[1]) for o, s in zip(outs, shapes)]


def mm(a, b, da=1, db=0):
    return lax.dot_general(a, b, (((da,), (db,)), ((), ())), preferred_element_type=F32)


def rope(values, cosine, sine):
    return values * cosine + pltpu.roll(values, values.shape[1] // 2, 1) * sine


class AttentionGrad:
    def __init__(self, branch, w_out, raw, tables, gains, seg_col, seg_row, grads, gain_grads,
                 w_buf, q_buf, k_buf, v_buf, mask, k_rot, v_low, dk, dv, sems):
        self.branch, self.w_out, self.raw, self.tables, self.gains = branch, w_out, raw, tables, gains
        self.seg_col, self.seg_row, self.grads, self.gain_grads = seg_col, seg_row, grads, gain_grads
        self.w_buf, self.q_buf, self.k_buf, self.v_buf, self.mask = w_buf, q_buf, k_buf, v_buf, mask
        self.k_rot, self.v_low, self.dk, self.dv, self.sems = k_rot, v_low, dk, dv, sems
        self.cols = w_buf.shape[1]
        self.query_cols = w_out.shape[0]
        self.key_cols = k_buf.shape[1]
        self.count = self.query_cols // self.cols
        self.per_key = self.count // (self.key_cols // HEAD_DIM)

    def fetch(self, t, slot):
        at = pl.ds(pl.multiple_of(t * self.cols, self.cols), self.cols)
        return (
            pltpu.make_async_copy(self.w_out.at[at, :], self.w_buf.at[slot], self.sems.at[0, slot]),
            pltpu.make_async_copy(self.raw.at[:, at], self.q_buf.at[slot], self.sems.at[1, slot]),
        )

    def prepare(self):
        q, k = self.query_cols, self.key_cols
        key = pltpu.make_async_copy(self.raw.at[:, pl.ds(q, k)], self.k_buf, self.sems.at[2, 0])
        value = pltpu.make_async_copy(self.raw.at[:, pl.ds(q + k, k)], self.v_buf, self.sems.at[2, 1])
        key.start()
        value.start()
        for c in self.fetch(0, 0):
            c.start()
        self.mask[...] = allowed_mask(self.seg_col, self.seg_row)
        self.gain_grads[...] = jnp.zeros_like(self.gain_grads)
        key.wait()
        value.wait()

    def normed(self, raw, which):
        scale = lax.rsqrt(jnp.mean(raw * raw, 1, keepdims=True) + EPS)
        return scale, (raw * scale) * self.gains[which : which + 1, :]

    def back(self, rot_grad, raw, scale, which):
        cosine, sine = self.tables[0], self.tables[1]
        grad = rope(rot_grad, cosine, -sine)
        part = jnp.sum(grad * raw * scale, 0, keepdims=True)
        self.gain_grads[which : which + 1, :] = self.gain_grads[which : which + 1, :] + part
        weighted = grad * self.gains[which : which + 1, :]
        mean = jnp.mean(weighted * raw, 1, keepdims=True)
        return scale * weighted - raw * (scale * scale * scale) * mean

    def step(self, t):
        slot = lax.rem(t, 2)
        last = t + 1 < self.count

        @pl.when(last)
        def _():
            for c in self.fetch(t + 1, 1 - slot):
                c.start()

        for c in self.fetch(t, slot):
            c.wait()
        cosine, sine = self.tables[0], self.tables[1]
        at_key = pl.ds(pl.multiple_of(t // self.per_key * HEAD_DIM, HEAD_DIM), HEAD_DIM)

        @pl.when(lax.rem(t, self.per_key) == 0)
        def _():
            _, key = self.normed(self.k_buf[:, at_key], 1)
            self.k_rot[...] = rope(key, cosine, sine).astype(BF16)
            self.v_low[...] = self.v_buf[:, at_key].astype(BF16)
            self.dk[...] = jnp.zeros_like(self.dk)
            self.dv[...] = jnp.zeros_like(self.dv)

        score_scale = 1.0 / math.sqrt(HEAD_DIM)
        out_grad = mm(self.branch[...], self.w_buf[slot], 1, 1).astype(BF16)
        mask = self.mask[...] > 0.0
        k_rot, v_low = self.k_rot[...], self.v_low[...]
        for h in range(self.cols // HEAD_DIM):
            here = slice(h * HEAD_DIM, (h + 1) * HEAD_DIM)
            raw = self.q_buf[slot, :, here]
            scale, query = self.normed(raw, 0)
            q_rot = rope(query, cosine, sine).astype(BF16)
            d_out = out_grad[:, here]
            scores = mm(q_rot, k_rot, 1, 1) * score_scale
            raised = jnp.where(mask, jnp.exp(scores), 0.0)
            probs = raised / jnp.sum(raised, 1, keepdims=True)
            self.dv[...] += mm(probs.astype(BF16), d_out, 0, 0)
            d_probs = mm(d_out, v_low, 1, 1)
            d_scores = (probs * (d_probs - jnp.sum(probs * d_probs, 1, keepdims=True))).astype(BF16)
            dq = mm(d_scores, k_rot) * score_scale
            self.dk[...] += mm(d_scores, q_rot, 0, 0)
            at = pl.ds(pl.multiple_of(t * self.cols + h * HEAD_DIM, HEAD_DIM), HEAD_DIM)
            self.grads[:, at] = self.back(dq, raw, scale, 0).astype(BF16)

        @pl.when(lax.rem(t, self.per_key) == self.per_key - 1)
        def _():
            raw = self.k_buf[:, at_key]
            scale, _ = self.normed(raw, 1)
            shift = pl.multiple_of(t // self.per_key * HEAD_DIM, HEAD_DIM)
            self.grads[:, pl.ds(self.query_cols + shift, HEAD_DIM)] = self.back(
                self.dk[...] * score_scale, raw, scale, 1
            ).astype(BF16)
            self.grads[:, pl.ds(self.query_cols + self.key_cols + shift, HEAD_DIM)] = self.dv[...].astype(BF16)


def scatter_attention_kernel(nz, plan, term, branch, w_out, raw, tables, gains, seg_col, seg_row,
                             total, grads, gain_grads, *scratch):
    buffers, rest = scratch[: Scatter.BUFFERS], scratch[Scatter.BUFFERS :]
    send, recv, local = rest[:3]
    z, e = place()
    greet(z, e, nz)
    s = Scatter(nz, [term], [total], *[[b] for b in buffers], send, recv, local)
    a = AttentionGrad(branch, w_out, raw, tables, gains, seg_col, seg_row, grads, gain_grads, *rest[3:])
    s.begin()
    a.prepare()
    steps = s.steps()
    run_beside(a.count, a.step, steps, plan)
    for j in range(nz):
        s.drain(j)


def run_beside(count, work, steps, plan):
    bounds = [sum(plan[:t]) for t in range(len(plan) + 1)]

    def body(t, _):
        for k in range(count):
            todo = steps[bounds[k] : bounds[k + 1]]
            if todo:
                @pl.when(t == k)
                def _():
                    for step in todo:
                        step()
        work(t)
        return 0

    lax.fori_loop(0, count, body, 0)
    for step in steps[bounds[count] :]:
        step()


def scatter_with_attention(terms, branch, w_out, raw, tables, gains, segments, collective_id):
    nz, width = lax.axis_size("dp"), lax.axis_size("expert")
    devices = nz * width
    length = branch.shape[0]
    shape = (terms.shape[0] // (4 * devices), terms.shape[1])
    term = terms.reshape((nz, width, 4) + shape)
    heads = 4
    cols = heads * HEAD_DIM
    key_cols = (raw.shape[1] - w_out.shape[0]) // 2
    vmem = pl.BlockSpec(memory_space=pltpu.VMEM)
    hbm = pl.BlockSpec(memory_space=pl.ANY)
    plan = [3, 1, 1, 1, 1, 1, 1, 1]
    total, grads, gain_grads = pl.pallas_call(
        functools.partial(scatter_attention_kernel, nz, plan),
        out_shape=[
            jax.ShapeDtypeStruct((4,) + shape, F32),
            jax.ShapeDtypeStruct(raw.shape, BF16),
            jax.ShapeDtypeStruct((2, HEAD_DIM), F32),
        ],
        in_specs=[hbm, vmem, hbm, hbm, vmem, vmem, vmem, vmem],
        out_specs=[vmem, vmem, vmem],
        scratch_shapes=scatter_buffers(nz, width, [(shape, terms.dtype)])
        + [
            pltpu.VMEM((2, cols, w_out.shape[1]), BF16),
            pltpu.VMEM((2, length, cols), F32),
            pltpu.VMEM((length, key_cols), F32),
            pltpu.VMEM((length, key_cols), F32),
            pltpu.VMEM((length, length), F32),
            pltpu.VMEM((length, HEAD_DIM), BF16),
            pltpu.VMEM((length, HEAD_DIM), BF16),
            pltpu.VMEM((length, HEAD_DIM), F32),
            pltpu.VMEM((length, HEAD_DIM), F32),
            pltpu.SemaphoreType.DMA((3, 2)),
        ],
        compiler_params=pltpu.CompilerParams(
            collective_id=collective_id, has_side_effects=True, vmem_limit_bytes=VMEM_LIMIT
        ),
        name="scatter_attention",
    )(term, branch, w_out, raw, tables, gains, segments[:, None], segments[None, :])
    return total.reshape(4 * shape[0], shape[1]), grads, gain_grads


TILE = 512


class ExpertWork:
    def __init__(self, nz, cap, group, all_rows, all_tables, all_grads, weights, outs, bufs, sems):
        self.nz, self.cap, self.group = nz, cap, group
        self.all_rows, self.all_tables, self.all_grads = all_rows, all_tables, all_grads
        self.weights, self.outs, self.bufs, self.sems = weights, outs, bufs, sems
        self.z, self.e = place()
        self.width = all_rows.shape[1]
        self.per = self.width // group

    def weight_copies(self):
        return [pltpu.make_async_copy(w, b, self.sems.at[0, i]) for i, (w, b) in enumerate(zip(self.weights, self.bufs[:3]))]

    def inputs(self, t, slot):
        j, part = t // self.per, lax.rem(t, self.per)
        at = self.block(part)
        zz = line_place(self.z, self.nz, j)
        x, tab, g = self.bufs[3:6]
        return (
            pltpu.make_async_copy(self.all_rows.at[zz, at], x.at[slot], self.sems.at[1 + slot, 0]),
            pltpu.make_async_copy(self.all_tables.at[zz, at], tab.at[slot], self.sems.at[1 + slot, 1]),
            pltpu.make_async_copy(self.all_grads.at[zz, at], g.at[slot], self.sems.at[1 + slot, 2]),
        )

    def flat(self, t):
        step = self.group * self.cap
        return pl.ds(pl.multiple_of(t * step, step), step)

    def row_results(self, t):
        pairs = zip(self.bufs[8:10], self.outs[3:5])
        return [pltpu.make_async_copy(b, o.at[self.flat(t)], self.sems.at[3, i]) for i, (b, o) in enumerate(pairs)]

    def hidden_results(self, t):
        pairs = zip(self.bufs[10:13], self.outs[5:8])
        return [pltpu.make_async_copy(b, o.at[self.flat(t)], self.sems.at[3, 2 + i]) for i, (b, o) in enumerate(pairs)]

    def term_results(self, t, n, cols):
        at = self.block(lax.rem(t, self.per))
        zz = line_place(self.z, self.nz, t // self.per)
        pairs = zip(self.bufs[6:8], self.outs[:2])
        return [
            pltpu.make_async_copy(b.at[:, :, cols], o.at[zz, at, :, cols], self.sems.at[4 + i, n])
            for i, (b, o) in enumerate(pairs)
        ]

    def begin(self):
        for c in self.weight_copies():
            c.start()

    def block(self, part):
        near = self.e // self.group
        return pl.ds(jnp.where(part == 0, near, 1 - near) * self.group, self.group)

    def ready(self, j, part):
        for c in self.inputs(jnp.int32(j * self.per + part), part):
            c.start()

    def step(self, t, hook):
        slot = lax.rem(t, 2)
        hook(0)
        cap, group = self.cap, self.group
        wg, wu, wd, xb, tb, gb, yb, rb, rowb, downb, actb, gpb, upb, cotb = self.bufs
        for c in self.inputs(t, slot):
            c.wait()

        @pl.when(t == 0)
        def _():
            for c in self.weight_copies():
                c.wait()

        self.free(t, self.row_results)
        length, width = xb.shape[2] * xb.shape[3], xb.shape[4]
        lanes = tb.shape[4]
        me = self.z * self.width + self.e
        total = self.nz * self.width
        lane = lax.broadcasted_iota(jnp.int32, (8, lanes), 1)
        row = lax.broadcasted_iota(jnp.int32, (8, lanes), 0)
        gate_lanes = jnp.logical_and(row == 0, jnp.logical_or(lane == me, lane == total + me))
        rank_lane = jnp.logical_and(row == 1, lane == 2 * total + me)
        select = jnp.where(jnp.logical_or(gate_lanes, rank_lane), 1.0, 0.0).astype(BF16)
        slots = lax.broadcasted_iota(jnp.int32, (cap, length), 0).astype(F32)
        picks, gates = [], []
        for s in range(group):
            info = mm(select, tb[slot, s].reshape(length, lanes), 1, 1)
            hit = slots == info[1:2]
            pick = hit.astype(BF16)
            picks.append(pick)
            gate = jnp.sum(jnp.where(hit, info[0:1], 0.0), 1, keepdims=True)
            gates.append(gate)
            at = pl.ds(s * cap, cap)
            rowb[at, :] = mm(pick, xb[slot, s].reshape(length, width)).astype(BF16)
            cot = mm(pick, gb[slot, s].reshape(length, width))
            cotb[at, :] = cot.astype(BF16)
            downb[at, :] = (gate * cot).astype(BF16)
        for c in self.row_results(t):
            c.start()
        hook(1)
        gate_all = jnp.concatenate(gates, 0)
        rows = rowb[...]
        pre_gate = mm(rows, wg[...])
        pre_up = mm(rows, wu[...])
        sig = jax.nn.sigmoid(pre_gate)
        silu = pre_gate * sig
        self.free(t, self.hidden_results)
        actb[...] = (silu * pre_up).astype(BF16)
        hook(2)
        act_grad = mm(downb[...], wd[...], 1, 1)
        gpb[...] = (act_grad * pre_up * sig * (1.0 + pre_gate * (1.0 - sig))).astype(BF16)
        upb[...] = (act_grad * silu).astype(BF16)
        for c in self.hidden_results(t):
            c.start()
        gg = jnp.zeros((group * cap, 1), F32)
        for n in range(width // TILE):
            hook(3 + n)
            cols = pl.ds(n * TILE, TILE)
            self.free(t, lambda s: self.term_results(s, n, cols))
            out = mm(actb[...], wd[:, cols]).astype(BF16).astype(F32)
            gg = gg + jnp.sum(out * cotb[:, cols].astype(F32), 1, keepdims=True)
            out = (out * gate_all).astype(BF16)
            back = (mm(gpb[...], wg[cols, :], 1, 1) + mm(upb[...], wu[cols, :], 1, 1)).astype(BF16)
            for s in range(group):
                part = slice(s * cap, (s + 1) * cap)
                yb[s, :, cols] = mm(picks[s], out[part], 0, 0).astype(BF16)
                rb[s, :, cols] = mm(picks[s], back[part], 0, 0).astype(BF16)
            for c in self.term_results(t, n, cols):
                c.start()
        near = self.e // group
        block = jnp.where(lax.rem(t, self.per) == 0, near, 1 - near)
        first = line_place(self.z, self.nz, t // self.per) * self.width + block * group
        for s in range(group):
            self.outs[2][first + s] = jnp.sum(
                picks[s].astype(F32) * gg[s * cap : (s + 1) * cap], 0, keepdims=True
            )

    def free(self, t, copies):
        @pl.when(t > 0)
        def _():
            for c in copies(t - 1):
                c.wait()

    def end(self):
        t = jnp.int32(self.nz * self.per - 1)
        for c in self.row_results(t) + self.hidden_results(t):
            c.wait()
        for n in range(self.bufs[13].shape[1] // TILE):
            for c in self.term_results(t, n, pl.ds(n * TILE, TILE)):
                c.wait()


def line_place(z, nz, j):
    near = jnp.minimum(z, nz - 1 - z)
    step = (j + 1) // 2
    zigzag = jnp.where(lax.rem(j, 2) == 0, z + step, z - step)
    tail = jnp.where(z < nz - 1 - z, j, nz - 1 - j)
    return jnp.where(j <= 2 * near, zigzag, tail)


def gather_expert_kernel(nz, cap, group, *refs):
    shards, all_grads, weights = refs[:2], refs[2], refs[3:6]
    gathered, outs = refs[6:8], refs[8:16]
    send, recv, local = refs[16:19]
    bufs, sems = refs[19:33], refs[33]
    z, e = place()
    greet(z, e, nz)
    g = Gather(nz, shards, gathered, send, recv, local)
    w = ExpertWork(nz, cap, group, gathered[0], gathered[1], all_grads, weights, outs, bufs, sems)
    w.begin()
    edge = jnp.logical_or(z == 0, z == nz - 1)
    plans = RELAYS.get(nz) or (relays_first(g, nz),) * 2

    def run(name):
        kind, j = name[0], int(name[1:])
        if kind == "N":
            g.shared_near(j)
            if j == 0:
                g.kept()
            w.ready(j, 0)
        elif kind == "A":
            g.shared_far(j)
            w.ready(j, 1)
        else:
            {"L": g.launch, "M": g.mates, "R": g.relay, "F": g.finish}[kind](j)

    def body(t, _):
        def hook(k):
            for plan, here in zip(plans, (edge, jnp.logical_not(edge))):
                for piece, part, names in plan:
                    if part == k:
                        @pl.when(jnp.logical_and(t == piece, here))
                        def _():
                            for name in names.split():
                                run(name)

        w.step(t, hook)
        return 0

    lax.fori_loop(0, nz * w.per, body, 0)
    w.end()
    for j in range(nz):
        g.drain(j, True)


def relays_first(g, nz):
    names = [{"launch": "L", "mates": "M", "relay": "R", "finish": "F"}[f.func.__name__] + str(f.args[0]) for f in g.steps()]
    head = [(0, 0, n) for n in names]
    return head + [(2 * j, 0, "N%d" % j) for j in range(nz)] + [(2 * j + 1, 0, "A%d" % j) for j in range(nz)]


RELAYS = {
    4: (
        (
            (0, 0, "L0 M0 L1"), (0, 0, "R0 N0"), (0, 2, "M1"), (0, 6, "R1"), (1, 0, "N1 F0 A0 L2"), (1, 2, "F1"), (1, 5, "M2 A1"),
            (2, 6, "R2"), (3, 1, "N2"), (3, 5, "L3"), (4, 0, "F2"), (4, 2, "A2"), (4, 4, "M3"), (5, 2, "R3"), (5, 5, "N3"),
            (6, 3, "F3"), (6, 6, "A3"),
        ),
        (
            (0, 0, "L0 M0 L1"), (0, 0, "R0 L2 N0"), (0, 2, "M1 M2"), (0, 6, "R1"), (1, 0, "N1 F0 A0 L3"), (1, 6, "M3 R2"), (2, 2, "N2"),
            (2, 6, "F1"), (3, 0, "A1"), (3, 6, "R3"), (4, 1, "N3"), (4, 6, "F2"), (5, 0, "A2"), (5, 2, "F3"), (5, 5, "A3"),
        ),
    )
}


def gather_with_experts(rows, table, all_grads, w_gate, w_up, w_down, cap, collective_id):
    nz, width = lax.axis_size("dp"), lax.axis_size("expert")
    devices, group = nz * width, 4
    length, model = rows.shape
    ff = w_gate.shape[1]
    quarter = length // 4
    shards = [a.reshape(4, quarter, a.shape[1]) for a in (rows, table)]
    step, picked = group * cap, devices * cap
    vmem = pl.BlockSpec(memory_space=pltpu.VMEM)
    hbm = pl.BlockSpec(memory_space=pl.ANY)
    block = lambda a: pltpu.VMEM((2, group) + a.shape, a.dtype)
    shape = lambda *dims: jax.ShapeDtypeStruct(dims, BF16)
    outs = pl.pallas_call(
        functools.partial(gather_expert_kernel, nz, cap, group),
        out_shape=[shape(nz, width, *s.shape) for s in shards]
        + [
            shape(nz, width, length, model),
            shape(nz, width, length, model),
            jax.ShapeDtypeStruct((devices, 1, length), F32),
            shape(picked, model),
            shape(picked, model),
            shape(picked, ff),
            shape(picked, ff),
            shape(picked, ff),
        ],
        in_specs=[vmem, vmem, hbm, hbm, hbm, hbm],
        out_specs=[hbm, hbm, hbm, hbm, vmem, hbm, hbm, hbm, hbm, hbm],
        scratch_shapes=gather_scratch(nz, 2)
        + [pltpu.VMEM(w.shape, BF16) for w in (w_gate, w_up, w_down)]
        + [block(shards[0]), block(shards[1]), block(shards[0])]
        + [pltpu.VMEM((group, length, model), BF16)] * 2
        + [pltpu.VMEM((step, n), BF16) for n in (model, model, ff, ff, ff, model)]
        + [pltpu.SemaphoreType.DMA((6, max(5, model // TILE)))],
        compiler_params=pltpu.CompilerParams(
            collective_id=collective_id, has_side_effects=True, vmem_limit_bytes=VMEM_LIMIT
        ),
        name="gather_experts",
    )(*shards, all_grads.reshape((nz, width) + shards[0].shape), w_gate, w_up, w_down)
    return outs[2:]


class Attention:
    def __init__(self, hidden, gain, w_mixed, w_out, tables, gains, seg_col, seg_row, raw, normed, attended, branch,
                 w_buf, o_buf, kv_buf, mask, k_rot, v_low, sems):
        self.hidden, self.gain, self.w_mixed, self.w_out = hidden, gain, w_mixed, w_out
        self.tables, self.gains, self.seg_col, self.seg_row = tables, gains, seg_col, seg_row
        self.raw, self.normed, self.attended, self.branch = raw, normed, attended, branch
        self.w_buf, self.o_buf, self.kv_buf, self.mask = w_buf, o_buf, kv_buf, mask
        self.k_rot, self.v_low, self.sems = k_rot, v_low, sems
        self.cols = o_buf.shape[1]
        self.query_cols = w_out.shape[0]
        self.key_cols = kv_buf.shape[1] // 2
        self.count = self.query_cols // self.cols
        self.per_key = self.count // (self.key_cols // HEAD_DIM)

    def fetch(self, t, slot):
        at = pl.ds(pl.multiple_of(t * self.cols, self.cols), self.cols)
        return (
            pltpu.make_async_copy(self.w_mixed.at[:, at], self.w_buf.at[slot], self.sems.at[0, slot]),
            pltpu.make_async_copy(self.w_out.at[at, :], self.o_buf.at[slot], self.sems.at[1, slot]),
        )

    def prepare(self):
        kv = pltpu.make_async_copy(
            self.w_mixed.at[:, pl.ds(self.query_cols, 2 * self.key_cols)], self.kv_buf, self.sems.at[2, 0]
        )
        kv.start()
        for c in self.fetch(0, 0):
            c.start()
        values = self.hidden[...].astype(F32)
        scale = lax.rsqrt(jnp.mean(values * values, 1, keepdims=True) + EPS)
        self.normed[...] = (values * scale * self.gain[...]).astype(BF16)
        self.branch[...] = jnp.zeros_like(self.branch)
        self.mask[...] = allowed_mask(self.seg_col, self.seg_row)
        kv.wait()
        self.raw[:, self.query_cols :] = mm(self.normed[...], self.kv_buf[...])

    def step(self, t):
        slot = lax.rem(t, 2)

        @pl.when(t + 1 < self.count)
        def _():
            for c in self.fetch(t + 1, 1 - slot):
                c.start()

        for c in self.fetch(t, slot):
            c.wait()
        cosine, sine = self.tables[0], self.tables[1]

        @pl.when(lax.rem(t, self.per_key) == 0)
        def _():
            shift = pl.multiple_of(t // self.per_key * HEAD_DIM, HEAD_DIM)
            key = head_norm(self.raw[:, pl.ds(self.query_cols + shift, HEAD_DIM)], self.gains[1:2, :])
            self.k_rot[...] = rope(key, cosine, sine).astype(BF16)
            self.v_low[...] = self.raw[:, pl.ds(self.query_cols + self.key_cols + shift, HEAD_DIM)].astype(BF16)

        at = pl.ds(pl.multiple_of(t * self.cols, self.cols), self.cols)
        query_raw = mm(self.normed[...], self.w_buf[slot])
        self.raw[:, at] = query_raw
        mask = self.mask[...] > 0.0
        k_rot, v_low = self.k_rot[...], self.v_low[...]
        outs = []
        for h in range(self.cols // HEAD_DIM):
            query = head_norm(query_raw[:, h * HEAD_DIM : (h + 1) * HEAD_DIM], self.gains[0:1, :])
            q_rot = rope(query, cosine, sine).astype(BF16)
            scores = mm(q_rot, k_rot, 1, 1) * (1.0 / math.sqrt(HEAD_DIM))
            raised = jnp.where(mask, jnp.exp(scores), 0.0)
            probs = (raised / jnp.sum(raised, 1, keepdims=True)).astype(BF16)
            outs.append(mm(probs, v_low).astype(BF16))
        out = jnp.concatenate(outs, 1)
        self.attended[:, at] = out
        self.branch[...] += mm(out, self.o_buf[slot])


def head_norm(raw, gain):
    return raw * lax.rsqrt(jnp.mean(raw * raw, 1, keepdims=True) + EPS) * gain


def allowed_mask(seg_col, seg_row):
    length = seg_col.shape[0]
    row = lax.broadcasted_iota(jnp.int32, (length, length), 0)
    col = lax.broadcasted_iota(jnp.int32, (length, length), 1)
    same = seg_col[...] == seg_row[...]
    return jnp.where(jnp.logical_and(same, col <= row), 1.0, 0.0)


def gather_attention_kernel(nz, plan, shard, hidden, gain, w_mixed, w_out, tables, gains, seg_col, seg_row,
                            gathered, raw, normed, attended, branch, *scratch):
    z, e = place()
    greet(z, e, nz)
    g = Gather(nz, [shard], [gathered], *scratch[:3])
    a = Attention(hidden, gain, w_mixed, w_out, tables, gains, seg_col, seg_row, raw, normed, attended, branch, *scratch[3:])
    steps = g.steps()
    steps[0]()
    a.prepare()
    run_beside(a.count, a.step, steps[1:], plan)
    for j in range(nz):
        g.shared_near(j)
        g.shared_far(j)
    for j in range(nz):
        g.drain(j)


def gather_with_attention(rows, hidden, gain, w_mixed, w_out, tables, gains, segments, collective_id):
    nz, width = lax.axis_size("dp"), lax.axis_size("expert")
    length, model = hidden.shape
    shard = rows.reshape(4, rows.shape[0] // 4, rows.shape[1])
    cols = 4 * HEAD_DIM
    mixed, query_cols = w_mixed.shape[1], w_out.shape[0]
    vmem = pl.BlockSpec(memory_space=pltpu.VMEM)
    hbm = pl.BlockSpec(memory_space=pl.ANY)
    gathered, raw, normed, attended, branch = pl.pallas_call(
        functools.partial(gather_attention_kernel, nz, [1, 0, 1, 1, 0, 1, 2, 2]),
        out_shape=[
            jax.ShapeDtypeStruct((nz, width) + shard.shape, shard.dtype),
            jax.ShapeDtypeStruct((length, mixed), F32),
            jax.ShapeDtypeStruct((length, model), BF16),
            jax.ShapeDtypeStruct((length, query_cols), BF16),
            jax.ShapeDtypeStruct((length, model), F32),
        ],
        in_specs=[vmem, vmem, vmem, hbm, hbm, vmem, vmem, vmem, vmem],
        out_specs=[hbm, vmem, vmem, vmem, vmem],
        scratch_shapes=gather_scratch(nz, 1)
        + [
            pltpu.VMEM((2, model, cols), BF16),
            pltpu.VMEM((2, cols, model), BF16),
            pltpu.VMEM((model, mixed - query_cols), BF16),
            pltpu.VMEM((length, length), F32),
            pltpu.VMEM((length, HEAD_DIM), BF16),
            pltpu.VMEM((length, HEAD_DIM), BF16),
            pltpu.SemaphoreType.DMA((3, 2)),
        ],
        compiler_params=pltpu.CompilerParams(
            collective_id=collective_id, has_side_effects=True, vmem_limit_bytes=VMEM_LIMIT
        ),
        name="gather_attention",
    )(shard, hidden, gain, w_mixed, w_out, tables, gains, segments[:, None], segments[None, :])
    return gathered, raw, normed, attended, branch


def pack_columns(columns, rows, lanes, dtype):
    parts = [c.astype(dtype) for c in columns]
    used = sum(c.shape[1] for c in parts)
    return jnp.concatenate(parts + [jnp.zeros((rows, lanes - used), dtype)], 1)


def spread(vector, devices, rows):
    blocks = vector.reshape(devices, -1)
    return jnp.pad(blocks, ((0, 0), (0, rows - blocks.shape[1]))).reshape(devices * rows, 1)


def per_device_gather(
    hidden_in,
    segment_ids,
    expert_ids,
    attn_gain,
    query_gain,
    key_gain,
    w_query,
    w_key,
    w_value,
    w_output,
    mlp_gain,
    w_router,
    w_gate,
    w_up,
    w_down,
    out_grad,
):
    devices = lax.axis_size(("dp", "expert"))
    me = lax.axis_index(("dp", "expert"))
    length, choices = expert_ids.shape
    width = hidden_in.shape[1]
    experts_total = devices
    capacity = 5 * length * choices // (4 * experts_total)
    query_cols, key_cols = w_query.shape[1], w_key.shape[1]
    rows = w_query.shape[0]
    head_rows = query_gain.shape[0]

    column = lambda v: jnp.pad(v, (0, rows - v.shape[0]))[:, None]
    lanes = 128 * pl.cdiv(experts_total + 4, 128)
    small = pack_columns(
        [w_router, column(attn_gain), column(mlp_gain), column(query_gain), column(key_gain)], rows, lanes, BF16
    )
    w_mixed = jnp.concatenate([w_query, w_key, w_value], 1)
    w_mixed, w_out, small = gather_all([w_mixed, w_output, small], 1)
    router = small[:, :experts_total]
    attn_gain, mlp_gain = small[:, experts_total], small[:, experts_total + 1]
    heads_of = small.reshape(devices, rows, lanes)[:, :head_rows]
    query_gain = heads_of[:, :, experts_total + 2].reshape(-1)
    key_gain = heads_of[:, :, experts_total + 3].reshape(-1)

    plain_in = hidden_in.astype(F32)
    inv_attn = rms_scale(plain_in)
    cosine_table, sine_table = rope_tables(jnp.arange(length) % TOK_DEV, HEAD_DIM)
    cosine, sine = cosine_table[:, 0], sine_table[:, 0]
    tables = jnp.stack([jnp.concatenate([cosine, cosine], 1), jnp.concatenate([-sine, sine], 1)])
    head_gains = jnp.stack([query_gain, key_gain]).astype(F32)
    all_grads, mixed, normed_attn, attended, branch = gather_with_attention(
        out_grad, hidden_in, attn_gain.astype(F32)[None, :], w_mixed, w_out, tables, head_gains, segment_ids, 3
    )
    residual = plain_in + branch

    inv_mlp = rms_scale(residual)
    normed_mlp = (residual * inv_mlp * mlp_gain).astype(BF16)
    logits = jnp.dot(normed_mlp, router, preferred_element_type=F32)
    chosen = jnp.any(expert_ids[:, :, None] == jnp.arange(experts_total)[None, None, :], 1)
    raised = jnp.where(chosen, jnp.exp(logits), 0.0)
    gate = raised / jnp.sum(raised, -1, keepdims=True)
    position = jnp.arange(length)
    not_after = (position[None, :] <= position[:, None]).astype(BF16)
    rank = jnp.dot(not_after, chosen.astype(BF16), preferred_element_type=F32) - 1.0
    rank = jnp.where(chosen, rank, -1.0)
    gate_high = lax.reduce_precision(gate, 8, 7)
    table = pack_columns([gate_high, gate - gate_high, rank], length, 128 * pl.cdiv(3 * experts_total, 128), BF16)

    y_terms, r_terms, gate_terms, rows_in, down_in, act, gate_pre_grad, up_pre_grad = gather_with_experts(
        normed_mlp, table, all_grads, w_gate[0], w_up[0], w_down[0], capacity, 2
    )
    is_me = (jnp.arange(experts_total) == me).astype(F32)
    gate_terms = (gate_terms * is_me[None, :, None]).reshape(devices * experts_total, length)
    row_grad_sum, gate_grad = scatter_sum([r_terms.reshape(devices * length, width), gate_terms], 4)
    grad_w_down = jnp.dot(act.T, down_in, preferred_element_type=F32)[None]
    grad_w_gate = jnp.dot(rows_in.T, gate_pre_grad, preferred_element_type=F32)[None]
    grad_w_up = jnp.dot(rows_in.T, up_pre_grad, preferred_element_type=F32)[None]

    gate_grad = gate_grad.T
    sel_grad = gate * (gate_grad - jnp.sum(gate * gate_grad, -1, keepdims=True))
    logit_grad = jnp.where(chosen, sel_grad, 0.0).astype(BF16)
    grad_w_router = jnp.dot(normed_mlp.T, logit_grad, preferred_element_type=F32)
    normed_mlp_grad = row_grad_sum + jnp.dot(logit_grad, router.T, preferred_element_type=F32)
    grad_mlp_gain = jnp.sum(normed_mlp_grad * residual * inv_mlp, 0)
    residual_grad = out_grad.astype(F32) + norm_grad(normed_mlp_grad, residual, inv_mlp, mlp_gain)

    branch_grad = residual_grad.astype(BF16)
    grad_w_output = jnp.dot(attended.T, branch_grad, preferred_element_type=F32).astype(BF16)
    mixed_out, mixed_grad, gain_grads = scatter_with_attention(
        y_terms.reshape(devices * length, width), branch_grad, w_out, mixed, tables, head_gains, segment_ids, 5
    )
    block_out = residual + mixed_out
    grad_query_gain, grad_key_gain = gain_grads[0], gain_grads[1]
    grad_w_mixed = jnp.dot(normed_attn.T, mixed_grad, preferred_element_type=F32).astype(BF16)
    normed_attn_grad = jnp.dot(mixed_grad, w_mixed.T, preferred_element_type=F32)
    grad_attn_gain = jnp.sum(normed_attn_grad * plain_in * inv_attn, 0)
    grad_in = residual_grad + norm_grad(normed_attn_grad, plain_in, inv_attn, attn_gain)

    small_grads = pack_columns(
        [
            grad_w_router,
            grad_attn_gain[:, None],
            grad_mlp_gain[:, None],
            spread(grad_query_gain, devices, rows),
            spread(grad_key_gain, devices, rows),
        ],
        width,
        lanes,
        F32,
    )
    share_mixed, share_w_output, share_small = scatter_sum([grad_w_mixed, grad_w_output, small_grads], 6)
    return (
        block_out,
        grad_in,
        share_small[:, experts_total],
        share_small[:head_rows, experts_total + 2],
        share_small[:head_rows, experts_total + 3],
        share_mixed[:, :query_cols],
        share_mixed[:, query_cols : query_cols + key_cols],
        share_mixed[:, query_cols + key_cols :],
        share_w_output,
        share_small[:, experts_total + 1],
        share_small[:, :experts_total],
        grad_w_gate,
        grad_w_up,
        grad_w_down,
    )


def per_device(*arguments):
    expert_ids, w_gate = arguments[2], arguments[12]
    devices, width = lax.axis_size(("dp", "expert")), lax.axis_size("expert")
    length, choices = expert_ids.shape
    capacity = 5 * length * choices // (4 * devices)
    dense = devices <= 4 * choices and w_gate.shape[0] == 1 and width == 8
    if dense and capacity % 16 == 0 and devices % 4 == 0:
        return per_device_gather(*arguments)
    return per_device_exchange(*arguments)


def solution(mesh):
    in_specs = (
        P(("dp", "expert"), None),
        P(("dp", "expert")),
        P(("dp", "expert"), None),
        P(("dp", "expert")),
        P(("dp", "expert")),
        P(("dp", "expert")),
        P(("dp", "expert"), None),
        P(("dp", "expert"), None),
        P(("dp", "expert"), None),
        P(("dp", "expert"), None),
        P(("dp", "expert")),
        P(("dp", "expert"), None),
        P(("dp", "expert"), None, None),
        P(("dp", "expert"), None, None),
        P(("dp", "expert"), None, None),
        P(("dp", "expert"), None),
    )
    out_specs = (
        P(("dp", "expert"), None),
        P(("dp", "expert"), None),
        P(("dp", "expert")),
        P(("dp", "expert")),
        P(("dp", "expert")),
        P(("dp", "expert"), None),
        P(("dp", "expert"), None),
        P(("dp", "expert"), None),
        P(("dp", "expert"), None),
        P(("dp", "expert")),
        P(("dp", "expert"), None),
        P(("dp", "expert"), None, None),
        P(("dp", "expert"), None, None),
        P(("dp", "expert"), None, None),
    )
    return jax.shard_map(
        per_device, mesh=mesh, in_specs=in_specs, out_specs=out_specs, check_vma=False
    )
```

```python
import functools
import math

import jax
import jax.numpy as jnp
from jax import lax
from jax.experimental import pallas as pl
from jax.experimental.pallas import tpu as pltpu
from jax.sharding import PartitionSpec as P

F32, BF16 = jnp.float32, jnp.bfloat16
MESH = pl.DeviceIdType.MESH
VMEM_LIMIT = 63 * 1024 * 1024


HEADS = 32
KV_HEADS = 4
HEAD_DIM = 128
TOK_DEV = 256


EPS = 1e-06
ROPE_BASE = 1000000.0


def rms_scale(values):
    return lax.rsqrt(jnp.mean(values * values, -1, keepdims=True) + EPS)


def norm_grad(upstream, values, inverse, gain_vec):
    weighted = upstream * gain_vec
    return inverse * weighted - values * inverse**3 * jnp.mean(weighted * values, -1, keepdims=True)


def rope_tables(positions, head_dim):
    half_dim = head_dim // 2
    frequency = ROPE_BASE ** (-(jnp.arange(half_dim).astype(jnp.float32) * 2.0 / head_dim))
    angles = positions.astype(jnp.float32)[:, None] * frequency[None, :]
    return (jnp.cos(angles)[:, None, :], jnp.sin(angles)[:, None, :])


def rotate(values, cosine_table, sine_table):
    half_dim = values.shape[-1] // 2
    first_half = values[..., :half_dim]
    second_half = values[..., half_dim:]
    return jnp.concatenate(
        [
            first_half * cosine_table - second_half * sine_table,
            second_half * cosine_table + first_half * sine_table,
        ],
        -1,
    )


def unrotate(values, cosine_table, sine_table):
    half_dim = values.shape[-1] // 2
    first_half = values[..., :half_dim]
    second_half = values[..., half_dim:]
    return jnp.concatenate(
        [
            first_half * cosine_table + second_half * sine_table,
            second_half * cosine_table - first_half * sine_table,
        ],
        -1,
    )


def attend(query_rot, key_rot, value_rows, allowed):
    score_scale = 1.0 / math.sqrt(HEAD_DIM)
    scores = (
        jnp.einsum("qkgd,tkd->kgqt", query_rot, key_rot, preferred_element_type=jnp.float32)
        * score_scale
    )
    exp_scores = jnp.where(allowed, jnp.exp(scores), 0.0)
    totals = jnp.sum(exp_scores, -1, keepdims=True)
    probs_low = (exp_scores / totals).astype(jnp.bfloat16)
    attended = jnp.einsum(
        "kgqt,tkd->qkgd", probs_low, value_rows, preferred_element_type=jnp.float32
    ).astype(jnp.bfloat16)
    return (attended, jnp.log(totals))


def attend_grad(query_rot, key_rot, value_rows, allowed, log_totals, attended_grad):
    score_scale = 1.0 / math.sqrt(HEAD_DIM)
    scores = (
        jnp.einsum("qkgd,tkd->kgqt", query_rot, key_rot, preferred_element_type=jnp.float32)
        * score_scale
    )
    probs_back = jnp.where(allowed, jnp.exp(scores - log_totals), 0.0)
    probs_low = probs_back.astype(jnp.bfloat16)
    value_sum_grad = jnp.einsum(
        "kgqt,qkgd->tkd", probs_low, attended_grad, preferred_element_type=jnp.float32
    )
    prob_grad = jnp.einsum(
        "qkgd,tkd->kgqt", attended_grad, value_rows, preferred_element_type=jnp.float32
    )
    score_grad = (
        probs_back * (prob_grad - jnp.sum(probs_back * prob_grad, -1, keepdims=True))
    ).astype(jnp.bfloat16)
    query_rot_grad = (
        jnp.einsum("kgqt,tkd->qkgd", score_grad, key_rot, preferred_element_type=jnp.float32)
        * score_scale
    )
    key_rot_grad = (
        jnp.einsum("kgqt,qkgd->tkd", score_grad, query_rot, preferred_element_type=jnp.float32)
        * score_scale
    )
    return (query_rot_grad, key_rot_grad, value_sum_grad)


def mixer_forward(block_in, block_segments, weights):
    w_query, w_key, w_value, w_output, w_router, attn_gain, mlp_gain, query_gain, key_gain = weights
    row_count = block_in.shape[0]
    seq_count = row_count // TOK_DEV
    group_size = HEADS // KV_HEADS
    plain_in = block_in.astype(jnp.float32)
    inv_attn = rms_scale(plain_in)
    normed_attn = (plain_in * inv_attn * attn_gain).astype(jnp.bfloat16)
    query_raw = jnp.dot(normed_attn, w_query, preferred_element_type=jnp.float32).reshape(
        row_count, HEADS, HEAD_DIM
    )
    key_raw = jnp.dot(normed_attn, w_key, preferred_element_type=jnp.float32).reshape(
        row_count, KV_HEADS, HEAD_DIM
    )
    value_rows = jnp.dot(normed_attn, w_value, preferred_element_type=jnp.float32).astype(
        jnp.bfloat16
    )
    value_rows = value_rows.reshape(seq_count, TOK_DEV, KV_HEADS, HEAD_DIM)
    query_scale = rms_scale(query_raw)
    key_scale = rms_scale(key_raw)
    cosine_table, sine_table = rope_tables(jnp.arange(row_count) % TOK_DEV, HEAD_DIM)
    query_rot = rotate(query_raw * query_scale * query_gain, cosine_table, sine_table).astype(
        jnp.bfloat16
    )
    query_rot = query_rot.reshape(seq_count, TOK_DEV, KV_HEADS, group_size, HEAD_DIM)
    key_rot = rotate(key_raw * key_scale * key_gain, cosine_table, sine_table).astype(jnp.bfloat16)
    key_rot = key_rot.reshape(seq_count, TOK_DEV, KV_HEADS, HEAD_DIM)
    segments = block_segments.reshape(seq_count, TOK_DEV)
    position = jnp.arange(TOK_DEV)
    allowed = (segments[:, :, None] == segments[:, None, :]) & (
        position[None, None, :] <= position[None, :, None]
    )
    attended, log_totals = jax.vmap(attend)(query_rot, key_rot, value_rows, allowed)
    attended = attended.reshape(row_count, HEADS * HEAD_DIM)
    residual = plain_in + jnp.dot(attended, w_output, preferred_element_type=jnp.float32)
    saved_state = (
        plain_in,
        inv_attn,
        normed_attn,
        query_raw,
        key_raw,
        value_rows,
        query_scale,
        key_scale,
        query_rot,
        key_rot,
        allowed,
        log_totals,
        attended,
        cosine_table,
        sine_table,
    )
    return (residual, saved_state)


def mixer_backward(residual_grad, saved_state, weights):
    w_query, w_key, w_value, w_output, w_router, attn_gain, mlp_gain, query_gain, key_gain = weights
    (
        plain_in,
        inv_attn,
        normed_attn,
        query_raw,
        key_raw,
        value_rows,
        query_scale,
        key_scale,
        query_rot,
        key_rot,
        allowed,
        log_totals,
        attended,
        cosine_table,
        sine_table,
    ) = saved_state
    row_count = residual_grad.shape[0]
    seq_count = row_count // TOK_DEV
    group_size = HEADS // KV_HEADS
    branch_grad = residual_grad.astype(jnp.bfloat16)
    grad_w_output = jnp.dot(attended.T, branch_grad, preferred_element_type=jnp.float32)
    attended_grad = jnp.dot(branch_grad, w_output.T, preferred_element_type=jnp.float32).astype(
        jnp.bfloat16
    )
    attended_grad = attended_grad.reshape(seq_count, TOK_DEV, KV_HEADS, group_size, HEAD_DIM)
    query_rot_grad, key_rot_grad, value_sum_grad = jax.vmap(attend_grad)(
        query_rot, key_rot, value_rows, allowed, log_totals, attended_grad
    )
    query_normed_grad = unrotate(
        query_rot_grad.reshape(row_count, HEADS, HEAD_DIM), cosine_table, sine_table
    )
    key_normed_grad = unrotate(
        key_rot_grad.reshape(row_count, KV_HEADS, HEAD_DIM), cosine_table, sine_table
    )
    grad_query_gain = jnp.sum(query_normed_grad * query_raw * query_scale, (0, 1))
    grad_key_gain = jnp.sum(key_normed_grad * key_raw * key_scale, (0, 1))
    query_grad = norm_grad(query_normed_grad, query_raw, query_scale, query_gain).astype(
        jnp.bfloat16
    )
    query_grad = query_grad.reshape(row_count, HEADS * HEAD_DIM)
    key_grad = norm_grad(key_normed_grad, key_raw, key_scale, key_gain).astype(jnp.bfloat16)
    key_grad = key_grad.reshape(row_count, KV_HEADS * HEAD_DIM)
    value_grad = value_sum_grad.astype(jnp.bfloat16).reshape(row_count, KV_HEADS * HEAD_DIM)
    grad_w_query = jnp.dot(normed_attn.T, query_grad, preferred_element_type=jnp.float32)
    grad_w_key = jnp.dot(normed_attn.T, key_grad, preferred_element_type=jnp.float32)
    grad_w_value = jnp.dot(normed_attn.T, value_grad, preferred_element_type=jnp.float32)
    normed_attn_grad = (
        jnp.dot(query_grad, w_query.T, preferred_element_type=jnp.float32)
        + jnp.dot(key_grad, w_key.T, preferred_element_type=jnp.float32)
        + jnp.dot(value_grad, w_value.T, preferred_element_type=jnp.float32)
    )
    grad_attn_gain = jnp.sum(normed_attn_grad * plain_in * inv_attn, 0)
    grad_in = residual_grad + norm_grad(normed_attn_grad, plain_in, inv_attn, attn_gain)
    return (
        grad_in,
        (
            grad_attn_gain,
            grad_query_gain,
            grad_key_gain,
            grad_w_query,
            grad_w_key,
            grad_w_value,
            grad_w_output,
        ),
    )


def dispatch_table(expert_rows, experts, capacity):
    length, choices = expert_rows.shape
    flat_ids = expert_rows.reshape(length * choices)
    marks = (flat_ids[:, None] == jnp.arange(experts)[None, :]).astype(jnp.int32)
    earlier = jnp.cumsum(marks, 0) - marks
    destination = flat_ids * capacity + jnp.sum(earlier * marks, -1)
    pair_ids = (
        jnp.zeros((experts * capacity,), jnp.int32)
        .at[destination]
        .set(jnp.arange(length * choices, dtype=jnp.int32))
    )
    filled = jnp.zeros((experts * capacity,), jnp.bfloat16).at[destination].set(1.0)
    return (destination, pair_ids, filled)


def move_rows(row_block, section_name):
    if section_name == "dispatch":
        return lax.all_to_all(row_block, ("dp", "expert"), split_axis=0, concat_axis=0, tiled=True)
    if section_name == "combine":
        return lax.all_to_all(row_block, ("dp", "expert"), split_axis=0, concat_axis=0, tiled=True)
    if section_name == "grad_dispatch":
        return lax.all_to_all(row_block, ("dp", "expert"), split_axis=0, concat_axis=0, tiled=True)
    return lax.all_to_all(row_block, ("dp", "expert"), split_axis=0, concat_axis=0, tiled=True)


def per_device_exchange(
    hidden_in,
    segment_ids,
    expert_ids,
    attn_gain,
    query_gain,
    key_gain,
    w_query,
    w_key,
    w_value,
    w_output,
    mlp_gain,
    w_router,
    w_gate,
    w_up,
    w_down,
    out_grad,
):
    weights = (
        lax.all_gather(w_query, ("dp", "expert"), axis=0, tiled=True),
        lax.all_gather(w_key, ("dp", "expert"), axis=0, tiled=True),
        lax.all_gather(w_value, ("dp", "expert"), axis=0, tiled=True),
        lax.all_gather(w_output, ("dp", "expert"), axis=0, tiled=True),
        lax.all_gather(w_router, ("dp", "expert"), axis=0, tiled=True),
        lax.all_gather(attn_gain, ("dp", "expert"), axis=0, tiled=True),
        lax.all_gather(mlp_gain, ("dp", "expert"), axis=0, tiled=True),
        lax.all_gather(query_gain, ("dp", "expert"), axis=0, tiled=True),
        lax.all_gather(key_gain, ("dp", "expert"), axis=0, tiled=True),
    )
    residual, saved_state = mixer_forward(hidden_in, segment_ids, weights)
    full_router = weights[4]
    full_mlp_gain = weights[6]
    inv_mlp = rms_scale(residual)
    normed_mlp = (residual * inv_mlp * full_mlp_gain).astype(jnp.bfloat16)
    logits = jnp.dot(normed_mlp, full_router, preferred_element_type=jnp.float32)
    device_count = lax.axis_size(("dp", "expert"))
    local_experts = w_gate.shape[0]
    experts = local_experts * device_count
    length, choices = expert_ids.shape
    model_width = hidden_in.shape[1]
    capacity = 5 * length * choices // (4 * experts)
    one_hot = expert_ids[:, :, None] == jnp.arange(experts)[None, None, :]
    chosen = jnp.sum(jnp.where(one_hot, logits[:, None, :], 0.0), -1)
    raised = jnp.exp(chosen)
    gate_weights = raised / jnp.sum(raised, -1, keepdims=True)
    destination, pair_ids, filled = dispatch_table(expert_ids, experts, capacity)
    send_rows = normed_mlp[pair_ids // choices] * filled[:, None]
    received = move_rows(
        send_rows.reshape(device_count, local_experts * capacity, model_width), "dispatch"
    )
    received = received.reshape(device_count, local_experts, capacity, model_width)
    pre_gate = jnp.einsum("secd,edf->secf", received, w_gate, preferred_element_type=jnp.float32)
    pre_up = jnp.einsum("secd,edf->secf", received, w_up, preferred_element_type=jnp.float32)
    gate_sigmoid = jax.nn.sigmoid(pre_gate)
    silu_gate = pre_gate * gate_sigmoid
    activation = (silu_gate * pre_up).astype(jnp.bfloat16)
    expert_out = jnp.einsum(
        "secf,efd->secd", activation, w_down, preferred_element_type=jnp.float32
    ).astype(jnp.bfloat16)
    returned = move_rows(
        expert_out.reshape(device_count, local_experts * capacity, model_width), "combine"
    )
    picked = returned.reshape(experts * capacity, model_width)[destination].reshape(
        length, choices, model_width
    )
    block_out = residual + jnp.sum(gate_weights[:, :, None] * picked.astype(jnp.float32), 1)
    weights = (
        lax.all_gather(w_query, ("dp", "expert"), axis=0, tiled=True),
        lax.all_gather(w_key, ("dp", "expert"), axis=0, tiled=True),
        lax.all_gather(w_value, ("dp", "expert"), axis=0, tiled=True),
        lax.all_gather(w_output, ("dp", "expert"), axis=0, tiled=True),
        lax.all_gather(w_router, ("dp", "expert"), axis=0, tiled=True),
        lax.all_gather(attn_gain, ("dp", "expert"), axis=0, tiled=True),
        lax.all_gather(mlp_gain, ("dp", "expert"), axis=0, tiled=True),
        lax.all_gather(query_gain, ("dp", "expert"), axis=0, tiled=True),
        lax.all_gather(key_gain, ("dp", "expert"), axis=0, tiled=True),
    )
    full_router = weights[4]
    full_mlp_gain = weights[6]
    cotangent = out_grad.astype(jnp.float32)
    gate_grad = jnp.sum(cotangent[:, None, :] * picked.astype(jnp.float32), -1)
    down_in = (
        (gate_weights[:, :, None] * cotangent[:, None, :])
        .astype(jnp.bfloat16)
        .reshape(length * choices, model_width)
    )
    send_grad = down_in[pair_ids] * filled[:, None]
    recv_grad = move_rows(
        send_grad.reshape(device_count, local_experts * capacity, model_width), "grad_dispatch"
    )
    recv_grad = recv_grad.reshape(device_count, local_experts, capacity, model_width)
    act_grad = jnp.einsum("secd,efd->secf", recv_grad, w_down, preferred_element_type=jnp.float32)
    grad_w_down = jnp.einsum(
        "secf,secd->efd", activation, recv_grad, preferred_element_type=jnp.float32
    )
    gate_pre_grad = (
        act_grad * pre_up * gate_sigmoid * (1.0 + pre_gate * (1.0 - gate_sigmoid))
    ).astype(jnp.bfloat16)
    up_pre_grad = (act_grad * silu_gate).astype(jnp.bfloat16)
    grad_w_gate = jnp.einsum(
        "secd,secf->edf", received, gate_pre_grad, preferred_element_type=jnp.float32
    )
    grad_w_up = jnp.einsum(
        "secd,secf->edf", received, up_pre_grad, preferred_element_type=jnp.float32
    )
    row_grad = (
        jnp.einsum("secf,edf->secd", gate_pre_grad, w_gate, preferred_element_type=jnp.float32)
        + jnp.einsum("secf,edf->secd", up_pre_grad, w_up, preferred_element_type=jnp.float32)
    ).astype(jnp.bfloat16)
    row_back = move_rows(
        row_grad.reshape(device_count, local_experts * capacity, model_width), "grad_return"
    )
    row_back = row_back.reshape(experts * capacity, model_width)[destination].reshape(
        length, choices, model_width
    )
    sel_grad = gate_weights * (gate_grad - jnp.sum(gate_weights * gate_grad, -1, keepdims=True))
    logit_grad = jnp.sum(jnp.where(one_hot, sel_grad[:, :, None], 0.0), 1).astype(jnp.bfloat16)
    grad_w_router = jnp.dot(normed_mlp.T, logit_grad, preferred_element_type=jnp.float32)
    normed_mlp_grad = jnp.sum(row_back.astype(jnp.float32), 1) + jnp.dot(
        logit_grad, full_router.T, preferred_element_type=jnp.float32
    )
    grad_mlp_gain = jnp.sum(normed_mlp_grad * residual * inv_mlp, 0)
    residual_grad = cotangent + norm_grad(normed_mlp_grad, residual, inv_mlp, full_mlp_gain)
    grad_in, mixer_terms = mixer_backward(residual_grad, saved_state, weights)
    (
        grad_attn_gain,
        grad_query_gain,
        grad_key_gain,
        grad_w_query,
        grad_w_key,
        grad_w_value,
        grad_w_output,
    ) = mixer_terms
    summed = (
        lax.psum_scatter(grad_w_query, ("dp", "expert"), scatter_dimension=0, tiled=True),
        lax.psum_scatter(grad_w_key, ("dp", "expert"), scatter_dimension=0, tiled=True),
        lax.psum_scatter(grad_w_value, ("dp", "expert"), scatter_dimension=0, tiled=True),
        lax.psum_scatter(grad_w_output, ("dp", "expert"), scatter_dimension=0, tiled=True),
        lax.psum_scatter(grad_w_router, ("dp", "expert"), scatter_dimension=0, tiled=True),
        lax.psum_scatter(grad_attn_gain, ("dp", "expert"), scatter_dimension=0, tiled=True),
        lax.psum_scatter(grad_mlp_gain, ("dp", "expert"), scatter_dimension=0, tiled=True),
        lax.psum_scatter(grad_query_gain, ("dp", "expert"), scatter_dimension=0, tiled=True),
        lax.psum_scatter(grad_key_gain, ("dp", "expert"), scatter_dimension=0, tiled=True),
    )
    (
        share_w_query,
        share_w_key,
        share_w_value,
        share_w_output,
        share_w_router,
        share_attn_gain,
        share_mlp_gain,
        share_query_gain,
        share_key_gain,
    ) = summed
    return (
        block_out,
        grad_in,
        share_attn_gain,
        share_query_gain,
        share_key_gain,
        share_w_query,
        share_w_key,
        share_w_value,
        share_w_output,
        share_mlp_gain,
        share_w_router,
        grad_w_gate,
        grad_w_up,
        grad_w_down,
    )


def place():
    z = lax.axis_index("dp")
    e = lax.axis_index("expert")
    return z, e


def line_order(z, nz, j, inner=False):
    near = jnp.minimum(z, nz - 1 - z)
    step = (j + 1) // 2
    step = step if j % 2 == 0 else -step
    if inner:
        step = jnp.where(z < nz - 1 - z, -step, step)
    tail = jnp.where(z < nz - 1 - z, j, nz - 1 - j)
    return jnp.where(j <= 2 * near, z + step, tail)


def greet(z, e, nz):
    barrier = pltpu.get_barrier_semaphore()
    for mate in (e ^ 1, e ^ 2, e ^ 4):
        pl.semaphore_signal(barrier, inc=1, device_id=(z, mate), device_id_type=MESH)

    @pl.when(z > 0)
    def _():
        pl.semaphore_signal(barrier, inc=1, device_id=(z - 1, e), device_id_type=MESH)

    @pl.when(z < nz - 1)
    def _():
        pl.semaphore_signal(barrier, inc=1, device_id=(z + 1, e), device_id_type=MESH)

    ends = (z > 0).astype(jnp.int32) + (z < nz - 1).astype(jnp.int32)
    pl.semaphore_wait(barrier, 3 + ends)


class Gather:
    Z, ZX, ZY, X3, X2, XQ, Y3, Y2, YQ, P0, PX3, PXQ, PY3, PYQ, PDX, PDY = range(16)
    KINDS = 16
    WHOLE, LOW, HIGH, LOW3, HIGH3, Q0, Q3 = (0, 4), (0, 2), (2, 2), (0, 3), (1, 3), (0, 1), (3, 1)

    def __init__(self, nz, shards, outs, send, recv, local):
        self.nz, self.shards, self.outs = nz, shards, outs
        self.send, self.recv, self.local = send, recv, local
        self.z, self.e = place()
        self.p, self.x, self.y, self.d = self.e ^ 1, self.e ^ 2, self.e ^ 4, self.e ^ 6

    def zz(self, j):
        return line_order(self.z, self.nz, j)

    def part(self, ref, piece):
        return ref.at[pl.ds(piece[0], piece[1])]

    def copy(self, i, kind, zz, ee, piece, dev, mine=False, sem=None):
        dst = self.part(self.outs[i].at[zz, ee], piece)
        return pltpu.make_async_remote_copy(
            src_ref=self.part(self.shards[i], piece) if mine else dst,
            dst_ref=dst,
            send_sem=self.send.at[i, zz, kind] if sem is None else sem,
            recv_sem=self.recv.at[i, zz, kind],
            device_id=dev,
            device_id_type=MESH,
        )

    def start(self, kind, zz, ee, piece, dev, mine=False):
        for i in range(len(self.outs)):
            self.copy(i, kind, zz, ee, piece, dev, mine).start()

    def arrived(self, kind, zz, ee, piece):
        for i in range(len(self.outs)):
            self.copy(i, kind, zz, ee, piece, (self.z, self.e)).wait_recv()

    def sent(self, kind, zz, ee, piece, mine=False):
        for i in range(len(self.outs)):
            self.copy(i, kind, zz, ee, piece, (self.z, self.e), mine).wait_send()

    def along(self, j, kind, ee, piece, act):
        z, e, nz = self.z, self.e, self.nz
        zz, mine = self.zz(j), j == 0 and kind == self.Z
        for i in range(len(self.outs)):
            @pl.when(jnp.logical_and(zz <= z, z < nz - 1))
            def _():
                act(self.copy(i, kind, zz, ee, piece, (z + 1, e), mine))

            @pl.when(jnp.logical_and(zz >= z, z > 0))
            def _():
                sem = self.local.at[1 + kind, i] if j == 0 else None
                act(self.copy(i, kind, zz, ee, piece, (z - 1, e), mine, sem))

    def keep(self, i):
        return pltpu.make_async_copy(self.shards[i], self.outs[i].at[self.z, self.e], self.local.at[0, i])

    def kept(self):
        for i in range(len(self.outs)):
            self.keep(i).wait()

    def launch(self, j):
        self.launch_line(j)
        self.launch_plane(j)

    def launch_line(self, j):
        e, zz, mine = self.e, self.zz(j), j == 0
        if not mine:
            self.arrived(self.Z, zz, e, self.WHOLE)
        else:
            self.start(self.XQ, zz, e, self.Q3, (self.z, self.x), mine)
            self.start(self.YQ, zz, e, self.Q0, (self.z, self.y), mine)
        self.along(j, self.Z, e, self.WHOLE, lambda c: c.start())

    def launch_plane(self, j):
        z, e, zz, mine = self.z, self.e, self.zz(j), j == 0
        self.start(self.X3, zz, e, self.LOW3, (z, self.x), mine)
        self.start(self.Y3, zz, e, self.HIGH3, (z, self.y), mine)
        self.start(self.P0, zz, e, self.WHOLE, (z, self.p), mine)
        if mine:
            for i in range(len(self.outs)):
                self.keep(i).start()

    def mates(self, j):
        zz, mine = self.zz(j), j == 0
        self.arrived(self.XQ if mine else self.ZX, zz, self.x, self.Q3)
        self.along(j, self.ZX, self.x, self.Q3, lambda c: c.start())
        self.start(self.PXQ, zz, self.x, self.Q3, (self.z, self.p))
        self.arrived(self.YQ if mine else self.ZY, zz, self.y, self.Q0)
        self.along(j, self.ZY, self.y, self.Q0, lambda c: c.start())
        self.start(self.PYQ, zz, self.y, self.Q0, (self.z, self.p))

    def relay(self, j):
        zz = self.zz(j)
        self.arrived(self.X3, zz, self.x, self.LOW3)
        self.start(self.Y2, zz, self.x, self.HIGH, (self.z, self.y))
        self.start(self.PX3, zz, self.x, self.LOW3, (self.z, self.p))
        self.arrived(self.Y3, zz, self.y, self.HIGH3)
        self.start(self.X2, zz, self.y, self.LOW, (self.z, self.x))
        self.start(self.PY3, zz, self.y, self.HIGH3, (self.z, self.p))

    def finish(self, j):
        zz = self.zz(j)
        self.arrived(self.X2, zz, self.d, self.LOW)
        self.start(self.PDX, zz, self.d, self.LOW, (self.z, self.p))
        self.arrived(self.Y2, zz, self.d, self.HIGH)
        self.start(self.PDY, zz, self.d, self.HIGH, (self.z, self.p))

    def shared_near(self, j):
        zz, p = self.zz(j), self.p
        self.arrived(self.P0, zz, p, self.WHOLE)
        self.arrived(self.PXQ, zz, p ^ 2, self.Q3)
        self.arrived(self.PX3, zz, p ^ 2, self.LOW3)

    def shared_far(self, j):
        zz, p = self.zz(j), self.p
        self.arrived(self.PYQ, zz, p ^ 4, self.Q0)
        self.arrived(self.PY3, zz, p ^ 4, self.HIGH3)
        self.arrived(self.PDX, zz, p ^ 6, self.LOW)
        self.arrived(self.PDY, zz, p ^ 6, self.HIGH)

    def drain(self, j, kept=False):
        zz, e, mine = self.zz(j), self.e, j == 0
        if mine:
            self.sent(self.XQ, zz, e, self.Q3, mine)
            self.sent(self.YQ, zz, e, self.Q0, mine)
            if not kept:
                self.kept()
        for kind, ee, piece in ((self.Z, e, self.WHOLE), (self.ZX, self.x, self.Q3), (self.ZY, self.y, self.Q0)):
            self.along(j, kind, ee, piece, lambda c: c.wait_send())
        self.sent(self.X3, zz, e, self.LOW3, mine)
        self.sent(self.Y3, zz, e, self.HIGH3, mine)
        self.sent(self.P0, zz, e, self.WHOLE, mine)
        self.sent(self.PXQ, zz, self.x, self.Q3)
        self.sent(self.PYQ, zz, self.y, self.Q0)
        self.sent(self.Y2, zz, self.x, self.HIGH)
        self.sent(self.X2, zz, self.y, self.LOW)
        self.sent(self.PX3, zz, self.x, self.LOW3)
        self.sent(self.PY3, zz, self.y, self.HIGH3)
        self.sent(self.PDX, zz, self.d, self.LOW)
        self.sent(self.PDY, zz, self.d, self.HIGH)

    def steps(self):
        n = self.nz
        todo = [(self.launch, 0), (self.mates, 0)]
        for j in range(1, n + 2):
            todo += [(self.launch, j), (self.mates, j - 1) if j > 1 else None, (self.relay, j - 1), (self.finish, j - 2)]
        return [functools.partial(f, j) for f, j in filter(None, todo) if 0 <= j < n]


def gather_kernel(nz, count, *refs):
    shards, outs = refs[:count], refs[count : 2 * count]
    send, recv, local = refs[2 * count :]
    z, e = place()
    greet(z, e, nz)
    g = Gather(nz, shards, outs, send, recv, local)
    for step in g.steps():
        step()
    for j in range(nz):
        g.shared_near(j)
        g.shared_far(j)
    for j in range(nz):
        g.drain(j)


def gather_scratch(nz, count):
    return [
        pltpu.SemaphoreType.DMA((count, nz, Gather.KINDS)),
        pltpu.SemaphoreType.DMA((count, nz, Gather.KINDS)),
        pltpu.SemaphoreType.DMA((4, count)),
    ]


def gather_all(arrays, collective_id):
    nz, width = lax.axis_size("dp"), lax.axis_size("expert")
    count = len(arrays)
    parts = [a.reshape((4, a.shape[0] // 4) + a.shape[1:]) for a in arrays]
    outs = pl.pallas_call(
        functools.partial(gather_kernel, nz, count),
        out_shape=[jax.ShapeDtypeStruct((nz, width) + h.shape, h.dtype) for h in parts],
        in_specs=[pl.BlockSpec(memory_space=pltpu.VMEM)] * count,
        out_specs=[pl.BlockSpec(memory_space=pl.ANY)] * count,
        scratch_shapes=gather_scratch(nz, count),
        compiler_params=pltpu.CompilerParams(
            collective_id=collective_id, has_side_effects=True, vmem_limit_bytes=VMEM_LIMIT
        ),
        name="gather_all",
    )(*parts)
    return [o.reshape((nz * width * a.shape[0],) + a.shape[1:]) for o, a in zip(outs, arrays)]


def accumulate(dst, src):
    rows = dst.shape[0]
    block = 32 if rows % 32 == 0 else rows

    def body(r, _):
        at = pl.ds(pl.multiple_of(r * block, block), block)
        dst[at, :] = dst[at, :] + src[at, :]
        return 0

    lax.fori_loop(0, rows // block, body, 0)


class Scatter:
    X2, Y2, X3, Y3, Z, ZB, ZX, ZXB, ZY, ZYB, XQ, YQ = range(4, 16)
    KINDS = 16
    BUFFERS = 9

    def __init__(self, nz, terms, outs, sums, temps, from_x2, from_y2, from_x3, from_y3, from_z, from_zm, from_q, send, recv, local):
        self.nz, self.terms, self.outs = nz, terms, outs
        self.sums, self.temps = sums, temps
        self.from_x2, self.from_y2, self.from_x3, self.from_y3 = from_x2, from_y2, from_x3, from_y3
        self.from_z, self.from_zm, self.from_q = from_z, from_zm, from_q
        self.send, self.recv, self.local = send, recv, local
        self.count = len(terms)
        self.z, self.e = place()
        self.core, self.chip = self.e % 2, self.e // 2
        self.p, self.x, self.y = self.e ^ 1, self.e ^ 2, self.e ^ 4
        self.chips = (self.chip ^ 3, self.chip ^ 1, self.chip ^ 2, self.chip)

    def zz(self, j):
        return line_order(self.z, self.nz, self.nz - 1 - j, True)

    def remote(self, i, kind, zz, src, dst, dev):
        return pltpu.make_async_remote_copy(
            src_ref=src, dst_ref=dst, send_sem=self.send.at[i, zz, kind], recv_sem=self.recv.at[i, zz, kind],
            device_id=dev, device_id_type=MESH)

    def quarters(self, i, zz, q, first, n):
        return self.sums[i].at[zz, q, pl.ds(first, n)]

    def pair(self, i, j, q):
        zz, chip = self.zz(j), self.chips[q]
        return self.remote(i, q, zz, self.terms[i].at[zz, chip * 2 + (1 - self.core)], self.sums[i].at[zz, q],
                           (self.z, self.p))

    def load(self, i, j, q):
        slot = q % 2
        return pltpu.make_async_copy(
            self.terms[i].at[self.zz(j), self.chips[q] * 2 + self.core], self.temps[i].at[slot], self.local.at[i, slot])

    def x2(self, i, zz):
        return self.remote(i, self.X2, zz, self.quarters(i, zz, 0, 0, 2), self.from_x2[i].at[zz], (self.z, self.x))

    def y2(self, i, zz):
        return self.remote(i, self.Y2, zz, self.quarters(i, zz, 0, 2, 2), self.from_y2[i].at[zz], (self.z, self.y))

    def x3(self, i, zz):
        return self.remote(i, self.X3, zz, self.quarters(i, zz, 1, 0, 3), self.from_x3[i].at[zz], (self.z, self.x))

    def y3(self, i, zz):
        return self.remote(i, self.Y3, zz, self.quarters(i, zz, 2, 1, 3), self.from_y3[i].at[zz], (self.z, self.y))

    def xq(self, i):
        return self.remote(i, self.XQ, self.z, self.quarters(i, self.z, 1, 3, 1), self.from_q[i].at[pl.ds(0, 1)], (self.z, self.x))

    def yq(self, i):
        return self.remote(i, self.YQ, self.z, self.quarters(i, self.z, 2, 0, 1), self.from_q[i].at[pl.ds(1, 1)], (self.z, self.y))

    def line(self, i, zz, which, dz, last=False):
        slot = self.nz if last else zz
        kind = (self.Z, self.ZX, self.ZY)[which] + int(last)
        src = (self.sums[i].at[zz, 3], self.quarters(i, zz, 1, 3, 1), self.quarters(i, zz, 2, 0, 1))[which]
        dst = self.from_z[i].at[slot] if which == 0 else self.from_zm[i].at[slot, pl.ds(which - 1, 1)]
        return self.remote(i, kind, zz, src, dst, (self.z + dz, self.e))

    def add(self, i, zz, q, first, n, src):
        for k in range(n):
            accumulate(self.sums[i].at[zz, q, first + k], src.at[k])

    def begin(self):
        for j in range(self.nz):
            for q in range(4):
                for i in range(self.count):
                    self.pair(i, j, q).start()
        for i in range(self.count):
            self.load(i, 0, 0).start()

    def first(self, j):
        zz = self.zz(j)
        for q in range(4):
            for i in range(self.count):
                if q < 3:
                    self.load(i, j, q + 1).start()
                elif j < self.nz - 1:
                    self.load(i, j + 1, 0).start()
                self.pair(i, j, q).wait_recv()
                self.load(i, j, q).wait()
                self.add(i, zz, q, 0, 4, self.temps[i].at[q % 2])
                if q == 0:
                    self.x2(i, zz).start()
                    self.y2(i, zz).start()

    def second(self, j):
        zz = self.zz(j)
        for i in range(self.count):
            self.y2(i, zz).wait_recv()
            self.add(i, zz, 1, 2, 2, self.from_y2[i].at[zz])
            self.x3(i, zz).start()
            self.x2(i, zz).wait_recv()
            self.add(i, zz, 2, 0, 2, self.from_x2[i].at[zz])
            self.y3(i, zz).start()
            for which in (1, 2):
                self.flow(i, j, which)

    def flow(self, i, j, which):
        z, nz, zz = self.z, self.nz, self.zz(j)
        q, first, n = ((3, 0, 4), (1, 3, 1), (2, 0, 1))[which]

        def came(slot):
            ref = self.from_z[i].at[slot] if which == 0 else self.from_zm[i].at[slot, pl.ds(which - 1, 1)]
            self.add(i, zz, q, first, n, ref)

        if j < nz - 1:
            @pl.when(jnp.logical_or(jnp.logical_and(zz > z, z > 0), jnp.logical_and(zz < z, z < nz - 1)))
            def _():
                self.line(i, zz, which, 1).wait_recv()
                came(zz)

            @pl.when(zz > z)
            def _():
                self.line(i, zz, which, 1).start()

            @pl.when(zz < z - 1)
            def _():
                self.line(i, zz, which, -1).start()

            @pl.when(zz == z - 1)
            def _():
                self.line(i, zz, which, -1, True).start()
        else:
            @pl.when(z > 0)
            def _():
                self.line(i, zz, which, 1).wait_recv()
                came(zz)

            @pl.when(z < nz - 1)
            def _():
                self.line(i, zz, which, -1, True).wait_recv()
                came(nz)

            if which == 1:
                self.xq(i).start()
            if which == 2:
                self.yq(i).start()

    def third(self, j):
        zz = self.zz(j)
        for i in range(self.count):
            self.x3(i, zz).wait_recv()
            self.add(i, zz, 3, 0, 3, self.from_x3[i].at[zz])
            self.y3(i, zz).wait_recv()
            self.add(i, zz, 3, 1, 3, self.from_y3[i].at[zz])
            self.flow(i, j, 0)

    def result(self):
        for i in range(self.count):
            self.xq(i).wait_recv()
            self.add(i, self.z, 3, 3, 1, self.from_q[i].at[pl.ds(0, 1)])
            self.yq(i).wait_recv()
            self.add(i, self.z, 3, 0, 1, self.from_q[i].at[pl.ds(1, 1)])
            self.outs[i][...] = self.sums[i][self.z, 3].astype(self.outs[i].dtype)

    def drain(self, j):
        z, nz = self.z, self.nz
        zz = self.zz(j)
        for i in range(self.count):
            for q in range(4):
                self.pair(i, j, q).wait_send()
            for c in (self.x2, self.y2, self.x3, self.y3):
                c(i, zz).wait_send()
            if j < nz - 1:
                for which in range(3):
                    @pl.when(zz > z)
                    def _():
                        self.line(i, zz, which, 1).wait_send()

                    @pl.when(zz < z - 1)
                    def _():
                        self.line(i, zz, which, -1).wait_send()

                    @pl.when(zz == z - 1)
                    def _():
                        self.line(i, zz, which, -1, True).wait_send()
            else:
                self.xq(i).wait_send()
                self.yq(i).wait_send()

    def steps(self):
        todo = []
        for j in range(self.nz + 2):
            todo += [(self.first, j), (self.second, j - 1), (self.third, j - 2)]
        return [functools.partial(f, j) for f, j in todo if 0 <= j < self.nz] + [self.result]


def scatter_kernel(nz, count, *refs):
    groups = [refs[k * count : (k + 1) * count] for k in range(2 + Scatter.BUFFERS)]
    send, recv, local = refs[(2 + Scatter.BUFFERS) * count :]
    z, e = place()
    greet(z, e, nz)
    s = Scatter(nz, *groups, send, recv, local)
    s.begin()
    for step in s.steps():
        step()
    for j in range(nz):
        s.drain(j)


def scatter_buffers(nz, width, kinds):
    leads = ((nz, width // 2, 4), (2, 4), (nz, 2), (nz, 2), (nz, 3), (nz, 3), (nz + 1, 4), (nz + 1, 2), (2,))
    return [pltpu.VMEM(lead + shape, dtype) for lead in leads for shape, dtype in kinds] + [
        pltpu.SemaphoreType.DMA((len(kinds), nz, Scatter.KINDS)),
        pltpu.SemaphoreType.DMA((len(kinds), nz, Scatter.KINDS)),
        pltpu.SemaphoreType.DMA((len(kinds), 2)),
    ]


def scatter_sum(arrays, collective_id):
    nz, width = lax.axis_size("dp"), lax.axis_size("expert")
    count = len(arrays)
    devices = nz * width
    terms = [a.reshape(nz, width, 4, a.shape[0] // (4 * devices), a.shape[1]) for a in arrays]
    shapes = [t.shape[3:] for t in terms]
    outs = pl.pallas_call(
        functools.partial(scatter_kernel, nz, count),
        out_shape=[jax.ShapeDtypeStruct((4,) + s, jnp.float32) for s in shapes],
        in_specs=[pl.BlockSpec(memory_space=pl.ANY)] * count,
        out_specs=[pl.BlockSpec(memory_space=pltpu.VMEM)] * count,
        scratch_shapes=scatter_buffers(nz, width, [(s, a.dtype) for s, a in zip(shapes, arrays)]),
        compiler_params=pltpu.CompilerParams(
            collective_id=collective_id, has_side_effects=True, vmem_limit_bytes=VMEM_LIMIT
        ),
        name="scatter_sum",
    )(*terms)
    return [o.reshape(4 * s[0], s[1]) for o, s in zip(outs, shapes)]


def mm(a, b, da=1, db=0):
    return lax.dot_general(a, b, (((da,), (db,)), ((), ())), preferred_element_type=F32)


def rope(values, cosine, sine):
    return values * cosine + pltpu.roll(values, values.shape[1] // 2, 1) * sine


class AttentionGrad:
    def __init__(self, branch, w_out, raw, tables, gains, seg_col, seg_row, normed, attended, w_mixed,
                 grads, gain_grads, normed_grad, grad_out, grad_mixed,
                 w_buf, q_buf, k_buf, v_buf, mask, k_rot, v_low, dk, dv, a_buf, m_buf, out_stage, mixed_stage, sems):
        self.normed, self.attended, self.w_mixed = normed, attended, w_mixed
        self.normed_grad, self.grad_out, self.grad_mixed = normed_grad, grad_out, grad_mixed
        self.a_buf, self.m_buf, self.out_stage, self.mixed_stage = a_buf, m_buf, out_stage, mixed_stage
        self.branch, self.w_out, self.raw, self.tables, self.gains = branch, w_out, raw, tables, gains
        self.seg_col, self.seg_row, self.grads, self.gain_grads = seg_col, seg_row, grads, gain_grads
        self.w_buf, self.q_buf, self.k_buf, self.v_buf, self.mask = w_buf, q_buf, k_buf, v_buf, mask
        self.k_rot, self.v_low, self.dk, self.dv, self.sems = k_rot, v_low, dk, dv, sems
        self.cols = w_buf.shape[0]
        self.query_cols = w_out.shape[0]
        self.key_cols = k_buf.shape[1]
        self.count = self.query_cols // self.cols
        self.per_key = self.count // (self.key_cols // HEAD_DIM)
        self.total = self.count + 2 * self.key_cols // self.cols

    def at(self, t):
        return pl.ds(pl.multiple_of(t * self.cols, self.cols), self.cols)

    def fetch(self, t, slot):
        at = self.at(t)
        return pltpu.make_async_copy(self.raw.at[:, at], self.q_buf.at[slot], self.sems.at[1, slot])

    def fetch_out(self, t):
        at = self.at(t)
        return (
            pltpu.make_async_copy(self.w_out.at[at, :], self.w_buf, self.sems.at[0, 0]),
            pltpu.make_async_copy(self.attended.at[:, at], self.a_buf, self.sems.at[3, 0]),
        )

    def fetch_mixed(self, t):
        return pltpu.make_async_copy(self.w_mixed.at[:, self.at(t)], self.m_buf, self.sems.at[4, 0])

    def put_out(self, t):
        return pltpu.make_async_copy(self.out_stage, self.grad_out.at[self.at(t), :], self.sems.at[5, 0])

    def put_mixed(self, t):
        return pltpu.make_async_copy(self.mixed_stage, self.grad_mixed.at[:, self.at(t)], self.sems.at[5, 1])

    def prepare(self):
        q, k = self.query_cols, self.key_cols
        key = pltpu.make_async_copy(self.raw.at[:, pl.ds(q, k)], self.k_buf, self.sems.at[2, 0])
        value = pltpu.make_async_copy(self.raw.at[:, pl.ds(q + k, k)], self.v_buf, self.sems.at[2, 1])
        key.start()
        value.start()
        for c in self.fetch_out(0):
            c.start()
        self.fetch(0, 0).start()
        self.fetch_mixed(0).start()
        self.normed_grad[...] = jnp.zeros_like(self.normed_grad)
        self.mask[...] = allowed_mask(self.seg_col, self.seg_row)
        self.gain_grads[...] = jnp.zeros_like(self.gain_grads)
        key.wait()
        value.wait()

    def scaled(self, raw, which):
        scale = lax.rsqrt(jnp.mean(raw * raw, 1, keepdims=True) + EPS)
        return scale, (raw * scale) * self.gains[which : which + 1, :]

    def back(self, rot_grad, raw, scale, which):
        cosine, sine = self.tables[0], self.tables[1]
        grad = rope(rot_grad, cosine, -sine)
        part = jnp.sum(grad * raw * scale, 0, keepdims=True)
        self.gain_grads[which : which + 1, :] = self.gain_grads[which : which + 1, :] + part
        weighted = grad * self.gains[which : which + 1, :]
        mean = jnp.mean(weighted * raw, 1, keepdims=True)
        return scale * weighted - raw * (scale * scale * scale) * mean

    def step(self, t):
        slot = lax.rem(t, 2)

        @pl.when(t + 1 < self.count)
        def _():
            self.fetch(t + 1, 1 - slot).start()

        @pl.when(t < self.count)
        def _():
            self.heads(t, slot)

        self.fetch_mixed(t).wait()
        grads = self.grads[:, self.at(t)]
        self.normed_grad[...] += mm(grads, self.m_buf[...], 1, 1)

        @pl.when(t + 1 < self.total)
        def _():
            self.fetch_mixed(t + 1).start()

        @pl.when(t > 0)
        def _():
            self.put_mixed(t - 1).wait()

        self.mixed_stage[...] = mm(self.normed[...], grads, 0, 0).astype(BF16)
        self.put_mixed(t).start()

    def end(self):
        self.put_mixed(self.total - 1).wait()
        self.put_out(self.count - 1).wait()

    def heads(self, t, slot):
        self.fetch(t, slot).wait()
        for c in self.fetch_out(t):
            c.wait()

        @pl.when(t > 0)
        def _():
            self.put_out(t - 1).wait()

        self.out_stage[...] = mm(self.a_buf[...], self.branch[...], 0, 0).astype(BF16)
        self.put_out(t).start()
        cosine, sine = self.tables[0], self.tables[1]
        at_key = pl.ds(pl.multiple_of(t // self.per_key * HEAD_DIM, HEAD_DIM), HEAD_DIM)

        @pl.when(lax.rem(t, self.per_key) == 0)
        def _():
            _, key = self.scaled(self.k_buf[:, at_key], 1)
            self.k_rot[...] = rope(key, cosine, sine).astype(BF16)
            self.v_low[...] = self.v_buf[:, at_key].astype(BF16)
            self.dk[...] = jnp.zeros_like(self.dk)
            self.dv[...] = jnp.zeros_like(self.dv)

        score_scale = 1.0 / math.sqrt(HEAD_DIM)
        out_grad = mm(self.branch[...], self.w_buf[...], 1, 1).astype(BF16)

        @pl.when(t + 1 < self.count)
        def _():
            for c in self.fetch_out(t + 1):
                c.start()

        mask = self.mask[...] > 0.0
        k_rot, v_low = self.k_rot[...], self.v_low[...]
        for h in range(self.cols // HEAD_DIM):
            here = slice(h * HEAD_DIM, (h + 1) * HEAD_DIM)
            raw = self.q_buf[slot, :, here]
            scale, query = self.scaled(raw, 0)
            q_rot = rope(query, cosine, sine).astype(BF16)
            d_out = out_grad[:, here]
            scores = mm(q_rot, k_rot, 1, 1) * score_scale
            raised = jnp.where(mask, jnp.exp(scores), 0.0)
            probs = raised / jnp.sum(raised, 1, keepdims=True)
            self.dv[...] += mm(probs.astype(BF16), d_out, 0, 0)
            d_probs = mm(d_out, v_low, 1, 1)
            d_scores = (probs * (d_probs - jnp.sum(probs * d_probs, 1, keepdims=True))).astype(BF16)
            dq = mm(d_scores, k_rot) * score_scale
            self.dk[...] += mm(d_scores, q_rot, 0, 0)
            at = pl.ds(pl.multiple_of(t * self.cols + h * HEAD_DIM, HEAD_DIM), HEAD_DIM)
            self.grads[:, at] = self.back(dq, raw, scale, 0).astype(BF16)

        @pl.when(lax.rem(t, self.per_key) == self.per_key - 1)
        def _():
            raw = self.k_buf[:, at_key]
            scale, _ = self.scaled(raw, 1)
            shift = pl.multiple_of(t // self.per_key * HEAD_DIM, HEAD_DIM)
            self.grads[:, pl.ds(self.query_cols + shift, HEAD_DIM)] = self.back(
                self.dk[...] * score_scale, raw, scale, 1
            ).astype(BF16)
            self.grads[:, pl.ds(self.query_cols + self.key_cols + shift, HEAD_DIM)] = self.dv[...].astype(BF16)


def scatter_attention_kernel(nz, plan, term, *refs):
    inputs, (total, *outs), scratch = refs[:10], refs[10:16], refs[16:]
    buffers, rest = scratch[: Scatter.BUFFERS], scratch[Scatter.BUFFERS :]
    send, recv, local = rest[:3]
    z, e = place()
    greet(z, e, nz)
    s = Scatter(nz, [term], [total], *[[b] for b in buffers], send, recv, local)
    a = AttentionGrad(*inputs, *outs, *rest[3:])
    s.begin()
    a.prepare()
    steps = s.steps()
    run_beside(a.total, a.step, steps, plan)
    a.end()
    for j in range(nz):
        s.drain(j)


def run_beside(count, work, steps, plan):
    bounds = [sum(plan[:t]) for t in range(len(plan) + 1)]

    def body(t, _):
        for k in range(count):
            todo = steps[bounds[k] : bounds[k + 1]]
            if todo:
                @pl.when(t == k)
                def _():
                    for step in todo:
                        step()
        work(t)
        return 0

    lax.fori_loop(0, count, body, 0)
    for step in steps[bounds[count] :]:
        step()


def scatter_with_attention(terms, branch, w_out, raw, tables, gains, segments, normed, attended, w_mixed, collective_id):
    nz, width = lax.axis_size("dp"), lax.axis_size("expert")
    devices = nz * width
    length, model = branch.shape
    shape = (terms.shape[0] // (4 * devices), terms.shape[1])
    term = terms.reshape((nz, width, 4) + shape)
    heads = 4
    cols = heads * HEAD_DIM
    key_cols = (raw.shape[1] - w_out.shape[0]) // 2
    vmem = pl.BlockSpec(memory_space=pltpu.VMEM)
    hbm = pl.BlockSpec(memory_space=pl.ANY)
    plan = [3, 1, 1, 1, 1, 1, 1, 1, 1, 0]
    total, grads, gain_grads, normed_grad, grad_out, grad_mixed = pl.pallas_call(
        functools.partial(scatter_attention_kernel, nz, plan),
        out_shape=[
            jax.ShapeDtypeStruct((4,) + shape, F32),
            jax.ShapeDtypeStruct(raw.shape, BF16),
            jax.ShapeDtypeStruct((2, HEAD_DIM), F32),
            jax.ShapeDtypeStruct((length, model), F32),
            jax.ShapeDtypeStruct(w_out.shape, BF16),
            jax.ShapeDtypeStruct(w_mixed.shape, BF16),
        ],
        in_specs=[hbm, vmem, hbm, hbm, vmem, vmem, vmem, vmem, vmem, hbm, hbm],
        out_specs=[vmem, vmem, vmem, vmem, hbm, hbm],
        scratch_shapes=scatter_buffers(nz, width, [(shape, terms.dtype)])
        + [
            pltpu.VMEM((cols, model), BF16),
            pltpu.VMEM((2, length, cols), F32),
            pltpu.VMEM((length, key_cols), F32),
            pltpu.VMEM((length, key_cols), F32),
            pltpu.VMEM((length, length), F32),
            pltpu.VMEM((length, HEAD_DIM), BF16),
            pltpu.VMEM((length, HEAD_DIM), BF16),
            pltpu.VMEM((length, HEAD_DIM), F32),
            pltpu.VMEM((length, HEAD_DIM), F32),
            pltpu.VMEM((length, cols), BF16),
            pltpu.VMEM((model, cols), BF16),
            pltpu.VMEM((cols, model), BF16),
            pltpu.VMEM((model, cols), BF16),
            pltpu.SemaphoreType.DMA((6, 2)),
        ],
        compiler_params=pltpu.CompilerParams(
            collective_id=collective_id, has_side_effects=True, vmem_limit_bytes=VMEM_LIMIT
        ),
        name="scatter_attention",
    )(term, branch, w_out, raw, tables, gains, segments[:, None], segments[None, :], normed, attended, w_mixed)
    return total.reshape(4 * shape[0], shape[1]), gain_grads, normed_grad, grad_out, grad_mixed


TILE = 512


class ExpertWork:
    def __init__(self, nz, cap, group, orders, all_rows, all_tables, all_grads, weights, outs, bufs, sems):
        self.nz, self.cap, self.group = nz, cap, group
        self.all_rows, self.all_tables, self.all_grads = all_rows, all_tables, all_grads
        self.weights, self.outs, self.bufs, self.sems = weights, outs, bufs, sems
        self.z, self.e = place()
        self.width = all_rows.shape[1]
        self.orders = orders
        self.edge = jnp.logical_or(self.z == 0, self.z == nz - 1)

    def weight_copies(self):
        return [pltpu.make_async_copy(w, b, self.sems.at[0, i]) for i, (w, b) in enumerate(zip(self.weights, self.bufs[:3]))]

    def place_of(self, t):
        zz, half = jnp.int32(0), jnp.int32(0)
        for p, (ends, middle) in enumerate(zip(*self.orders)):
            for here, (j, h) in ((self.edge, ends), (jnp.logical_not(self.edge), middle)):
                here = jnp.logical_and(here, t == p)
                zz = jnp.where(here, line_order(self.z, self.nz, j), zz)
                half = jnp.where(here, h, half)
        near = self.e // self.group
        return zz, jnp.where(half == 0, near, 1 - near) * self.group

    def inputs(self, t, slot):
        zz, first = self.place_of(t)
        at = pl.ds(first, self.group)
        x, tab, g = self.bufs[3:6]
        return (
            pltpu.make_async_copy(self.all_rows.at[zz, at], x.at[slot], self.sems.at[1 + slot, 0]),
            pltpu.make_async_copy(self.all_tables.at[zz, at], tab.at[slot], self.sems.at[1 + slot, 1]),
            pltpu.make_async_copy(self.all_grads.at[zz, at], g.at[slot], self.sems.at[1 + slot, 2]),
        )

    def flat(self, t):
        step = self.group * self.cap
        return pl.ds(pl.multiple_of(t * step, step), step)

    def row_results(self, t):
        pairs = zip(self.bufs[8:10], self.outs[3:5])
        return [pltpu.make_async_copy(b, o.at[self.flat(t)], self.sems.at[3, i]) for i, (b, o) in enumerate(pairs)]

    def hidden_results(self, t):
        pairs = zip(self.bufs[10:13], self.outs[5:8])
        return [pltpu.make_async_copy(b, o.at[self.flat(t)], self.sems.at[3, 2 + i]) for i, (b, o) in enumerate(pairs)]

    def term_results(self, t, n, cols):
        zz, first = self.place_of(t)
        at = pl.ds(first, self.group)
        pairs = zip(self.bufs[6:8], self.outs[:2])
        return [
            pltpu.make_async_copy(b.at[:, :, cols], o.at[zz, at, :, cols], self.sems.at[4 + i, n])
            for i, (b, o) in enumerate(pairs)
        ]

    def begin(self):
        for c in self.weight_copies():
            c.start()

    def ready(self, p):
        for c in self.inputs(jnp.int32(p), p % 2):
            c.start()

    def step(self, t, hook):
        slot = lax.rem(t, 2)
        hook(0)
        cap, group = self.cap, self.group
        wg, wu, wd, xb, tb, gb, yb, rb, rowb, downb, actb, gpb, upb, cotb = self.bufs
        for c in self.inputs(t, slot):
            c.wait()

        @pl.when(t == 0)
        def _():
            for c in self.weight_copies():
                c.wait()

        self.free(t, self.row_results)
        length, width = xb.shape[2] * xb.shape[3], xb.shape[4]
        lanes = tb.shape[4]
        me = self.z * self.width + self.e
        total = self.nz * self.width
        lane = lax.broadcasted_iota(jnp.int32, (8, lanes), 1)
        row = lax.broadcasted_iota(jnp.int32, (8, lanes), 0)
        gate_lanes = jnp.logical_and(row == 0, jnp.logical_or(lane == me, lane == total + me))
        rank_lane = jnp.logical_and(row == 1, lane == 2 * total + me)
        select = jnp.where(jnp.logical_or(gate_lanes, rank_lane), 1.0, 0.0).astype(BF16)
        slots = lax.broadcasted_iota(jnp.int32, (cap, length), 0).astype(F32)
        picks, gates = [], []
        for s in range(group):
            info = mm(select, tb[slot, s].reshape(length, lanes), 1, 1)
            hit = slots == info[1:2]
            pick = hit.astype(BF16)
            picks.append(pick)
            gate = jnp.sum(jnp.where(hit, info[0:1], 0.0), 1, keepdims=True)
            gates.append(gate)
            at = pl.ds(s * cap, cap)
            rowb[at, :] = mm(pick, xb[slot, s].reshape(length, width)).astype(BF16)
            cot = mm(pick, gb[slot, s].reshape(length, width))
            cotb[at, :] = cot.astype(BF16)
            downb[at, :] = (gate * cot).astype(BF16)
        for c in self.row_results(t):
            c.start()
        hook(1)
        gate_all = jnp.concatenate(gates, 0)
        rows = rowb[...]
        pre_gate = mm(rows, wg[...])
        pre_up = mm(rows, wu[...])
        sig = jax.nn.sigmoid(pre_gate)
        silu = pre_gate * sig
        self.free(t, self.hidden_results)
        actb[...] = (silu * pre_up).astype(BF16)
        hook(2)
        act_grad = mm(downb[...], wd[...], 1, 1)
        gpb[...] = (act_grad * pre_up * sig * (1.0 + pre_gate * (1.0 - sig))).astype(BF16)
        upb[...] = (act_grad * silu).astype(BF16)
        for c in self.hidden_results(t):
            c.start()
        gg = jnp.zeros((group * cap, 1), F32)
        for n in range(width // TILE):
            hook(3 + n)
            cols = pl.ds(n * TILE, TILE)
            self.free(t, lambda s: self.term_results(s, n, cols))
            out = mm(actb[...], wd[:, cols]).astype(BF16).astype(F32)
            gg = gg + jnp.sum(out * cotb[:, cols].astype(F32), 1, keepdims=True)
            out = (out * gate_all).astype(BF16)
            back = (mm(gpb[...], wg[cols, :], 1, 1) + mm(upb[...], wu[cols, :], 1, 1)).astype(BF16)
            for s in range(group):
                part = slice(s * cap, (s + 1) * cap)
                yb[s, :, cols] = mm(picks[s], out[part], 0, 0).astype(BF16)
                rb[s, :, cols] = mm(picks[s], back[part], 0, 0).astype(BF16)
            for c in self.term_results(t, n, cols):
                c.start()
        zz, first = self.place_of(t)
        first = zz * self.width + first
        for s in range(group):
            self.outs[2][first + s] = jnp.sum(
                picks[s].astype(F32) * gg[s * cap : (s + 1) * cap], 0, keepdims=True
            )

    def free(self, t, copies):
        @pl.when(t > 0)
        def _():
            for c in copies(t - 1):
                c.wait()

    def end(self):
        t = jnp.int32(len(self.orders[0]) - 1)
        for c in self.row_results(t) + self.hidden_results(t):
            c.wait()
        for n in range(self.bufs[13].shape[1] // TILE):
            for c in self.term_results(t, n, pl.ds(n * TILE, TILE)):
                c.wait()


def gather_expert_kernel(nz, cap, group, *refs):
    shards, all_grads, weights = refs[:2], refs[2], refs[3:6]
    gathered, outs = refs[6:8], refs[8:16]
    send, recv, local = refs[16:19]
    bufs, sems = refs[19:33], refs[33]
    z, e = place()
    greet(z, e, nz)
    g = Gather(nz, shards, gathered, send, recv, local)
    plain = tuple((j, h) for j in range(nz) for h in range(2))
    orders = ORDERS.get(nz) or (plain, plain)
    plans = RELAYS.get(nz) or (relays_first(g, orders[0]),) * 2
    w = ExpertWork(nz, cap, group, orders, gathered[0], gathered[1], all_grads, weights, outs, bufs, sems)
    w.begin()
    relays = {"L": g.launch_line, "K": g.launch_plane, "M": g.mates, "R": g.relay, "F": g.finish}

    def run(name, order):
        kind, j = name[0], int(name[1:])
        if kind == "I":
            place, half = order[j]
            (g.shared_far if half else g.shared_near)(place)
            if place == 0 and half == 0:
                g.kept()
            w.ready(j)
        else:
            relays[kind](j)

    def body(t, _):
        def hook(k):
            for plan, order, here in zip(plans, orders, (w.edge, jnp.logical_not(w.edge))):
                for piece, part, names in plan:
                    if part == k:
                        @pl.when(jnp.logical_and(t == piece, here))
                        def _():
                            for name in names.split():
                                run(name, order)

        w.step(t, hook)
        return 0

    lax.fori_loop(0, len(orders[0]), body, 0)
    w.end()
    for j in range(nz):
        g.drain(j, True)


def relays_first(g, order):
    head = []
    for f in g.steps():
        kind, j = f.func.__name__, f.args[0]
        names = {"launch": "L%d K%d", "mates": "M%d", "relay": "R%d", "finish": "F%d"}[kind]
        head.append((0, 0, names.replace("%d", str(j))))
    return head + [(p, 0, "I%d" % p) for p in range(len(order))]


ORDERS = {
    4: (
        ((0, 0), (1, 0), (0, 1), (1, 1), (2, 0), (2, 1), (3, 0), (3, 1)),
        ((0, 0), (1, 0), (0, 1), (2, 0), (1, 1), (3, 0), (2, 1), (3, 1)),
    )
}
RELAYS = {
    4: (
        (
            (0, 0, "L0 K0 M0"),
            (0, 0, "L1 K1 R0"),
            (0, 0, "I0"),
            (0, 1, "M1"),
            (0, 5, "R1"),
            (1, 0, "I1"),
            (1, 2, "F0"),
            (1, 4, "L2 K2 I2"),
            (2, 1, "F1"),
            (2, 2, "M2 I3"),
            (3, 2, "R2"),
            (3, 4, "I4"),
            (4, 1, "L3 K3"),
            (4, 2, "F2"),
            (4, 5, "I5 M3"),
            (5, 3, "R3"),
            (5, 5, "I6"),
            (6, 3, "F3"),
            (6, 6, "I7"),
        ),
        (
            (0, 0, "L0 K0 M0"),
            (0, 0, "L1 L2 K1"),
            (0, 0, "R0 K2 I0"),
            (0, 1, "M1 M2"),
            (0, 4, "R1"),
            (0, 6, "I1"),
            (1, 2, "F0"),
            (1, 4, "L3 K3 I2"),
            (2, 2, "M3"),
            (2, 3, "R2"),
            (2, 5, "I3"),
            (3, 2, "F1"),
            (3, 5, "I4"),
            (4, 4, "R3"),
            (4, 6, "I5"),
            (5, 2, "F2"),
            (5, 5, "I6"),
            (6, 1, "F3"),
            (6, 3, "I7"),
        ),
    )
}


def gather_with_experts(rows, table, all_grads, w_gate, w_up, w_down, cap, collective_id):
    nz, width = lax.axis_size("dp"), lax.axis_size("expert")
    devices, group = nz * width, 4
    length, model = rows.shape
    ff = w_gate.shape[1]
    quarter = length // 4
    shards = [a.reshape(4, quarter, a.shape[1]) for a in (rows, table)]
    step, picked = group * cap, devices * cap
    vmem = pl.BlockSpec(memory_space=pltpu.VMEM)
    hbm = pl.BlockSpec(memory_space=pl.ANY)
    block = lambda a: pltpu.VMEM((2, group) + a.shape, a.dtype)
    shape = lambda *dims: jax.ShapeDtypeStruct(dims, BF16)
    outs = pl.pallas_call(
        functools.partial(gather_expert_kernel, nz, cap, group),
        out_shape=[shape(nz, width, *s.shape) for s in shards]
        + [
            shape(nz, width, length, model),
            shape(nz, width, length, model),
            jax.ShapeDtypeStruct((devices, 1, length), F32),
            shape(picked, model),
            shape(picked, model),
            shape(picked, ff),
            shape(picked, ff),
            shape(picked, ff),
        ],
        in_specs=[vmem, vmem, hbm, hbm, hbm, hbm],
        out_specs=[hbm, hbm, hbm, hbm, vmem, hbm, hbm, hbm, hbm, hbm],
        scratch_shapes=gather_scratch(nz, 2)
        + [pltpu.VMEM(w.shape, BF16) for w in (w_gate, w_up, w_down)]
        + [block(shards[0]), block(shards[1]), block(shards[0])]
        + [pltpu.VMEM((group, length, model), BF16)] * 2
        + [pltpu.VMEM((step, n), BF16) for n in (model, model, ff, ff, ff, model)]
        + [pltpu.SemaphoreType.DMA((6, max(5, model // TILE)))],
        compiler_params=pltpu.CompilerParams(
            collective_id=collective_id, has_side_effects=True, vmem_limit_bytes=VMEM_LIMIT
        ),
        name="gather_experts",
    )(*shards, all_grads.reshape((nz, width) + shards[0].shape), w_gate, w_up, w_down)
    return outs[2:]


class Attention:
    def __init__(self, hidden, gain, w_mixed, w_out, tables, gains, seg_col, seg_row, raw, normed, attended, branch,
                 w_buf, o_buf, kv_buf, mask, k_rot, v_low, sems):
        self.hidden, self.gain, self.w_mixed, self.w_out = hidden, gain, w_mixed, w_out
        self.tables, self.gains, self.seg_col, self.seg_row = tables, gains, seg_col, seg_row
        self.raw, self.normed, self.attended, self.branch = raw, normed, attended, branch
        self.w_buf, self.o_buf, self.kv_buf, self.mask = w_buf, o_buf, kv_buf, mask
        self.k_rot, self.v_low, self.sems = k_rot, v_low, sems
        self.cols = o_buf.shape[1]
        self.query_cols = w_out.shape[0]
        self.key_cols = kv_buf.shape[1] // 2
        self.count = self.query_cols // self.cols
        self.per_key = self.count // (self.key_cols // HEAD_DIM)

    def fetch(self, t, slot):
        at = pl.ds(pl.multiple_of(t * self.cols, self.cols), self.cols)
        return (
            pltpu.make_async_copy(self.w_mixed.at[:, at], self.w_buf.at[slot], self.sems.at[0, slot]),
            pltpu.make_async_copy(self.w_out.at[at, :], self.o_buf.at[slot], self.sems.at[1, slot]),
        )

    def prepare(self):
        kv = pltpu.make_async_copy(
            self.w_mixed.at[:, pl.ds(self.query_cols, 2 * self.key_cols)], self.kv_buf, self.sems.at[2, 0]
        )
        kv.start()
        for c in self.fetch(0, 0):
            c.start()
        values = self.hidden[...].astype(F32)
        scale = lax.rsqrt(jnp.mean(values * values, 1, keepdims=True) + EPS)
        self.normed[...] = (values * scale * self.gain[...]).astype(BF16)
        self.branch[...] = jnp.zeros_like(self.branch)
        self.mask[...] = allowed_mask(self.seg_col, self.seg_row)
        kv.wait()
        self.raw[:, self.query_cols :] = mm(self.normed[...], self.kv_buf[...])

    def step(self, t):
        slot = lax.rem(t, 2)

        @pl.when(t + 1 < self.count)
        def _():
            for c in self.fetch(t + 1, 1 - slot):
                c.start()

        for c in self.fetch(t, slot):
            c.wait()
        cosine, sine = self.tables[0], self.tables[1]

        @pl.when(lax.rem(t, self.per_key) == 0)
        def _():
            shift = pl.multiple_of(t // self.per_key * HEAD_DIM, HEAD_DIM)
            key = head_norm(self.raw[:, pl.ds(self.query_cols + shift, HEAD_DIM)], self.gains[1:2, :])
            self.k_rot[...] = rope(key, cosine, sine).astype(BF16)
            self.v_low[...] = self.raw[:, pl.ds(self.query_cols + self.key_cols + shift, HEAD_DIM)].astype(BF16)

        at = pl.ds(pl.multiple_of(t * self.cols, self.cols), self.cols)
        query_raw = mm(self.normed[...], self.w_buf[slot])
        self.raw[:, at] = query_raw
        mask = self.mask[...] > 0.0
        k_rot, v_low = self.k_rot[...], self.v_low[...]
        outs = []
        for h in range(self.cols // HEAD_DIM):
            query = head_norm(query_raw[:, h * HEAD_DIM : (h + 1) * HEAD_DIM], self.gains[0:1, :])
            q_rot = rope(query, cosine, sine).astype(BF16)
            scores = mm(q_rot, k_rot, 1, 1) * (1.0 / math.sqrt(HEAD_DIM))
            raised = jnp.where(mask, jnp.exp(scores), 0.0)
            probs = (raised / jnp.sum(raised, 1, keepdims=True)).astype(BF16)
            outs.append(mm(probs, v_low).astype(BF16))
        out = jnp.concatenate(outs, 1)
        self.attended[:, at] = out
        self.branch[...] += mm(out, self.o_buf[slot])


def head_norm(raw, gain):
    return raw * lax.rsqrt(jnp.mean(raw * raw, 1, keepdims=True) + EPS) * gain


def allowed_mask(seg_col, seg_row):
    length = seg_col.shape[0]
    row = lax.broadcasted_iota(jnp.int32, (length, length), 0)
    col = lax.broadcasted_iota(jnp.int32, (length, length), 1)
    same = seg_col[...] == seg_row[...]
    return jnp.where(jnp.logical_and(same, col <= row), 1.0, 0.0)


def gather_attention_kernel(nz, plan, shard, hidden, gain, w_mixed, w_out, tables, gains, seg_col, seg_row,
                            gathered, raw, normed, attended, branch, *scratch):
    z, e = place()
    greet(z, e, nz)
    g = Gather(nz, [shard], [gathered], *scratch[:3])
    a = Attention(hidden, gain, w_mixed, w_out, tables, gains, seg_col, seg_row, raw, normed, attended, branch, *scratch[3:])
    steps = g.steps()
    steps[0]()
    a.prepare()
    run_beside(a.count, a.step, steps[1:], plan)
    for j in range(nz):
        g.shared_near(j)
        g.shared_far(j)
    for j in range(nz):
        g.drain(j)


def gather_with_attention(rows, hidden, gain, w_mixed, w_out, tables, gains, segments, collective_id):
    nz, width = lax.axis_size("dp"), lax.axis_size("expert")
    length, model = hidden.shape
    shard = rows.reshape(4, rows.shape[0] // 4, rows.shape[1])
    cols = 4 * HEAD_DIM
    mixed, query_cols = w_mixed.shape[1], w_out.shape[0]
    vmem = pl.BlockSpec(memory_space=pltpu.VMEM)
    hbm = pl.BlockSpec(memory_space=pl.ANY)
    gathered, raw, normed, attended, branch = pl.pallas_call(
        functools.partial(gather_attention_kernel, nz, [1, 0, 1, 1, 0, 1, 2, 2]),
        out_shape=[
            jax.ShapeDtypeStruct((nz, width) + shard.shape, shard.dtype),
            jax.ShapeDtypeStruct((length, mixed), F32),
            jax.ShapeDtypeStruct((length, model), BF16),
            jax.ShapeDtypeStruct((length, query_cols), BF16),
            jax.ShapeDtypeStruct((length, model), F32),
        ],
        in_specs=[vmem, vmem, vmem, hbm, hbm, vmem, vmem, vmem, vmem],
        out_specs=[hbm, vmem, vmem, vmem, vmem],
        scratch_shapes=gather_scratch(nz, 1)
        + [
            pltpu.VMEM((2, model, cols), BF16),
            pltpu.VMEM((2, cols, model), BF16),
            pltpu.VMEM((model, mixed - query_cols), BF16),
            pltpu.VMEM((length, length), F32),
            pltpu.VMEM((length, HEAD_DIM), BF16),
            pltpu.VMEM((length, HEAD_DIM), BF16),
            pltpu.SemaphoreType.DMA((3, 2)),
        ],
        compiler_params=pltpu.CompilerParams(
            collective_id=collective_id, has_side_effects=True, vmem_limit_bytes=VMEM_LIMIT
        ),
        name="gather_attention",
    )(shard, hidden, gain, w_mixed, w_out, tables, gains, segments[:, None], segments[None, :])
    return gathered, raw, normed, attended, branch


def pack_columns(columns, rows, lanes, dtype):
    parts = [c.astype(dtype) for c in columns]
    used = sum(c.shape[1] for c in parts)
    return jnp.concatenate(parts + [jnp.zeros((rows, lanes - used), dtype)], 1)


def spread(vector, devices, rows):
    blocks = vector.reshape(devices, -1)
    return jnp.pad(blocks, ((0, 0), (0, rows - blocks.shape[1]))).reshape(devices * rows, 1)


def per_device_gather(
    hidden_in,
    segment_ids,
    expert_ids,
    attn_gain,
    query_gain,
    key_gain,
    w_query,
    w_key,
    w_value,
    w_output,
    mlp_gain,
    w_router,
    w_gate,
    w_up,
    w_down,
    out_grad,
):
    devices = lax.axis_size(("dp", "expert"))
    me = lax.axis_index(("dp", "expert"))
    length, choices = expert_ids.shape
    width = hidden_in.shape[1]
    experts_total = devices
    capacity = 5 * length * choices // (4 * experts_total)
    query_cols, key_cols = w_query.shape[1], w_key.shape[1]
    rows = w_query.shape[0]
    head_rows = query_gain.shape[0]

    column = lambda v: jnp.pad(v, (0, rows - v.shape[0]))[:, None]
    lanes = 128 * pl.cdiv(experts_total + 4, 128)
    small = pack_columns(
        [w_router, column(attn_gain), column(mlp_gain), column(query_gain), column(key_gain)], rows, lanes, BF16
    )
    w_mixed = jnp.concatenate([w_query, w_key, w_value], 1)
    w_mixed, w_out, small = gather_all([w_mixed, w_output, small], 1)
    router = small[:, :experts_total]
    attn_gain, mlp_gain = small[:, experts_total], small[:, experts_total + 1]
    heads_of = small.reshape(devices, rows, lanes)[:, :head_rows]
    query_gain = heads_of[:, :, experts_total + 2].reshape(-1)
    key_gain = heads_of[:, :, experts_total + 3].reshape(-1)

    plain_in = hidden_in.astype(F32)
    inv_attn = rms_scale(plain_in)
    cosine_table, sine_table = rope_tables(jnp.arange(length) % TOK_DEV, HEAD_DIM)
    cosine, sine = cosine_table[:, 0], sine_table[:, 0]
    tables = jnp.stack([jnp.concatenate([cosine, cosine], 1), jnp.concatenate([-sine, sine], 1)])
    head_gains = jnp.stack([query_gain, key_gain]).astype(F32)
    all_grads, mixed, normed_attn, attended, branch = gather_with_attention(
        out_grad, hidden_in, attn_gain.astype(F32)[None, :], w_mixed, w_out, tables, head_gains, segment_ids, 3
    )
    residual = plain_in + branch

    inv_mlp = rms_scale(residual)
    normed_mlp = (residual * inv_mlp * mlp_gain).astype(BF16)
    logits = jnp.dot(normed_mlp, router, preferred_element_type=F32)
    chosen = jnp.any(expert_ids[:, :, None] == jnp.arange(experts_total)[None, None, :], 1)
    raised = jnp.where(chosen, jnp.exp(logits), 0.0)
    gate = raised / jnp.sum(raised, -1, keepdims=True)
    position = jnp.arange(length)
    not_after = (position[None, :] <= position[:, None]).astype(BF16)
    rank = jnp.dot(not_after, chosen.astype(BF16), preferred_element_type=F32) - 1.0
    rank = jnp.where(chosen, rank, -1.0)
    gate_high = lax.reduce_precision(gate, 8, 7)
    table = pack_columns([gate_high, gate - gate_high, rank], length, 128 * pl.cdiv(3 * experts_total, 128), BF16)

    y_terms, r_terms, gate_terms, rows_in, down_in, act, gate_pre_grad, up_pre_grad = gather_with_experts(
        normed_mlp, table, all_grads, w_gate[0], w_up[0], w_down[0], capacity, 2
    )
    is_me = (jnp.arange(experts_total) == me).astype(F32)
    gate_terms = (gate_terms * is_me[None, :, None]).reshape(devices * experts_total, length)
    row_grad_sum, gate_grad = scatter_sum([r_terms.reshape(devices * length, width), gate_terms], 4)
    grad_w_down = jnp.dot(act.T, down_in, preferred_element_type=F32)[None]
    grad_w_gate = jnp.dot(rows_in.T, gate_pre_grad, preferred_element_type=F32)[None]
    grad_w_up = jnp.dot(rows_in.T, up_pre_grad, preferred_element_type=F32)[None]

    gate_grad = gate_grad.T
    sel_grad = gate * (gate_grad - jnp.sum(gate * gate_grad, -1, keepdims=True))
    logit_grad = jnp.where(chosen, sel_grad, 0.0).astype(BF16)
    grad_w_router = jnp.dot(normed_mlp.T, logit_grad, preferred_element_type=F32)
    normed_mlp_grad = row_grad_sum + jnp.dot(logit_grad, router.T, preferred_element_type=F32)
    grad_mlp_gain = jnp.sum(normed_mlp_grad * residual * inv_mlp, 0)
    residual_grad = out_grad.astype(F32) + norm_grad(normed_mlp_grad, residual, inv_mlp, mlp_gain)

    branch_grad = residual_grad.astype(BF16)
    mixed_out, gain_grads, normed_attn_grad, grad_w_output, grad_w_mixed = scatter_with_attention(
        y_terms.reshape(devices * length, width), branch_grad, w_out, mixed, tables, head_gains, segment_ids,
        normed_attn, attended, w_mixed, 5,
    )
    block_out = residual + mixed_out
    grad_query_gain, grad_key_gain = gain_grads[0], gain_grads[1]
    grad_attn_gain = jnp.sum(normed_attn_grad * plain_in * inv_attn, 0)
    grad_in = residual_grad + norm_grad(normed_attn_grad, plain_in, inv_attn, attn_gain)

    small_grads = pack_columns(
        [
            grad_w_router,
            grad_attn_gain[:, None],
            grad_mlp_gain[:, None],
            spread(grad_query_gain, devices, rows),
            spread(grad_key_gain, devices, rows),
        ],
        width,
        lanes,
        F32,
    )
    share_mixed, share_w_output, share_small = scatter_sum([grad_w_mixed, grad_w_output, small_grads], 6)
    return (
        block_out,
        grad_in,
        share_small[:, experts_total],
        share_small[:head_rows, experts_total + 2],
        share_small[:head_rows, experts_total + 3],
        share_mixed[:, :query_cols],
        share_mixed[:, query_cols : query_cols + key_cols],
        share_mixed[:, query_cols + key_cols :],
        share_w_output,
        share_small[:, experts_total + 1],
        share_small[:, :experts_total],
        grad_w_gate,
        grad_w_up,
        grad_w_down,
    )


def per_device(*arguments):
    expert_ids, w_gate = arguments[2], arguments[12]
    devices, width = lax.axis_size(("dp", "expert")), lax.axis_size("expert")
    length, choices = expert_ids.shape
    capacity = 5 * length * choices // (4 * devices)
    dense = devices <= 4 * choices and w_gate.shape[0] == 1 and width == 8
    if dense and capacity % 16 == 0 and devices % 4 == 0:
        return per_device_gather(*arguments)
    return per_device_exchange(*arguments)


def solution(mesh):
    in_specs = (
        P(("dp", "expert"), None),
        P(("dp", "expert")),
        P(("dp", "expert"), None),
        P(("dp", "expert")),
        P(("dp", "expert")),
        P(("dp", "expert")),
        P(("dp", "expert"), None),
        P(("dp", "expert"), None),
        P(("dp", "expert"), None),
        P(("dp", "expert"), None),
        P(("dp", "expert")),
        P(("dp", "expert"), None),
        P(("dp", "expert"), None, None),
        P(("dp", "expert"), None, None),
        P(("dp", "expert"), None, None),
        P(("dp", "expert"), None),
    )
    out_specs = (
        P(("dp", "expert"), None),
        P(("dp", "expert"), None),
        P(("dp", "expert")),
        P(("dp", "expert")),
        P(("dp", "expert")),
        P(("dp", "expert"), None),
        P(("dp", "expert"), None),
        P(("dp", "expert"), None),
        P(("dp", "expert"), None),
        P(("dp", "expert")),
        P(("dp", "expert"), None),
        P(("dp", "expert"), None, None),
        P(("dp", "expert"), None, None),
        P(("dp", "expert"), None, None),
    )
    return jax.shard_map(
        per_device, mesh=mesh, in_specs=in_specs, out_specs=out_specs, check_vma=False
    )
```

```python
import functools
import math

import jax
import jax.numpy as jnp
from jax import lax
from jax.experimental import pallas as pl
from jax.experimental.pallas import tpu as pltpu
from jax.sharding import PartitionSpec as P

F32, BF16 = jnp.float32, jnp.bfloat16
MESH = pl.DeviceIdType.MESH
VMEM_LIMIT = 63 * 1024 * 1024


HEADS = 32
KV_HEADS = 4
HEAD_DIM = 128
TOK_DEV = 256


EPS = 1e-06
ROPE_BASE = 1000000.0


def rms_scale(values):
    return lax.rsqrt(jnp.mean(values * values, -1, keepdims=True) + EPS)


def norm_grad(upstream, values, inverse, gain_vec):
    weighted = upstream * gain_vec
    return inverse * weighted - values * inverse**3 * jnp.mean(weighted * values, -1, keepdims=True)


def rope_tables(positions, head_dim):
    half_dim = head_dim // 2
    frequency = ROPE_BASE ** (-(jnp.arange(half_dim).astype(jnp.float32) * 2.0 / head_dim))
    angles = positions.astype(jnp.float32)[:, None] * frequency[None, :]
    return (jnp.cos(angles)[:, None, :], jnp.sin(angles)[:, None, :])


def rotate(values, cosine_table, sine_table):
    half_dim = values.shape[-1] // 2
    first_half = values[..., :half_dim]
    second_half = values[..., half_dim:]
    return jnp.concatenate(
        [
            first_half * cosine_table - second_half * sine_table,
            second_half * cosine_table + first_half * sine_table,
        ],
        -1,
    )


def unrotate(values, cosine_table, sine_table):
    half_dim = values.shape[-1] // 2
    first_half = values[..., :half_dim]
    second_half = values[..., half_dim:]
    return jnp.concatenate(
        [
            first_half * cosine_table + second_half * sine_table,
            second_half * cosine_table - first_half * sine_table,
        ],
        -1,
    )


def attend(query_rot, key_rot, value_rows, allowed):
    score_scale = 1.0 / math.sqrt(HEAD_DIM)
    scores = (
        jnp.einsum("qkgd,tkd->kgqt", query_rot, key_rot, preferred_element_type=jnp.float32)
        * score_scale
    )
    exp_scores = jnp.where(allowed, jnp.exp(scores), 0.0)
    totals = jnp.sum(exp_scores, -1, keepdims=True)
    probs_low = (exp_scores / totals).astype(jnp.bfloat16)
    attended = jnp.einsum(
        "kgqt,tkd->qkgd", probs_low, value_rows, preferred_element_type=jnp.float32
    ).astype(jnp.bfloat16)
    return (attended, jnp.log(totals))


def attend_grad(query_rot, key_rot, value_rows, allowed, log_totals, attended_grad):
    score_scale = 1.0 / math.sqrt(HEAD_DIM)
    scores = (
        jnp.einsum("qkgd,tkd->kgqt", query_rot, key_rot, preferred_element_type=jnp.float32)
        * score_scale
    )
    probs_back = jnp.where(allowed, jnp.exp(scores - log_totals), 0.0)
    probs_low = probs_back.astype(jnp.bfloat16)
    value_sum_grad = jnp.einsum(
        "kgqt,qkgd->tkd", probs_low, attended_grad, preferred_element_type=jnp.float32
    )
    prob_grad = jnp.einsum(
        "qkgd,tkd->kgqt", attended_grad, value_rows, preferred_element_type=jnp.float32
    )
    score_grad = (
        probs_back * (prob_grad - jnp.sum(probs_back * prob_grad, -1, keepdims=True))
    ).astype(jnp.bfloat16)
    query_rot_grad = (
        jnp.einsum("kgqt,tkd->qkgd", score_grad, key_rot, preferred_element_type=jnp.float32)
        * score_scale
    )
    key_rot_grad = (
        jnp.einsum("kgqt,qkgd->tkd", score_grad, query_rot, preferred_element_type=jnp.float32)
        * score_scale
    )
    return (query_rot_grad, key_rot_grad, value_sum_grad)


def mixer_forward(block_in, block_segments, weights):
    w_query, w_key, w_value, w_output, w_router, attn_gain, mlp_gain, query_gain, key_gain = weights
    row_count = block_in.shape[0]
    seq_count = row_count // TOK_DEV
    group_size = HEADS // KV_HEADS
    plain_in = block_in.astype(jnp.float32)
    inv_attn = rms_scale(plain_in)
    normed_attn = (plain_in * inv_attn * attn_gain).astype(jnp.bfloat16)
    query_raw = jnp.dot(normed_attn, w_query, preferred_element_type=jnp.float32).reshape(
        row_count, HEADS, HEAD_DIM
    )
    key_raw = jnp.dot(normed_attn, w_key, preferred_element_type=jnp.float32).reshape(
        row_count, KV_HEADS, HEAD_DIM
    )
    value_rows = jnp.dot(normed_attn, w_value, preferred_element_type=jnp.float32).astype(
        jnp.bfloat16
    )
    value_rows = value_rows.reshape(seq_count, TOK_DEV, KV_HEADS, HEAD_DIM)
    query_scale = rms_scale(query_raw)
    key_scale = rms_scale(key_raw)
    cosine_table, sine_table = rope_tables(jnp.arange(row_count) % TOK_DEV, HEAD_DIM)
    query_rot = rotate(query_raw * query_scale * query_gain, cosine_table, sine_table).astype(
        jnp.bfloat16
    )
    query_rot = query_rot.reshape(seq_count, TOK_DEV, KV_HEADS, group_size, HEAD_DIM)
    key_rot = rotate(key_raw * key_scale * key_gain, cosine_table, sine_table).astype(jnp.bfloat16)
    key_rot = key_rot.reshape(seq_count, TOK_DEV, KV_HEADS, HEAD_DIM)
    segments = block_segments.reshape(seq_count, TOK_DEV)
    position = jnp.arange(TOK_DEV)
    allowed = (segments[:, :, None] == segments[:, None, :]) & (
        position[None, None, :] <= position[None, :, None]
    )
    attended, log_totals = jax.vmap(attend)(query_rot, key_rot, value_rows, allowed)
    attended = attended.reshape(row_count, HEADS * HEAD_DIM)
    residual = plain_in + jnp.dot(attended, w_output, preferred_element_type=jnp.float32)
    saved_state = (
        plain_in,
        inv_attn,
        normed_attn,
        query_raw,
        key_raw,
        value_rows,
        query_scale,
        key_scale,
        query_rot,
        key_rot,
        allowed,
        log_totals,
        attended,
        cosine_table,
        sine_table,
    )
    return (residual, saved_state)


def mixer_backward(residual_grad, saved_state, weights):
    w_query, w_key, w_value, w_output, w_router, attn_gain, mlp_gain, query_gain, key_gain = weights
    (
        plain_in,
        inv_attn,
        normed_attn,
        query_raw,
        key_raw,
        value_rows,
        query_scale,
        key_scale,
        query_rot,
        key_rot,
        allowed,
        log_totals,
        attended,
        cosine_table,
        sine_table,
    ) = saved_state
    row_count = residual_grad.shape[0]
    seq_count = row_count // TOK_DEV
    group_size = HEADS // KV_HEADS
    branch_grad = residual_grad.astype(jnp.bfloat16)
    grad_w_output = jnp.dot(attended.T, branch_grad, preferred_element_type=jnp.float32)
    attended_grad = jnp.dot(branch_grad, w_output.T, preferred_element_type=jnp.float32).astype(
        jnp.bfloat16
    )
    attended_grad = attended_grad.reshape(seq_count, TOK_DEV, KV_HEADS, group_size, HEAD_DIM)
    query_rot_grad, key_rot_grad, value_sum_grad = jax.vmap(attend_grad)(
        query_rot, key_rot, value_rows, allowed, log_totals, attended_grad
    )
    query_normed_grad = unrotate(
        query_rot_grad.reshape(row_count, HEADS, HEAD_DIM), cosine_table, sine_table
    )
    key_normed_grad = unrotate(
        key_rot_grad.reshape(row_count, KV_HEADS, HEAD_DIM), cosine_table, sine_table
    )
    grad_query_gain = jnp.sum(query_normed_grad * query_raw * query_scale, (0, 1))
    grad_key_gain = jnp.sum(key_normed_grad * key_raw * key_scale, (0, 1))
    query_grad = norm_grad(query_normed_grad, query_raw, query_scale, query_gain).astype(
        jnp.bfloat16
    )
    query_grad = query_grad.reshape(row_count, HEADS * HEAD_DIM)
    key_grad = norm_grad(key_normed_grad, key_raw, key_scale, key_gain).astype(jnp.bfloat16)
    key_grad = key_grad.reshape(row_count, KV_HEADS * HEAD_DIM)
    value_grad = value_sum_grad.astype(jnp.bfloat16).reshape(row_count, KV_HEADS * HEAD_DIM)
    grad_w_query = jnp.dot(normed_attn.T, query_grad, preferred_element_type=jnp.float32)
    grad_w_key = jnp.dot(normed_attn.T, key_grad, preferred_element_type=jnp.float32)
    grad_w_value = jnp.dot(normed_attn.T, value_grad, preferred_element_type=jnp.float32)
    normed_attn_grad = (
        jnp.dot(query_grad, w_query.T, preferred_element_type=jnp.float32)
        + jnp.dot(key_grad, w_key.T, preferred_element_type=jnp.float32)
        + jnp.dot(value_grad, w_value.T, preferred_element_type=jnp.float32)
    )
    grad_attn_gain = jnp.sum(normed_attn_grad * plain_in * inv_attn, 0)
    grad_in = residual_grad + norm_grad(normed_attn_grad, plain_in, inv_attn, attn_gain)
    return (
        grad_in,
        (
            grad_attn_gain,
            grad_query_gain,
            grad_key_gain,
            grad_w_query,
            grad_w_key,
            grad_w_value,
            grad_w_output,
        ),
    )


def dispatch_table(expert_rows, experts, capacity):
    length, choices = expert_rows.shape
    flat_ids = expert_rows.reshape(length * choices)
    marks = (flat_ids[:, None] == jnp.arange(experts)[None, :]).astype(jnp.int32)
    earlier = jnp.cumsum(marks, 0) - marks
    destination = flat_ids * capacity + jnp.sum(earlier * marks, -1)
    pair_ids = (
        jnp.zeros((experts * capacity,), jnp.int32)
        .at[destination]
        .set(jnp.arange(length * choices, dtype=jnp.int32))
    )
    filled = jnp.zeros((experts * capacity,), jnp.bfloat16).at[destination].set(1.0)
    return (destination, pair_ids, filled)


def move_rows(row_block, section_name):
    if section_name == "dispatch":
        return lax.all_to_all(row_block, ("dp", "expert"), split_axis=0, concat_axis=0, tiled=True)
    if section_name == "combine":
        return lax.all_to_all(row_block, ("dp", "expert"), split_axis=0, concat_axis=0, tiled=True)
    if section_name == "grad_dispatch":
        return lax.all_to_all(row_block, ("dp", "expert"), split_axis=0, concat_axis=0, tiled=True)
    return lax.all_to_all(row_block, ("dp", "expert"), split_axis=0, concat_axis=0, tiled=True)


def per_device_exchange(
    hidden_in,
    segment_ids,
    expert_ids,
    attn_gain,
    query_gain,
    key_gain,
    w_query,
    w_key,
    w_value,
    w_output,
    mlp_gain,
    w_router,
    w_gate,
    w_up,
    w_down,
    out_grad,
):
    weights = (
        lax.all_gather(w_query, ("dp", "expert"), axis=0, tiled=True),
        lax.all_gather(w_key, ("dp", "expert"), axis=0, tiled=True),
        lax.all_gather(w_value, ("dp", "expert"), axis=0, tiled=True),
        lax.all_gather(w_output, ("dp", "expert"), axis=0, tiled=True),
        lax.all_gather(w_router, ("dp", "expert"), axis=0, tiled=True),
        lax.all_gather(attn_gain, ("dp", "expert"), axis=0, tiled=True),
        lax.all_gather(mlp_gain, ("dp", "expert"), axis=0, tiled=True),
        lax.all_gather(query_gain, ("dp", "expert"), axis=0, tiled=True),
        lax.all_gather(key_gain, ("dp", "expert"), axis=0, tiled=True),
    )
    residual, saved_state = mixer_forward(hidden_in, segment_ids, weights)
    full_router = weights[4]
    full_mlp_gain = weights[6]
    inv_mlp = rms_scale(residual)
    normed_mlp = (residual * inv_mlp * full_mlp_gain).astype(jnp.bfloat16)
    logits = jnp.dot(normed_mlp, full_router, preferred_element_type=jnp.float32)
    device_count = lax.axis_size(("dp", "expert"))
    local_experts = w_gate.shape[0]
    experts = local_experts * device_count
    length, choices = expert_ids.shape
    model_width = hidden_in.shape[1]
    capacity = 5 * length * choices // (4 * experts)
    one_hot = expert_ids[:, :, None] == jnp.arange(experts)[None, None, :]
    chosen = jnp.sum(jnp.where(one_hot, logits[:, None, :], 0.0), -1)
    raised = jnp.exp(chosen)
    gate_weights = raised / jnp.sum(raised, -1, keepdims=True)
    destination, pair_ids, filled = dispatch_table(expert_ids, experts, capacity)
    send_rows = normed_mlp[pair_ids // choices] * filled[:, None]
    received = move_rows(
        send_rows.reshape(device_count, local_experts * capacity, model_width), "dispatch"
    )
    received = received.reshape(device_count, local_experts, capacity, model_width)
    pre_gate = jnp.einsum("secd,edf->secf", received, w_gate, preferred_element_type=jnp.float32)
    pre_up = jnp.einsum("secd,edf->secf", received, w_up, preferred_element_type=jnp.float32)
    gate_sigmoid = jax.nn.sigmoid(pre_gate)
    silu_gate = pre_gate * gate_sigmoid
    activation = (silu_gate * pre_up).astype(jnp.bfloat16)
    expert_out = jnp.einsum(
        "secf,efd->secd", activation, w_down, preferred_element_type=jnp.float32
    ).astype(jnp.bfloat16)
    returned = move_rows(
        expert_out.reshape(device_count, local_experts * capacity, model_width), "combine"
    )
    picked = returned.reshape(experts * capacity, model_width)[destination].reshape(
        length, choices, model_width
    )
    block_out = residual + jnp.sum(gate_weights[:, :, None] * picked.astype(jnp.float32), 1)
    weights = (
        lax.all_gather(w_query, ("dp", "expert"), axis=0, tiled=True),
        lax.all_gather(w_key, ("dp", "expert"), axis=0, tiled=True),
        lax.all_gather(w_value, ("dp", "expert"), axis=0, tiled=True),
        lax.all_gather(w_output, ("dp", "expert"), axis=0, tiled=True),
        lax.all_gather(w_router, ("dp", "expert"), axis=0, tiled=True),
        lax.all_gather(attn_gain, ("dp", "expert"), axis=0, tiled=True),
        lax.all_gather(mlp_gain, ("dp", "expert"), axis=0, tiled=True),
        lax.all_gather(query_gain, ("dp", "expert"), axis=0, tiled=True),
        lax.all_gather(key_gain, ("dp", "expert"), axis=0, tiled=True),
    )
    full_router = weights[4]
    full_mlp_gain = weights[6]
    cotangent = out_grad.astype(jnp.float32)
    gate_grad = jnp.sum(cotangent[:, None, :] * picked.astype(jnp.float32), -1)
    down_in = (
        (gate_weights[:, :, None] * cotangent[:, None, :])
        .astype(jnp.bfloat16)
        .reshape(length * choices, model_width)
    )
    send_grad = down_in[pair_ids] * filled[:, None]
    recv_grad = move_rows(
        send_grad.reshape(device_count, local_experts * capacity, model_width), "grad_dispatch"
    )
    recv_grad = recv_grad.reshape(device_count, local_experts, capacity, model_width)
    act_grad = jnp.einsum("secd,efd->secf", recv_grad, w_down, preferred_element_type=jnp.float32)
    grad_w_down = jnp.einsum(
        "secf,secd->efd", activation, recv_grad, preferred_element_type=jnp.float32
    )
    gate_pre_grad = (
        act_grad * pre_up * gate_sigmoid * (1.0 + pre_gate * (1.0 - gate_sigmoid))
    ).astype(jnp.bfloat16)
    up_pre_grad = (act_grad * silu_gate).astype(jnp.bfloat16)
    grad_w_gate = jnp.einsum(
        "secd,secf->edf", received, gate_pre_grad, preferred_element_type=jnp.float32
    )
    grad_w_up = jnp.einsum(
        "secd,secf->edf", received, up_pre_grad, preferred_element_type=jnp.float32
    )
    row_grad = (
        jnp.einsum("secf,edf->secd", gate_pre_grad, w_gate, preferred_element_type=jnp.float32)
        + jnp.einsum("secf,edf->secd", up_pre_grad, w_up, preferred_element_type=jnp.float32)
    ).astype(jnp.bfloat16)
    row_back = move_rows(
        row_grad.reshape(device_count, local_experts * capacity, model_width), "grad_return"
    )
    row_back = row_back.reshape(experts * capacity, model_width)[destination].reshape(
        length, choices, model_width
    )
    sel_grad = gate_weights * (gate_grad - jnp.sum(gate_weights * gate_grad, -1, keepdims=True))
    logit_grad = jnp.sum(jnp.where(one_hot, sel_grad[:, :, None], 0.0), 1).astype(jnp.bfloat16)
    grad_w_router = jnp.dot(normed_mlp.T, logit_grad, preferred_element_type=jnp.float32)
    normed_mlp_grad = jnp.sum(row_back.astype(jnp.float32), 1) + jnp.dot(
        logit_grad, full_router.T, preferred_element_type=jnp.float32
    )
    grad_mlp_gain = jnp.sum(normed_mlp_grad * residual * inv_mlp, 0)
    residual_grad = cotangent + norm_grad(normed_mlp_grad, residual, inv_mlp, full_mlp_gain)
    grad_in, mixer_terms = mixer_backward(residual_grad, saved_state, weights)
    (
        grad_attn_gain,
        grad_query_gain,
        grad_key_gain,
        grad_w_query,
        grad_w_key,
        grad_w_value,
        grad_w_output,
    ) = mixer_terms
    summed = (
        lax.psum_scatter(grad_w_query, ("dp", "expert"), scatter_dimension=0, tiled=True),
        lax.psum_scatter(grad_w_key, ("dp", "expert"), scatter_dimension=0, tiled=True),
        lax.psum_scatter(grad_w_value, ("dp", "expert"), scatter_dimension=0, tiled=True),
        lax.psum_scatter(grad_w_output, ("dp", "expert"), scatter_dimension=0, tiled=True),
        lax.psum_scatter(grad_w_router, ("dp", "expert"), scatter_dimension=0, tiled=True),
        lax.psum_scatter(grad_attn_gain, ("dp", "expert"), scatter_dimension=0, tiled=True),
        lax.psum_scatter(grad_mlp_gain, ("dp", "expert"), scatter_dimension=0, tiled=True),
        lax.psum_scatter(grad_query_gain, ("dp", "expert"), scatter_dimension=0, tiled=True),
        lax.psum_scatter(grad_key_gain, ("dp", "expert"), scatter_dimension=0, tiled=True),
    )
    (
        share_w_query,
        share_w_key,
        share_w_value,
        share_w_output,
        share_w_router,
        share_attn_gain,
        share_mlp_gain,
        share_query_gain,
        share_key_gain,
    ) = summed
    return (
        block_out,
        grad_in,
        share_attn_gain,
        share_query_gain,
        share_key_gain,
        share_w_query,
        share_w_key,
        share_w_value,
        share_w_output,
        share_mlp_gain,
        share_w_router,
        grad_w_gate,
        grad_w_up,
        grad_w_down,
    )


def place():
    z = lax.axis_index("dp")
    e = lax.axis_index("expert")
    return z, e


def line_order(z, nz, j, inner=False):
    near = jnp.minimum(z, nz - 1 - z)
    step = (j + 1) // 2
    step = step if j % 2 == 0 else -step
    if inner:
        step = jnp.where(z < nz - 1 - z, -step, step)
    tail = jnp.where(z < nz - 1 - z, j, nz - 1 - j)
    return jnp.where(j <= 2 * near, z + step, tail)


def greet(z, e, nz):
    barrier = pltpu.get_barrier_semaphore()
    for mate in (e ^ 1, e ^ 2, e ^ 4):
        pl.semaphore_signal(barrier, inc=1, device_id=(z, mate), device_id_type=MESH)

    @pl.when(z > 0)
    def _():
        pl.semaphore_signal(barrier, inc=1, device_id=(z - 1, e), device_id_type=MESH)

    @pl.when(z < nz - 1)
    def _():
        pl.semaphore_signal(barrier, inc=1, device_id=(z + 1, e), device_id_type=MESH)

    ends = (z > 0).astype(jnp.int32) + (z < nz - 1).astype(jnp.int32)
    pl.semaphore_wait(barrier, 3 + ends)


class Gather:
    Z, ZX, ZY, X3, X2, XQ, Y3, Y2, YQ, P0, PX3, PXQ, PY3, PYQ, PDX, PDY = range(16)
    KINDS = 16
    WHOLE, LOW, HIGH, LOW3, HIGH3, Q0, Q3 = (0, 4), (0, 2), (2, 2), (0, 3), (1, 3), (0, 1), (3, 1)

    def __init__(self, nz, shards, outs, send, recv, local):
        self.nz, self.shards, self.outs = nz, shards, outs
        self.send, self.recv, self.local = send, recv, local
        self.z, self.e = place()
        self.p, self.x, self.y, self.d = self.e ^ 1, self.e ^ 2, self.e ^ 4, self.e ^ 6

    def zz(self, j):
        return line_order(self.z, self.nz, j)

    def part(self, ref, piece):
        return ref.at[pl.ds(piece[0], piece[1])]

    def copy(self, i, kind, zz, ee, piece, dev, mine=False, sem=None):
        dst = self.part(self.outs[i].at[zz, ee], piece)
        return pltpu.make_async_remote_copy(
            src_ref=self.part(self.shards[i], piece) if mine else dst,
            dst_ref=dst,
            send_sem=self.send.at[i, zz, kind] if sem is None else sem,
            recv_sem=self.recv.at[i, zz, kind],
            device_id=dev,
            device_id_type=MESH,
        )

    def start(self, kind, zz, ee, piece, dev, mine=False):
        for i in range(len(self.outs)):
            self.copy(i, kind, zz, ee, piece, dev, mine).start()

    def arrived(self, kind, zz, ee, piece):
        for i in range(len(self.outs)):
            self.copy(i, kind, zz, ee, piece, (self.z, self.e)).wait_recv()

    def sent(self, kind, zz, ee, piece, mine=False):
        for i in range(len(self.outs)):
            self.copy(i, kind, zz, ee, piece, (self.z, self.e), mine).wait_send()

    def along(self, j, kind, ee, piece, act):
        z, e, nz = self.z, self.e, self.nz
        zz, mine = self.zz(j), j == 0 and kind == self.Z
        for i in range(len(self.outs)):
            @pl.when(jnp.logical_and(zz <= z, z < nz - 1))
            def _():
                act(self.copy(i, kind, zz, ee, piece, (z + 1, e), mine))

            @pl.when(jnp.logical_and(zz >= z, z > 0))
            def _():
                sem = self.local.at[1 + kind, i] if j == 0 else None
                act(self.copy(i, kind, zz, ee, piece, (z - 1, e), mine, sem))

    def keep(self, i):
        return pltpu.make_async_copy(self.shards[i], self.outs[i].at[self.z, self.e], self.local.at[0, i])

    def kept(self):
        for i in range(len(self.outs)):
            self.keep(i).wait()

    def launch(self, j):
        self.launch_line(j)
        self.launch_plane(j)

    def launch_line(self, j):
        e, zz, mine = self.e, self.zz(j), j == 0
        if not mine:
            self.arrived(self.Z, zz, e, self.WHOLE)
        else:
            self.start(self.XQ, zz, e, self.Q3, (self.z, self.x), mine)
            self.start(self.YQ, zz, e, self.Q0, (self.z, self.y), mine)
        self.along(j, self.Z, e, self.WHOLE, lambda c: c.start())

    def launch_plane(self, j):
        z, e, zz, mine = self.z, self.e, self.zz(j), j == 0
        self.start(self.X3, zz, e, self.LOW3, (z, self.x), mine)
        self.start(self.Y3, zz, e, self.HIGH3, (z, self.y), mine)
        self.start(self.P0, zz, e, self.WHOLE, (z, self.p), mine)
        if mine:
            for i in range(len(self.outs)):
                self.keep(i).start()

    def mates(self, j):
        zz, mine = self.zz(j), j == 0
        self.arrived(self.XQ if mine else self.ZX, zz, self.x, self.Q3)
        self.along(j, self.ZX, self.x, self.Q3, lambda c: c.start())
        self.start(self.PXQ, zz, self.x, self.Q3, (self.z, self.p))
        self.arrived(self.YQ if mine else self.ZY, zz, self.y, self.Q0)
        self.along(j, self.ZY, self.y, self.Q0, lambda c: c.start())
        self.start(self.PYQ, zz, self.y, self.Q0, (self.z, self.p))

    def relay(self, j):
        zz = self.zz(j)
        self.arrived(self.X3, zz, self.x, self.LOW3)
        self.start(self.Y2, zz, self.x, self.HIGH, (self.z, self.y))
        self.start(self.PX3, zz, self.x, self.LOW3, (self.z, self.p))
        self.arrived(self.Y3, zz, self.y, self.HIGH3)
        self.start(self.X2, zz, self.y, self.LOW, (self.z, self.x))
        self.start(self.PY3, zz, self.y, self.HIGH3, (self.z, self.p))

    def finish(self, j):
        zz = self.zz(j)
        self.arrived(self.X2, zz, self.d, self.LOW)
        self.start(self.PDX, zz, self.d, self.LOW, (self.z, self.p))
        self.arrived(self.Y2, zz, self.d, self.HIGH)
        self.start(self.PDY, zz, self.d, self.HIGH, (self.z, self.p))

    def shared_near(self, j):
        zz, p = self.zz(j), self.p
        self.arrived(self.P0, zz, p, self.WHOLE)
        self.arrived(self.PXQ, zz, p ^ 2, self.Q3)
        self.arrived(self.PX3, zz, p ^ 2, self.LOW3)

    def shared_far(self, j):
        zz, p = self.zz(j), self.p
        self.arrived(self.PYQ, zz, p ^ 4, self.Q0)
        self.arrived(self.PY3, zz, p ^ 4, self.HIGH3)
        self.arrived(self.PDX, zz, p ^ 6, self.LOW)
        self.arrived(self.PDY, zz, p ^ 6, self.HIGH)

    def drain(self, j, kept=False):
        zz, e, mine = self.zz(j), self.e, j == 0
        if mine:
            self.sent(self.XQ, zz, e, self.Q3, mine)
            self.sent(self.YQ, zz, e, self.Q0, mine)
            if not kept:
                self.kept()
        for kind, ee, piece in ((self.Z, e, self.WHOLE), (self.ZX, self.x, self.Q3), (self.ZY, self.y, self.Q0)):
            self.along(j, kind, ee, piece, lambda c: c.wait_send())
        self.sent(self.X3, zz, e, self.LOW3, mine)
        self.sent(self.Y3, zz, e, self.HIGH3, mine)
        self.sent(self.P0, zz, e, self.WHOLE, mine)
        self.sent(self.PXQ, zz, self.x, self.Q3)
        self.sent(self.PYQ, zz, self.y, self.Q0)
        self.sent(self.Y2, zz, self.x, self.HIGH)
        self.sent(self.X2, zz, self.y, self.LOW)
        self.sent(self.PX3, zz, self.x, self.LOW3)
        self.sent(self.PY3, zz, self.y, self.HIGH3)
        self.sent(self.PDX, zz, self.d, self.LOW)
        self.sent(self.PDY, zz, self.d, self.HIGH)

    def steps(self):
        n = self.nz
        todo = [(self.launch, 0), (self.mates, 0)]
        for j in range(1, n + 2):
            todo += [(self.launch, j), (self.mates, j - 1) if j > 1 else None, (self.relay, j - 1), (self.finish, j - 2)]
        return [functools.partial(f, j) for f, j in filter(None, todo) if 0 <= j < n]


def gather_kernel(nz, count, *refs):
    shards, outs = refs[:count], refs[count : 2 * count]
    send, recv, local = refs[2 * count :]
    z, e = place()
    greet(z, e, nz)
    g = Gather(nz, shards, outs, send, recv, local)
    for step in g.steps():
        step()
    for j in range(nz):
        g.shared_near(j)
        g.shared_far(j)
    for j in range(nz):
        g.drain(j)


def gather_scratch(nz, count):
    return [
        pltpu.SemaphoreType.DMA((count, nz, Gather.KINDS)),
        pltpu.SemaphoreType.DMA((count, nz, Gather.KINDS)),
        pltpu.SemaphoreType.DMA((4, count)),
    ]


def gather_all(arrays, collective_id):
    nz, width = lax.axis_size("dp"), lax.axis_size("expert")
    count = len(arrays)
    parts = [a.reshape((4, a.shape[0] // 4) + a.shape[1:]) for a in arrays]
    outs = pl.pallas_call(
        functools.partial(gather_kernel, nz, count),
        out_shape=[jax.ShapeDtypeStruct((nz, width) + h.shape, h.dtype) for h in parts],
        in_specs=[pl.BlockSpec(memory_space=pltpu.VMEM)] * count,
        out_specs=[pl.BlockSpec(memory_space=pl.ANY)] * count,
        scratch_shapes=gather_scratch(nz, count),
        compiler_params=pltpu.CompilerParams(
            collective_id=collective_id, has_side_effects=True, vmem_limit_bytes=VMEM_LIMIT
        ),
        name="gather_all",
    )(*parts)
    return [o.reshape((nz * width * a.shape[0],) + a.shape[1:]) for o, a in zip(outs, arrays)]


def accumulate(dst, src):
    rows = dst.shape[0]
    block = 32 if rows % 32 == 0 else rows
    if rows == block:
        dst[...] = dst[...] + src[...]
        return

    def body(r, _):
        at = pl.ds(pl.multiple_of(r * block, block), block)
        dst[at, :] = dst[at, :] + src[at, :]
        return 0

    lax.fori_loop(0, rows // block, body, 0)


class Scatter:
    X2, Y2, X3, Y3, Z, ZB, ZX, ZXB, ZY, ZYB, XQ, YQ = range(4, 16)
    KINDS = 16
    BUFFERS = 9

    def __init__(self, nz, terms, outs, sums, temps, from_x2, from_y2, from_x3, from_y3, from_z, from_zm, from_q, send, recv, local):
        self.nz, self.terms, self.outs = nz, terms, outs
        self.sums, self.temps = sums, temps
        self.from_x2, self.from_y2, self.from_x3, self.from_y3 = from_x2, from_y2, from_x3, from_y3
        self.from_z, self.from_zm, self.from_q = from_z, from_zm, from_q
        self.send, self.recv, self.local = send, recv, local
        self.count = len(terms)
        self.z, self.e = place()
        self.core, self.chip = self.e % 2, self.e // 2
        self.p, self.x, self.y = self.e ^ 1, self.e ^ 2, self.e ^ 4
        self.chips = (self.chip ^ 3, self.chip ^ 1, self.chip ^ 2, self.chip)

    def zz(self, j):
        return line_order(self.z, self.nz, self.nz - 1 - j, True)

    def remote(self, i, kind, zz, src, dst, dev):
        return pltpu.make_async_remote_copy(
            src_ref=src, dst_ref=dst, send_sem=self.send.at[i, zz, kind], recv_sem=self.recv.at[i, zz, kind],
            device_id=dev, device_id_type=MESH)

    def quarters(self, i, zz, q, first, n):
        return self.sums[i].at[zz, q, pl.ds(first, n)]

    def pair(self, i, j, q):
        zz, chip = self.zz(j), self.chips[q]
        return self.remote(i, q, zz, self.terms[i].at[zz, chip * 2 + (1 - self.core)], self.sums[i].at[zz, q],
                           (self.z, self.p))

    def load(self, i, j, q):
        slot = q % 2
        return pltpu.make_async_copy(
            self.terms[i].at[self.zz(j), self.chips[q] * 2 + self.core], self.temps[i].at[slot], self.local.at[i, slot])

    def x2(self, i, zz):
        return self.remote(i, self.X2, zz, self.quarters(i, zz, 0, 0, 2), self.from_x2[i].at[zz], (self.z, self.x))

    def y2(self, i, zz):
        return self.remote(i, self.Y2, zz, self.quarters(i, zz, 0, 2, 2), self.from_y2[i].at[zz], (self.z, self.y))

    def x3(self, i, zz):
        return self.remote(i, self.X3, zz, self.quarters(i, zz, 1, 0, 3), self.from_x3[i].at[zz], (self.z, self.x))

    def y3(self, i, zz):
        return self.remote(i, self.Y3, zz, self.quarters(i, zz, 2, 1, 3), self.from_y3[i].at[zz], (self.z, self.y))

    def xq(self, i):
        return self.remote(i, self.XQ, self.z, self.quarters(i, self.z, 1, 3, 1), self.from_q[i].at[pl.ds(0, 1)], (self.z, self.x))

    def yq(self, i):
        return self.remote(i, self.YQ, self.z, self.quarters(i, self.z, 2, 0, 1), self.from_q[i].at[pl.ds(1, 1)], (self.z, self.y))

    def line(self, i, zz, which, dz, last=False):
        slot = self.nz if last else zz
        kind = (self.Z, self.ZX, self.ZY)[which] + int(last)
        src = (self.sums[i].at[zz, 3], self.quarters(i, zz, 1, 3, 1), self.quarters(i, zz, 2, 0, 1))[which]
        dst = self.from_z[i].at[slot] if which == 0 else self.from_zm[i].at[slot, pl.ds(which - 1, 1)]
        return self.remote(i, kind, zz, src, dst, (self.z + dz, self.e))

    def add(self, i, zz, q, first, n, src):
        for k in range(n):
            accumulate(self.sums[i].at[zz, q, first + k], src.at[k])

    def begin(self):
        for j in range(self.nz):
            for q in range(4):
                for i in range(self.count):
                    self.pair(i, j, q).start()
        for i in range(self.count):
            self.load(i, 0, 0).start()

    def first(self, j):
        zz = self.zz(j)
        for q in range(4):
            for i in range(self.count):
                if q < 3:
                    self.load(i, j, q + 1).start()
                elif j < self.nz - 1:
                    self.load(i, j + 1, 0).start()
                self.pair(i, j, q).wait_recv()
                self.load(i, j, q).wait()
                self.add(i, zz, q, 0, 4, self.temps[i].at[q % 2])
                if q == 0:
                    self.x2(i, zz).start()
                    self.y2(i, zz).start()

    def second(self, j):
        zz = self.zz(j)
        for i in range(self.count):
            self.y2(i, zz).wait_recv()
            self.add(i, zz, 1, 2, 2, self.from_y2[i].at[zz])
            self.x3(i, zz).start()
            self.x2(i, zz).wait_recv()
            self.add(i, zz, 2, 0, 2, self.from_x2[i].at[zz])
            self.y3(i, zz).start()
            for which in (1, 2):
                self.flow(i, j, which)

    def flow(self, i, j, which):
        z, nz, zz = self.z, self.nz, self.zz(j)
        q, first, n = ((3, 0, 4), (1, 3, 1), (2, 0, 1))[which]

        def came(slot):
            ref = self.from_z[i].at[slot] if which == 0 else self.from_zm[i].at[slot, pl.ds(which - 1, 1)]
            self.add(i, zz, q, first, n, ref)

        if j < nz - 1:
            @pl.when(jnp.logical_or(jnp.logical_and(zz > z, z > 0), jnp.logical_and(zz < z, z < nz - 1)))
            def _():
                self.line(i, zz, which, 1).wait_recv()
                came(zz)

            @pl.when(zz > z)
            def _():
                self.line(i, zz, which, 1).start()

            @pl.when(zz < z - 1)
            def _():
                self.line(i, zz, which, -1).start()

            @pl.when(zz == z - 1)
            def _():
                self.line(i, zz, which, -1, True).start()
        else:
            @pl.when(z > 0)
            def _():
                self.line(i, zz, which, 1).wait_recv()
                came(zz)

            @pl.when(z < nz - 1)
            def _():
                self.line(i, zz, which, -1, True).wait_recv()
                came(nz)

            if which == 1:
                self.xq(i).start()
            if which == 2:
                self.yq(i).start()

    def third(self, j):
        zz = self.zz(j)
        for i in range(self.count):
            self.x3(i, zz).wait_recv()
            self.add(i, zz, 3, 0, 3, self.from_x3[i].at[zz])
            self.y3(i, zz).wait_recv()
            self.add(i, zz, 3, 1, 3, self.from_y3[i].at[zz])
            self.flow(i, j, 0)

    def result(self):
        for i in range(self.count):
            self.xq(i).wait_recv()
            self.add(i, self.z, 3, 3, 1, self.from_q[i].at[pl.ds(0, 1)])
            self.yq(i).wait_recv()
            self.add(i, self.z, 3, 0, 1, self.from_q[i].at[pl.ds(1, 1)])
            self.outs[i][...] = self.sums[i][self.z, 3].astype(self.outs[i].dtype)

    def drain(self, j):
        z, nz = self.z, self.nz
        zz = self.zz(j)
        for i in range(self.count):
            for q in range(4):
                self.pair(i, j, q).wait_send()
            for c in (self.x2, self.y2, self.x3, self.y3):
                c(i, zz).wait_send()
            if j < nz - 1:
                for which in range(3):
                    @pl.when(zz > z)
                    def _():
                        self.line(i, zz, which, 1).wait_send()

                    @pl.when(zz < z - 1)
                    def _():
                        self.line(i, zz, which, -1).wait_send()

                    @pl.when(zz == z - 1)
                    def _():
                        self.line(i, zz, which, -1, True).wait_send()
            else:
                self.xq(i).wait_send()
                self.yq(i).wait_send()

    def steps(self):
        todo = []
        for j in range(self.nz + 2):
            todo += [(self.first, j), (self.second, j - 1), (self.third, j - 2)]
        return [functools.partial(f, j) for f, j in todo if 0 <= j < self.nz] + [self.result]


def scatter_kernel(nz, count, *refs):
    groups = [refs[k * count : (k + 1) * count] for k in range(2 + Scatter.BUFFERS)]
    send, recv, local = refs[(2 + Scatter.BUFFERS) * count :]
    z, e = place()
    greet(z, e, nz)
    s = Scatter(nz, *groups, send, recv, local)
    s.begin()
    for step in s.steps():
        step()
    for j in range(nz):
        s.drain(j)


def scatter_buffers(nz, width, kinds):
    leads = ((nz, width // 2, 4), (2, 4), (nz, 2), (nz, 2), (nz, 3), (nz, 3), (nz + 1, 4), (nz + 1, 2), (2,))
    return [pltpu.VMEM(lead + shape, dtype) for lead in leads for shape, dtype in kinds] + [
        pltpu.SemaphoreType.DMA((len(kinds), nz, Scatter.KINDS)),
        pltpu.SemaphoreType.DMA((len(kinds), nz, Scatter.KINDS)),
        pltpu.SemaphoreType.DMA((len(kinds), 2)),
    ]


def scatter_sum(arrays, collective_id):
    nz, width = lax.axis_size("dp"), lax.axis_size("expert")
    count = len(arrays)
    devices = nz * width
    terms = [a.reshape(nz, width, 4, a.shape[0] // (4 * devices), a.shape[1]) for a in arrays]
    shapes = [t.shape[3:] for t in terms]
    outs = pl.pallas_call(
        functools.partial(scatter_kernel, nz, count),
        out_shape=[jax.ShapeDtypeStruct((4,) + s, jnp.float32) for s in shapes],
        in_specs=[pl.BlockSpec(memory_space=pl.ANY)] * count,
        out_specs=[pl.BlockSpec(memory_space=pltpu.VMEM)] * count,
        scratch_shapes=scatter_buffers(nz, width, [(s, a.dtype) for s, a in zip(shapes, arrays)]),
        compiler_params=pltpu.CompilerParams(
            collective_id=collective_id, has_side_effects=True, vmem_limit_bytes=VMEM_LIMIT
        ),
        name="scatter_sum",
    )(*terms)
    return [o.reshape(4 * s[0], s[1]) for o, s in zip(outs, shapes)]


def mm(a, b, da=1, db=0):
    return lax.dot_general(a, b, (((da,), (db,)), ((), ())), preferred_element_type=F32)


def rope(values, cosine, sine):
    return values * cosine + pltpu.roll(values, values.shape[1] // 2, 1) * sine


class AttentionGrad:
    def __init__(self, branch, w_out, raw, tables, gains, seg_col, seg_row, normed, attended, w_mixed,
                 grads, gain_grads, normed_grad, grad_out, grad_mixed,
                 w_buf, q_buf, k_buf, v_buf, mask, k_rot, v_low, dk, dv, a_buf, m_buf, out_stage, mixed_stage, sems):
        self.normed, self.attended, self.w_mixed = normed, attended, w_mixed
        self.normed_grad, self.grad_out, self.grad_mixed = normed_grad, grad_out, grad_mixed
        self.a_buf, self.m_buf, self.out_stage, self.mixed_stage = a_buf, m_buf, out_stage, mixed_stage
        self.branch, self.w_out, self.raw, self.tables, self.gains = branch, w_out, raw, tables, gains
        self.seg_col, self.seg_row, self.grads, self.gain_grads = seg_col, seg_row, grads, gain_grads
        self.w_buf, self.q_buf, self.k_buf, self.v_buf, self.mask = w_buf, q_buf, k_buf, v_buf, mask
        self.k_rot, self.v_low, self.dk, self.dv, self.sems = k_rot, v_low, dk, dv, sems
        self.cols = w_buf.shape[0]
        self.query_cols = w_out.shape[0]
        self.key_cols = k_buf.shape[1]
        self.count = self.query_cols // self.cols
        self.per_key = self.count // (self.key_cols // HEAD_DIM)
        self.total = self.count + 2 * self.key_cols // self.cols

    def at(self, t):
        return pl.ds(pl.multiple_of(t * self.cols, self.cols), self.cols)

    def fetch(self, t, slot):
        at = self.at(t)
        return pltpu.make_async_copy(self.raw.at[:, at], self.q_buf.at[slot], self.sems.at[1, slot])

    def fetch_out(self, t):
        at = self.at(t)
        return (
            pltpu.make_async_copy(self.w_out.at[at, :], self.w_buf, self.sems.at[0, 0]),
            pltpu.make_async_copy(self.attended.at[:, at], self.a_buf, self.sems.at[3, 0]),
        )

    def fetch_mixed(self, t):
        return pltpu.make_async_copy(self.w_mixed.at[:, self.at(t)], self.m_buf, self.sems.at[4, 0])

    def put_out(self, t):
        return pltpu.make_async_copy(self.out_stage, self.grad_out.at[self.at(t), :], self.sems.at[5, 0])

    def put_mixed(self, t):
        return pltpu.make_async_copy(self.mixed_stage, self.grad_mixed.at[:, self.at(t)], self.sems.at[5, 1])

    def prepare(self):
        q, k = self.query_cols, self.key_cols
        key = pltpu.make_async_copy(self.raw.at[:, pl.ds(q, k)], self.k_buf, self.sems.at[2, 0])
        value = pltpu.make_async_copy(self.raw.at[:, pl.ds(q + k, k)], self.v_buf, self.sems.at[2, 1])
        key.start()
        value.start()
        for c in self.fetch_out(0):
            c.start()
        self.fetch(0, 0).start()
        self.fetch_mixed(0).start()
        self.normed_grad[...] = jnp.zeros_like(self.normed_grad)
        self.mask[...] = allowed_mask(self.seg_col, self.seg_row)
        self.gain_grads[...] = jnp.zeros_like(self.gain_grads)
        key.wait()
        value.wait()

    def scaled(self, raw, which):
        scale = lax.rsqrt(jnp.mean(raw * raw, 1, keepdims=True) + EPS)
        return scale, (raw * scale) * self.gains[which : which + 1, :]

    def back(self, rot_grad, raw, scale, which):
        cosine, sine = self.tables[0], self.tables[1]
        grad = rope(rot_grad, cosine, -sine)
        part = jnp.sum(grad * raw * scale, 0, keepdims=True)
        self.gain_grads[which : which + 1, :] = self.gain_grads[which : which + 1, :] + part
        weighted = grad * self.gains[which : which + 1, :]
        mean = jnp.mean(weighted * raw, 1, keepdims=True)
        return scale * weighted - raw * (scale * scale * scale) * mean

    def step(self, t):
        slot = lax.rem(t, 2)

        @pl.when(t + 1 < self.count)
        def _():
            self.fetch(t + 1, 1 - slot).start()

        @pl.when(t < self.count)
        def _():
            self.heads(t, slot)

        self.fetch_mixed(t).wait()
        grads = self.grads[:, self.at(t)]
        self.normed_grad[...] += mm(grads, self.m_buf[...], 1, 1)

        @pl.when(t + 1 < self.total)
        def _():
            self.fetch_mixed(t + 1).start()

        @pl.when(t > 0)
        def _():
            self.put_mixed(t - 1).wait()

        self.mixed_stage[...] = mm(self.normed[...], grads, 0, 0).astype(BF16)
        self.put_mixed(t).start()

    def end(self):
        self.put_mixed(self.total - 1).wait()
        self.put_out(self.count - 1).wait()

    def heads(self, t, slot):
        self.fetch(t, slot).wait()
        for c in self.fetch_out(t):
            c.wait()

        @pl.when(t > 0)
        def _():
            self.put_out(t - 1).wait()

        self.out_stage[...] = mm(self.a_buf[...], self.branch[...], 0, 0).astype(BF16)
        self.put_out(t).start()
        cosine, sine = self.tables[0], self.tables[1]
        at_key = pl.ds(pl.multiple_of(t // self.per_key * HEAD_DIM, HEAD_DIM), HEAD_DIM)

        @pl.when(lax.rem(t, self.per_key) == 0)
        def _():
            _, key = self.scaled(self.k_buf[:, at_key], 1)
            self.k_rot[...] = rope(key, cosine, sine).astype(BF16)
            self.v_low[...] = self.v_buf[:, at_key].astype(BF16)
            self.dk[...] = jnp.zeros_like(self.dk)
            self.dv[...] = jnp.zeros_like(self.dv)

        score_scale = 1.0 / math.sqrt(HEAD_DIM)
        out_grad = mm(self.branch[...], self.w_buf[...], 1, 1).astype(BF16)

        @pl.when(t + 1 < self.count)
        def _():
            for c in self.fetch_out(t + 1):
                c.start()

        mask = self.mask[...] > 0.0
        k_rot, v_low = self.k_rot[...], self.v_low[...]
        for h in range(self.cols // HEAD_DIM):
            here = slice(h * HEAD_DIM, (h + 1) * HEAD_DIM)
            raw = self.q_buf[slot, :, here]
            scale, query = self.scaled(raw, 0)
            q_rot = rope(query, cosine, sine).astype(BF16)
            d_out = out_grad[:, here]
            scores = mm(q_rot, k_rot, 1, 1) * score_scale
            raised = jnp.where(mask, jnp.exp(scores), 0.0)
            probs = raised / jnp.sum(raised, 1, keepdims=True)
            self.dv[...] += mm(probs.astype(BF16), d_out, 0, 0)
            d_probs = mm(d_out, v_low, 1, 1)
            d_scores = (probs * (d_probs - jnp.sum(probs * d_probs, 1, keepdims=True))).astype(BF16)
            dq = mm(d_scores, k_rot) * score_scale
            self.dk[...] += mm(d_scores, q_rot, 0, 0)
            at = pl.ds(pl.multiple_of(t * self.cols + h * HEAD_DIM, HEAD_DIM), HEAD_DIM)
            self.grads[:, at] = self.back(dq, raw, scale, 0).astype(BF16)

        @pl.when(lax.rem(t, self.per_key) == self.per_key - 1)
        def _():
            raw = self.k_buf[:, at_key]
            scale, _ = self.scaled(raw, 1)
            shift = pl.multiple_of(t // self.per_key * HEAD_DIM, HEAD_DIM)
            self.grads[:, pl.ds(self.query_cols + shift, HEAD_DIM)] = self.back(
                self.dk[...] * score_scale, raw, scale, 1
            ).astype(BF16)
            self.grads[:, pl.ds(self.query_cols + self.key_cols + shift, HEAD_DIM)] = self.dv[...].astype(BF16)


def scatter_attention_kernel(nz, plan, term, *refs):
    inputs, (total, *outs), scratch = refs[:10], refs[10:16], refs[16:]
    buffers, rest = scratch[: Scatter.BUFFERS], scratch[Scatter.BUFFERS :]
    send, recv, local = rest[:3]
    z, e = place()
    greet(z, e, nz)
    s = Scatter(nz, [term], [total], *[[b] for b in buffers], send, recv, local)
    a = AttentionGrad(*inputs, *outs, *rest[3:])
    s.begin()
    a.prepare()
    steps = s.steps()
    run_beside(a.total, a.step, steps, plan)
    a.end()
    for j in range(nz):
        s.drain(j)


def run_beside(count, work, steps, plan):
    bounds = [sum(plan[:t]) for t in range(len(plan) + 1)]

    def body(t, _):
        for k in range(count):
            todo = steps[bounds[k] : bounds[k + 1]]
            if todo:
                @pl.when(t == k)
                def _():
                    for step in todo:
                        step()
        work(t)
        return 0

    lax.fori_loop(0, count, body, 0)
    for step in steps[bounds[count] :]:
        step()


def scatter_with_attention(terms, branch, w_out, raw, tables, gains, segments, normed, attended, w_mixed, collective_id):
    nz, width = lax.axis_size("dp"), lax.axis_size("expert")
    devices = nz * width
    length, model = branch.shape
    shape = (terms.shape[0] // (4 * devices), terms.shape[1])
    term = terms.reshape((nz, width, 4) + shape)
    heads = 4
    cols = heads * HEAD_DIM
    key_cols = (raw.shape[1] - w_out.shape[0]) // 2
    vmem = pl.BlockSpec(memory_space=pltpu.VMEM)
    hbm = pl.BlockSpec(memory_space=pl.ANY)
    plan = [3, 1, 1, 1, 1, 1, 1, 1, 1, 0]
    total, grads, gain_grads, normed_grad, grad_out, grad_mixed = pl.pallas_call(
        functools.partial(scatter_attention_kernel, nz, plan),
        out_shape=[
            jax.ShapeDtypeStruct((4,) + shape, F32),
            jax.ShapeDtypeStruct(raw.shape, BF16),
            jax.ShapeDtypeStruct((2, HEAD_DIM), F32),
            jax.ShapeDtypeStruct((length, model), F32),
            jax.ShapeDtypeStruct(w_out.shape, BF16),
            jax.ShapeDtypeStruct(w_mixed.shape, BF16),
        ],
        in_specs=[hbm, vmem, hbm, hbm, vmem, vmem, vmem, vmem, vmem, hbm, hbm],
        out_specs=[vmem, vmem, vmem, vmem, hbm, hbm],
        scratch_shapes=scatter_buffers(nz, width, [(shape, terms.dtype)])
        + [
            pltpu.VMEM((cols, model), BF16),
            pltpu.VMEM((2, length, cols), F32),
            pltpu.VMEM((length, key_cols), F32),
            pltpu.VMEM((length, key_cols), F32),
            pltpu.VMEM((length, length), F32),
            pltpu.VMEM((length, HEAD_DIM), BF16),
            pltpu.VMEM((length, HEAD_DIM), BF16),
            pltpu.VMEM((length, HEAD_DIM), F32),
            pltpu.VMEM((length, HEAD_DIM), F32),
            pltpu.VMEM((length, cols), BF16),
            pltpu.VMEM((model, cols), BF16),
            pltpu.VMEM((cols, model), BF16),
            pltpu.VMEM((model, cols), BF16),
            pltpu.SemaphoreType.DMA((6, 2)),
        ],
        compiler_params=pltpu.CompilerParams(
            collective_id=collective_id, has_side_effects=True, vmem_limit_bytes=VMEM_LIMIT
        ),
        name="scatter_attention",
    )(term, branch, w_out, raw, tables, gains, segments[:, None], segments[None, :], normed, attended, w_mixed)
    return total.reshape(4 * shape[0], shape[1]), gain_grads, normed_grad, grad_out, grad_mixed


TILE = 512


class ExpertWork:
    def __init__(self, nz, cap, group, orders, all_rows, all_tables, all_grads, weights, outs, bufs, sems):
        self.nz, self.cap, self.group = nz, cap, group
        self.all_rows, self.all_tables, self.all_grads = all_rows, all_tables, all_grads
        self.weights, self.outs, self.bufs, self.sems = weights, outs, bufs, sems
        self.z, self.e = place()
        self.width = all_rows.shape[1]
        self.orders = orders
        self.edge = jnp.logical_or(self.z == 0, self.z == nz - 1)

    def weight_copies(self):
        return [pltpu.make_async_copy(w, b, self.sems.at[0, i]) for i, (w, b) in enumerate(zip(self.weights, self.bufs[:3]))]

    def place_of(self, t):
        zz, half = jnp.int32(0), jnp.int32(0)
        for p, (ends, middle) in enumerate(zip(*self.orders)):
            for here, (j, h) in ((self.edge, ends), (jnp.logical_not(self.edge), middle)):
                here = jnp.logical_and(here, t == p)
                zz = jnp.where(here, line_order(self.z, self.nz, j), zz)
                half = jnp.where(here, h, half)
        near = self.e // self.group
        return zz, jnp.where(half == 0, near, 1 - near) * self.group

    def inputs(self, t, slot):
        zz, first = self.place_of(t)
        at = pl.ds(first, self.group)
        x, tab, g = self.bufs[3:6]
        return (
            pltpu.make_async_copy(self.all_rows.at[zz, at], x.at[slot], self.sems.at[1 + slot, 0]),
            pltpu.make_async_copy(self.all_tables.at[zz, at], tab.at[slot], self.sems.at[1 + slot, 1]),
            pltpu.make_async_copy(self.all_grads.at[zz, at], g.at[slot], self.sems.at[1 + slot, 2]),
        )

    def flat(self, t):
        step = self.group * self.cap
        return pl.ds(pl.multiple_of(t * step, step), step)

    def row_results(self, t):
        pairs = zip(self.bufs[8:10], self.outs[3:5])
        return [pltpu.make_async_copy(b, o.at[self.flat(t)], self.sems.at[3, i]) for i, (b, o) in enumerate(pairs)]

    def hidden_results(self, t):
        pairs = zip(self.bufs[10:13], self.outs[5:8])
        return [pltpu.make_async_copy(b, o.at[self.flat(t)], self.sems.at[3, 2 + i]) for i, (b, o) in enumerate(pairs)]

    def term_results(self, t, n, cols):
        zz, first = self.place_of(t)
        at = pl.ds(first, self.group)
        pairs = zip(self.bufs[6:8], self.outs[:2])
        return [
            pltpu.make_async_copy(b.at[:, :, cols], o.at[zz, at, :, cols], self.sems.at[4 + i, n])
            for i, (b, o) in enumerate(pairs)
        ]

    def begin(self):
        for c in self.weight_copies():
            c.start()

    def ready(self, p):
        for c in self.inputs(jnp.int32(p), p % 2):
            c.start()

    def step(self, t, hook):
        slot = lax.rem(t, 2)
        hook(0)
        cap, group = self.cap, self.group
        wg, wu, wd, xb, tb, gb, yb, rb, rowb, downb, actb, gpb, upb, cotb = self.bufs
        for c in self.inputs(t, slot):
            c.wait()

        @pl.when(t == 0)
        def _():
            for c in self.weight_copies():
                c.wait()

        self.free(t, self.row_results)
        length, width = xb.shape[2] * xb.shape[3], xb.shape[4]
        lanes = tb.shape[4]
        me = self.z * self.width + self.e
        total = self.nz * self.width
        lane = lax.broadcasted_iota(jnp.int32, (8, lanes), 1)
        row = lax.broadcasted_iota(jnp.int32, (8, lanes), 0)
        gate_lanes = jnp.logical_and(row == 0, jnp.logical_or(lane == me, lane == total + me))
        rank_lane = jnp.logical_and(row == 1, lane == 2 * total + me)
        select = jnp.where(jnp.logical_or(gate_lanes, rank_lane), 1.0, 0.0).astype(BF16)
        slots = lax.broadcasted_iota(jnp.int32, (cap, length), 0).astype(F32)
        picks, gates = [], []
        for s in range(group):
            info = mm(select, tb[slot, s].reshape(length, lanes), 1, 1)
            hit = slots == info[1:2]
            pick = hit.astype(BF16)
            picks.append(pick)
            gate = jnp.sum(jnp.where(hit, info[0:1], 0.0), 1, keepdims=True)
            gates.append(gate)
            at = pl.ds(s * cap, cap)
            rowb[at, :] = mm(pick, xb[slot, s].reshape(length, width)).astype(BF16)
            cot = mm(pick, gb[slot, s].reshape(length, width))
            cotb[at, :] = cot.astype(BF16)
            downb[at, :] = (gate * cot).astype(BF16)
        for c in self.row_results(t):
            c.start()
        hook(1)
        gate_all = jnp.concatenate(gates, 0)
        rows = rowb[...]
        pre_gate = mm(rows, wg[...])
        pre_up = mm(rows, wu[...])
        sig = jax.nn.sigmoid(pre_gate)
        silu = pre_gate * sig
        self.free(t, self.hidden_results)
        actb[...] = (silu * pre_up).astype(BF16)
        hook(2)
        act_grad = mm(downb[...], wd[...], 1, 1)
        gpb[...] = (act_grad * pre_up * sig * (1.0 + pre_gate * (1.0 - sig))).astype(BF16)
        upb[...] = (act_grad * silu).astype(BF16)
        for c in self.hidden_results(t):
            c.start()
        gg = jnp.zeros((group * cap, 1), F32)
        for n in range(width // TILE):
            hook(3 + n)
            cols = pl.ds(n * TILE, TILE)
            self.free(t, lambda s: self.term_results(s, n, cols))
            out = mm(actb[...], wd[:, cols]).astype(BF16).astype(F32)
            gg = gg + jnp.sum(out * cotb[:, cols].astype(F32), 1, keepdims=True)
            out = (out * gate_all).astype(BF16)
            back = (mm(gpb[...], wg[cols, :], 1, 1) + mm(upb[...], wu[cols, :], 1, 1)).astype(BF16)
            for s in range(group):
                part = slice(s * cap, (s + 1) * cap)
                yb[s, :, cols] = mm(picks[s], out[part], 0, 0).astype(BF16)
                rb[s, :, cols] = mm(picks[s], back[part], 0, 0).astype(BF16)
            for c in self.term_results(t, n, cols):
                c.start()
        zz, first = self.place_of(t)
        first = zz * self.width + first
        for s in range(group):
            self.outs[2][first + s] = jnp.sum(
                picks[s].astype(F32) * gg[s * cap : (s + 1) * cap], 0, keepdims=True
            )

    def free(self, t, copies):
        @pl.when(t > 0)
        def _():
            for c in copies(t - 1):
                c.wait()

    def end(self):
        t = jnp.int32(len(self.orders[0]) - 1)
        for c in self.row_results(t) + self.hidden_results(t):
            c.wait()
        for n in range(self.bufs[13].shape[1] // TILE):
            for c in self.term_results(t, n, pl.ds(n * TILE, TILE)):
                c.wait()


def gather_expert_kernel(nz, cap, group, *refs):
    shards, all_grads, weights = refs[:2], refs[2], refs[3:6]
    gathered, outs = refs[6:8], refs[8:16]
    send, recv, local = refs[16:19]
    bufs, sems = refs[19:33], refs[33]
    z, e = place()
    greet(z, e, nz)
    g = Gather(nz, shards, gathered, send, recv, local)
    plain = tuple((j, h) for j in range(nz) for h in range(2))
    orders = ORDERS.get(nz) or (plain, plain)
    plans = RELAYS.get(nz) or (relays_first(g, orders[0]),) * 2
    w = ExpertWork(nz, cap, group, orders, gathered[0], gathered[1], all_grads, weights, outs, bufs, sems)
    w.begin()
    relays = {"L": g.launch_line, "K": g.launch_plane, "M": g.mates, "R": g.relay, "F": g.finish}

    def run(name, order):
        kind, j = name[0], int(name[1:])
        if kind == "I":
            place, half = order[j]
            (g.shared_far if half else g.shared_near)(place)
            if place == 0 and half == 0:
                g.kept()
            w.ready(j)
        else:
            relays[kind](j)

    def body(t, _):
        def hook(k):
            for plan, order, here in zip(plans, orders, (w.edge, jnp.logical_not(w.edge))):
                for piece, part, names in plan:
                    if part == k:
                        @pl.when(jnp.logical_and(t == piece, here))
                        def _():
                            for name in names.split():
                                run(name, order)

        w.step(t, hook)
        return 0

    lax.fori_loop(0, len(orders[0]), body, 0)
    w.end()
    for j in range(nz):
        g.drain(j, True)


def relays_first(g, order):
    head = []
    for f in g.steps():
        kind, j = f.func.__name__, f.args[0]
        names = {"launch": "L%d K%d", "mates": "M%d", "relay": "R%d", "finish": "F%d"}[kind]
        head.append((0, 0, names.replace("%d", str(j))))
    return head + [(p, 0, "I%d" % p) for p in range(len(order))]


ORDERS = {
    4: (
        ((0, 0), (1, 0), (0, 1), (1, 1), (2, 0), (2, 1), (3, 0), (3, 1)),
        ((0, 0), (1, 0), (0, 1), (2, 0), (1, 1), (3, 0), (2, 1), (3, 1)),
    )
}
RELAYS = {
    4: (
        (
            (0, 0, "L0 K0 M0"),
            (0, 0, "L1 K1 R0"),
            (0, 0, "I0"),
            (0, 1, "M1"),
            (0, 5, "R1"),
            (1, 0, "I1"),
            (1, 2, "F0"),
            (1, 4, "L2 K2 I2"),
            (2, 1, "F1"),
            (2, 2, "M2 I3"),
            (3, 2, "R2"),
            (3, 4, "I4"),
            (4, 1, "L3 K3"),
            (4, 2, "F2"),
            (4, 5, "I5 M3"),
            (5, 3, "R3"),
            (5, 5, "I6"),
            (6, 3, "F3"),
            (6, 6, "I7"),
        ),
        (
            (0, 0, "L0 K0 M0"),
            (0, 0, "L1 L2 K1"),
            (0, 0, "R0 K2 I0"),
            (0, 1, "M1 M2"),
            (0, 4, "R1"),
            (0, 6, "I1"),
            (1, 2, "F0"),
            (1, 4, "L3 K3 I2"),
            (2, 2, "M3"),
            (2, 3, "R2"),
            (2, 5, "I3"),
            (3, 2, "F1"),
            (3, 5, "I4"),
            (4, 4, "R3"),
            (4, 6, "I5"),
            (5, 2, "F2"),
            (5, 5, "I6"),
            (6, 1, "F3"),
            (6, 3, "I7"),
        ),
    )
}


def gather_with_experts(rows, table, all_grads, w_gate, w_up, w_down, cap, collective_id):
    nz, width = lax.axis_size("dp"), lax.axis_size("expert")
    devices, group = nz * width, 4
    length, model = rows.shape
    ff = w_gate.shape[1]
    quarter = length // 4
    shards = [a.reshape(4, quarter, a.shape[1]) for a in (rows, table)]
    step, picked = group * cap, devices * cap
    vmem = pl.BlockSpec(memory_space=pltpu.VMEM)
    hbm = pl.BlockSpec(memory_space=pl.ANY)
    block = lambda a: pltpu.VMEM((2, group) + a.shape, a.dtype)
    shape = lambda *dims: jax.ShapeDtypeStruct(dims, BF16)
    outs = pl.pallas_call(
        functools.partial(gather_expert_kernel, nz, cap, group),
        out_shape=[shape(nz, width, *s.shape) for s in shards]
        + [
            shape(nz, width, length, model),
            shape(nz, width, length, model),
            jax.ShapeDtypeStruct((devices, 1, length), F32),
            shape(picked, model),
            shape(picked, model),
            shape(picked, ff),
            shape(picked, ff),
            shape(picked, ff),
        ],
        in_specs=[vmem, vmem, hbm, hbm, hbm, hbm],
        out_specs=[hbm, hbm, hbm, hbm, vmem, hbm, hbm, hbm, hbm, hbm],
        scratch_shapes=gather_scratch(nz, 2)
        + [pltpu.VMEM(w.shape, BF16) for w in (w_gate, w_up, w_down)]
        + [block(shards[0]), block(shards[1]), block(shards[0])]
        + [pltpu.VMEM((group, length, model), BF16)] * 2
        + [pltpu.VMEM((step, n), BF16) for n in (model, model, ff, ff, ff, model)]
        + [pltpu.SemaphoreType.DMA((6, max(5, model // TILE)))],
        compiler_params=pltpu.CompilerParams(
            collective_id=collective_id, has_side_effects=True, vmem_limit_bytes=VMEM_LIMIT
        ),
        name="gather_experts",
    )(*shards, all_grads.reshape((nz, width) + shards[0].shape), w_gate, w_up, w_down)
    return outs[2:]


class Attention:
    def __init__(self, hidden, gain, w_mixed, w_out, tables, gains, seg_col, seg_row, raw, normed, attended, branch,
                 w_buf, o_buf, kv_buf, mask, k_rot, v_low, sems):
        self.hidden, self.gain, self.w_mixed, self.w_out = hidden, gain, w_mixed, w_out
        self.tables, self.gains, self.seg_col, self.seg_row = tables, gains, seg_col, seg_row
        self.raw, self.normed, self.attended, self.branch = raw, normed, attended, branch
        self.w_buf, self.o_buf, self.kv_buf, self.mask = w_buf, o_buf, kv_buf, mask
        self.k_rot, self.v_low, self.sems = k_rot, v_low, sems
        self.cols = o_buf.shape[1]
        self.query_cols = w_out.shape[0]
        self.key_cols = kv_buf.shape[1] // 2
        self.count = self.query_cols // self.cols
        self.per_key = self.count // (self.key_cols // HEAD_DIM)

    def fetch(self, t, slot):
        at = pl.ds(pl.multiple_of(t * self.cols, self.cols), self.cols)
        return (
            pltpu.make_async_copy(self.w_mixed.at[:, at], self.w_buf.at[slot], self.sems.at[0, slot]),
            pltpu.make_async_copy(self.w_out.at[at, :], self.o_buf.at[slot], self.sems.at[1, slot]),
        )

    def prepare(self):
        kv = pltpu.make_async_copy(
            self.w_mixed.at[:, pl.ds(self.query_cols, 2 * self.key_cols)], self.kv_buf, self.sems.at[2, 0]
        )
        kv.start()
        for c in self.fetch(0, 0):
            c.start()
        values = self.hidden[...].astype(F32)
        scale = lax.rsqrt(jnp.mean(values * values, 1, keepdims=True) + EPS)
        self.normed[...] = (values * scale * self.gain[...]).astype(BF16)
        self.branch[...] = jnp.zeros_like(self.branch)
        self.mask[...] = allowed_mask(self.seg_col, self.seg_row)
        kv.wait()
        self.raw[:, self.query_cols :] = mm(self.normed[...], self.kv_buf[...])

    def step(self, t):
        slot = lax.rem(t, 2)

        @pl.when(t + 1 < self.count)
        def _():
            for c in self.fetch(t + 1, 1 - slot):
                c.start()

        for c in self.fetch(t, slot):
            c.wait()
        cosine, sine = self.tables[0], self.tables[1]

        @pl.when(lax.rem(t, self.per_key) == 0)
        def _():
            shift = pl.multiple_of(t // self.per_key * HEAD_DIM, HEAD_DIM)
            key = head_norm(self.raw[:, pl.ds(self.query_cols + shift, HEAD_DIM)], self.gains[1:2, :])
            self.k_rot[...] = rope(key, cosine, sine).astype(BF16)
            self.v_low[...] = self.raw[:, pl.ds(self.query_cols + self.key_cols + shift, HEAD_DIM)].astype(BF16)

        at = pl.ds(pl.multiple_of(t * self.cols, self.cols), self.cols)
        query_raw = mm(self.normed[...], self.w_buf[slot])
        self.raw[:, at] = query_raw
        mask = self.mask[...] > 0.0
        k_rot, v_low = self.k_rot[...], self.v_low[...]
        outs = []
        for h in range(self.cols // HEAD_DIM):
            query = head_norm(query_raw[:, h * HEAD_DIM : (h + 1) * HEAD_DIM], self.gains[0:1, :])
            q_rot = rope(query, cosine, sine).astype(BF16)
            scores = mm(q_rot, k_rot, 1, 1) * (1.0 / math.sqrt(HEAD_DIM))
            raised = jnp.where(mask, jnp.exp(scores), 0.0)
            probs = (raised / jnp.sum(raised, 1, keepdims=True)).astype(BF16)
            outs.append(mm(probs, v_low).astype(BF16))
        out = jnp.concatenate(outs, 1)
        self.attended[:, at] = out
        self.branch[...] += mm(out, self.o_buf[slot])


def head_norm(raw, gain):
    return raw * lax.rsqrt(jnp.mean(raw * raw, 1, keepdims=True) + EPS) * gain


def allowed_mask(seg_col, seg_row):
    length = seg_col.shape[0]
    row = lax.broadcasted_iota(jnp.int32, (length, length), 0)
    col = lax.broadcasted_iota(jnp.int32, (length, length), 1)
    same = seg_col[...] == seg_row[...]
    return jnp.where(jnp.logical_and(same, col <= row), 1.0, 0.0)


def gather_attention_kernel(nz, plan, shard, hidden, gain, w_mixed, w_out, tables, gains, seg_col, seg_row,
                            gathered, raw, normed, attended, branch, *scratch):
    z, e = place()
    greet(z, e, nz)
    g = Gather(nz, [shard], [gathered], *scratch[:3])
    a = Attention(hidden, gain, w_mixed, w_out, tables, gains, seg_col, seg_row, raw, normed, attended, branch, *scratch[3:])
    steps = g.steps()
    steps[0]()
    a.prepare()
    run_beside(a.count, a.step, steps[1:], plan)
    for j in range(nz):
        g.shared_near(j)
        g.shared_far(j)
    for j in range(nz):
        g.drain(j)


def gather_with_attention(rows, hidden, gain, w_mixed, w_out, tables, gains, segments, collective_id):
    nz, width = lax.axis_size("dp"), lax.axis_size("expert")
    length, model = hidden.shape
    shard = rows.reshape(4, rows.shape[0] // 4, rows.shape[1])
    cols = 4 * HEAD_DIM
    mixed, query_cols = w_mixed.shape[1], w_out.shape[0]
    vmem = pl.BlockSpec(memory_space=pltpu.VMEM)
    hbm = pl.BlockSpec(memory_space=pl.ANY)
    gathered, raw, normed, attended, branch = pl.pallas_call(
        functools.partial(gather_attention_kernel, nz, [1, 0, 1, 1, 0, 1, 2, 2]),
        out_shape=[
            jax.ShapeDtypeStruct((nz, width) + shard.shape, shard.dtype),
            jax.ShapeDtypeStruct((length, mixed), F32),
            jax.ShapeDtypeStruct((length, model), BF16),
            jax.ShapeDtypeStruct((length, query_cols), BF16),
            jax.ShapeDtypeStruct((length, model), F32),
        ],
        in_specs=[vmem, vmem, vmem, hbm, hbm, vmem, vmem, vmem, vmem],
        out_specs=[hbm, vmem, vmem, vmem, vmem],
        scratch_shapes=gather_scratch(nz, 1)
        + [
            pltpu.VMEM((2, model, cols), BF16),
            pltpu.VMEM((2, cols, model), BF16),
            pltpu.VMEM((model, mixed - query_cols), BF16),
            pltpu.VMEM((length, length), F32),
            pltpu.VMEM((length, HEAD_DIM), BF16),
            pltpu.VMEM((length, HEAD_DIM), BF16),
            pltpu.SemaphoreType.DMA((3, 2)),
        ],
        compiler_params=pltpu.CompilerParams(
            collective_id=collective_id, has_side_effects=True, vmem_limit_bytes=VMEM_LIMIT
        ),
        name="gather_attention",
    )(shard, hidden, gain, w_mixed, w_out, tables, gains, segments[:, None], segments[None, :])
    return gathered, raw, normed, attended, branch


class ExpertGrads:
    TILE = 256

    def __init__(self, rows, down, act, gate_pre, up_pre, grad_gate, grad_up, grad_down,
                 tile, gate_buf, up_buf, gate_stage, up_stage, sems):
        self.rows, self.down, self.act, self.gate_pre, self.up_pre = rows, down, act, gate_pre, up_pre
        self.grad_gate, self.grad_up, self.grad_down = grad_gate, grad_up, grad_down
        self.tile, self.gate_buf, self.up_buf = tile, gate_buf, up_buf
        self.gate_stage, self.up_stage, self.sems = gate_stage, up_stage, sems
        self.half = rows.shape[1] // self.TILE
        self.count = 2 * self.half

    def at(self, t):
        return pl.ds(pl.multiple_of(lax.rem(t, self.half) * self.TILE, self.TILE), self.TILE)

    def each(self, t, act):
        slot = lax.rem(t, 2)
        for source, here in ((self.rows, t < self.half), (self.down, t >= self.half)):
            @pl.when(here)
            def _():
                act(pltpu.make_async_copy(source.at[:, self.at(t)], self.tile.at[slot], self.sems.at[0, slot]))

    def hidden(self, source, buf, k):
        return pltpu.make_async_copy(source, buf, self.sems.at[1, k])

    def put(self, t, act):
        for out, here in ((self.grad_gate, t < self.half), (self.grad_down, t >= self.half)):
            @pl.when(here)
            def _():
                act(pltpu.make_async_copy(self.gate_stage, out.at[self.at(t), :], self.sems.at[2, 0]))

    def put_up(self, t):
        return pltpu.make_async_copy(self.up_stage, self.grad_up.at[self.at(t), :], self.sems.at[2, 1])

    def prepare(self):
        self.hidden(self.gate_pre, self.gate_buf, 0).start()
        self.hidden(self.up_pre, self.up_buf, 1).start()
        self.each(jnp.int32(0), lambda c: c.start())

    def step(self, t):
        slot = lax.rem(t, 2)

        @pl.when(t + 1 < self.count)
        def _():
            self.each(t + 1, lambda c: c.start())

        @pl.when(t == 0)
        def _():
            self.hidden(self.gate_pre, self.gate_buf, 0).wait()
            self.hidden(self.up_pre, self.up_buf, 1).wait()

        @pl.when(t == self.half)
        def _():
            copy = self.hidden(self.act, self.gate_buf, 0)
            copy.start()
            copy.wait()

        self.each(t, lambda c: c.wait())

        @pl.when(t > 0)
        def _():
            self.put(t - 1, lambda c: c.wait())

        self.gate_stage[...] = mm(self.tile[slot], self.gate_buf[...], 0, 0)
        self.put(t, lambda c: c.start())

        @pl.when(t < self.half)
        def _():
            @pl.when(t > 0)
            def _():
                self.put_up(t - 1).wait()

            self.up_stage[...] = mm(self.tile[slot], self.up_buf[...], 0, 0)
            self.put_up(t).start()

    def end(self):
        self.put(jnp.int32(self.count - 1), lambda c: c.wait())
        self.put_up(jnp.int32(self.half - 1)).wait()


def scatter_grads_kernel(nz, plan, count, *refs):
    terms, inputs = refs[:count], refs[count : count + 5]
    totals, outs = refs[count + 5 : 2 * count + 5], refs[2 * count + 5 : 2 * count + 8]
    scratch = refs[2 * count + 8 :]
    groups = [scratch[k * count : (k + 1) * count] for k in range(Scatter.BUFFERS)]
    rest = scratch[Scatter.BUFFERS * count :]
    z, e = place()
    greet(z, e, nz)
    s = Scatter(nz, terms, totals, *groups, *rest[:3])
    w = ExpertGrads(*inputs, *outs, *rest[3:])
    s.begin()
    w.prepare()
    run_beside(w.count, w.step, s.steps(), plan)
    w.end()
    for j in range(nz):
        s.drain(j)


def scatter_with_grads(arrays, rows, down, act, gate_pre, up_pre, collective_id):
    nz, width = lax.axis_size("dp"), lax.axis_size("expert")
    count, devices = len(arrays), nz * width
    terms = [a.reshape(nz, width, 4, a.shape[0] // (4 * devices), a.shape[1]) for a in arrays]
    shapes = [t.shape[3:] for t in terms]
    picked, model = rows.shape
    ff = act.shape[1]
    tile = ExpertGrads.TILE
    vmem = pl.BlockSpec(memory_space=pltpu.VMEM)
    hbm = pl.BlockSpec(memory_space=pl.ANY)
    plan = [3, 1, 0, 0, 0, 0, 3, 0, 0, 0, 0, 2] + [0] * 16
    outs = pl.pallas_call(
        functools.partial(scatter_grads_kernel, nz, plan, count),
        out_shape=[jax.ShapeDtypeStruct((4,) + s, F32) for s in shapes] + [jax.ShapeDtypeStruct((model, ff), F32)] * 3,
        in_specs=[hbm] * (count + 5),
        out_specs=[vmem] * count + [hbm] * 3,
        scratch_shapes=scatter_buffers(nz, width, [(s, a.dtype) for s, a in zip(shapes, arrays)])
        + [
            pltpu.VMEM((2, picked, tile), BF16),
            pltpu.VMEM((picked, ff), BF16),
            pltpu.VMEM((picked, ff), BF16),
            pltpu.VMEM((tile, ff), F32),
            pltpu.VMEM((tile, ff), F32),
            pltpu.SemaphoreType.DMA((3, 2)),
        ],
        compiler_params=pltpu.CompilerParams(
            collective_id=collective_id, has_side_effects=True, vmem_limit_bytes=VMEM_LIMIT
        ),
        name="scatter_grads",
    )(*terms, rows, down, act, gate_pre, up_pre)
    return [o.reshape(4 * s[0], s[1]) for o, s in zip(outs, shapes)] + list(outs[count:])


def pack_columns(columns, rows, lanes, dtype):
    parts = [c.astype(dtype) for c in columns]
    used = sum(c.shape[1] for c in parts)
    return jnp.concatenate(parts + [jnp.zeros((rows, lanes - used), dtype)], 1)


def spread(vector, devices, rows):
    blocks = vector.reshape(devices, -1)
    return jnp.pad(blocks, ((0, 0), (0, rows - blocks.shape[1]))).reshape(devices * rows, 1)


def per_device_gather(
    hidden_in,
    segment_ids,
    expert_ids,
    attn_gain,
    query_gain,
    key_gain,
    w_query,
    w_key,
    w_value,
    w_output,
    mlp_gain,
    w_router,
    w_gate,
    w_up,
    w_down,
    out_grad,
):
    devices = lax.axis_size(("dp", "expert"))
    me = lax.axis_index(("dp", "expert"))
    length, choices = expert_ids.shape
    width = hidden_in.shape[1]
    experts_total = devices
    capacity = 5 * length * choices // (4 * experts_total)
    query_cols, key_cols = w_query.shape[1], w_key.shape[1]
    rows = w_query.shape[0]
    head_rows = query_gain.shape[0]

    column = lambda v: jnp.pad(v, (0, rows - v.shape[0]))[:, None]
    lanes = 128 * pl.cdiv(experts_total + 4, 128)
    small = pack_columns(
        [w_router, column(attn_gain), column(mlp_gain), column(query_gain), column(key_gain)], rows, lanes, BF16
    )
    w_mixed = jnp.concatenate([w_query, w_key, w_value], 1)
    w_mixed, w_out, small = gather_all([w_mixed, w_output, small], 1)
    router = small[:, :experts_total]
    attn_gain, mlp_gain = small[:, experts_total], small[:, experts_total + 1]
    heads_of = small.reshape(devices, rows, lanes)[:, :head_rows]
    query_gain = heads_of[:, :, experts_total + 2].reshape(-1)
    key_gain = heads_of[:, :, experts_total + 3].reshape(-1)

    plain_in = hidden_in.astype(F32)
    inv_attn = rms_scale(plain_in)
    cosine_table, sine_table = rope_tables(jnp.arange(length) % TOK_DEV, HEAD_DIM)
    cosine, sine = cosine_table[:, 0], sine_table[:, 0]
    tables = jnp.stack([jnp.concatenate([cosine, cosine], 1), jnp.concatenate([-sine, sine], 1)])
    head_gains = jnp.stack([query_gain, key_gain]).astype(F32)
    all_grads, mixed, normed_attn, attended, branch = gather_with_attention(
        out_grad, hidden_in, attn_gain.astype(F32)[None, :], w_mixed, w_out, tables, head_gains, segment_ids, 3
    )
    residual = plain_in + branch

    inv_mlp = rms_scale(residual)
    normed_mlp = (residual * inv_mlp * mlp_gain).astype(BF16)
    logits = jnp.dot(normed_mlp, router, preferred_element_type=F32)
    chosen = jnp.any(expert_ids[:, :, None] == jnp.arange(experts_total)[None, None, :], 1)
    raised = jnp.where(chosen, jnp.exp(logits), 0.0)
    gate = raised / jnp.sum(raised, -1, keepdims=True)
    position = jnp.arange(length)
    not_after = (position[None, :] <= position[:, None]).astype(BF16)
    rank = jnp.dot(not_after, chosen.astype(BF16), preferred_element_type=F32) - 1.0
    rank = jnp.where(chosen, rank, -1.0)
    gate_high = lax.reduce_precision(gate, 8, 7)
    table = pack_columns([gate_high, gate - gate_high, rank], length, 128 * pl.cdiv(3 * experts_total, 128), BF16)

    y_terms, r_terms, gate_terms, rows_in, down_in, act, gate_pre_grad, up_pre_grad = gather_with_experts(
        normed_mlp, table, all_grads, w_gate[0], w_up[0], w_down[0], capacity, 2
    )
    is_me = (jnp.arange(experts_total) == me).astype(F32)
    gate_terms = (gate_terms * is_me[None, :, None]).reshape(devices * experts_total, length)
    row_grad_sum, gate_grad, grad_w_gate, grad_w_up, grad_w_down = scatter_with_grads(
        [r_terms.reshape(devices * length, width), gate_terms], rows_in, down_in, act, gate_pre_grad, up_pre_grad, 4
    )
    grad_w_gate, grad_w_up, grad_w_down = grad_w_gate[None], grad_w_up[None], grad_w_down.T[None]

    gate_grad = gate_grad.T
    sel_grad = gate * (gate_grad - jnp.sum(gate * gate_grad, -1, keepdims=True))
    logit_grad = jnp.where(chosen, sel_grad, 0.0).astype(BF16)
    grad_w_router = jnp.dot(normed_mlp.T, logit_grad, preferred_element_type=F32)
    normed_mlp_grad = row_grad_sum + jnp.dot(logit_grad, router.T, preferred_element_type=F32)
    grad_mlp_gain = jnp.sum(normed_mlp_grad * residual * inv_mlp, 0)
    residual_grad = out_grad.astype(F32) + norm_grad(normed_mlp_grad, residual, inv_mlp, mlp_gain)

    branch_grad = residual_grad.astype(BF16)
    mixed_out, gain_grads, normed_attn_grad, grad_w_output, grad_w_mixed = scatter_with_attention(
        y_terms.reshape(devices * length, width), branch_grad, w_out, mixed, tables, head_gains, segment_ids,
        normed_attn, attended, w_mixed, 5,
    )
    block_out = residual + mixed_out
    grad_query_gain, grad_key_gain = gain_grads[0], gain_grads[1]
    grad_attn_gain = jnp.sum(normed_attn_grad * plain_in * inv_attn, 0)
    grad_in = residual_grad + norm_grad(normed_attn_grad, plain_in, inv_attn, attn_gain)

    small_grads = pack_columns(
        [
            grad_w_router,
            grad_attn_gain[:, None],
            grad_mlp_gain[:, None],
            spread(grad_query_gain, devices, rows),
            spread(grad_key_gain, devices, rows),
        ],
        width,
        lanes,
        F32,
    )
    share_mixed, share_w_output, share_small = scatter_sum([grad_w_mixed, grad_w_output, small_grads], 6)
    return (
        block_out,
        grad_in,
        share_small[:, experts_total],
        share_small[:head_rows, experts_total + 2],
        share_small[:head_rows, experts_total + 3],
        share_mixed[:, :query_cols],
        share_mixed[:, query_cols : query_cols + key_cols],
        share_mixed[:, query_cols + key_cols :],
        share_w_output,
        share_small[:, experts_total + 1],
        share_small[:, :experts_total],
        grad_w_gate,
        grad_w_up,
        grad_w_down,
    )


def per_device(*arguments):
    expert_ids, w_gate = arguments[2], arguments[12]
    devices, width = lax.axis_size(("dp", "expert")), lax.axis_size("expert")
    length, choices = expert_ids.shape
    capacity = 5 * length * choices // (4 * devices)
    dense = devices <= 4 * choices and w_gate.shape[0] == 1 and width == 8
    if dense and capacity % 16 == 0 and devices % 4 == 0:
        return per_device_gather(*arguments)
    return per_device_exchange(*arguments)


def solution(mesh):
    in_specs = (
        P(("dp", "expert"), None),
        P(("dp", "expert")),
        P(("dp", "expert"), None),
        P(("dp", "expert")),
        P(("dp", "expert")),
        P(("dp", "expert")),
        P(("dp", "expert"), None),
        P(("dp", "expert"), None),
        P(("dp", "expert"), None),
        P(("dp", "expert"), None),
        P(("dp", "expert")),
        P(("dp", "expert"), None),
        P(("dp", "expert"), None, None),
        P(("dp", "expert"), None, None),
        P(("dp", "expert"), None, None),
        P(("dp", "expert"), None),
    )
    out_specs = (
        P(("dp", "expert"), None),
        P(("dp", "expert"), None),
        P(("dp", "expert")),
        P(("dp", "expert")),
        P(("dp", "expert")),
        P(("dp", "expert"), None),
        P(("dp", "expert"), None),
        P(("dp", "expert"), None),
        P(("dp", "expert"), None),
        P(("dp", "expert")),
        P(("dp", "expert"), None),
        P(("dp", "expert"), None, None),
        P(("dp", "expert"), None, None),
        P(("dp", "expert"), None, None),
    )
    return jax.shard_map(
        per_device, mesh=mesh, in_specs=in_specs, out_specs=out_specs, check_vma=False
    )
```

```python
import functools
import math

import jax
import jax.numpy as jnp
from jax import lax
from jax.experimental import pallas as pl
from jax.experimental.pallas import tpu as pltpu
from jax.sharding import PartitionSpec as P

F32, BF16 = jnp.float32, jnp.bfloat16
MESH = pl.DeviceIdType.MESH
VMEM_LIMIT = 63 * 1024 * 1024


HEADS = 32
KV_HEADS = 4
HEAD_DIM = 128
TOK_DEV = 256


EPS = 1e-06
ROPE_BASE = 1000000.0


def rms_scale(values):
    return lax.rsqrt(jnp.mean(values * values, -1, keepdims=True) + EPS)


def norm_grad(upstream, values, inverse, gain_vec):
    weighted = upstream * gain_vec
    return inverse * weighted - values * inverse**3 * jnp.mean(weighted * values, -1, keepdims=True)


def rope_tables(positions, head_dim):
    half_dim = head_dim // 2
    frequency = ROPE_BASE ** (-(jnp.arange(half_dim).astype(jnp.float32) * 2.0 / head_dim))
    angles = positions.astype(jnp.float32)[:, None] * frequency[None, :]
    return (jnp.cos(angles)[:, None, :], jnp.sin(angles)[:, None, :])


def rotate(values, cosine_table, sine_table):
    half_dim = values.shape[-1] // 2
    first_half = values[..., :half_dim]
    second_half = values[..., half_dim:]
    return jnp.concatenate(
        [
            first_half * cosine_table - second_half * sine_table,
            second_half * cosine_table + first_half * sine_table,
        ],
        -1,
    )


def unrotate(values, cosine_table, sine_table):
    half_dim = values.shape[-1] // 2
    first_half = values[..., :half_dim]
    second_half = values[..., half_dim:]
    return jnp.concatenate(
        [
            first_half * cosine_table + second_half * sine_table,
            second_half * cosine_table - first_half * sine_table,
        ],
        -1,
    )


def attend(query_rot, key_rot, value_rows, allowed):
    score_scale = 1.0 / math.sqrt(HEAD_DIM)
    scores = (
        jnp.einsum("qkgd,tkd->kgqt", query_rot, key_rot, preferred_element_type=jnp.float32)
        * score_scale
    )
    exp_scores = jnp.where(allowed, jnp.exp(scores), 0.0)
    totals = jnp.sum(exp_scores, -1, keepdims=True)
    probs_low = (exp_scores / totals).astype(jnp.bfloat16)
    attended = jnp.einsum(
        "kgqt,tkd->qkgd", probs_low, value_rows, preferred_element_type=jnp.float32
    ).astype(jnp.bfloat16)
    return (attended, jnp.log(totals))


def attend_grad(query_rot, key_rot, value_rows, allowed, log_totals, attended_grad):
    score_scale = 1.0 / math.sqrt(HEAD_DIM)
    scores = (
        jnp.einsum("qkgd,tkd->kgqt", query_rot, key_rot, preferred_element_type=jnp.float32)
        * score_scale
    )
    probs_back = jnp.where(allowed, jnp.exp(scores - log_totals), 0.0)
    probs_low = probs_back.astype(jnp.bfloat16)
    value_sum_grad = jnp.einsum(
        "kgqt,qkgd->tkd", probs_low, attended_grad, preferred_element_type=jnp.float32
    )
    prob_grad = jnp.einsum(
        "qkgd,tkd->kgqt", attended_grad, value_rows, preferred_element_type=jnp.float32
    )
    score_grad = (
        probs_back * (prob_grad - jnp.sum(probs_back * prob_grad, -1, keepdims=True))
    ).astype(jnp.bfloat16)
    query_rot_grad = (
        jnp.einsum("kgqt,tkd->qkgd", score_grad, key_rot, preferred_element_type=jnp.float32)
        * score_scale
    )
    key_rot_grad = (
        jnp.einsum("kgqt,qkgd->tkd", score_grad, query_rot, preferred_element_type=jnp.float32)
        * score_scale
    )
    return (query_rot_grad, key_rot_grad, value_sum_grad)


def mixer_forward(block_in, block_segments, weights):
    w_query, w_key, w_value, w_output, w_router, attn_gain, mlp_gain, query_gain, key_gain = weights
    row_count = block_in.shape[0]
    seq_count = row_count // TOK_DEV
    group_size = HEADS // KV_HEADS
    plain_in = block_in.astype(jnp.float32)
    inv_attn = rms_scale(plain_in)
    normed_attn = (plain_in * inv_attn * attn_gain).astype(jnp.bfloat16)
    query_raw = jnp.dot(normed_attn, w_query, preferred_element_type=jnp.float32).reshape(
        row_count, HEADS, HEAD_DIM
    )
    key_raw = jnp.dot(normed_attn, w_key, preferred_element_type=jnp.float32).reshape(
        row_count, KV_HEADS, HEAD_DIM
    )
    value_rows = jnp.dot(normed_attn, w_value, preferred_element_type=jnp.float32).astype(
        jnp.bfloat16
    )
    value_rows = value_rows.reshape(seq_count, TOK_DEV, KV_HEADS, HEAD_DIM)
    query_scale = rms_scale(query_raw)
    key_scale = rms_scale(key_raw)
    cosine_table, sine_table = rope_tables(jnp.arange(row_count) % TOK_DEV, HEAD_DIM)
    query_rot = rotate(query_raw * query_scale * query_gain, cosine_table, sine_table).astype(
        jnp.bfloat16
    )
    query_rot = query_rot.reshape(seq_count, TOK_DEV, KV_HEADS, group_size, HEAD_DIM)
    key_rot = rotate(key_raw * key_scale * key_gain, cosine_table, sine_table).astype(jnp.bfloat16)
    key_rot = key_rot.reshape(seq_count, TOK_DEV, KV_HEADS, HEAD_DIM)
    segments = block_segments.reshape(seq_count, TOK_DEV)
    position = jnp.arange(TOK_DEV)
    allowed = (segments[:, :, None] == segments[:, None, :]) & (
        position[None, None, :] <= position[None, :, None]
    )
    attended, log_totals = jax.vmap(attend)(query_rot, key_rot, value_rows, allowed)
    attended = attended.reshape(row_count, HEADS * HEAD_DIM)
    residual = plain_in + jnp.dot(attended, w_output, preferred_element_type=jnp.float32)
    saved_state = (
        plain_in,
        inv_attn,
        normed_attn,
        query_raw,
        key_raw,
        value_rows,
        query_scale,
        key_scale,
        query_rot,
        key_rot,
        allowed,
        log_totals,
        attended,
        cosine_table,
        sine_table,
    )
    return (residual, saved_state)


def mixer_backward(residual_grad, saved_state, weights):
    w_query, w_key, w_value, w_output, w_router, attn_gain, mlp_gain, query_gain, key_gain = weights
    (
        plain_in,
        inv_attn,
        normed_attn,
        query_raw,
        key_raw,
        value_rows,
        query_scale,
        key_scale,
        query_rot,
        key_rot,
        allowed,
        log_totals,
        attended,
        cosine_table,
        sine_table,
    ) = saved_state
    row_count = residual_grad.shape[0]
    seq_count = row_count // TOK_DEV
    group_size = HEADS // KV_HEADS
    branch_grad = residual_grad.astype(jnp.bfloat16)
    grad_w_output = jnp.dot(attended.T, branch_grad, preferred_element_type=jnp.float32)
    attended_grad = jnp.dot(branch_grad, w_output.T, preferred_element_type=jnp.float32).astype(
        jnp.bfloat16
    )
    attended_grad = attended_grad.reshape(seq_count, TOK_DEV, KV_HEADS, group_size, HEAD_DIM)
    query_rot_grad, key_rot_grad, value_sum_grad = jax.vmap(attend_grad)(
        query_rot, key_rot, value_rows, allowed, log_totals, attended_grad
    )
    query_normed_grad = unrotate(
        query_rot_grad.reshape(row_count, HEADS, HEAD_DIM), cosine_table, sine_table
    )
    key_normed_grad = unrotate(
        key_rot_grad.reshape(row_count, KV_HEADS, HEAD_DIM), cosine_table, sine_table
    )
    grad_query_gain = jnp.sum(query_normed_grad * query_raw * query_scale, (0, 1))
    grad_key_gain = jnp.sum(key_normed_grad * key_raw * key_scale, (0, 1))
    query_grad = norm_grad(query_normed_grad, query_raw, query_scale, query_gain).astype(
        jnp.bfloat16
    )
    query_grad = query_grad.reshape(row_count, HEADS * HEAD_DIM)
    key_grad = norm_grad(key_normed_grad, key_raw, key_scale, key_gain).astype(jnp.bfloat16)
    key_grad = key_grad.reshape(row_count, KV_HEADS * HEAD_DIM)
    value_grad = value_sum_grad.astype(jnp.bfloat16).reshape(row_count, KV_HEADS * HEAD_DIM)
    grad_w_query = jnp.dot(normed_attn.T, query_grad, preferred_element_type=jnp.float32)
    grad_w_key = jnp.dot(normed_attn.T, key_grad, preferred_element_type=jnp.float32)
    grad_w_value = jnp.dot(normed_attn.T, value_grad, preferred_element_type=jnp.float32)
    normed_attn_grad = (
        jnp.dot(query_grad, w_query.T, preferred_element_type=jnp.float32)
        + jnp.dot(key_grad, w_key.T, preferred_element_type=jnp.float32)
        + jnp.dot(value_grad, w_value.T, preferred_element_type=jnp.float32)
    )
    grad_attn_gain = jnp.sum(normed_attn_grad * plain_in * inv_attn, 0)
    grad_in = residual_grad + norm_grad(normed_attn_grad, plain_in, inv_attn, attn_gain)
    return (
        grad_in,
        (
            grad_attn_gain,
            grad_query_gain,
            grad_key_gain,
            grad_w_query,
            grad_w_key,
            grad_w_value,
            grad_w_output,
        ),
    )


def dispatch_table(expert_rows, experts, capacity):
    length, choices = expert_rows.shape
    flat_ids = expert_rows.reshape(length * choices)
    marks = (flat_ids[:, None] == jnp.arange(experts)[None, :]).astype(jnp.int32)
    earlier = jnp.cumsum(marks, 0) - marks
    destination = flat_ids * capacity + jnp.sum(earlier * marks, -1)
    pair_ids = (
        jnp.zeros((experts * capacity,), jnp.int32)
        .at[destination]
        .set(jnp.arange(length * choices, dtype=jnp.int32))
    )
    filled = jnp.zeros((experts * capacity,), jnp.bfloat16).at[destination].set(1.0)
    return (destination, pair_ids, filled)


def move_rows(row_block, section_name):
    if section_name == "dispatch":
        return lax.all_to_all(row_block, ("dp", "expert"), split_axis=0, concat_axis=0, tiled=True)
    if section_name == "combine":
        return lax.all_to_all(row_block, ("dp", "expert"), split_axis=0, concat_axis=0, tiled=True)
    if section_name == "grad_dispatch":
        return lax.all_to_all(row_block, ("dp", "expert"), split_axis=0, concat_axis=0, tiled=True)
    return lax.all_to_all(row_block, ("dp", "expert"), split_axis=0, concat_axis=0, tiled=True)


def per_device_exchange(
    hidden_in,
    segment_ids,
    expert_ids,
    attn_gain,
    query_gain,
    key_gain,
    w_query,
    w_key,
    w_value,
    w_output,
    mlp_gain,
    w_router,
    w_gate,
    w_up,
    w_down,
    out_grad,
):
    weights = (
        lax.all_gather(w_query, ("dp", "expert"), axis=0, tiled=True),
        lax.all_gather(w_key, ("dp", "expert"), axis=0, tiled=True),
        lax.all_gather(w_value, ("dp", "expert"), axis=0, tiled=True),
        lax.all_gather(w_output, ("dp", "expert"), axis=0, tiled=True),
        lax.all_gather(w_router, ("dp", "expert"), axis=0, tiled=True),
        lax.all_gather(attn_gain, ("dp", "expert"), axis=0, tiled=True),
        lax.all_gather(mlp_gain, ("dp", "expert"), axis=0, tiled=True),
        lax.all_gather(query_gain, ("dp", "expert"), axis=0, tiled=True),
        lax.all_gather(key_gain, ("dp", "expert"), axis=0, tiled=True),
    )
    residual, saved_state = mixer_forward(hidden_in, segment_ids, weights)
    full_router = weights[4]
    full_mlp_gain = weights[6]
    inv_mlp = rms_scale(residual)
    normed_mlp = (residual * inv_mlp * full_mlp_gain).astype(jnp.bfloat16)
    logits = jnp.dot(normed_mlp, full_router, preferred_element_type=jnp.float32)
    device_count = lax.axis_size(("dp", "expert"))
    local_experts = w_gate.shape[0]
    experts = local_experts * device_count
    length, choices = expert_ids.shape
    model_width = hidden_in.shape[1]
    capacity = 5 * length * choices // (4 * experts)
    one_hot = expert_ids[:, :, None] == jnp.arange(experts)[None, None, :]
    chosen = jnp.sum(jnp.where(one_hot, logits[:, None, :], 0.0), -1)
    raised = jnp.exp(chosen)
    gate_weights = raised / jnp.sum(raised, -1, keepdims=True)
    destination, pair_ids, filled = dispatch_table(expert_ids, experts, capacity)
    send_rows = normed_mlp[pair_ids // choices] * filled[:, None]
    received = move_rows(
        send_rows.reshape(device_count, local_experts * capacity, model_width), "dispatch"
    )
    received = received.reshape(device_count, local_experts, capacity, model_width)
    pre_gate = jnp.einsum("secd,edf->secf", received, w_gate, preferred_element_type=jnp.float32)
    pre_up = jnp.einsum("secd,edf->secf", received, w_up, preferred_element_type=jnp.float32)
    gate_sigmoid = jax.nn.sigmoid(pre_gate)
    silu_gate = pre_gate * gate_sigmoid
    activation = (silu_gate * pre_up).astype(jnp.bfloat16)
    expert_out = jnp.einsum(
        "secf,efd->secd", activation, w_down, preferred_element_type=jnp.float32
    ).astype(jnp.bfloat16)
    returned = move_rows(
        expert_out.reshape(device_count, local_experts * capacity, model_width), "combine"
    )
    picked = returned.reshape(experts * capacity, model_width)[destination].reshape(
        length, choices, model_width
    )
    block_out = residual + jnp.sum(gate_weights[:, :, None] * picked.astype(jnp.float32), 1)
    weights = (
        lax.all_gather(w_query, ("dp", "expert"), axis=0, tiled=True),
        lax.all_gather(w_key, ("dp", "expert"), axis=0, tiled=True),
        lax.all_gather(w_value, ("dp", "expert"), axis=0, tiled=True),
        lax.all_gather(w_output, ("dp", "expert"), axis=0, tiled=True),
        lax.all_gather(w_router, ("dp", "expert"), axis=0, tiled=True),
        lax.all_gather(attn_gain, ("dp", "expert"), axis=0, tiled=True),
        lax.all_gather(mlp_gain, ("dp", "expert"), axis=0, tiled=True),
        lax.all_gather(query_gain, ("dp", "expert"), axis=0, tiled=True),
        lax.all_gather(key_gain, ("dp", "expert"), axis=0, tiled=True),
    )
    full_router = weights[4]
    full_mlp_gain = weights[6]
    cotangent = out_grad.astype(jnp.float32)
    gate_grad = jnp.sum(cotangent[:, None, :] * picked.astype(jnp.float32), -1)
    down_in = (
        (gate_weights[:, :, None] * cotangent[:, None, :])
        .astype(jnp.bfloat16)
        .reshape(length * choices, model_width)
    )
    send_grad = down_in[pair_ids] * filled[:, None]
    recv_grad = move_rows(
        send_grad.reshape(device_count, local_experts * capacity, model_width), "grad_dispatch"
    )
    recv_grad = recv_grad.reshape(device_count, local_experts, capacity, model_width)
    act_grad = jnp.einsum("secd,efd->secf", recv_grad, w_down, preferred_element_type=jnp.float32)
    grad_w_down = jnp.einsum(
        "secf,secd->efd", activation, recv_grad, preferred_element_type=jnp.float32
    )
    gate_pre_grad = (
        act_grad * pre_up * gate_sigmoid * (1.0 + pre_gate * (1.0 - gate_sigmoid))
    ).astype(jnp.bfloat16)
    up_pre_grad = (act_grad * silu_gate).astype(jnp.bfloat16)
    grad_w_gate = jnp.einsum(
        "secd,secf->edf", received, gate_pre_grad, preferred_element_type=jnp.float32
    )
    grad_w_up = jnp.einsum(
        "secd,secf->edf", received, up_pre_grad, preferred_element_type=jnp.float32
    )
    row_grad = (
        jnp.einsum("secf,edf->secd", gate_pre_grad, w_gate, preferred_element_type=jnp.float32)
        + jnp.einsum("secf,edf->secd", up_pre_grad, w_up, preferred_element_type=jnp.float32)
    ).astype(jnp.bfloat16)
    row_back = move_rows(
        row_grad.reshape(device_count, local_experts * capacity, model_width), "grad_return"
    )
    row_back = row_back.reshape(experts * capacity, model_width)[destination].reshape(
        length, choices, model_width
    )
    sel_grad = gate_weights * (gate_grad - jnp.sum(gate_weights * gate_grad, -1, keepdims=True))
    logit_grad = jnp.sum(jnp.where(one_hot, sel_grad[:, :, None], 0.0), 1).astype(jnp.bfloat16)
    grad_w_router = jnp.dot(normed_mlp.T, logit_grad, preferred_element_type=jnp.float32)
    normed_mlp_grad = jnp.sum(row_back.astype(jnp.float32), 1) + jnp.dot(
        logit_grad, full_router.T, preferred_element_type=jnp.float32
    )
    grad_mlp_gain = jnp.sum(normed_mlp_grad * residual * inv_mlp, 0)
    residual_grad = cotangent + norm_grad(normed_mlp_grad, residual, inv_mlp, full_mlp_gain)
    grad_in, mixer_terms = mixer_backward(residual_grad, saved_state, weights)
    (
        grad_attn_gain,
        grad_query_gain,
        grad_key_gain,
        grad_w_query,
        grad_w_key,
        grad_w_value,
        grad_w_output,
    ) = mixer_terms
    summed = (
        lax.psum_scatter(grad_w_query, ("dp", "expert"), scatter_dimension=0, tiled=True),
        lax.psum_scatter(grad_w_key, ("dp", "expert"), scatter_dimension=0, tiled=True),
        lax.psum_scatter(grad_w_value, ("dp", "expert"), scatter_dimension=0, tiled=True),
        lax.psum_scatter(grad_w_output, ("dp", "expert"), scatter_dimension=0, tiled=True),
        lax.psum_scatter(grad_w_router, ("dp", "expert"), scatter_dimension=0, tiled=True),
        lax.psum_scatter(grad_attn_gain, ("dp", "expert"), scatter_dimension=0, tiled=True),
        lax.psum_scatter(grad_mlp_gain, ("dp", "expert"), scatter_dimension=0, tiled=True),
        lax.psum_scatter(grad_query_gain, ("dp", "expert"), scatter_dimension=0, tiled=True),
        lax.psum_scatter(grad_key_gain, ("dp", "expert"), scatter_dimension=0, tiled=True),
    )
    (
        share_w_query,
        share_w_key,
        share_w_value,
        share_w_output,
        share_w_router,
        share_attn_gain,
        share_mlp_gain,
        share_query_gain,
        share_key_gain,
    ) = summed
    return (
        block_out,
        grad_in,
        share_attn_gain,
        share_query_gain,
        share_key_gain,
        share_w_query,
        share_w_key,
        share_w_value,
        share_w_output,
        share_mlp_gain,
        share_w_router,
        grad_w_gate,
        grad_w_up,
        grad_w_down,
    )


def place():
    z = lax.axis_index("dp")
    e = lax.axis_index("expert")
    return z, e


def line_order(z, nz, j, inner=False):
    near = jnp.minimum(z, nz - 1 - z)
    step = (j + 1) // 2
    step = step if j % 2 == 0 else -step
    if inner:
        step = jnp.where(z < nz - 1 - z, -step, step)
    tail = jnp.where(z < nz - 1 - z, j, nz - 1 - j)
    return jnp.where(j <= 2 * near, z + step, tail)


def greet(z, e, nz):
    barrier = pltpu.get_barrier_semaphore()
    for mate in (e ^ 1, e ^ 2, e ^ 4):
        pl.semaphore_signal(barrier, inc=1, device_id=(z, mate), device_id_type=MESH)

    @pl.when(z > 0)
    def _():
        pl.semaphore_signal(barrier, inc=1, device_id=(z - 1, e), device_id_type=MESH)

    @pl.when(z < nz - 1)
    def _():
        pl.semaphore_signal(barrier, inc=1, device_id=(z + 1, e), device_id_type=MESH)

    ends = (z > 0).astype(jnp.int32) + (z < nz - 1).astype(jnp.int32)
    pl.semaphore_wait(barrier, 3 + ends)


class Gather:
    Z, ZX, ZY, X3, X2, XQ, Y3, Y2, YQ, P0, PX3, PXQ, PY3, PYQ, PDX, PDY = range(16)
    KINDS = 16
    WHOLE, LOW, HIGH, LOW3, HIGH3, Q0, Q3 = (0, 4), (0, 2), (2, 2), (0, 3), (1, 3), (0, 1), (3, 1)

    def __init__(self, nz, shards, outs, send, recv, local):
        self.nz, self.shards, self.outs = nz, shards, outs
        self.send, self.recv, self.local = send, recv, local
        self.z, self.e = place()
        self.p, self.x, self.y, self.d = self.e ^ 1, self.e ^ 2, self.e ^ 4, self.e ^ 6

    def zz(self, j):
        return line_order(self.z, self.nz, j)

    def part(self, ref, piece):
        return ref.at[pl.ds(piece[0], piece[1])]

    def copy(self, i, kind, zz, ee, piece, dev, mine=False, sem=None):
        dst = self.part(self.outs[i].at[zz, ee], piece)
        return pltpu.make_async_remote_copy(
            src_ref=self.part(self.shards[i], piece) if mine else dst,
            dst_ref=dst,
            send_sem=self.send.at[i, zz, kind] if sem is None else sem,
            recv_sem=self.recv.at[i, zz, kind],
            device_id=dev,
            device_id_type=MESH,
        )

    def start(self, kind, zz, ee, piece, dev, mine=False):
        for i in range(len(self.outs)):
            self.copy(i, kind, zz, ee, piece, dev, mine).start()

    def arrived(self, kind, zz, ee, piece):
        for i in range(len(self.outs)):
            self.copy(i, kind, zz, ee, piece, (self.z, self.e)).wait_recv()

    def sent(self, kind, zz, ee, piece, mine=False):
        for i in range(len(self.outs)):
            self.copy(i, kind, zz, ee, piece, (self.z, self.e), mine).wait_send()

    def along(self, j, kind, ee, piece, act):
        z, e, nz = self.z, self.e, self.nz
        zz, mine = self.zz(j), j == 0 and kind == self.Z
        for i in range(len(self.outs)):
            @pl.when(jnp.logical_and(zz <= z, z < nz - 1))
            def _():
                act(self.copy(i, kind, zz, ee, piece, (z + 1, e), mine))

            @pl.when(jnp.logical_and(zz >= z, z > 0))
            def _():
                sem = self.local.at[1 + kind, i] if j == 0 else None
                act(self.copy(i, kind, zz, ee, piece, (z - 1, e), mine, sem))

    def keep(self, i):
        return pltpu.make_async_copy(self.shards[i], self.outs[i].at[self.z, self.e], self.local.at[0, i])

    def kept(self):
        for i in range(len(self.outs)):
            self.keep(i).wait()

    def launch(self, j):
        self.launch_line(j)
        self.launch_plane(j)

    def launch_line(self, j):
        e, zz, mine = self.e, self.zz(j), j == 0
        if not mine:
            self.arrived(self.Z, zz, e, self.WHOLE)
        else:
            self.start(self.XQ, zz, e, self.Q3, (self.z, self.x), mine)
            self.start(self.YQ, zz, e, self.Q0, (self.z, self.y), mine)
        self.along(j, self.Z, e, self.WHOLE, lambda c: c.start())

    def launch_plane(self, j):
        z, e, zz, mine = self.z, self.e, self.zz(j), j == 0
        self.start(self.X3, zz, e, self.LOW3, (z, self.x), mine)
        self.start(self.Y3, zz, e, self.HIGH3, (z, self.y), mine)
        self.start(self.P0, zz, e, self.WHOLE, (z, self.p), mine)
        if mine:
            for i in range(len(self.outs)):
                self.keep(i).start()

    def mates(self, j):
        zz, mine = self.zz(j), j == 0
        self.arrived(self.XQ if mine else self.ZX, zz, self.x, self.Q3)
        self.along(j, self.ZX, self.x, self.Q3, lambda c: c.start())
        self.start(self.PXQ, zz, self.x, self.Q3, (self.z, self.p))
        self.arrived(self.YQ if mine else self.ZY, zz, self.y, self.Q0)
        self.along(j, self.ZY, self.y, self.Q0, lambda c: c.start())
        self.start(self.PYQ, zz, self.y, self.Q0, (self.z, self.p))

    def relay(self, j):
        zz = self.zz(j)
        self.arrived(self.X3, zz, self.x, self.LOW3)
        self.start(self.Y2, zz, self.x, self.HIGH, (self.z, self.y))
        self.start(self.PX3, zz, self.x, self.LOW3, (self.z, self.p))
        self.arrived(self.Y3, zz, self.y, self.HIGH3)
        self.start(self.X2, zz, self.y, self.LOW, (self.z, self.x))
        self.start(self.PY3, zz, self.y, self.HIGH3, (self.z, self.p))

    def finish(self, j):
        zz = self.zz(j)
        self.arrived(self.X2, zz, self.d, self.LOW)
        self.start(self.PDX, zz, self.d, self.LOW, (self.z, self.p))
        self.arrived(self.Y2, zz, self.d, self.HIGH)
        self.start(self.PDY, zz, self.d, self.HIGH, (self.z, self.p))

    def shared_near(self, j):
        zz, p = self.zz(j), self.p
        self.arrived(self.P0, zz, p, self.WHOLE)
        self.arrived(self.PXQ, zz, p ^ 2, self.Q3)
        self.arrived(self.PX3, zz, p ^ 2, self.LOW3)

    def shared_far(self, j):
        zz, p = self.zz(j), self.p
        self.arrived(self.PYQ, zz, p ^ 4, self.Q0)
        self.arrived(self.PY3, zz, p ^ 4, self.HIGH3)
        self.arrived(self.PDX, zz, p ^ 6, self.LOW)
        self.arrived(self.PDY, zz, p ^ 6, self.HIGH)

    def drain(self, j, kept=False):
        zz, e, mine = self.zz(j), self.e, j == 0
        if mine:
            self.sent(self.XQ, zz, e, self.Q3, mine)
            self.sent(self.YQ, zz, e, self.Q0, mine)
            if not kept:
                self.kept()
        for kind, ee, piece in ((self.Z, e, self.WHOLE), (self.ZX, self.x, self.Q3), (self.ZY, self.y, self.Q0)):
            self.along(j, kind, ee, piece, lambda c: c.wait_send())
        self.sent(self.X3, zz, e, self.LOW3, mine)
        self.sent(self.Y3, zz, e, self.HIGH3, mine)
        self.sent(self.P0, zz, e, self.WHOLE, mine)
        self.sent(self.PXQ, zz, self.x, self.Q3)
        self.sent(self.PYQ, zz, self.y, self.Q0)
        self.sent(self.Y2, zz, self.x, self.HIGH)
        self.sent(self.X2, zz, self.y, self.LOW)
        self.sent(self.PX3, zz, self.x, self.LOW3)
        self.sent(self.PY3, zz, self.y, self.HIGH3)
        self.sent(self.PDX, zz, self.d, self.LOW)
        self.sent(self.PDY, zz, self.d, self.HIGH)

    def steps(self):
        n = self.nz
        todo = [(self.launch, 0), (self.mates, 0)]
        for j in range(1, n + 2):
            todo += [(self.launch, j), (self.mates, j - 1) if j > 1 else None, (self.relay, j - 1), (self.finish, j - 2)]
        return [functools.partial(f, j) for f, j in filter(None, todo) if 0 <= j < n]


def gather_kernel(nz, count, *refs):
    shards, outs = refs[:count], refs[count : 2 * count]
    send, recv, local = refs[2 * count :]
    z, e = place()
    greet(z, e, nz)
    g = Gather(nz, shards, outs, send, recv, local)
    for step in g.steps():
        step()
    for j in range(nz):
        g.shared_near(j)
        g.shared_far(j)
    for j in range(nz):
        g.drain(j)


def gather_scratch(nz, count):
    return [
        pltpu.SemaphoreType.DMA((count, nz, Gather.KINDS)),
        pltpu.SemaphoreType.DMA((count, nz, Gather.KINDS)),
        pltpu.SemaphoreType.DMA((4, count)),
    ]


def gather_all(arrays, collective_id):
    nz, width = lax.axis_size("dp"), lax.axis_size("expert")
    count = len(arrays)
    parts = [a.reshape((4, a.shape[0] // 4) + a.shape[1:]) for a in arrays]
    outs = pl.pallas_call(
        functools.partial(gather_kernel, nz, count),
        out_shape=[jax.ShapeDtypeStruct((nz, width) + h.shape, h.dtype) for h in parts],
        in_specs=[pl.BlockSpec(memory_space=pltpu.VMEM)] * count,
        out_specs=[pl.BlockSpec(memory_space=pl.ANY)] * count,
        scratch_shapes=gather_scratch(nz, count),
        compiler_params=pltpu.CompilerParams(
            collective_id=collective_id, has_side_effects=True, vmem_limit_bytes=VMEM_LIMIT
        ),
        name="gather_all",
    )(*parts)
    return [o.reshape((nz * width * a.shape[0],) + a.shape[1:]) for o, a in zip(outs, arrays)]


def accumulate(dst, src):
    rows = dst.shape[0]
    block = 32 if rows % 32 == 0 else rows
    if rows == block:
        dst[...] = dst[...] + src[...]
        return

    def body(r, _):
        at = pl.ds(pl.multiple_of(r * block, block), block)
        dst[at, :] = dst[at, :] + src[at, :]
        return 0

    lax.fori_loop(0, rows // block, body, 0)


class Scatter:
    X2, Y2, X3, Y3, Z, ZB, ZX, ZXB, ZY, ZYB, XQ, YQ = range(4, 16)
    KINDS = 16
    BUFFERS = 9

    def __init__(self, nz, terms, outs, sums, temps, from_x2, from_y2, from_x3, from_y3, from_z, from_zm, from_q, send, recv, local):
        self.nz, self.terms, self.outs = nz, terms, outs
        self.sums, self.temps = sums, temps
        self.from_x2, self.from_y2, self.from_x3, self.from_y3 = from_x2, from_y2, from_x3, from_y3
        self.from_z, self.from_zm, self.from_q = from_z, from_zm, from_q
        self.send, self.recv, self.local = send, recv, local
        self.count = len(terms)
        self.z, self.e = place()
        self.core, self.chip = self.e % 2, self.e // 2
        self.p, self.x, self.y = self.e ^ 1, self.e ^ 2, self.e ^ 4
        self.chips = (self.chip ^ 3, self.chip ^ 1, self.chip ^ 2, self.chip)

    def zz(self, j):
        return line_order(self.z, self.nz, self.nz - 1 - j, True)

    def remote(self, i, kind, zz, src, dst, dev):
        return pltpu.make_async_remote_copy(
            src_ref=src, dst_ref=dst, send_sem=self.send.at[i, zz, kind], recv_sem=self.recv.at[i, zz, kind],
            device_id=dev, device_id_type=MESH)

    def quarters(self, i, zz, q, first, n):
        return self.sums[i].at[zz, q, pl.ds(first, n)]

    def pair(self, i, j, q):
        zz, chip = self.zz(j), self.chips[q]
        return self.remote(i, q, zz, self.terms[i].at[zz, chip * 2 + (1 - self.core)], self.sums[i].at[zz, q],
                           (self.z, self.p))

    def load(self, i, j, q):
        slot = q % 2
        return pltpu.make_async_copy(
            self.terms[i].at[self.zz(j), self.chips[q] * 2 + self.core], self.temps[i].at[slot], self.local.at[i, slot])

    def x2(self, i, zz):
        return self.remote(i, self.X2, zz, self.quarters(i, zz, 0, 0, 2), self.from_x2[i].at[zz], (self.z, self.x))

    def y2(self, i, zz):
        return self.remote(i, self.Y2, zz, self.quarters(i, zz, 0, 2, 2), self.from_y2[i].at[zz], (self.z, self.y))

    def x3(self, i, zz):
        return self.remote(i, self.X3, zz, self.quarters(i, zz, 1, 0, 3), self.from_x3[i].at[zz], (self.z, self.x))

    def y3(self, i, zz):
        return self.remote(i, self.Y3, zz, self.quarters(i, zz, 2, 1, 3), self.from_y3[i].at[zz], (self.z, self.y))

    def xq(self, i):
        return self.remote(i, self.XQ, self.z, self.quarters(i, self.z, 1, 3, 1), self.from_q[i].at[pl.ds(0, 1)], (self.z, self.x))

    def yq(self, i):
        return self.remote(i, self.YQ, self.z, self.quarters(i, self.z, 2, 0, 1), self.from_q[i].at[pl.ds(1, 1)], (self.z, self.y))

    def line(self, i, zz, which, dz, last=False):
        slot = self.nz if last else zz
        kind = (self.Z, self.ZX, self.ZY)[which] + int(last)
        src = (self.sums[i].at[zz, 3], self.quarters(i, zz, 1, 3, 1), self.quarters(i, zz, 2, 0, 1))[which]
        dst = self.from_z[i].at[slot] if which == 0 else self.from_zm[i].at[slot, pl.ds(which - 1, 1)]
        return self.remote(i, kind, zz, src, dst, (self.z + dz, self.e))

    def add(self, i, zz, q, first, n, src):
        for k in range(n):
            accumulate(self.sums[i].at[zz, q, first + k], src.at[k])

    def begin(self):
        for j in range(self.nz):
            for q in range(4):
                for i in range(self.count):
                    self.pair(i, j, q).start()
        for i in range(self.count):
            self.load(i, 0, 0).start()

    def first(self, j):
        zz = self.zz(j)
        for q in range(4):
            for i in range(self.count):
                if q < 3:
                    self.load(i, j, q + 1).start()
                elif j < self.nz - 1:
                    self.load(i, j + 1, 0).start()
                self.pair(i, j, q).wait_recv()
                self.load(i, j, q).wait()
                self.add(i, zz, q, 0, 4, self.temps[i].at[q % 2])
                if q == 0:
                    self.x2(i, zz).start()
                    self.y2(i, zz).start()

    def second(self, j):
        zz = self.zz(j)
        for i in range(self.count):
            self.y2(i, zz).wait_recv()
            self.add(i, zz, 1, 2, 2, self.from_y2[i].at[zz])
            self.x3(i, zz).start()
            self.x2(i, zz).wait_recv()
            self.add(i, zz, 2, 0, 2, self.from_x2[i].at[zz])
            self.y3(i, zz).start()
        for i in range(self.count):
            for which in (1, 2):
                self.flow(i, j, which)

    def flow(self, i, j, which):
        z, nz, zz = self.z, self.nz, self.zz(j)
        q, first, n = ((3, 0, 4), (1, 3, 1), (2, 0, 1))[which]

        def came(slot):
            ref = self.from_z[i].at[slot] if which == 0 else self.from_zm[i].at[slot, pl.ds(which - 1, 1)]
            self.add(i, zz, q, first, n, ref)

        if j < nz - 1:
            @pl.when(jnp.logical_or(jnp.logical_and(zz > z, z > 0), jnp.logical_and(zz < z, z < nz - 1)))
            def _():
                self.line(i, zz, which, 1).wait_recv()
                came(zz)

            @pl.when(zz > z)
            def _():
                self.line(i, zz, which, 1).start()

            @pl.when(zz < z - 1)
            def _():
                self.line(i, zz, which, -1).start()

            @pl.when(zz == z - 1)
            def _():
                self.line(i, zz, which, -1, True).start()
        else:
            @pl.when(z > 0)
            def _():
                self.line(i, zz, which, 1).wait_recv()
                came(zz)

            @pl.when(z < nz - 1)
            def _():
                self.line(i, zz, which, -1, True).wait_recv()
                came(nz)

            if which == 1:
                self.xq(i).start()
            if which == 2:
                self.yq(i).start()

    def third(self, j):
        zz = self.zz(j)
        for i in range(self.count):
            self.x3(i, zz).wait_recv()
            self.add(i, zz, 3, 0, 3, self.from_x3[i].at[zz])
            self.y3(i, zz).wait_recv()
            self.add(i, zz, 3, 1, 3, self.from_y3[i].at[zz])
        for i in range(self.count):
            self.flow(i, j, 0)

    def result(self):
        for i in range(self.count):
            self.xq(i).wait_recv()
            self.add(i, self.z, 3, 3, 1, self.from_q[i].at[pl.ds(0, 1)])
            self.yq(i).wait_recv()
            self.add(i, self.z, 3, 0, 1, self.from_q[i].at[pl.ds(1, 1)])
            self.outs[i][...] = self.sums[i][self.z, 3].astype(self.outs[i].dtype)

    def drain(self, j):
        z, nz = self.z, self.nz
        zz = self.zz(j)
        for i in range(self.count):
            for q in range(4):
                self.pair(i, j, q).wait_send()
            for c in (self.x2, self.y2, self.x3, self.y3):
                c(i, zz).wait_send()
            if j < nz - 1:
                for which in range(3):
                    @pl.when(zz > z)
                    def _():
                        self.line(i, zz, which, 1).wait_send()

                    @pl.when(zz < z - 1)
                    def _():
                        self.line(i, zz, which, -1).wait_send()

                    @pl.when(zz == z - 1)
                    def _():
                        self.line(i, zz, which, -1, True).wait_send()
            else:
                self.xq(i).wait_send()
                self.yq(i).wait_send()

    def steps(self):
        todo = []
        for j in range(self.nz + 2):
            todo += [(self.first, j), (self.second, j - 1), (self.third, j - 2)]
        return [functools.partial(f, j) for f, j in todo if 0 <= j < self.nz] + [self.result]


def scatter_kernel(nz, count, *refs):
    groups = [refs[k * count : (k + 1) * count] for k in range(2 + Scatter.BUFFERS)]
    send, recv, local = refs[(2 + Scatter.BUFFERS) * count :]
    z, e = place()
    greet(z, e, nz)
    s = Scatter(nz, *groups, send, recv, local)
    s.begin()
    for step in s.steps():
        step()
    for j in range(nz):
        s.drain(j)


def scatter_buffers(nz, width, kinds):
    leads = ((nz, width // 2, 4), (2, 4), (nz, 2), (nz, 2), (nz, 3), (nz, 3), (nz + 1, 4), (nz + 1, 2), (2,))
    return [pltpu.VMEM(lead + shape, dtype) for lead in leads for shape, dtype in kinds] + [
        pltpu.SemaphoreType.DMA((len(kinds), nz, Scatter.KINDS)),
        pltpu.SemaphoreType.DMA((len(kinds), nz, Scatter.KINDS)),
        pltpu.SemaphoreType.DMA((len(kinds), 2)),
    ]


def scatter_sum(arrays, collective_id):
    nz, width = lax.axis_size("dp"), lax.axis_size("expert")
    count = len(arrays)
    devices = nz * width
    terms = [a.reshape(nz, width, 4, a.shape[0] // (4 * devices), a.shape[1]) for a in arrays]
    shapes = [t.shape[3:] for t in terms]
    outs = pl.pallas_call(
        functools.partial(scatter_kernel, nz, count),
        out_shape=[jax.ShapeDtypeStruct((4,) + s, jnp.float32) for s in shapes],
        in_specs=[pl.BlockSpec(memory_space=pl.ANY)] * count,
        out_specs=[pl.BlockSpec(memory_space=pltpu.VMEM)] * count,
        scratch_shapes=scatter_buffers(nz, width, [(s, a.dtype) for s, a in zip(shapes, arrays)]),
        compiler_params=pltpu.CompilerParams(
            collective_id=collective_id, has_side_effects=True, vmem_limit_bytes=VMEM_LIMIT
        ),
        name="scatter_sum",
    )(*terms)
    return [o.reshape(4 * s[0], s[1]) for o, s in zip(outs, shapes)]


def mm(a, b, da=1, db=0):
    return lax.dot_general(a, b, (((da,), (db,)), ((), ())), preferred_element_type=F32)


def rope(values, cosine, sine):
    return values * cosine + pltpu.roll(values, values.shape[1] // 2, 1) * sine


class AttentionGrad:
    def __init__(self, branch, w_out, raw, tables, gains, seg_col, seg_row, normed, attended, w_mixed,
                 grads, gain_grads, normed_grad, grad_out, grad_mixed,
                 w_buf, q_buf, k_buf, v_buf, mask, k_rot, v_low, dk, dv, a_buf, m_buf, out_stage, mixed_stage, sems):
        self.normed, self.attended, self.w_mixed = normed, attended, w_mixed
        self.normed_grad, self.grad_out, self.grad_mixed = normed_grad, grad_out, grad_mixed
        self.a_buf, self.m_buf, self.out_stage, self.mixed_stage = a_buf, m_buf, out_stage, mixed_stage
        self.branch, self.w_out, self.raw, self.tables, self.gains = branch, w_out, raw, tables, gains
        self.seg_col, self.seg_row, self.grads, self.gain_grads = seg_col, seg_row, grads, gain_grads
        self.w_buf, self.q_buf, self.k_buf, self.v_buf, self.mask = w_buf, q_buf, k_buf, v_buf, mask
        self.k_rot, self.v_low, self.dk, self.dv, self.sems = k_rot, v_low, dk, dv, sems
        self.cols = w_buf.shape[0]
        self.query_cols = w_out.shape[0]
        self.key_cols = k_buf.shape[1]
        self.count = self.query_cols // self.cols
        self.per_key = self.count // (self.key_cols // HEAD_DIM)
        self.total = self.count + 2 * self.key_cols // self.cols

    def at(self, t):
        return pl.ds(pl.multiple_of(t * self.cols, self.cols), self.cols)

    def fetch(self, t, slot):
        at = self.at(t)
        return pltpu.make_async_copy(self.raw.at[:, at], self.q_buf.at[slot], self.sems.at[1, slot])

    def fetch_out(self, t):
        at = self.at(t)
        return (
            pltpu.make_async_copy(self.w_out.at[at, :], self.w_buf, self.sems.at[0, 0]),
            pltpu.make_async_copy(self.attended.at[:, at], self.a_buf, self.sems.at[3, 0]),
        )

    def fetch_mixed(self, t):
        return pltpu.make_async_copy(self.w_mixed.at[:, self.at(t)], self.m_buf, self.sems.at[4, 0])

    def put_out(self, t):
        return pltpu.make_async_copy(self.out_stage, self.grad_out.at[self.at(t), :], self.sems.at[5, 0])

    def put_mixed(self, t):
        return pltpu.make_async_copy(self.mixed_stage, self.grad_mixed.at[:, self.at(t)], self.sems.at[5, 1])

    def prepare(self):
        q, k = self.query_cols, self.key_cols
        key = pltpu.make_async_copy(self.raw.at[:, pl.ds(q, k)], self.k_buf, self.sems.at[2, 0])
        value = pltpu.make_async_copy(self.raw.at[:, pl.ds(q + k, k)], self.v_buf, self.sems.at[2, 1])
        key.start()
        value.start()
        for c in self.fetch_out(0):
            c.start()
        self.fetch(0, 0).start()
        self.fetch_mixed(0).start()
        self.normed_grad[...] = jnp.zeros_like(self.normed_grad)
        self.mask[...] = allowed_mask(self.seg_col, self.seg_row)
        self.gain_grads[...] = jnp.zeros_like(self.gain_grads)
        key.wait()
        value.wait()

    def scaled(self, raw, which):
        scale = lax.rsqrt(jnp.mean(raw * raw, 1, keepdims=True) + EPS)
        return scale, (raw * scale) * self.gains[which : which + 1, :]

    def back(self, rot_grad, raw, scale, which):
        cosine, sine = self.tables[0], self.tables[1]
        grad = rope(rot_grad, cosine, -sine)
        part = jnp.sum(grad * raw * scale, 0, keepdims=True)
        self.gain_grads[which : which + 1, :] = self.gain_grads[which : which + 1, :] + part
        weighted = grad * self.gains[which : which + 1, :]
        mean = jnp.mean(weighted * raw, 1, keepdims=True)
        return scale * weighted - raw * (scale * scale * scale) * mean

    def step(self, t):
        slot = lax.rem(t, 2)

        @pl.when(t + 1 < self.count)
        def _():
            self.fetch(t + 1, 1 - slot).start()

        @pl.when(t < self.count)
        def _():
            self.heads(t, slot)

        self.fetch_mixed(t).wait()
        grads = self.grads[:, self.at(t)]
        self.normed_grad[...] += mm(grads, self.m_buf[...], 1, 1)

        @pl.when(t + 1 < self.total)
        def _():
            self.fetch_mixed(t + 1).start()

        @pl.when(t > 0)
        def _():
            self.put_mixed(t - 1).wait()

        self.mixed_stage[...] = mm(self.normed[...], grads, 0, 0).astype(BF16)
        self.put_mixed(t).start()

    def end(self):
        self.put_mixed(self.total - 1).wait()
        self.put_out(self.count - 1).wait()

    def heads(self, t, slot):
        self.fetch(t, slot).wait()
        for c in self.fetch_out(t):
            c.wait()

        @pl.when(t > 0)
        def _():
            self.put_out(t - 1).wait()

        self.out_stage[...] = mm(self.a_buf[...], self.branch[...], 0, 0).astype(BF16)
        self.put_out(t).start()
        cosine, sine = self.tables[0], self.tables[1]
        at_key = pl.ds(pl.multiple_of(t // self.per_key * HEAD_DIM, HEAD_DIM), HEAD_DIM)

        @pl.when(lax.rem(t, self.per_key) == 0)
        def _():
            _, key = self.scaled(self.k_buf[:, at_key], 1)
            self.k_rot[...] = rope(key, cosine, sine).astype(BF16)
            self.v_low[...] = self.v_buf[:, at_key].astype(BF16)
            self.dk[...] = jnp.zeros_like(self.dk)
            self.dv[...] = jnp.zeros_like(self.dv)

        score_scale = 1.0 / math.sqrt(HEAD_DIM)
        out_grad = mm(self.branch[...], self.w_buf[...], 1, 1).astype(BF16)

        @pl.when(t + 1 < self.count)
        def _():
            for c in self.fetch_out(t + 1):
                c.start()

        mask = self.mask[...] > 0.0
        k_rot, v_low = self.k_rot[...], self.v_low[...]
        for h in range(self.cols // HEAD_DIM):
            here = slice(h * HEAD_DIM, (h + 1) * HEAD_DIM)
            raw = self.q_buf[slot, :, here]
            scale, query = self.scaled(raw, 0)
            q_rot = rope(query, cosine, sine).astype(BF16)
            d_out = out_grad[:, here]
            scores = mm(q_rot, k_rot, 1, 1) * score_scale
            raised = jnp.where(mask, jnp.exp(scores), 0.0)
            probs = raised / jnp.sum(raised, 1, keepdims=True)
            self.dv[...] += mm(probs.astype(BF16), d_out, 0, 0)
            d_probs = mm(d_out, v_low, 1, 1)
            d_scores = (probs * (d_probs - jnp.sum(probs * d_probs, 1, keepdims=True))).astype(BF16)
            dq = mm(d_scores, k_rot) * score_scale
            self.dk[...] += mm(d_scores, q_rot, 0, 0)
            at = pl.ds(pl.multiple_of(t * self.cols + h * HEAD_DIM, HEAD_DIM), HEAD_DIM)
            self.grads[:, at] = self.back(dq, raw, scale, 0).astype(BF16)

        @pl.when(lax.rem(t, self.per_key) == self.per_key - 1)
        def _():
            raw = self.k_buf[:, at_key]
            scale, _ = self.scaled(raw, 1)
            shift = pl.multiple_of(t // self.per_key * HEAD_DIM, HEAD_DIM)
            self.grads[:, pl.ds(self.query_cols + shift, HEAD_DIM)] = self.back(
                self.dk[...] * score_scale, raw, scale, 1
            ).astype(BF16)
            self.grads[:, pl.ds(self.query_cols + self.key_cols + shift, HEAD_DIM)] = self.dv[...].astype(BF16)


def scatter_attention_kernel(nz, plan, term, *refs):
    inputs, (total, *outs), scratch = refs[:10], refs[10:16], refs[16:]
    buffers, rest = scratch[: Scatter.BUFFERS], scratch[Scatter.BUFFERS :]
    send, recv, local = rest[:3]
    z, e = place()
    greet(z, e, nz)
    s = Scatter(nz, [term], [total], *[[b] for b in buffers], send, recv, local)
    a = AttentionGrad(*inputs, *outs, *rest[3:])
    s.begin()
    a.prepare()
    steps = s.steps()
    run_beside(a.total, a.step, steps, plan)
    a.end()
    for j in range(nz):
        s.drain(j)


def run_beside(count, work, steps, plan):
    bounds = [sum(plan[:t]) for t in range(len(plan) + 1)]

    def body(t, _):
        for k in range(count):
            todo = steps[bounds[k] : bounds[k + 1]]
            if todo:
                @pl.when(t == k)
                def _():
                    for step in todo:
                        step()
        work(t)
        return 0

    lax.fori_loop(0, count, body, 0)
    for step in steps[bounds[count] :]:
        step()


def scatter_with_attention(terms, branch, w_out, raw, tables, gains, segments, normed, attended, w_mixed, collective_id):
    nz, width = lax.axis_size("dp"), lax.axis_size("expert")
    devices = nz * width
    length, model = branch.shape
    shape = (terms.shape[0] // (4 * devices), terms.shape[1])
    term = terms.reshape((nz, width, 4) + shape)
    heads = 4
    cols = heads * HEAD_DIM
    key_cols = (raw.shape[1] - w_out.shape[0]) // 2
    vmem = pl.BlockSpec(memory_space=pltpu.VMEM)
    hbm = pl.BlockSpec(memory_space=pl.ANY)
    plan = [3, 1, 1, 1, 1, 1, 1, 1, 1, 0]
    total, grads, gain_grads, normed_grad, grad_out, grad_mixed = pl.pallas_call(
        functools.partial(scatter_attention_kernel, nz, plan),
        out_shape=[
            jax.ShapeDtypeStruct((4,) + shape, F32),
            jax.ShapeDtypeStruct(raw.shape, BF16),
            jax.ShapeDtypeStruct((2, HEAD_DIM), F32),
            jax.ShapeDtypeStruct((length, model), F32),
            jax.ShapeDtypeStruct(w_out.shape, BF16),
            jax.ShapeDtypeStruct(w_mixed.shape, BF16),
        ],
        in_specs=[hbm, vmem, hbm, hbm, vmem, vmem, vmem, vmem, vmem, hbm, hbm],
        out_specs=[vmem, vmem, vmem, vmem, hbm, hbm],
        scratch_shapes=scatter_buffers(nz, width, [(shape, terms.dtype)])
        + [
            pltpu.VMEM((cols, model), BF16),
            pltpu.VMEM((2, length, cols), F32),
            pltpu.VMEM((length, key_cols), F32),
            pltpu.VMEM((length, key_cols), F32),
            pltpu.VMEM((length, length), F32),
            pltpu.VMEM((length, HEAD_DIM), BF16),
            pltpu.VMEM((length, HEAD_DIM), BF16),
            pltpu.VMEM((length, HEAD_DIM), F32),
            pltpu.VMEM((length, HEAD_DIM), F32),
            pltpu.VMEM((length, cols), BF16),
            pltpu.VMEM((model, cols), BF16),
            pltpu.VMEM((cols, model), BF16),
            pltpu.VMEM((model, cols), BF16),
            pltpu.SemaphoreType.DMA((6, 2)),
        ],
        compiler_params=pltpu.CompilerParams(
            collective_id=collective_id, has_side_effects=True, vmem_limit_bytes=VMEM_LIMIT
        ),
        name="scatter_attention",
    )(term, branch, w_out, raw, tables, gains, segments[:, None], segments[None, :], normed, attended, w_mixed)
    return total.reshape(4 * shape[0], shape[1]), gain_grads, normed_grad, grad_out, grad_mixed


TILE = 512


class ExpertWork:
    def __init__(self, nz, cap, group, orders, all_rows, all_tables, all_grads, weights, outs, bufs, sems):
        self.nz, self.cap, self.group = nz, cap, group
        self.all_rows, self.all_tables, self.all_grads = all_rows, all_tables, all_grads
        self.weights, self.outs, self.bufs, self.sems = weights, outs, bufs, sems
        self.z, self.e = place()
        self.width = all_rows.shape[1]
        self.orders = orders
        self.edge = jnp.logical_or(self.z == 0, self.z == nz - 1)

    def weight_copies(self):
        return [pltpu.make_async_copy(w, b, self.sems.at[0, i]) for i, (w, b) in enumerate(zip(self.weights, self.bufs[:3]))]

    def place_of(self, t):
        zz, half = jnp.int32(0), jnp.int32(0)
        for p, (ends, middle) in enumerate(zip(*self.orders)):
            for here, (j, h) in ((self.edge, ends), (jnp.logical_not(self.edge), middle)):
                here = jnp.logical_and(here, t == p)
                zz = jnp.where(here, line_order(self.z, self.nz, j), zz)
                half = jnp.where(here, h, half)
        near = self.e // self.group
        return zz, jnp.where(half == 0, near, 1 - near) * self.group

    def inputs(self, t, slot):
        zz, first = self.place_of(t)
        at = pl.ds(first, self.group)
        x, tab, g = self.bufs[3:6]
        return (
            pltpu.make_async_copy(self.all_rows.at[zz, at], x.at[slot], self.sems.at[1 + slot, 0]),
            pltpu.make_async_copy(self.all_tables.at[zz, at], tab.at[slot], self.sems.at[1 + slot, 1]),
            pltpu.make_async_copy(self.all_grads.at[zz, at], g.at[slot], self.sems.at[1 + slot, 2]),
        )

    def flat(self, t):
        step = self.group * self.cap
        return pl.ds(pl.multiple_of(t * step, step), step)

    def row_results(self, t):
        pairs = zip(self.bufs[8:10], self.outs[3:5])
        return [pltpu.make_async_copy(b, o.at[self.flat(t)], self.sems.at[3, i]) for i, (b, o) in enumerate(pairs)]

    def hidden_results(self, t):
        pairs = zip(self.bufs[10:13], self.outs[5:8])
        return [pltpu.make_async_copy(b, o.at[self.flat(t)], self.sems.at[3, 2 + i]) for i, (b, o) in enumerate(pairs)]

    def term_results(self, t, n, cols):
        zz, first = self.place_of(t)
        at = pl.ds(first, self.group)
        pairs = zip(self.bufs[6:8], self.outs[:2])
        return [
            pltpu.make_async_copy(b.at[:, :, cols], o.at[zz, at, :, cols], self.sems.at[4 + i, n])
            for i, (b, o) in enumerate(pairs)
        ]

    def begin(self):
        for c in self.weight_copies():
            c.start()

    def ready(self, p):
        for c in self.inputs(jnp.int32(p), p % 2):
            c.start()

    def step(self, t, hook):
        slot = lax.rem(t, 2)
        hook(0)
        cap, group = self.cap, self.group
        wg, wu, wd, xb, tb, gb, yb, rb, rowb, downb, actb, gpb, upb, cotb = self.bufs
        for c in self.inputs(t, slot):
            c.wait()

        @pl.when(t == 0)
        def _():
            for c in self.weight_copies():
                c.wait()

        self.free(t, self.row_results)
        length, width = xb.shape[2] * xb.shape[3], xb.shape[4]
        lanes = tb.shape[4]
        me = self.z * self.width + self.e
        total = self.nz * self.width
        lane = lax.broadcasted_iota(jnp.int32, (8, lanes), 1)
        row = lax.broadcasted_iota(jnp.int32, (8, lanes), 0)
        gate_lanes = jnp.logical_and(row == 0, jnp.logical_or(lane == me, lane == total + me))
        rank_lane = jnp.logical_and(row == 1, lane == 2 * total + me)
        select = jnp.where(jnp.logical_or(gate_lanes, rank_lane), 1.0, 0.0).astype(BF16)
        slots = lax.broadcasted_iota(jnp.int32, (cap, length), 0).astype(F32)
        picks, gates = [], []
        for s in range(group):
            info = mm(select, tb[slot, s].reshape(length, lanes), 1, 1)
            hit = slots == info[1:2]
            pick = hit.astype(BF16)
            picks.append(pick)
            gate = jnp.sum(jnp.where(hit, info[0:1], 0.0), 1, keepdims=True)
            gates.append(gate)
            at = pl.ds(s * cap, cap)
            rowb[at, :] = mm(pick, xb[slot, s].reshape(length, width)).astype(BF16)
            cot = mm(pick, gb[slot, s].reshape(length, width))
            cotb[at, :] = cot.astype(BF16)
            downb[at, :] = (gate * cot).astype(BF16)
        for c in self.row_results(t):
            c.start()
        hook(1)
        gate_all = jnp.concatenate(gates, 0)
        rows = rowb[...]
        pre_gate = mm(rows, wg[...])
        pre_up = mm(rows, wu[...])
        sig = jax.nn.sigmoid(pre_gate)
        silu = pre_gate * sig
        self.free(t, self.hidden_results)
        actb[...] = (silu * pre_up).astype(BF16)
        hook(2)
        act_grad = mm(downb[...], wd[...], 1, 1)
        gpb[...] = (act_grad * pre_up * sig * (1.0 + pre_gate * (1.0 - sig))).astype(BF16)
        upb[...] = (act_grad * silu).astype(BF16)
        for c in self.hidden_results(t):
            c.start()
        gg = jnp.zeros((group * cap, 1), F32)
        for n in range(width // TILE):
            hook(3 + n)
            cols = pl.ds(n * TILE, TILE)
            self.free(t, lambda s: self.term_results(s, n, cols))
            out = mm(actb[...], wd[:, cols]).astype(BF16).astype(F32)
            gg = gg + jnp.sum(out * cotb[:, cols].astype(F32), 1, keepdims=True)
            out = (out * gate_all).astype(BF16)
            back = (mm(gpb[...], wg[cols, :], 1, 1) + mm(upb[...], wu[cols, :], 1, 1)).astype(BF16)
            for s in range(group):
                part = slice(s * cap, (s + 1) * cap)
                yb[s, :, cols] = mm(picks[s], out[part], 0, 0).astype(BF16)
                rb[s, :, cols] = mm(picks[s], back[part], 0, 0).astype(BF16)
            for c in self.term_results(t, n, cols):
                c.start()
        zz, first = self.place_of(t)
        first = zz * self.width + first
        for s in range(group):
            self.outs[2][first + s] = jnp.sum(
                picks[s].astype(F32) * gg[s * cap : (s + 1) * cap], 0, keepdims=True
            )

    def free(self, t, copies):
        @pl.when(t > 0)
        def _():
            for c in copies(t - 1):
                c.wait()

    def end(self):
        t = jnp.int32(len(self.orders[0]) - 1)
        for c in self.row_results(t) + self.hidden_results(t):
            c.wait()
        for n in range(self.bufs[13].shape[1] // TILE):
            for c in self.term_results(t, n, pl.ds(n * TILE, TILE)):
                c.wait()


def gather_expert_kernel(nz, cap, group, *refs):
    shards, all_grads, weights = refs[:2], refs[2], refs[3:6]
    gathered, outs = refs[6:8], refs[8:16]
    send, recv, local = refs[16:19]
    bufs, sems = refs[19:33], refs[33]
    z, e = place()
    greet(z, e, nz)
    g = Gather(nz, shards, gathered, send, recv, local)
    plain = tuple((j, h) for j in range(nz) for h in range(2))
    orders = ORDERS.get(nz) or (plain, plain)
    plans = RELAYS.get(nz) or (relays_first(g, orders[0]),) * 2
    w = ExpertWork(nz, cap, group, orders, gathered[0], gathered[1], all_grads, weights, outs, bufs, sems)
    w.begin()
    relays = {"L": g.launch_line, "K": g.launch_plane, "M": g.mates, "R": g.relay, "F": g.finish}

    def run(name, order):
        kind, j = name[0], int(name[1:])
        if kind == "I":
            place, half = order[j]
            (g.shared_far if half else g.shared_near)(place)
            if place == 0 and half == 0:
                g.kept()
            w.ready(j)
        else:
            relays[kind](j)

    def body(t, _):
        def hook(k):
            for plan, order, here in zip(plans, orders, (w.edge, jnp.logical_not(w.edge))):
                for piece, part, names in plan:
                    if part == k:
                        @pl.when(jnp.logical_and(t == piece, here))
                        def _():
                            for name in names.split():
                                run(name, order)

        w.step(t, hook)
        return 0

    lax.fori_loop(0, len(orders[0]), body, 0)
    w.end()
    for j in range(nz):
        g.drain(j, True)


def relays_first(g, order):
    head = []
    for f in g.steps():
        kind, j = f.func.__name__, f.args[0]
        names = {"launch": "L%d K%d", "mates": "M%d", "relay": "R%d", "finish": "F%d"}[kind]
        head.append((0, 0, names.replace("%d", str(j))))
    return head + [(p, 0, "I%d" % p) for p in range(len(order))]


ORDERS = {
    4: (
        ((0, 0), (1, 0), (0, 1), (1, 1), (2, 0), (2, 1), (3, 0), (3, 1)),
        ((0, 0), (1, 0), (0, 1), (2, 0), (1, 1), (3, 0), (2, 1), (3, 1)),
    )
}
RELAYS = {
    4: (
        (
            (0, 0, "L0 K0 M0"),
            (0, 0, "L1 K1 R0"),
            (0, 0, "I0"),
            (0, 1, "M1"),
            (0, 5, "R1"),
            (1, 0, "I1"),
            (1, 2, "F0"),
            (1, 4, "L2 K2 I2"),
            (2, 1, "F1"),
            (2, 2, "M2 I3"),
            (3, 2, "R2"),
            (3, 4, "I4"),
            (4, 1, "L3 K3"),
            (4, 2, "F2"),
            (4, 5, "I5 M3"),
            (5, 3, "R3"),
            (5, 5, "I6"),
            (6, 3, "F3"),
            (6, 6, "I7"),
        ),
        (
            (0, 0, "L0 K0 M0"),
            (0, 0, "L1 L2 K1"),
            (0, 0, "R0 K2 I0"),
            (0, 1, "M1 M2"),
            (0, 4, "R1"),
            (0, 6, "I1"),
            (1, 2, "F0"),
            (1, 4, "L3 K3 I2"),
            (2, 2, "M3"),
            (2, 3, "R2"),
            (2, 5, "I3"),
            (3, 2, "F1"),
            (3, 5, "I4"),
            (4, 4, "R3"),
            (4, 6, "I5"),
            (5, 2, "F2"),
            (5, 5, "I6"),
            (6, 1, "F3"),
            (6, 3, "I7"),
        ),
    )
}


def gather_with_experts(rows, table, all_grads, w_gate, w_up, w_down, cap, collective_id):
    nz, width = lax.axis_size("dp"), lax.axis_size("expert")
    devices, group = nz * width, 4
    length, model = rows.shape
    ff = w_gate.shape[1]
    quarter = length // 4
    shards = [a.reshape(4, quarter, a.shape[1]) for a in (rows, table)]
    step, picked = group * cap, devices * cap
    vmem = pl.BlockSpec(memory_space=pltpu.VMEM)
    hbm = pl.BlockSpec(memory_space=pl.ANY)
    block = lambda a: pltpu.VMEM((2, group) + a.shape, a.dtype)
    shape = lambda *dims: jax.ShapeDtypeStruct(dims, BF16)
    outs = pl.pallas_call(
        functools.partial(gather_expert_kernel, nz, cap, group),
        out_shape=[shape(nz, width, *s.shape) for s in shards]
        + [
            shape(nz, width, length, model),
            shape(nz, width, length, model),
            jax.ShapeDtypeStruct((devices, 1, length), F32),
            shape(picked, model),
            shape(picked, model),
            shape(picked, ff),
            shape(picked, ff),
            shape(picked, ff),
        ],
        in_specs=[vmem, vmem, hbm, hbm, hbm, hbm],
        out_specs=[hbm, hbm, hbm, hbm, vmem, hbm, hbm, hbm, hbm, hbm],
        scratch_shapes=gather_scratch(nz, 2)
        + [pltpu.VMEM(w.shape, BF16) for w in (w_gate, w_up, w_down)]
        + [block(shards[0]), block(shards[1]), block(shards[0])]
        + [pltpu.VMEM((group, length, model), BF16)] * 2
        + [pltpu.VMEM((step, n), BF16) for n in (model, model, ff, ff, ff, model)]
        + [pltpu.SemaphoreType.DMA((6, max(5, model // TILE)))],
        compiler_params=pltpu.CompilerParams(
            collective_id=collective_id, has_side_effects=True, vmem_limit_bytes=VMEM_LIMIT
        ),
        name="gather_experts",
    )(*shards, all_grads.reshape((nz, width) + shards[0].shape), w_gate, w_up, w_down)
    return outs[2:]


class Attention:
    def __init__(self, columns, hidden, w_mixed, w_out, small, head_map, tables, seg_col, seg_row, raw, normed, attended, branch,
                 w_buf, o_buf, kv_buf, small_buf, gains, mask, k_rot, v_low, sems):
        self.columns, self.hidden, self.w_mixed, self.w_out = columns, hidden, w_mixed, w_out
        self.small, self.head_map, self.small_buf = small, head_map, small_buf
        self.tables, self.gains, self.seg_col, self.seg_row = tables, gains, seg_col, seg_row
        self.raw, self.normed, self.attended, self.branch = raw, normed, attended, branch
        self.w_buf, self.o_buf, self.kv_buf, self.mask = w_buf, o_buf, kv_buf, mask
        self.k_rot, self.v_low, self.sems = k_rot, v_low, sems
        self.cols = w_buf.shape[-1]
        self.query_cols = attended.shape[1]
        self.key_cols = kv_buf.shape[-1] // 2
        self.count = self.query_cols // self.cols
        self.per_key = self.count // (self.key_cols // HEAD_DIM)

    def fetch(self, t, slot):
        at = pl.ds(pl.multiple_of(t * self.cols, self.cols), self.cols)
        owners = self.o_buf.shape[1]
        blocks = self.w_out.shape[1] // owners
        return (
            pltpu.make_async_copy(self.w_mixed.at[:, :, :, :, at], self.w_buf.at[slot], self.sems.at[0, slot]),
            pltpu.make_async_copy(
                self.w_out.at[t // blocks, pl.ds(lax.rem(t, blocks) * owners, owners)], self.o_buf.at[slot], self.sems.at[1, slot]
            ),
        )

    def prepare(self):
        kv = pltpu.make_async_copy(
            self.w_mixed.at[:, :, :, :, pl.ds(self.query_cols, 2 * self.key_cols)], self.kv_buf, self.sems.at[2, 0]
        )
        small = pltpu.make_async_copy(self.small, self.small_buf, self.sems.at[2, 1])
        small.start()
        kv.start()
        for c in self.fetch(0, 0):
            c.start()
        values = self.hidden[...].astype(F32)
        scale = lax.rsqrt(jnp.mean(values * values, 1, keepdims=True) + EPS)
        small.wait()
        model, lanes = values.shape[1], self.small_buf.shape[-1]
        lane = lax.broadcasted_iota(jnp.int32, (8, lanes), 1)
        row = lax.broadcasted_iota(jnp.int32, (8, lanes), 0)
        select = jnp.zeros((8, lanes), F32)
        for k, column in enumerate(self.columns):
            select = jnp.where(jnp.logical_and(row == k, lane == column), 1.0, select)
        info = mm(select.astype(BF16), self.small_buf[...].reshape(model, lanes), 1, 1)
        self.normed[...] = (values * scale * info[0:1]).astype(BF16)
        self.gains[...] = mm(info.astype(BF16), self.head_map[...])
        self.branch[...] = jnp.zeros_like(self.branch)
        self.mask[...] = allowed_mask(self.seg_col, self.seg_row)
        kv.wait()
        self.raw[:, self.query_cols :] = mm(self.normed[...], self.kv_buf[...].reshape(model, 2 * self.key_cols))

    def step(self, t):
        slot = lax.rem(t, 2)

        @pl.when(t + 1 < self.count)
        def _():
            for c in self.fetch(t + 1, 1 - slot):
                c.start()

        for c in self.fetch(t, slot):
            c.wait()
        cosine, sine = self.tables[0], self.tables[1]

        @pl.when(lax.rem(t, self.per_key) == 0)
        def _():
            shift = pl.multiple_of(t // self.per_key * HEAD_DIM, HEAD_DIM)
            key = head_norm(self.raw[:, pl.ds(self.query_cols + shift, HEAD_DIM)], self.gains[2:3, :])
            self.k_rot[...] = rope(key, cosine, sine).astype(BF16)
            self.v_low[...] = self.raw[:, pl.ds(self.query_cols + self.key_cols + shift, HEAD_DIM)].astype(BF16)

        at = pl.ds(pl.multiple_of(t * self.cols, self.cols), self.cols)
        query_raw = mm(self.normed[...], self.w_buf[slot].reshape(self.normed.shape[1], self.cols))
        self.raw[:, at] = query_raw
        mask = self.mask[...] > 0.0
        k_rot, v_low = self.k_rot[...], self.v_low[...]
        outs = []
        for h in range(self.cols // HEAD_DIM):
            query = head_norm(query_raw[:, h * HEAD_DIM : (h + 1) * HEAD_DIM], self.gains[1:2, :])
            q_rot = rope(query, cosine, sine).astype(BF16)
            scores = mm(q_rot, k_rot, 1, 1) * (1.0 / math.sqrt(HEAD_DIM))
            raised = jnp.where(mask, jnp.exp(scores), 0.0)
            probs = (raised / jnp.sum(raised, 1, keepdims=True)).astype(BF16)
            outs.append(mm(probs, v_low).astype(BF16))
        out = jnp.concatenate(outs, 1)
        self.attended[:, at] = out
        self.branch[...] += mm(out, self.o_buf[slot].reshape(self.cols, self.normed.shape[1]))


def head_norm(raw, gain):
    return raw * lax.rsqrt(jnp.mean(raw * raw, 1, keepdims=True) + EPS) * gain


def allowed_mask(seg_col, seg_row):
    length = seg_col.shape[0]
    row = lax.broadcasted_iota(jnp.int32, (length, length), 0)
    col = lax.broadcasted_iota(jnp.int32, (length, length), 1)
    same = seg_col[...] == seg_row[...]
    return jnp.where(jnp.logical_and(same, col <= row), 1.0, 0.0)


def gather_attention_kernel(nz, plan, columns, *refs):
    shards, inputs = refs[:4], refs[4:9]
    gathered, outs = refs[9:13], refs[13:17]
    scratch = refs[17:]
    z, e = place()
    greet(z, e, nz)
    w = Gather(nz, shards[:3], gathered[:3], *scratch[:3])
    g = Gather(nz, shards[3:], gathered[3:], *scratch[3:6])
    hidden, head_map, tables, seg_col, seg_row = inputs
    a = Attention(columns, hidden, *gathered[:3], head_map, tables, seg_col, seg_row, *outs, *scratch[6:])
    first, steps = w.steps(), g.steps()
    for step in first[:-2]:
        step()
    steps[0]()
    first[-2]()
    steps[1]()
    first[-1]()
    for j in range(nz):
        w.shared_near(j)
        w.shared_far(j)
    w.kept()
    a.prepare()
    run_beside(a.count, a.step, steps[2:], plan)
    for j in range(nz):
        g.shared_near(j)
        g.shared_far(j)
    for j in range(nz):
        w.drain(j, True)
        g.drain(j)


def gather_with_attention(w_mixed, w_out, small, rows, columns, hidden, head_map, tables, segments, collective_id):
    nz, width = lax.axis_size("dp"), lax.axis_size("expert")
    length, model = hidden.shape
    shards = [a.reshape((4, a.shape[0] // 4) + a.shape[1:]) for a in (w_mixed, w_out, small, rows)]
    cols = 4 * HEAD_DIM
    mixed, query_cols = w_mixed.shape[1], w_out.shape[0] * nz * width
    owners = cols // w_out.shape[0]
    vmem = pl.BlockSpec(memory_space=pltpu.VMEM)
    hbm = pl.BlockSpec(memory_space=pl.ANY)
    lead = (nz, width) + shards[0].shape[:2]
    outs = pl.pallas_call(
        functools.partial(gather_attention_kernel, nz, [0, 0, 2, 1, 1, 1, 2, 2], columns),
        out_shape=[jax.ShapeDtypeStruct((nz, width) + s.shape, s.dtype) for s in shards]
        + [
            jax.ShapeDtypeStruct((length, mixed), F32),
            jax.ShapeDtypeStruct((length, model), BF16),
            jax.ShapeDtypeStruct((length, query_cols), BF16),
            jax.ShapeDtypeStruct((length, model), F32),
        ],
        in_specs=[vmem] * 9,
        out_specs=[hbm] * 4 + [vmem] * 4,
        scratch_shapes=gather_scratch(nz, 3)
        + gather_scratch(nz, 1)
        + [
            pltpu.VMEM((2,) + lead + (cols,), BF16),
            pltpu.VMEM((2, owners) + shards[1].shape, BF16),
            pltpu.VMEM(lead + (mixed - query_cols,), BF16),
            pltpu.VMEM((nz, width) + shards[2].shape, BF16),
            pltpu.VMEM((8, HEAD_DIM), F32),
            pltpu.VMEM((length, length), F32),
            pltpu.VMEM((length, HEAD_DIM), BF16),
            pltpu.VMEM((length, HEAD_DIM), BF16),
            pltpu.SemaphoreType.DMA((3, 2)),
        ],
        compiler_params=pltpu.CompilerParams(
            collective_id=collective_id, has_side_effects=True, vmem_limit_bytes=VMEM_LIMIT
        ),
        name="gather_attention",
    )(*shards, hidden, head_map, tables, segments[:, None], segments[None, :])
    whole = [o.reshape((-1, o.shape[-1])) for o in outs[:4]]
    return whole + list(outs[4:])


class ExpertGrads:
    TILE = 256

    def __init__(self, rows, down, act, gate_pre, up_pre, grad_gate, grad_up, grad_down,
                 tile, gate_buf, up_buf, gate_stage, up_stage, sems):
        self.rows, self.down, self.act, self.gate_pre, self.up_pre = rows, down, act, gate_pre, up_pre
        self.grad_gate, self.grad_up, self.grad_down = grad_gate, grad_up, grad_down
        self.tile, self.gate_buf, self.up_buf = tile, gate_buf, up_buf
        self.gate_stage, self.up_stage, self.sems = gate_stage, up_stage, sems
        self.half = rows.shape[1] // self.TILE
        self.count = 2 * self.half

    def at(self, t):
        return pl.ds(pl.multiple_of(lax.rem(t, self.half) * self.TILE, self.TILE), self.TILE)

    def each(self, t, act):
        slot = lax.rem(t, 2)
        for source, here in ((self.rows, t < self.half), (self.down, t >= self.half)):
            @pl.when(here)
            def _():
                act(pltpu.make_async_copy(source.at[:, self.at(t)], self.tile.at[slot], self.sems.at[0, slot]))

    def hidden(self, source, buf, k):
        return pltpu.make_async_copy(source, buf, self.sems.at[1, k])

    def put(self, t, act):
        for out, here in ((self.grad_gate, t < self.half), (self.grad_down, t >= self.half)):
            @pl.when(here)
            def _():
                act(pltpu.make_async_copy(self.gate_stage, out.at[self.at(t), :], self.sems.at[2, 0]))

    def put_up(self, t):
        return pltpu.make_async_copy(self.up_stage, self.grad_up.at[self.at(t), :], self.sems.at[2, 1])

    def prepare(self):
        self.hidden(self.gate_pre, self.gate_buf, 0).start()
        self.hidden(self.up_pre, self.up_buf, 1).start()
        self.each(jnp.int32(0), lambda c: c.start())

    def step(self, t):
        slot = lax.rem(t, 2)

        @pl.when(t + 1 < self.count)
        def _():
            self.each(t + 1, lambda c: c.start())

        @pl.when(t == 0)
        def _():
            self.hidden(self.gate_pre, self.gate_buf, 0).wait()
            self.hidden(self.up_pre, self.up_buf, 1).wait()

        @pl.when(t == self.half)
        def _():
            copy = self.hidden(self.act, self.gate_buf, 0)
            copy.start()
            copy.wait()

        self.each(t, lambda c: c.wait())

        @pl.when(t > 0)
        def _():
            self.put(t - 1, lambda c: c.wait())

        self.gate_stage[...] = mm(self.tile[slot], self.gate_buf[...], 0, 0)
        self.put(t, lambda c: c.start())

        @pl.when(t < self.half)
        def _():
            @pl.when(t > 0)
            def _():
                self.put_up(t - 1).wait()

            self.up_stage[...] = mm(self.tile[slot], self.up_buf[...], 0, 0)
            self.put_up(t).start()

    def end(self):
        self.put(jnp.int32(self.count - 1), lambda c: c.wait())
        self.put_up(jnp.int32(self.half - 1)).wait()


def scatter_grads_kernel(nz, plan, count, *refs):
    terms, inputs = refs[:count], refs[count : count + 5]
    totals, outs = refs[count + 5 : 2 * count + 5], refs[2 * count + 5 : 2 * count + 8]
    scratch = refs[2 * count + 8 :]
    groups = [scratch[k * count : (k + 1) * count] for k in range(Scatter.BUFFERS)]
    rest = scratch[Scatter.BUFFERS * count :]
    z, e = place()
    greet(z, e, nz)
    s = Scatter(nz, terms, totals, *groups, *rest[:3])
    w = ExpertGrads(*inputs, *outs, *rest[3:])
    s.begin()
    w.prepare()
    run_beside(w.count, w.step, s.steps(), plan)
    w.end()
    for j in range(nz):
        s.drain(j)


def scatter_with_grads(arrays, rows, down, act, gate_pre, up_pre, collective_id):
    nz, width = lax.axis_size("dp"), lax.axis_size("expert")
    count, devices = len(arrays), nz * width
    terms = [a.reshape(nz, width, 4, a.shape[0] // (4 * devices), a.shape[1]) for a in arrays]
    shapes = [t.shape[3:] for t in terms]
    picked, model = rows.shape
    ff = act.shape[1]
    tile = ExpertGrads.TILE
    vmem = pl.BlockSpec(memory_space=pltpu.VMEM)
    hbm = pl.BlockSpec(memory_space=pl.ANY)
    plan = [3, 1, 0, 0, 0, 0, 3, 0, 0, 0, 0, 2] + [0] * 16
    outs = pl.pallas_call(
        functools.partial(scatter_grads_kernel, nz, plan, count),
        out_shape=[jax.ShapeDtypeStruct((4,) + s, F32) for s in shapes] + [jax.ShapeDtypeStruct((model, ff), F32)] * 3,
        in_specs=[hbm] * (count + 5),
        out_specs=[vmem] * count + [hbm] * 3,
        scratch_shapes=scatter_buffers(nz, width, [(s, a.dtype) for s, a in zip(shapes, arrays)])
        + [
            pltpu.VMEM((2, picked, tile), BF16),
            pltpu.VMEM((picked, ff), BF16),
            pltpu.VMEM((picked, ff), BF16),
            pltpu.VMEM((tile, ff), F32),
            pltpu.VMEM((tile, ff), F32),
            pltpu.SemaphoreType.DMA((3, 2)),
        ],
        compiler_params=pltpu.CompilerParams(
            collective_id=collective_id, has_side_effects=True, vmem_limit_bytes=VMEM_LIMIT
        ),
        name="scatter_grads",
    )(*terms, rows, down, act, gate_pre, up_pre)
    return [o.reshape(4 * s[0], s[1]) for o, s in zip(outs, shapes)] + list(outs[count:])


def pack_columns(columns, rows, lanes, dtype):
    parts = [c.astype(dtype) for c in columns]
    used = sum(c.shape[1] for c in parts)
    return jnp.concatenate(parts + [jnp.zeros((rows, lanes - used), dtype)], 1)


def spread(vector, devices, rows):
    blocks = vector.reshape(devices, -1)
    return jnp.pad(blocks, ((0, 0), (0, rows - blocks.shape[1]))).reshape(devices * rows, 1)


def per_device_gather(
    hidden_in,
    segment_ids,
    expert_ids,
    attn_gain,
    query_gain,
    key_gain,
    w_query,
    w_key,
    w_value,
    w_output,
    mlp_gain,
    w_router,
    w_gate,
    w_up,
    w_down,
    out_grad,
):
    devices = lax.axis_size(("dp", "expert"))
    me = lax.axis_index(("dp", "expert"))
    length, choices = expert_ids.shape
    width = hidden_in.shape[1]
    experts_total = devices
    capacity = 5 * length * choices // (4 * experts_total)
    query_cols, key_cols = w_query.shape[1], w_key.shape[1]
    rows = w_query.shape[0]
    head_rows = query_gain.shape[0]

    column = lambda v: jnp.pad(v, (0, rows - v.shape[0]))[:, None]
    lanes = 128 * pl.cdiv(experts_total + 4, 128)
    small = pack_columns(
        [w_router, column(attn_gain), column(mlp_gain), column(query_gain), column(key_gain)], rows, lanes, BF16
    )
    w_mixed = jnp.concatenate([w_query, w_key, w_value], 1)

    cosine_table, sine_table = rope_tables(jnp.arange(length) % TOK_DEV, HEAD_DIM)
    cosine, sine = cosine_table[:, 0], sine_table[:, 0]
    tables = jnp.stack([jnp.concatenate([cosine, cosine], 1), jnp.concatenate([-sine, sine], 1)])
    lane = jnp.arange(HEAD_DIM)
    head_map = (jnp.arange(width)[:, None] == (lane // head_rows * rows + lane % head_rows)[None, :]).astype(BF16)
    columns = (experts_total, experts_total + 2, experts_total + 3)
    w_mixed, w_out, small, all_grads, mixed, normed_attn, attended, branch = gather_with_attention(
        w_mixed, w_output, small, out_grad, columns, hidden_in, head_map, tables, segment_ids, 3
    )
    router = small[:, :experts_total]
    attn_gain, mlp_gain = small[:, experts_total], small[:, experts_total + 1]
    heads_of = small.reshape(devices, rows, lanes)[:, :head_rows]
    query_gain = heads_of[:, :, experts_total + 2].reshape(-1)
    key_gain = heads_of[:, :, experts_total + 3].reshape(-1)

    head_gains = jnp.stack([query_gain, key_gain]).astype(F32)
    plain_in = hidden_in.astype(F32)
    inv_attn = rms_scale(plain_in)
    residual = plain_in + branch

    inv_mlp = rms_scale(residual)
    normed_mlp = (residual * inv_mlp * mlp_gain).astype(BF16)
    logits = jnp.dot(normed_mlp, router, preferred_element_type=F32)
    chosen = jnp.any(expert_ids[:, :, None] == jnp.arange(experts_total)[None, None, :], 1)
    raised = jnp.where(chosen, jnp.exp(logits), 0.0)
    gate = raised / jnp.sum(raised, -1, keepdims=True)
    position = jnp.arange(length)
    not_after = (position[None, :] <= position[:, None]).astype(BF16)
    rank = jnp.dot(not_after, chosen.astype(BF16), preferred_element_type=F32) - 1.0
    rank = jnp.where(chosen, rank, -1.0)
    gate_high = lax.reduce_precision(gate, 8, 7)
    table = pack_columns([gate_high, gate - gate_high, rank], length, 128 * pl.cdiv(3 * experts_total, 128), BF16)

    y_terms, r_terms, gate_terms, rows_in, down_in, act, gate_pre_grad, up_pre_grad = gather_with_experts(
        normed_mlp, table, all_grads, w_gate[0], w_up[0], w_down[0], capacity, 2
    )
    is_me = (jnp.arange(experts_total) == me).astype(F32)
    gate_terms = (gate_terms * is_me[None, :, None]).reshape(devices * experts_total, length)
    row_grad_sum, gate_grad, grad_w_gate, grad_w_up, grad_w_down = scatter_with_grads(
        [r_terms.reshape(devices * length, width), gate_terms], rows_in, down_in, act, gate_pre_grad, up_pre_grad, 4
    )
    grad_w_gate, grad_w_up, grad_w_down = grad_w_gate[None], grad_w_up[None], grad_w_down.T[None]

    gate_grad = gate_grad.T
    sel_grad = gate * (gate_grad - jnp.sum(gate * gate_grad, -1, keepdims=True))
    logit_grad = jnp.where(chosen, sel_grad, 0.0).astype(BF16)
    grad_w_router = jnp.dot(normed_mlp.T, logit_grad, preferred_element_type=F32)
    normed_mlp_grad = row_grad_sum + jnp.dot(logit_grad, router.T, preferred_element_type=F32)
    grad_mlp_gain = jnp.sum(normed_mlp_grad * residual * inv_mlp, 0)
    residual_grad = out_grad.astype(F32) + norm_grad(normed_mlp_grad, residual, inv_mlp, mlp_gain)

    branch_grad = residual_grad.astype(BF16)
    mixed_out, gain_grads, normed_attn_grad, grad_w_output, grad_w_mixed = scatter_with_attention(
        y_terms.reshape(devices * length, width), branch_grad, w_out, mixed, tables, head_gains, segment_ids,
        normed_attn, attended, w_mixed, 5,
    )
    block_out = residual + mixed_out
    grad_query_gain, grad_key_gain = gain_grads[0], gain_grads[1]
    grad_attn_gain = jnp.sum(normed_attn_grad * plain_in * inv_attn, 0)
    grad_in = residual_grad + norm_grad(normed_attn_grad, plain_in, inv_attn, attn_gain)

    small_grads = pack_columns(
        [
            grad_w_router,
            grad_attn_gain[:, None],
            grad_mlp_gain[:, None],
            spread(grad_query_gain, devices, rows),
            spread(grad_key_gain, devices, rows),
        ],
        width,
        lanes,
        F32,
    )
    share_mixed, share_w_output, share_small = scatter_sum([grad_w_mixed, grad_w_output, small_grads], 6)
    return (
        block_out,
        grad_in,
        share_small[:, experts_total],
        share_small[:head_rows, experts_total + 2],
        share_small[:head_rows, experts_total + 3],
        share_mixed[:, :query_cols],
        share_mixed[:, query_cols : query_cols + key_cols],
        share_mixed[:, query_cols + key_cols :],
        share_w_output,
        share_small[:, experts_total + 1],
        share_small[:, :experts_total],
        grad_w_gate,
        grad_w_up,
        grad_w_down,
    )


def per_device(*arguments):
    expert_ids, w_gate = arguments[2], arguments[12]
    devices, width = lax.axis_size(("dp", "expert")), lax.axis_size("expert")
    length, choices = expert_ids.shape
    capacity = 5 * length * choices // (4 * devices)
    dense = devices <= 4 * choices and w_gate.shape[0] == 1 and width == 8
    if dense and capacity % 16 == 0 and devices % 4 == 0:
        return per_device_gather(*arguments)
    return per_device_exchange(*arguments)


def solution(mesh):
    in_specs = (
        P(("dp", "expert"), None),
        P(("dp", "expert")),
        P(("dp", "expert"), None),
        P(("dp", "expert")),
        P(("dp", "expert")),
        P(("dp", "expert")),
        P(("dp", "expert"), None),
        P(("dp", "expert"), None),
        P(("dp", "expert"), None),
        P(("dp", "expert"), None),
        P(("dp", "expert")),
        P(("dp", "expert"), None),
        P(("dp", "expert"), None, None),
        P(("dp", "expert"), None, None),
        P(("dp", "expert"), None, None),
        P(("dp", "expert"), None),
    )
    out_specs = (
        P(("dp", "expert"), None),
        P(("dp", "expert"), None),
        P(("dp", "expert")),
        P(("dp", "expert")),
        P(("dp", "expert")),
        P(("dp", "expert"), None),
        P(("dp", "expert"), None),
        P(("dp", "expert"), None),
        P(("dp", "expert"), None),
        P(("dp", "expert")),
        P(("dp", "expert"), None),
        P(("dp", "expert"), None, None),
        P(("dp", "expert"), None, None),
        P(("dp", "expert"), None, None),
    )
    return jax.shard_map(
        per_device, mesh=mesh, in_specs=in_specs, out_specs=out_specs, check_vma=False
    )
```

```python
import functools
import math

import jax
import jax.numpy as jnp
from jax import lax
from jax.experimental import pallas as pl
from jax.experimental.pallas import tpu as pltpu
from jax.sharding import PartitionSpec as P

F32, BF16 = jnp.float32, jnp.bfloat16
MESH = pl.DeviceIdType.MESH
VMEM_LIMIT = 63 * 1024 * 1024


HEADS = 32
KV_HEADS = 4
HEAD_DIM = 128
TOK_DEV = 256


EPS = 1e-06
ROPE_BASE = 1000000.0


def rms_scale(values):
    return lax.rsqrt(jnp.mean(values * values, -1, keepdims=True) + EPS)


def norm_grad(upstream, values, inverse, gain_vec):
    weighted = upstream * gain_vec
    return inverse * weighted - values * inverse**3 * jnp.mean(weighted * values, -1, keepdims=True)


def rope_tables(positions, head_dim):
    half_dim = head_dim // 2
    frequency = ROPE_BASE ** (-(jnp.arange(half_dim).astype(jnp.float32) * 2.0 / head_dim))
    angles = positions.astype(jnp.float32)[:, None] * frequency[None, :]
    return (jnp.cos(angles)[:, None, :], jnp.sin(angles)[:, None, :])


def rotate(values, cosine_table, sine_table):
    half_dim = values.shape[-1] // 2
    first_half = values[..., :half_dim]
    second_half = values[..., half_dim:]
    return jnp.concatenate(
        [
            first_half * cosine_table - second_half * sine_table,
            second_half * cosine_table + first_half * sine_table,
        ],
        -1,
    )


def unrotate(values, cosine_table, sine_table):
    half_dim = values.shape[-1] // 2
    first_half = values[..., :half_dim]
    second_half = values[..., half_dim:]
    return jnp.concatenate(
        [
            first_half * cosine_table + second_half * sine_table,
            second_half * cosine_table - first_half * sine_table,
        ],
        -1,
    )


def attend(query_rot, key_rot, value_rows, allowed):
    score_scale = 1.0 / math.sqrt(HEAD_DIM)
    scores = (
        jnp.einsum("qkgd,tkd->kgqt", query_rot, key_rot, preferred_element_type=jnp.float32)
        * score_scale
    )
    exp_scores = jnp.where(allowed, jnp.exp(scores), 0.0)
    totals = jnp.sum(exp_scores, -1, keepdims=True)
    probs_low = (exp_scores / totals).astype(jnp.bfloat16)
    attended = jnp.einsum(
        "kgqt,tkd->qkgd", probs_low, value_rows, preferred_element_type=jnp.float32
    ).astype(jnp.bfloat16)
    return (attended, jnp.log(totals))


def attend_grad(query_rot, key_rot, value_rows, allowed, log_totals, attended_grad):
    score_scale = 1.0 / math.sqrt(HEAD_DIM)
    scores = (
        jnp.einsum("qkgd,tkd->kgqt", query_rot, key_rot, preferred_element_type=jnp.float32)
        * score_scale
    )
    probs_back = jnp.where(allowed, jnp.exp(scores - log_totals), 0.0)
    probs_low = probs_back.astype(jnp.bfloat16)
    value_sum_grad = jnp.einsum(
        "kgqt,qkgd->tkd", probs_low, attended_grad, preferred_element_type=jnp.float32
    )
    prob_grad = jnp.einsum(
        "qkgd,tkd->kgqt", attended_grad, value_rows, preferred_element_type=jnp.float32
    )
    score_grad = (
        probs_back * (prob_grad - jnp.sum(probs_back * prob_grad, -1, keepdims=True))
    ).astype(jnp.bfloat16)
    query_rot_grad = (
        jnp.einsum("kgqt,tkd->qkgd", score_grad, key_rot, preferred_element_type=jnp.float32)
        * score_scale
    )
    key_rot_grad = (
        jnp.einsum("kgqt,qkgd->tkd", score_grad, query_rot, preferred_element_type=jnp.float32)
        * score_scale
    )
    return (query_rot_grad, key_rot_grad, value_sum_grad)


def mixer_forward(block_in, block_segments, weights):
    w_query, w_key, w_value, w_output, w_router, attn_gain, mlp_gain, query_gain, key_gain = weights
    row_count = block_in.shape[0]
    seq_count = row_count // TOK_DEV
    group_size = HEADS // KV_HEADS
    plain_in = block_in.astype(jnp.float32)
    inv_attn = rms_scale(plain_in)
    normed_attn = (plain_in * inv_attn * attn_gain).astype(jnp.bfloat16)
    query_raw = jnp.dot(normed_attn, w_query, preferred_element_type=jnp.float32).reshape(
        row_count, HEADS, HEAD_DIM
    )
    key_raw = jnp.dot(normed_attn, w_key, preferred_element_type=jnp.float32).reshape(
        row_count, KV_HEADS, HEAD_DIM
    )
    value_rows = jnp.dot(normed_attn, w_value, preferred_element_type=jnp.float32).astype(
        jnp.bfloat16
    )
    value_rows = value_rows.reshape(seq_count, TOK_DEV, KV_HEADS, HEAD_DIM)
    query_scale = rms_scale(query_raw)
    key_scale = rms_scale(key_raw)
    cosine_table, sine_table = rope_tables(jnp.arange(row_count) % TOK_DEV, HEAD_DIM)
    query_rot = rotate(query_raw * query_scale * query_gain, cosine_table, sine_table).astype(
        jnp.bfloat16
    )
    query_rot = query_rot.reshape(seq_count, TOK_DEV, KV_HEADS, group_size, HEAD_DIM)
    key_rot = rotate(key_raw * key_scale * key_gain, cosine_table, sine_table).astype(jnp.bfloat16)
    key_rot = key_rot.reshape(seq_count, TOK_DEV, KV_HEADS, HEAD_DIM)
    segments = block_segments.reshape(seq_count, TOK_DEV)
    position = jnp.arange(TOK_DEV)
    allowed = (segments[:, :, None] == segments[:, None, :]) & (
        position[None, None, :] <= position[None, :, None]
    )
    attended, log_totals = jax.vmap(attend)(query_rot, key_rot, value_rows, allowed)
    attended = attended.reshape(row_count, HEADS * HEAD_DIM)
    residual = plain_in + jnp.dot(attended, w_output, preferred_element_type=jnp.float32)
    saved_state = (
        plain_in,
        inv_attn,
        normed_attn,
        query_raw,
        key_raw,
        value_rows,
        query_scale,
        key_scale,
        query_rot,
        key_rot,
        allowed,
        log_totals,
        attended,
        cosine_table,
        sine_table,
    )
    return (residual, saved_state)


def mixer_backward(residual_grad, saved_state, weights):
    w_query, w_key, w_value, w_output, w_router, attn_gain, mlp_gain, query_gain, key_gain = weights
    (
        plain_in,
        inv_attn,
        normed_attn,
        query_raw,
        key_raw,
        value_rows,
        query_scale,
        key_scale,
        query_rot,
        key_rot,
        allowed,
        log_totals,
        attended,
        cosine_table,
        sine_table,
    ) = saved_state
    row_count = residual_grad.shape[0]
    seq_count = row_count // TOK_DEV
    group_size = HEADS // KV_HEADS
    branch_grad = residual_grad.astype(jnp.bfloat16)
    grad_w_output = jnp.dot(attended.T, branch_grad, preferred_element_type=jnp.float32)
    attended_grad = jnp.dot(branch_grad, w_output.T, preferred_element_type=jnp.float32).astype(
        jnp.bfloat16
    )
    attended_grad = attended_grad.reshape(seq_count, TOK_DEV, KV_HEADS, group_size, HEAD_DIM)
    query_rot_grad, key_rot_grad, value_sum_grad = jax.vmap(attend_grad)(
        query_rot, key_rot, value_rows, allowed, log_totals, attended_grad
    )
    query_normed_grad = unrotate(
        query_rot_grad.reshape(row_count, HEADS, HEAD_DIM), cosine_table, sine_table
    )
    key_normed_grad = unrotate(
        key_rot_grad.reshape(row_count, KV_HEADS, HEAD_DIM), cosine_table, sine_table
    )
    grad_query_gain = jnp.sum(query_normed_grad * query_raw * query_scale, (0, 1))
    grad_key_gain = jnp.sum(key_normed_grad * key_raw * key_scale, (0, 1))
    query_grad = norm_grad(query_normed_grad, query_raw, query_scale, query_gain).astype(
        jnp.bfloat16
    )
    query_grad = query_grad.reshape(row_count, HEADS * HEAD_DIM)
    key_grad = norm_grad(key_normed_grad, key_raw, key_scale, key_gain).astype(jnp.bfloat16)
    key_grad = key_grad.reshape(row_count, KV_HEADS * HEAD_DIM)
    value_grad = value_sum_grad.astype(jnp.bfloat16).reshape(row_count, KV_HEADS * HEAD_DIM)
    grad_w_query = jnp.dot(normed_attn.T, query_grad, preferred_element_type=jnp.float32)
    grad_w_key = jnp.dot(normed_attn.T, key_grad, preferred_element_type=jnp.float32)
    grad_w_value = jnp.dot(normed_attn.T, value_grad, preferred_element_type=jnp.float32)
    normed_attn_grad = (
        jnp.dot(query_grad, w_query.T, preferred_element_type=jnp.float32)
        + jnp.dot(key_grad, w_key.T, preferred_element_type=jnp.float32)
        + jnp.dot(value_grad, w_value.T, preferred_element_type=jnp.float32)
    )
    grad_attn_gain = jnp.sum(normed_attn_grad * plain_in * inv_attn, 0)
    grad_in = residual_grad + norm_grad(normed_attn_grad, plain_in, inv_attn, attn_gain)
    return (
        grad_in,
        (
            grad_attn_gain,
            grad_query_gain,
            grad_key_gain,
            grad_w_query,
            grad_w_key,
            grad_w_value,
            grad_w_output,
        ),
    )


def dispatch_table(expert_rows, experts, capacity):
    length, choices = expert_rows.shape
    flat_ids = expert_rows.reshape(length * choices)
    marks = (flat_ids[:, None] == jnp.arange(experts)[None, :]).astype(jnp.int32)
    earlier = jnp.cumsum(marks, 0) - marks
    destination = flat_ids * capacity + jnp.sum(earlier * marks, -1)
    pair_ids = (
        jnp.zeros((experts * capacity,), jnp.int32)
        .at[destination]
        .set(jnp.arange(length * choices, dtype=jnp.int32))
    )
    filled = jnp.zeros((experts * capacity,), jnp.bfloat16).at[destination].set(1.0)
    return (destination, pair_ids, filled)


def move_rows(row_block, section_name):
    if section_name == "dispatch":
        return lax.all_to_all(row_block, ("dp", "expert"), split_axis=0, concat_axis=0, tiled=True)
    if section_name == "combine":
        return lax.all_to_all(row_block, ("dp", "expert"), split_axis=0, concat_axis=0, tiled=True)
    if section_name == "grad_dispatch":
        return lax.all_to_all(row_block, ("dp", "expert"), split_axis=0, concat_axis=0, tiled=True)
    return lax.all_to_all(row_block, ("dp", "expert"), split_axis=0, concat_axis=0, tiled=True)


def per_device_exchange(
    hidden_in,
    segment_ids,
    expert_ids,
    attn_gain,
    query_gain,
    key_gain,
    w_query,
    w_key,
    w_value,
    w_output,
    mlp_gain,
    w_router,
    w_gate,
    w_up,
    w_down,
    out_grad,
):
    weights = (
        lax.all_gather(w_query, ("dp", "expert"), axis=0, tiled=True),
        lax.all_gather(w_key, ("dp", "expert"), axis=0, tiled=True),
        lax.all_gather(w_value, ("dp", "expert"), axis=0, tiled=True),
        lax.all_gather(w_output, ("dp", "expert"), axis=0, tiled=True),
        lax.all_gather(w_router, ("dp", "expert"), axis=0, tiled=True),
        lax.all_gather(attn_gain, ("dp", "expert"), axis=0, tiled=True),
        lax.all_gather(mlp_gain, ("dp", "expert"), axis=0, tiled=True),
        lax.all_gather(query_gain, ("dp", "expert"), axis=0, tiled=True),
        lax.all_gather(key_gain, ("dp", "expert"), axis=0, tiled=True),
    )
    residual, saved_state = mixer_forward(hidden_in, segment_ids, weights)
    full_router = weights[4]
    full_mlp_gain = weights[6]
    inv_mlp = rms_scale(residual)
    normed_mlp = (residual * inv_mlp * full_mlp_gain).astype(jnp.bfloat16)
    logits = jnp.dot(normed_mlp, full_router, preferred_element_type=jnp.float32)
    device_count = lax.axis_size(("dp", "expert"))
    local_experts = w_gate.shape[0]
    experts = local_experts * device_count
    length, choices = expert_ids.shape
    model_width = hidden_in.shape[1]
    capacity = 5 * length * choices // (4 * experts)
    one_hot = expert_ids[:, :, None] == jnp.arange(experts)[None, None, :]
    chosen = jnp.sum(jnp.where(one_hot, logits[:, None, :], 0.0), -1)
    raised = jnp.exp(chosen)
    gate_weights = raised / jnp.sum(raised, -1, keepdims=True)
    destination, pair_ids, filled = dispatch_table(expert_ids, experts, capacity)
    send_rows = normed_mlp[pair_ids // choices] * filled[:, None]
    received = move_rows(
        send_rows.reshape(device_count, local_experts * capacity, model_width), "dispatch"
    )
    received = received.reshape(device_count, local_experts, capacity, model_width)
    pre_gate = jnp.einsum("secd,edf->secf", received, w_gate, preferred_element_type=jnp.float32)
    pre_up = jnp.einsum("secd,edf->secf", received, w_up, preferred_element_type=jnp.float32)
    gate_sigmoid = jax.nn.sigmoid(pre_gate)
    silu_gate = pre_gate * gate_sigmoid
    activation = (silu_gate * pre_up).astype(jnp.bfloat16)
    expert_out = jnp.einsum(
        "secf,efd->secd", activation, w_down, preferred_element_type=jnp.float32
    ).astype(jnp.bfloat16)
    returned = move_rows(
        expert_out.reshape(device_count, local_experts * capacity, model_width), "combine"
    )
    picked = returned.reshape(experts * capacity, model_width)[destination].reshape(
        length, choices, model_width
    )
    block_out = residual + jnp.sum(gate_weights[:, :, None] * picked.astype(jnp.float32), 1)
    weights = (
        lax.all_gather(w_query, ("dp", "expert"), axis=0, tiled=True),
        lax.all_gather(w_key, ("dp", "expert"), axis=0, tiled=True),
        lax.all_gather(w_value, ("dp", "expert"), axis=0, tiled=True),
        lax.all_gather(w_output, ("dp", "expert"), axis=0, tiled=True),
        lax.all_gather(w_router, ("dp", "expert"), axis=0, tiled=True),
        lax.all_gather(attn_gain, ("dp", "expert"), axis=0, tiled=True),
        lax.all_gather(mlp_gain, ("dp", "expert"), axis=0, tiled=True),
        lax.all_gather(query_gain, ("dp", "expert"), axis=0, tiled=True),
        lax.all_gather(key_gain, ("dp", "expert"), axis=0, tiled=True),
    )
    full_router = weights[4]
    full_mlp_gain = weights[6]
    cotangent = out_grad.astype(jnp.float32)
    gate_grad = jnp.sum(cotangent[:, None, :] * picked.astype(jnp.float32), -1)
    down_in = (
        (gate_weights[:, :, None] * cotangent[:, None, :])
        .astype(jnp.bfloat16)
        .reshape(length * choices, model_width)
    )
    send_grad = down_in[pair_ids] * filled[:, None]
    recv_grad = move_rows(
        send_grad.reshape(device_count, local_experts * capacity, model_width), "grad_dispatch"
    )
    recv_grad = recv_grad.reshape(device_count, local_experts, capacity, model_width)
    act_grad = jnp.einsum("secd,efd->secf", recv_grad, w_down, preferred_element_type=jnp.float32)
    grad_w_down = jnp.einsum(
        "secf,secd->efd", activation, recv_grad, preferred_element_type=jnp.float32
    )
    gate_pre_grad = (
        act_grad * pre_up * gate_sigmoid * (1.0 + pre_gate * (1.0 - gate_sigmoid))
    ).astype(jnp.bfloat16)
    up_pre_grad = (act_grad * silu_gate).astype(jnp.bfloat16)
    grad_w_gate = jnp.einsum(
        "secd,secf->edf", received, gate_pre_grad, preferred_element_type=jnp.float32
    )
    grad_w_up = jnp.einsum(
        "secd,secf->edf", received, up_pre_grad, preferred_element_type=jnp.float32
    )
    row_grad = (
        jnp.einsum("secf,edf->secd", gate_pre_grad, w_gate, preferred_element_type=jnp.float32)
        + jnp.einsum("secf,edf->secd", up_pre_grad, w_up, preferred_element_type=jnp.float32)
    ).astype(jnp.bfloat16)
    row_back = move_rows(
        row_grad.reshape(device_count, local_experts * capacity, model_width), "grad_return"
    )
    row_back = row_back.reshape(experts * capacity, model_width)[destination].reshape(
        length, choices, model_width
    )
    sel_grad = gate_weights * (gate_grad - jnp.sum(gate_weights * gate_grad, -1, keepdims=True))
    logit_grad = jnp.sum(jnp.where(one_hot, sel_grad[:, :, None], 0.0), 1).astype(jnp.bfloat16)
    grad_w_router = jnp.dot(normed_mlp.T, logit_grad, preferred_element_type=jnp.float32)
    normed_mlp_grad = jnp.sum(row_back.astype(jnp.float32), 1) + jnp.dot(
        logit_grad, full_router.T, preferred_element_type=jnp.float32
    )
    grad_mlp_gain = jnp.sum(normed_mlp_grad * residual * inv_mlp, 0)
    residual_grad = cotangent + norm_grad(normed_mlp_grad, residual, inv_mlp, full_mlp_gain)
    grad_in, mixer_terms = mixer_backward(residual_grad, saved_state, weights)
    (
        grad_attn_gain,
        grad_query_gain,
        grad_key_gain,
        grad_w_query,
        grad_w_key,
        grad_w_value,
        grad_w_output,
    ) = mixer_terms
    summed = (
        lax.psum_scatter(grad_w_query, ("dp", "expert"), scatter_dimension=0, tiled=True),
        lax.psum_scatter(grad_w_key, ("dp", "expert"), scatter_dimension=0, tiled=True),
        lax.psum_scatter(grad_w_value, ("dp", "expert"), scatter_dimension=0, tiled=True),
        lax.psum_scatter(grad_w_output, ("dp", "expert"), scatter_dimension=0, tiled=True),
        lax.psum_scatter(grad_w_router, ("dp", "expert"), scatter_dimension=0, tiled=True),
        lax.psum_scatter(grad_attn_gain, ("dp", "expert"), scatter_dimension=0, tiled=True),
        lax.psum_scatter(grad_mlp_gain, ("dp", "expert"), scatter_dimension=0, tiled=True),
        lax.psum_scatter(grad_query_gain, ("dp", "expert"), scatter_dimension=0, tiled=True),
        lax.psum_scatter(grad_key_gain, ("dp", "expert"), scatter_dimension=0, tiled=True),
    )
    (
        share_w_query,
        share_w_key,
        share_w_value,
        share_w_output,
        share_w_router,
        share_attn_gain,
        share_mlp_gain,
        share_query_gain,
        share_key_gain,
    ) = summed
    return (
        block_out,
        grad_in,
        share_attn_gain,
        share_query_gain,
        share_key_gain,
        share_w_query,
        share_w_key,
        share_w_value,
        share_w_output,
        share_mlp_gain,
        share_w_router,
        grad_w_gate,
        grad_w_up,
        grad_w_down,
    )


def place():
    z = lax.axis_index("dp")
    e = lax.axis_index("expert")
    return z, e


def line_order(z, nz, j, inner=False):
    near = jnp.minimum(z, nz - 1 - z)
    step = (j + 1) // 2
    step = step if j % 2 == 0 else -step
    if inner:
        step = jnp.where(z < nz - 1 - z, -step, step)
    tail = jnp.where(z < nz - 1 - z, j, nz - 1 - j)
    return jnp.where(j <= 2 * near, z + step, tail)


def greet(z, e, nz):
    barrier = pltpu.get_barrier_semaphore()
    for mate in (e ^ 1, e ^ 2, e ^ 4):
        pl.semaphore_signal(barrier, inc=1, device_id=(z, mate), device_id_type=MESH)

    @pl.when(z > 0)
    def _():
        pl.semaphore_signal(barrier, inc=1, device_id=(z - 1, e), device_id_type=MESH)

    @pl.when(z < nz - 1)
    def _():
        pl.semaphore_signal(barrier, inc=1, device_id=(z + 1, e), device_id_type=MESH)

    ends = (z > 0).astype(jnp.int32) + (z < nz - 1).astype(jnp.int32)
    pl.semaphore_wait(barrier, 3 + ends)


class Gather:
    Z, ZX, ZY, X3, X2, XQ, Y3, Y2, YQ, P0, PX3, PXQ, PY3, PYQ, PDX, PDY = range(16)
    KINDS = 16
    WHOLE, LOW, HIGH, LOW3, HIGH3, Q0, Q3 = (0, 4), (0, 2), (2, 2), (0, 3), (1, 3), (0, 1), (3, 1)

    def __init__(self, nz, shards, outs, send, recv, local):
        self.nz, self.shards, self.outs = nz, shards, outs
        self.send, self.recv, self.local = send, recv, local
        self.z, self.e = place()
        self.p, self.x, self.y, self.d = self.e ^ 1, self.e ^ 2, self.e ^ 4, self.e ^ 6

    def zz(self, j):
        return line_order(self.z, self.nz, j)

    def part(self, ref, piece):
        return ref.at[pl.ds(piece[0], piece[1])]

    def copy(self, i, kind, zz, ee, piece, dev, mine=False, sem=None):
        dst = self.part(self.outs[i].at[zz, ee], piece)
        return pltpu.make_async_remote_copy(
            src_ref=self.part(self.shards[i], piece) if mine else dst,
            dst_ref=dst,
            send_sem=self.send.at[i, zz, kind] if sem is None else sem,
            recv_sem=self.recv.at[i, zz, kind],
            device_id=dev,
            device_id_type=MESH,
        )

    def start(self, kind, zz, ee, piece, dev, mine=False):
        for i in range(len(self.outs)):
            self.copy(i, kind, zz, ee, piece, dev, mine).start()

    def arrived(self, kind, zz, ee, piece):
        for i in range(len(self.outs)):
            self.copy(i, kind, zz, ee, piece, (self.z, self.e)).wait_recv()

    def sent(self, kind, zz, ee, piece, mine=False):
        for i in range(len(self.outs)):
            self.copy(i, kind, zz, ee, piece, (self.z, self.e), mine).wait_send()

    def along(self, j, kind, ee, piece, act):
        z, e, nz = self.z, self.e, self.nz
        zz, mine = self.zz(j), j == 0 and kind == self.Z
        for i in range(len(self.outs)):
            @pl.when(jnp.logical_and(zz <= z, z < nz - 1))
            def _():
                act(self.copy(i, kind, zz, ee, piece, (z + 1, e), mine))

            @pl.when(jnp.logical_and(zz >= z, z > 0))
            def _():
                sem = self.local.at[1 + kind, i] if j == 0 else None
                act(self.copy(i, kind, zz, ee, piece, (z - 1, e), mine, sem))

    def keep(self, i):
        return pltpu.make_async_copy(self.shards[i], self.outs[i].at[self.z, self.e], self.local.at[0, i])

    def kept(self):
        for i in range(len(self.outs)):
            self.keep(i).wait()

    def launch(self, j):
        self.launch_line(j)
        self.launch_plane(j)

    def launch_line(self, j):
        e, zz, mine = self.e, self.zz(j), j == 0
        if not mine:
            self.arrived(self.Z, zz, e, self.WHOLE)
        else:
            self.start(self.XQ, zz, e, self.Q3, (self.z, self.x), mine)
            self.start(self.YQ, zz, e, self.Q0, (self.z, self.y), mine)
        self.along(j, self.Z, e, self.WHOLE, lambda c: c.start())

    def launch_plane(self, j):
        z, e, zz, mine = self.z, self.e, self.zz(j), j == 0
        self.start(self.X3, zz, e, self.LOW3, (z, self.x), mine)
        self.start(self.Y3, zz, e, self.HIGH3, (z, self.y), mine)
        self.start(self.P0, zz, e, self.WHOLE, (z, self.p), mine)
        if mine:
            for i in range(len(self.outs)):
                self.keep(i).start()

    def mates(self, j):
        zz, mine = self.zz(j), j == 0
        self.arrived(self.XQ if mine else self.ZX, zz, self.x, self.Q3)
        self.along(j, self.ZX, self.x, self.Q3, lambda c: c.start())
        self.start(self.PXQ, zz, self.x, self.Q3, (self.z, self.p))
        self.arrived(self.YQ if mine else self.ZY, zz, self.y, self.Q0)
        self.along(j, self.ZY, self.y, self.Q0, lambda c: c.start())
        self.start(self.PYQ, zz, self.y, self.Q0, (self.z, self.p))

    def relay(self, j):
        zz = self.zz(j)
        self.arrived(self.X3, zz, self.x, self.LOW3)
        self.start(self.Y2, zz, self.x, self.HIGH, (self.z, self.y))
        self.start(self.PX3, zz, self.x, self.LOW3, (self.z, self.p))
        self.arrived(self.Y3, zz, self.y, self.HIGH3)
        self.start(self.X2, zz, self.y, self.LOW, (self.z, self.x))
        self.start(self.PY3, zz, self.y, self.HIGH3, (self.z, self.p))

    def finish(self, j):
        zz = self.zz(j)
        self.arrived(self.X2, zz, self.d, self.LOW)
        self.start(self.PDX, zz, self.d, self.LOW, (self.z, self.p))
        self.arrived(self.Y2, zz, self.d, self.HIGH)
        self.start(self.PDY, zz, self.d, self.HIGH, (self.z, self.p))

    def shared_near(self, j):
        zz, p = self.zz(j), self.p
        self.arrived(self.P0, zz, p, self.WHOLE)
        self.arrived(self.PXQ, zz, p ^ 2, self.Q3)
        self.arrived(self.PX3, zz, p ^ 2, self.LOW3)

    def shared_far(self, j):
        zz, p = self.zz(j), self.p
        self.arrived(self.PYQ, zz, p ^ 4, self.Q0)
        self.arrived(self.PY3, zz, p ^ 4, self.HIGH3)
        self.arrived(self.PDX, zz, p ^ 6, self.LOW)
        self.arrived(self.PDY, zz, p ^ 6, self.HIGH)

    def drain(self, j, kept=False):
        zz, e, mine = self.zz(j), self.e, j == 0
        if mine:
            self.sent(self.XQ, zz, e, self.Q3, mine)
            self.sent(self.YQ, zz, e, self.Q0, mine)
            if not kept:
                self.kept()
        for kind, ee, piece in ((self.Z, e, self.WHOLE), (self.ZX, self.x, self.Q3), (self.ZY, self.y, self.Q0)):
            self.along(j, kind, ee, piece, lambda c: c.wait_send())
        self.sent(self.X3, zz, e, self.LOW3, mine)
        self.sent(self.Y3, zz, e, self.HIGH3, mine)
        self.sent(self.P0, zz, e, self.WHOLE, mine)
        self.sent(self.PXQ, zz, self.x, self.Q3)
        self.sent(self.PYQ, zz, self.y, self.Q0)
        self.sent(self.Y2, zz, self.x, self.HIGH)
        self.sent(self.X2, zz, self.y, self.LOW)
        self.sent(self.PX3, zz, self.x, self.LOW3)
        self.sent(self.PY3, zz, self.y, self.HIGH3)
        self.sent(self.PDX, zz, self.d, self.LOW)
        self.sent(self.PDY, zz, self.d, self.HIGH)

    def steps(self):
        n = self.nz
        todo = [(self.launch, 0), (self.mates, 0)]
        for j in range(1, n + 2):
            todo += [(self.launch, j), (self.mates, j - 1) if j > 1 else None, (self.relay, j - 1), (self.finish, j - 2)]
        return [functools.partial(f, j) for f, j in filter(None, todo) if 0 <= j < n]


def gather_kernel(nz, count, *refs):
    shards, outs = refs[:count], refs[count : 2 * count]
    send, recv, local = refs[2 * count :]
    z, e = place()
    greet(z, e, nz)
    g = Gather(nz, shards, outs, send, recv, local)
    for step in g.steps():
        step()
    for j in range(nz):
        g.shared_near(j)
        g.shared_far(j)
    for j in range(nz):
        g.drain(j)


def gather_scratch(nz, count):
    return [
        pltpu.SemaphoreType.DMA((count, nz, Gather.KINDS)),
        pltpu.SemaphoreType.DMA((count, nz, Gather.KINDS)),
        pltpu.SemaphoreType.DMA((4, count)),
    ]


def gather_all(arrays, collective_id):
    nz, width = lax.axis_size("dp"), lax.axis_size("expert")
    count = len(arrays)
    parts = [a.reshape((4, a.shape[0] // 4) + a.shape[1:]) for a in arrays]
    outs = pl.pallas_call(
        functools.partial(gather_kernel, nz, count),
        out_shape=[jax.ShapeDtypeStruct((nz, width) + h.shape, h.dtype) for h in parts],
        in_specs=[pl.BlockSpec(memory_space=pltpu.VMEM)] * count,
        out_specs=[pl.BlockSpec(memory_space=pl.ANY)] * count,
        scratch_shapes=gather_scratch(nz, count),
        compiler_params=pltpu.CompilerParams(
            collective_id=collective_id, has_side_effects=True, vmem_limit_bytes=VMEM_LIMIT
        ),
        name="gather_all",
    )(*parts)
    return [o.reshape((nz * width * a.shape[0],) + a.shape[1:]) for o, a in zip(outs, arrays)]


def accumulate(dst, src):
    rows = dst.shape[0]
    block = 32 if rows % 32 == 0 else rows
    if rows == block:
        dst[...] = dst[...] + src[...]
        return

    def body(r, _):
        at = pl.ds(pl.multiple_of(r * block, block), block)
        dst[at, :] = dst[at, :] + src[at, :]
        return 0

    lax.fori_loop(0, rows // block, body, 0)


class Scatter:
    X2, Y2, X3, Y3, Z, ZB, ZX, ZXB, ZY, ZYB, XQ, YQ = range(4, 16)
    KINDS = 16
    BUFFERS = 9

    def __init__(self, nz, terms, outs, sums, temps, from_x2, from_y2, from_x3, from_y3, from_z, from_zm, from_q, send, recv, local):
        self.nz, self.terms, self.outs = nz, terms, outs
        self.sums, self.temps = sums, temps
        self.from_x2, self.from_y2, self.from_x3, self.from_y3 = from_x2, from_y2, from_x3, from_y3
        self.from_z, self.from_zm, self.from_q = from_z, from_zm, from_q
        self.send, self.recv, self.local = send, recv, local
        self.count = len(terms)
        self.z, self.e = place()
        self.core, self.chip = self.e % 2, self.e // 2
        self.p, self.x, self.y = self.e ^ 1, self.e ^ 2, self.e ^ 4
        self.chips = (self.chip ^ 3, self.chip ^ 1, self.chip ^ 2, self.chip)

    def zz(self, j):
        return line_order(self.z, self.nz, self.nz - 1 - j, True)

    def remote(self, i, kind, zz, src, dst, dev):
        return pltpu.make_async_remote_copy(
            src_ref=src, dst_ref=dst, send_sem=self.send.at[i, zz, kind], recv_sem=self.recv.at[i, zz, kind],
            device_id=dev, device_id_type=MESH)

    def quarters(self, i, zz, q, first, n):
        return self.sums[i].at[zz, q, pl.ds(first, n)]

    def pair(self, i, j, q):
        zz, chip = self.zz(j), self.chips[q]
        return self.remote(i, q, zz, self.terms[i].at[zz, chip * 2 + (1 - self.core)], self.sums[i].at[zz, q],
                           (self.z, self.p))

    def load(self, i, j, q):
        slot = q % 2
        return pltpu.make_async_copy(
            self.terms[i].at[self.zz(j), self.chips[q] * 2 + self.core], self.temps[i].at[slot], self.local.at[i, slot])

    def x2(self, i, zz):
        return self.remote(i, self.X2, zz, self.quarters(i, zz, 0, 0, 2), self.from_x2[i].at[zz], (self.z, self.x))

    def y2(self, i, zz):
        return self.remote(i, self.Y2, zz, self.quarters(i, zz, 0, 2, 2), self.from_y2[i].at[zz], (self.z, self.y))

    def x3(self, i, zz):
        return self.remote(i, self.X3, zz, self.quarters(i, zz, 1, 0, 3), self.from_x3[i].at[zz], (self.z, self.x))

    def y3(self, i, zz):
        return self.remote(i, self.Y3, zz, self.quarters(i, zz, 2, 1, 3), self.from_y3[i].at[zz], (self.z, self.y))

    def xq(self, i):
        return self.remote(i, self.XQ, self.z, self.quarters(i, self.z, 1, 3, 1), self.from_q[i].at[pl.ds(0, 1)], (self.z, self.x))

    def yq(self, i):
        return self.remote(i, self.YQ, self.z, self.quarters(i, self.z, 2, 0, 1), self.from_q[i].at[pl.ds(1, 1)], (self.z, self.y))

    def line(self, i, zz, which, dz, last=False):
        slot = self.nz if last else zz
        kind = (self.Z, self.ZX, self.ZY)[which] + int(last)
        src = (self.sums[i].at[zz, 3], self.quarters(i, zz, 1, 3, 1), self.quarters(i, zz, 2, 0, 1))[which]
        dst = self.from_z[i].at[slot] if which == 0 else self.from_zm[i].at[slot, pl.ds(which - 1, 1)]
        return self.remote(i, kind, zz, src, dst, (self.z + dz, self.e))

    def add(self, i, zz, q, first, n, src):
        for k in range(n):
            accumulate(self.sums[i].at[zz, q, first + k], src.at[k])

    def begin(self):
        for j in range(self.nz):
            for q in range(4):
                for i in range(self.count):
                    self.pair(i, j, q).start()
        for i in range(self.count):
            self.load(i, 0, 0).start()

    def first(self, j):
        zz = self.zz(j)
        for q in range(4):
            for i in range(self.count):
                if q < 3:
                    self.load(i, j, q + 1).start()
                elif j < self.nz - 1:
                    self.load(i, j + 1, 0).start()
                self.pair(i, j, q).wait_recv()
                self.load(i, j, q).wait()
                self.add(i, zz, q, 0, 4, self.temps[i].at[q % 2])
                if q == 0:
                    self.x2(i, zz).start()
                    self.y2(i, zz).start()

    def second(self, j):
        zz = self.zz(j)
        for i in range(self.count):
            self.y2(i, zz).wait_recv()
            self.add(i, zz, 1, 2, 2, self.from_y2[i].at[zz])
            self.x3(i, zz).start()
            self.x2(i, zz).wait_recv()
            self.add(i, zz, 2, 0, 2, self.from_x2[i].at[zz])
            self.y3(i, zz).start()
        for i in range(self.count):
            for which in (1, 2):
                self.flow(i, j, which)

    def flow(self, i, j, which):
        z, nz, zz = self.z, self.nz, self.zz(j)
        q, first, n = ((3, 0, 4), (1, 3, 1), (2, 0, 1))[which]

        def came(slot):
            ref = self.from_z[i].at[slot] if which == 0 else self.from_zm[i].at[slot, pl.ds(which - 1, 1)]
            self.add(i, zz, q, first, n, ref)

        if j < nz - 1:
            @pl.when(jnp.logical_or(jnp.logical_and(zz > z, z > 0), jnp.logical_and(zz < z, z < nz - 1)))
            def _():
                self.line(i, zz, which, 1).wait_recv()
                came(zz)

            @pl.when(zz > z)
            def _():
                self.line(i, zz, which, 1).start()

            @pl.when(zz < z - 1)
            def _():
                self.line(i, zz, which, -1).start()

            @pl.when(zz == z - 1)
            def _():
                self.line(i, zz, which, -1, True).start()
        else:
            @pl.when(z > 0)
            def _():
                self.line(i, zz, which, 1).wait_recv()
                came(zz)

            @pl.when(z < nz - 1)
            def _():
                self.line(i, zz, which, -1, True).wait_recv()
                came(nz)

            if which == 1:
                self.xq(i).start()
            if which == 2:
                self.yq(i).start()

    def third(self, j):
        zz = self.zz(j)
        for i in range(self.count):
            self.x3(i, zz).wait_recv()
            self.add(i, zz, 3, 0, 3, self.from_x3[i].at[zz])
            self.y3(i, zz).wait_recv()
            self.add(i, zz, 3, 1, 3, self.from_y3[i].at[zz])
        for i in range(self.count):
            self.flow(i, j, 0)

    def result(self):
        for i in range(self.count):
            self.xq(i).wait_recv()
            self.add(i, self.z, 3, 3, 1, self.from_q[i].at[pl.ds(0, 1)])
            self.yq(i).wait_recv()
            self.add(i, self.z, 3, 0, 1, self.from_q[i].at[pl.ds(1, 1)])
            self.outs[i][...] = self.sums[i][self.z, 3].astype(self.outs[i].dtype)

    def drain(self, j):
        z, nz = self.z, self.nz
        zz = self.zz(j)
        for i in range(self.count):
            for q in range(4):
                self.pair(i, j, q).wait_send()
            for c in (self.x2, self.y2, self.x3, self.y3):
                c(i, zz).wait_send()
            if j < nz - 1:
                for which in range(3):
                    @pl.when(zz > z)
                    def _():
                        self.line(i, zz, which, 1).wait_send()

                    @pl.when(zz < z - 1)
                    def _():
                        self.line(i, zz, which, -1).wait_send()

                    @pl.when(zz == z - 1)
                    def _():
                        self.line(i, zz, which, -1, True).wait_send()
            else:
                self.xq(i).wait_send()
                self.yq(i).wait_send()

    def steps(self):
        todo = []
        for j in range(self.nz + 2):
            todo += [(self.first, j), (self.second, j - 1), (self.third, j - 2)]
        return [functools.partial(f, j) for f, j in todo if 0 <= j < self.nz] + [self.result]


def scatter_kernel(nz, count, *refs):
    groups = [refs[k * count : (k + 1) * count] for k in range(2 + Scatter.BUFFERS)]
    send, recv, local = refs[(2 + Scatter.BUFFERS) * count :]
    z, e = place()
    greet(z, e, nz)
    s = Scatter(nz, *groups, send, recv, local)
    s.begin()
    for step in s.steps():
        step()
    for j in range(nz):
        s.drain(j)


def scatter_buffers(nz, width, kinds):
    leads = ((nz, width // 2, 4), (2, 4), (nz, 2), (nz, 2), (nz, 3), (nz, 3), (nz + 1, 4), (nz + 1, 2), (2,))
    return [pltpu.VMEM(lead + shape, dtype) for lead in leads for shape, dtype in kinds] + [
        pltpu.SemaphoreType.DMA((len(kinds), nz, Scatter.KINDS)),
        pltpu.SemaphoreType.DMA((len(kinds), nz, Scatter.KINDS)),
        pltpu.SemaphoreType.DMA((len(kinds), 2)),
    ]


def scatter_sum(arrays, collective_id):
    nz, width = lax.axis_size("dp"), lax.axis_size("expert")
    count = len(arrays)
    devices = nz * width
    terms = [a.reshape(nz, width, 4, a.shape[0] // (4 * devices), a.shape[1]) for a in arrays]
    shapes = [t.shape[3:] for t in terms]
    outs = pl.pallas_call(
        functools.partial(scatter_kernel, nz, count),
        out_shape=[jax.ShapeDtypeStruct((4,) + s, jnp.float32) for s in shapes],
        in_specs=[pl.BlockSpec(memory_space=pl.ANY)] * count,
        out_specs=[pl.BlockSpec(memory_space=pltpu.VMEM)] * count,
        scratch_shapes=scatter_buffers(nz, width, [(s, a.dtype) for s, a in zip(shapes, arrays)]),
        compiler_params=pltpu.CompilerParams(
            collective_id=collective_id, has_side_effects=True, vmem_limit_bytes=VMEM_LIMIT
        ),
        name="scatter_sum",
    )(*terms)
    return [o.reshape(4 * s[0], s[1]) for o, s in zip(outs, shapes)]


def mm(a, b, da=1, db=0):
    return lax.dot_general(a, b, (((da,), (db,)), ((), ())), preferred_element_type=F32)


def rope(values, cosine, sine):
    return values * cosine + pltpu.roll(values, values.shape[1] // 2, 1) * sine


class AttentionGrad:
    def __init__(self, branch, w_out, raw, tables, gains, seg_col, seg_row, normed, attended, w_mixed,
                 grads, gain_grads, normed_grad, grad_out, grad_mixed,
                 w_buf, q_buf, k_buf, v_buf, mask, k_rot, v_low, dk, dv, a_buf, m_buf, out_stage, mixed_stage, sems):
        self.normed, self.attended, self.w_mixed = normed, attended, w_mixed
        self.normed_grad, self.grad_out, self.grad_mixed = normed_grad, grad_out, grad_mixed
        self.a_buf, self.m_buf, self.out_stage, self.mixed_stage = a_buf, m_buf, out_stage, mixed_stage
        self.branch, self.w_out, self.raw, self.tables, self.gains = branch, w_out, raw, tables, gains
        self.seg_col, self.seg_row, self.grads, self.gain_grads = seg_col, seg_row, grads, gain_grads
        self.w_buf, self.q_buf, self.k_buf, self.v_buf, self.mask = w_buf, q_buf, k_buf, v_buf, mask
        self.k_rot, self.v_low, self.dk, self.dv, self.sems = k_rot, v_low, dk, dv, sems
        self.cols = w_buf.shape[0]
        self.query_cols = w_out.shape[0]
        self.key_cols = k_buf.shape[1]
        self.count = self.query_cols // self.cols
        self.per_key = self.count // (self.key_cols // HEAD_DIM)
        self.total = self.count + 2 * self.key_cols // self.cols

    def at(self, t):
        return pl.ds(pl.multiple_of(t * self.cols, self.cols), self.cols)

    def fetch(self, t, slot):
        at = self.at(t)
        return pltpu.make_async_copy(self.raw.at[:, at], self.q_buf.at[slot], self.sems.at[1, slot])

    def fetch_out(self, t):
        at = self.at(t)
        return (
            pltpu.make_async_copy(self.w_out.at[at, :], self.w_buf, self.sems.at[0, 0]),
            pltpu.make_async_copy(self.attended.at[:, at], self.a_buf, self.sems.at[3, 0]),
        )

    def fetch_mixed(self, t):
        return pltpu.make_async_copy(self.w_mixed.at[:, self.at(t)], self.m_buf, self.sems.at[4, 0])

    def put_out(self, t):
        return pltpu.make_async_copy(self.out_stage, self.grad_out.at[self.at(t), :], self.sems.at[5, 0])

    def put_mixed(self, t):
        return pltpu.make_async_copy(self.mixed_stage, self.grad_mixed.at[:, self.at(t)], self.sems.at[5, 1])

    def prepare(self):
        q, k = self.query_cols, self.key_cols
        key = pltpu.make_async_copy(self.raw.at[:, pl.ds(q, k)], self.k_buf, self.sems.at[2, 0])
        value = pltpu.make_async_copy(self.raw.at[:, pl.ds(q + k, k)], self.v_buf, self.sems.at[2, 1])
        key.start()
        value.start()
        for c in self.fetch_out(0):
            c.start()
        self.fetch(0, 0).start()
        self.fetch_mixed(0).start()
        self.normed_grad[...] = jnp.zeros_like(self.normed_grad)
        self.mask[...] = allowed_mask(self.seg_col, self.seg_row)
        self.gain_grads[...] = jnp.zeros_like(self.gain_grads)
        key.wait()
        value.wait()

    def scaled(self, raw, which):
        scale = lax.rsqrt(jnp.mean(raw * raw, 1, keepdims=True) + EPS)
        return scale, (raw * scale) * self.gains[which : which + 1, :]

    def back(self, rot_grad, raw, scale, which):
        cosine, sine = self.tables[0], self.tables[1]
        grad = rope(rot_grad, cosine, -sine)
        part = jnp.sum(grad * raw * scale, 0, keepdims=True)
        self.gain_grads[which : which + 1, :] = self.gain_grads[which : which + 1, :] + part
        weighted = grad * self.gains[which : which + 1, :]
        mean = jnp.mean(weighted * raw, 1, keepdims=True)
        return scale * weighted - raw * (scale * scale * scale) * mean

    def step(self, t):
        slot = lax.rem(t, 2)

        @pl.when(t + 1 < self.count)
        def _():
            self.fetch(t + 1, 1 - slot).start()

        @pl.when(t < self.count)
        def _():
            self.heads(t, slot)

        self.fetch_mixed(t).wait()
        grads = self.grads[:, self.at(t)]
        self.normed_grad[...] += mm(grads, self.m_buf[...], 1, 1)

        @pl.when(t + 1 < self.total)
        def _():
            self.fetch_mixed(t + 1).start()

        @pl.when(t > 0)
        def _():
            self.put_mixed(t - 1).wait()

        self.mixed_stage[...] = mm(self.normed[...], grads, 0, 0).astype(BF16)
        self.put_mixed(t).start()

    def end(self):
        self.put_mixed(self.total - 1).wait()
        self.put_out(self.count - 1).wait()

    def heads(self, t, slot):
        self.fetch(t, slot).wait()
        for c in self.fetch_out(t):
            c.wait()

        @pl.when(t > 0)
        def _():
            self.put_out(t - 1).wait()

        self.out_stage[...] = mm(self.a_buf[...], self.branch[...], 0, 0).astype(BF16)
        self.put_out(t).start()
        cosine, sine = self.tables[0], self.tables[1]
        at_key = pl.ds(pl.multiple_of(t // self.per_key * HEAD_DIM, HEAD_DIM), HEAD_DIM)

        @pl.when(lax.rem(t, self.per_key) == 0)
        def _():
            _, key = self.scaled(self.k_buf[:, at_key], 1)
            self.k_rot[...] = rope(key, cosine, sine).astype(BF16)
            self.v_low[...] = self.v_buf[:, at_key].astype(BF16)
            self.dk[...] = jnp.zeros_like(self.dk)
            self.dv[...] = jnp.zeros_like(self.dv)

        score_scale = 1.0 / math.sqrt(HEAD_DIM)
        out_grad = mm(self.branch[...], self.w_buf[...], 1, 1).astype(BF16)

        @pl.when(t + 1 < self.count)
        def _():
            for c in self.fetch_out(t + 1):
                c.start()

        mask = self.mask[...] > 0.0
        k_rot, v_low = self.k_rot[...], self.v_low[...]
        for h in range(self.cols // HEAD_DIM):
            here = slice(h * HEAD_DIM, (h + 1) * HEAD_DIM)
            raw = self.q_buf[slot, :, here]
            scale, query = self.scaled(raw, 0)
            q_rot = rope(query, cosine, sine).astype(BF16)
            d_out = out_grad[:, here]
            scores = mm(q_rot, k_rot, 1, 1) * score_scale
            raised = jnp.where(mask, jnp.exp(scores), 0.0)
            probs = raised / jnp.sum(raised, 1, keepdims=True)
            self.dv[...] += mm(probs.astype(BF16), d_out, 0, 0)
            d_probs = mm(d_out, v_low, 1, 1)
            d_scores = (probs * (d_probs - jnp.sum(probs * d_probs, 1, keepdims=True))).astype(BF16)
            dq = mm(d_scores, k_rot) * score_scale
            self.dk[...] += mm(d_scores, q_rot, 0, 0)
            at = pl.ds(pl.multiple_of(t * self.cols + h * HEAD_DIM, HEAD_DIM), HEAD_DIM)
            self.grads[:, at] = self.back(dq, raw, scale, 0).astype(BF16)

        @pl.when(lax.rem(t, self.per_key) == self.per_key - 1)
        def _():
            raw = self.k_buf[:, at_key]
            scale, _ = self.scaled(raw, 1)
            shift = pl.multiple_of(t // self.per_key * HEAD_DIM, HEAD_DIM)
            self.grads[:, pl.ds(self.query_cols + shift, HEAD_DIM)] = self.back(
                self.dk[...] * score_scale, raw, scale, 1
            ).astype(BF16)
            self.grads[:, pl.ds(self.query_cols + self.key_cols + shift, HEAD_DIM)] = self.dv[...].astype(BF16)


def scatter_attention_kernel(nz, plan, term, *refs):
    inputs, (total, *outs), scratch = refs[:10], refs[10:16], refs[16:]
    buffers, rest = scratch[: Scatter.BUFFERS], scratch[Scatter.BUFFERS :]
    send, recv, local = rest[:3]
    z, e = place()
    greet(z, e, nz)
    s = Scatter(nz, [term], [total], *[[b] for b in buffers], send, recv, local)
    a = AttentionGrad(*inputs, *outs, *rest[3:])
    s.begin()
    a.prepare()
    steps = s.steps()
    run_beside(a.total, a.step, steps, plan)
    a.end()
    for j in range(nz):
        s.drain(j)


def run_beside(count, work, steps, plan):
    bounds = [sum(plan[:t]) for t in range(len(plan) + 1)]

    def body(t, _):
        for k in range(count):
            todo = steps[bounds[k] : bounds[k + 1]]
            if todo:
                @pl.when(t == k)
                def _():
                    for step in todo:
                        step()
        work(t)
        return 0

    lax.fori_loop(0, count, body, 0)
    for step in steps[bounds[count] :]:
        step()


def scatter_with_attention(terms, branch, w_out, raw, tables, gains, segments, normed, attended, w_mixed, collective_id):
    nz, width = lax.axis_size("dp"), lax.axis_size("expert")
    devices = nz * width
    length, model = branch.shape
    shape = (terms.shape[0] // (4 * devices), terms.shape[1])
    term = terms.reshape((nz, width, 4) + shape)
    heads = 4
    cols = heads * HEAD_DIM
    key_cols = (raw.shape[1] - w_out.shape[0]) // 2
    vmem = pl.BlockSpec(memory_space=pltpu.VMEM)
    hbm = pl.BlockSpec(memory_space=pl.ANY)
    plan = [3, 1, 1, 1, 1, 1, 1, 1, 1, 0]
    total, grads, gain_grads, normed_grad, grad_out, grad_mixed = pl.pallas_call(
        functools.partial(scatter_attention_kernel, nz, plan),
        out_shape=[
            jax.ShapeDtypeStruct((4,) + shape, F32),
            jax.ShapeDtypeStruct(raw.shape, BF16),
            jax.ShapeDtypeStruct((2, HEAD_DIM), F32),
            jax.ShapeDtypeStruct((length, model), F32),
            jax.ShapeDtypeStruct(w_out.shape, BF16),
            jax.ShapeDtypeStruct(w_mixed.shape, BF16),
        ],
        in_specs=[hbm, vmem, hbm, hbm, vmem, vmem, vmem, vmem, vmem, hbm, hbm],
        out_specs=[vmem, vmem, vmem, vmem, hbm, hbm],
        scratch_shapes=scatter_buffers(nz, width, [(shape, terms.dtype)])
        + [
            pltpu.VMEM((cols, model), BF16),
            pltpu.VMEM((2, length, cols), F32),
            pltpu.VMEM((length, key_cols), F32),
            pltpu.VMEM((length, key_cols), F32),
            pltpu.VMEM((length, length), F32),
            pltpu.VMEM((length, HEAD_DIM), BF16),
            pltpu.VMEM((length, HEAD_DIM), BF16),
            pltpu.VMEM((length, HEAD_DIM), F32),
            pltpu.VMEM((length, HEAD_DIM), F32),
            pltpu.VMEM((length, cols), BF16),
            pltpu.VMEM((model, cols), BF16),
            pltpu.VMEM((cols, model), BF16),
            pltpu.VMEM((model, cols), BF16),
            pltpu.SemaphoreType.DMA((6, 2)),
        ],
        compiler_params=pltpu.CompilerParams(
            collective_id=collective_id, has_side_effects=True, vmem_limit_bytes=VMEM_LIMIT
        ),
        name="scatter_attention",
    )(term, branch, w_out, raw, tables, gains, segments[:, None], segments[None, :], normed, attended, w_mixed)
    return total.reshape(4 * shape[0], shape[1]), gain_grads, normed_grad, grad_out, grad_mixed


TILE = 512


class ExpertWork:
    def __init__(self, nz, cap, group, orders, all_rows, all_tables, all_grads, weights, outs, bufs, sems):
        self.nz, self.cap, self.group = nz, cap, group
        self.all_rows, self.all_tables, self.all_grads = all_rows, all_tables, all_grads
        self.weights, self.outs, self.bufs, self.sems = weights, outs, bufs, sems
        self.z, self.e = place()
        self.width = all_rows.shape[1]
        self.orders = orders
        self.edge = jnp.logical_or(self.z == 0, self.z == nz - 1)

    def weight_copies(self):
        return [pltpu.make_async_copy(w, b, self.sems.at[0, i]) for i, (w, b) in enumerate(zip(self.weights, self.bufs[:3]))]

    def place_of(self, t):
        zz, half = jnp.int32(0), jnp.int32(0)
        for p, (ends, middle) in enumerate(zip(*self.orders)):
            for here, (j, h) in ((self.edge, ends), (jnp.logical_not(self.edge), middle)):
                here = jnp.logical_and(here, t == p)
                zz = jnp.where(here, line_order(self.z, self.nz, j), zz)
                half = jnp.where(here, h, half)
        near = self.e // self.group
        return zz, jnp.where(half == 0, near, 1 - near) * self.group

    def inputs(self, t, slot):
        zz, first = self.place_of(t)
        at = pl.ds(first, self.group)
        x, tab, g = self.bufs[3:6]
        return (
            pltpu.make_async_copy(self.all_rows.at[zz, at], x.at[slot], self.sems.at[1 + slot, 0]),
            pltpu.make_async_copy(self.all_tables.at[zz, at], tab.at[slot], self.sems.at[1 + slot, 1]),
            pltpu.make_async_copy(self.all_grads.at[zz, at], g.at[slot], self.sems.at[1 + slot, 2]),
        )

    def flat(self, t):
        step = self.group * self.cap
        return pl.ds(pl.multiple_of(t * step, step), step)

    def row_results(self, t):
        pairs = zip(self.bufs[8:10], self.outs[3:5])
        return [pltpu.make_async_copy(b, o.at[self.flat(t)], self.sems.at[3, i]) for i, (b, o) in enumerate(pairs)]

    def hidden_results(self, t):
        pairs = zip(self.bufs[10:13], self.outs[5:8])
        return [pltpu.make_async_copy(b, o.at[self.flat(t)], self.sems.at[3, 2 + i]) for i, (b, o) in enumerate(pairs)]

    def term_results(self, t, n, cols):
        zz, first = self.place_of(t)
        at = pl.ds(first, self.group)
        pairs = zip(self.bufs[6:8], self.outs[:2])
        return [
            pltpu.make_async_copy(b.at[:, :, cols], o.at[zz, at, :, cols], self.sems.at[4 + i, n])
            for i, (b, o) in enumerate(pairs)
        ]

    def begin(self):
        for c in self.weight_copies():
            c.start()

    def ready(self, p):
        for c in self.inputs(jnp.int32(p), p % 2):
            c.start()

    def step(self, t, hook):
        slot = lax.rem(t, 2)
        hook(0)
        cap, group = self.cap, self.group
        wg, wu, wd, xb, tb, gb, yb, rb, rowb, downb, actb, gpb, upb, cotb = self.bufs
        for c in self.inputs(t, slot):
            c.wait()

        @pl.when(t == 0)
        def _():
            for c in self.weight_copies():
                c.wait()

        self.free(t, self.row_results)
        length, width = xb.shape[2] * xb.shape[3], xb.shape[4]
        lanes = tb.shape[4]
        me = self.z * self.width + self.e
        total = self.nz * self.width
        lane = lax.broadcasted_iota(jnp.int32, (8, lanes), 1)
        row = lax.broadcasted_iota(jnp.int32, (8, lanes), 0)
        gate_lanes = jnp.logical_and(row == 0, jnp.logical_or(lane == me, lane == total + me))
        rank_lane = jnp.logical_and(row == 1, lane == 2 * total + me)
        select = jnp.where(jnp.logical_or(gate_lanes, rank_lane), 1.0, 0.0).astype(BF16)
        slots = lax.broadcasted_iota(jnp.int32, (cap, length), 0).astype(F32)
        picks, gates = [], []
        for s in range(group):
            info = mm(select, tb[slot, s].reshape(length, lanes), 1, 1)
            hit = slots == info[1:2]
            pick = hit.astype(BF16)
            picks.append(pick)
            gate = jnp.sum(jnp.where(hit, info[0:1], 0.0), 1, keepdims=True)
            gates.append(gate)
            at = pl.ds(s * cap, cap)
            rowb[at, :] = mm(pick, xb[slot, s].reshape(length, width)).astype(BF16)
            cot = mm(pick, gb[slot, s].reshape(length, width))
            cotb[at, :] = cot.astype(BF16)
            downb[at, :] = (gate * cot).astype(BF16)
        for c in self.row_results(t):
            c.start()
        hook(1)
        gate_all = jnp.concatenate(gates, 0)
        rows = rowb[...]
        pre_gate = mm(rows, wg[...])
        pre_up = mm(rows, wu[...])
        sig = jax.nn.sigmoid(pre_gate)
        silu = pre_gate * sig
        self.free(t, self.hidden_results)
        actb[...] = (silu * pre_up).astype(BF16)
        hook(2)
        act_grad = mm(downb[...], wd[...], 1, 1)
        gpb[...] = (act_grad * pre_up * sig * (1.0 + pre_gate * (1.0 - sig))).astype(BF16)
        upb[...] = (act_grad * silu).astype(BF16)
        for c in self.hidden_results(t):
            c.start()
        gg = jnp.zeros((group * cap, 1), F32)
        for n in range(width // TILE):
            hook(3 + n)
            cols = pl.ds(n * TILE, TILE)
            self.free(t, lambda s: self.term_results(s, n, cols))
            out = mm(actb[...], wd[:, cols]).astype(BF16).astype(F32)
            gg = gg + jnp.sum(out * cotb[:, cols].astype(F32), 1, keepdims=True)
            out = (out * gate_all).astype(BF16)
            back = (mm(gpb[...], wg[cols, :], 1, 1) + mm(upb[...], wu[cols, :], 1, 1)).astype(BF16)
            for s in range(group):
                part = slice(s * cap, (s + 1) * cap)
                yb[s, :, cols] = mm(picks[s], out[part], 0, 0).astype(BF16)
                rb[s, :, cols] = mm(picks[s], back[part], 0, 0).astype(BF16)
            for c in self.term_results(t, n, cols):
                c.start()
        zz, first = self.place_of(t)
        first = zz * self.width + first
        for s in range(group):
            self.outs[2][first + s] = jnp.sum(
                picks[s].astype(F32) * gg[s * cap : (s + 1) * cap], 0, keepdims=True
            )

    def free(self, t, copies):
        @pl.when(t > 0)
        def _():
            for c in copies(t - 1):
                c.wait()

    def end(self):
        t = jnp.int32(len(self.orders[0]) - 1)
        for c in self.row_results(t) + self.hidden_results(t):
            c.wait()
        for n in range(self.bufs[13].shape[1] // TILE):
            for c in self.term_results(t, n, pl.ds(n * TILE, TILE)):
                c.wait()


def gather_expert_kernel(nz, cap, group, *refs):
    shards, all_grads, weights = refs[:2], refs[2], refs[3:6]
    gathered, outs = refs[6:8], refs[8:16]
    send, recv, local = refs[16:19]
    bufs, sems = refs[19:33], refs[33]
    z, e = place()
    greet(z, e, nz)
    g = Gather(nz, shards, gathered, send, recv, local)
    plain = tuple((j, h) for j in range(nz) for h in range(2))
    orders = ORDERS.get(nz) or (plain, plain)
    plans = RELAYS.get(nz) or (relays_first(g, orders[0]),) * 2
    w = ExpertWork(nz, cap, group, orders, gathered[0], gathered[1], all_grads, weights, outs, bufs, sems)
    w.begin()
    relays = {"L": g.launch_line, "K": g.launch_plane, "M": g.mates, "R": g.relay, "F": g.finish}

    def run(name, order):
        kind, j = name[0], int(name[1:])
        if kind == "I":
            place, half = order[j]
            (g.shared_far if half else g.shared_near)(place)
            if place == 0 and half == 0:
                g.kept()
            w.ready(j)
        else:
            relays[kind](j)

    def body(t, _):
        def hook(k):
            for plan, order, here in zip(plans, orders, (w.edge, jnp.logical_not(w.edge))):
                for piece, part, names in plan:
                    if part == k:
                        @pl.when(jnp.logical_and(t == piece, here))
                        def _():
                            for name in names.split():
                                run(name, order)

        w.step(t, hook)
        return 0

    lax.fori_loop(0, len(orders[0]), body, 0)
    w.end()
    for j in range(nz):
        g.drain(j, True)


def relays_first(g, order):
    head = []
    for f in g.steps():
        kind, j = f.func.__name__, f.args[0]
        names = {"launch": "L%d K%d", "mates": "M%d", "relay": "R%d", "finish": "F%d"}[kind]
        head.append((0, 0, names.replace("%d", str(j))))
    return head + [(p, 0, "I%d" % p) for p in range(len(order))]


ORDERS = {
    4: (
        ((0, 0), (1, 0), (0, 1), (1, 1), (2, 0), (2, 1), (3, 0), (3, 1)),
        ((0, 0), (1, 0), (0, 1), (2, 0), (1, 1), (3, 0), (2, 1), (3, 1)),
    )
}
RELAYS = {
    4: (
        (
            (0, 0, "L0 K0 M0"),
            (0, 0, "L1 K1 R0"),
            (0, 0, "I0"),
            (0, 1, "M1"),
            (0, 5, "R1"),
            (1, 0, "I1"),
            (1, 2, "F0"),
            (1, 4, "L2 K2 I2"),
            (2, 1, "F1"),
            (2, 2, "M2 I3"),
            (3, 2, "R2"),
            (3, 4, "I4"),
            (4, 1, "L3 K3"),
            (4, 2, "F2"),
            (4, 5, "I5 M3"),
            (5, 3, "R3"),
            (5, 5, "I6"),
            (6, 3, "F3"),
            (6, 6, "I7"),
        ),
        (
            (0, 0, "L0 K0 M0"),
            (0, 0, "L1 L2 K1"),
            (0, 0, "R0 K2 I0"),
            (0, 1, "M1 M2"),
            (0, 4, "R1"),
            (0, 6, "I1"),
            (1, 2, "F0"),
            (1, 4, "L3 K3 I2"),
            (2, 2, "M3"),
            (2, 3, "R2"),
            (2, 5, "I3"),
            (3, 2, "F1"),
            (3, 5, "I4"),
            (4, 4, "R3"),
            (4, 6, "I5"),
            (5, 2, "F2"),
            (5, 5, "I6"),
            (6, 1, "F3"),
            (6, 3, "I7"),
        ),
    )
}


def gather_with_experts(rows, table, all_grads, w_gate, w_up, w_down, cap, collective_id):
    nz, width = lax.axis_size("dp"), lax.axis_size("expert")
    devices, group = nz * width, 4
    length, model = rows.shape
    ff = w_gate.shape[1]
    quarter = length // 4
    shards = [a.reshape(4, quarter, a.shape[1]) for a in (rows, table)]
    step, picked = group * cap, devices * cap
    vmem = pl.BlockSpec(memory_space=pltpu.VMEM)
    hbm = pl.BlockSpec(memory_space=pl.ANY)
    block = lambda a: pltpu.VMEM((2, group) + a.shape, a.dtype)
    shape = lambda *dims: jax.ShapeDtypeStruct(dims, BF16)
    outs = pl.pallas_call(
        functools.partial(gather_expert_kernel, nz, cap, group),
        out_shape=[shape(nz, width, *s.shape) for s in shards]
        + [
            shape(nz, width, length, model),
            shape(nz, width, length, model),
            jax.ShapeDtypeStruct((devices, 1, length), F32),
            shape(picked, model),
            shape(picked, model),
            shape(picked, ff),
            shape(picked, ff),
            shape(picked, ff),
        ],
        in_specs=[vmem, vmem, hbm, hbm, hbm, hbm],
        out_specs=[hbm, hbm, hbm, hbm, vmem, hbm, hbm, hbm, hbm, hbm],
        scratch_shapes=gather_scratch(nz, 2)
        + [pltpu.VMEM(w.shape, BF16) for w in (w_gate, w_up, w_down)]
        + [block(shards[0]), block(shards[1]), block(shards[0])]
        + [pltpu.VMEM((group, length, model), BF16)] * 2
        + [pltpu.VMEM((step, n), BF16) for n in (model, model, ff, ff, ff, model)]
        + [pltpu.SemaphoreType.DMA((6, max(5, model // TILE)))],
        compiler_params=pltpu.CompilerParams(
            collective_id=collective_id, has_side_effects=True, vmem_limit_bytes=VMEM_LIMIT
        ),
        name="gather_experts",
    )(*shards, all_grads.reshape((nz, width) + shards[0].shape), w_gate, w_up, w_down)
    return outs[2:]


class Attention:
    def __init__(self, columns, hidden, w_mixed, w_out, small, head_map, tables, seg_col, seg_row, raw, normed, attended, branch, wide_gains,
                 gains, w_buf, o_buf, kv_buf, small_buf, mask, k_rot, v_low, sems):
        self.wide_gains = wide_gains
        self.columns, self.hidden, self.w_mixed, self.w_out = columns, hidden, w_mixed, w_out
        self.small, self.head_map, self.small_buf = small, head_map, small_buf
        self.tables, self.gains, self.seg_col, self.seg_row = tables, gains, seg_col, seg_row
        self.raw, self.normed, self.attended, self.branch = raw, normed, attended, branch
        self.w_buf, self.o_buf, self.kv_buf, self.mask = w_buf, o_buf, kv_buf, mask
        self.k_rot, self.v_low, self.sems = k_rot, v_low, sems
        self.cols = w_buf.shape[-1]
        self.query_cols = attended.shape[1]
        self.key_cols = kv_buf.shape[-1] // 2
        self.count = self.query_cols // self.cols
        self.per_key = self.count // (self.key_cols // HEAD_DIM)

    def fetch(self, t, slot):
        at = pl.ds(pl.multiple_of(t * self.cols, self.cols), self.cols)
        owners = self.o_buf.shape[1]
        blocks = self.w_out.shape[1] // owners
        return (
            pltpu.make_async_copy(self.w_mixed.at[:, :, :, :, at], self.w_buf.at[slot], self.sems.at[0, slot]),
            pltpu.make_async_copy(
                self.w_out.at[t // blocks, pl.ds(lax.rem(t, blocks) * owners, owners)], self.o_buf.at[slot], self.sems.at[1, slot]
            ),
        )

    def prepare(self):
        kv = pltpu.make_async_copy(
            self.w_mixed.at[:, :, :, :, pl.ds(self.query_cols, 2 * self.key_cols)], self.kv_buf, self.sems.at[2, 0]
        )
        small = pltpu.make_async_copy(self.small, self.small_buf, self.sems.at[2, 1])
        small.start()
        kv.start()
        for c in self.fetch(0, 0):
            c.start()
        values = self.hidden[...].astype(F32)
        scale = lax.rsqrt(jnp.mean(values * values, 1, keepdims=True) + EPS)
        small.wait()
        model, lanes = values.shape[1], self.small_buf.shape[-1]
        lane = lax.broadcasted_iota(jnp.int32, (8, lanes), 1)
        row = lax.broadcasted_iota(jnp.int32, (8, lanes), 0)
        select = jnp.zeros((8, lanes), F32)
        for k, column in enumerate(self.columns):
            select = jnp.where(jnp.logical_and(row == k, lane == column), 1.0, select)
        info = mm(select.astype(BF16), self.small_buf[...].reshape(model, lanes), 1, 1)
        self.normed[...] = (values * scale * info[0:1]).astype(BF16)
        self.wide_gains[...] = info
        self.gains[...] = mm(info.astype(BF16), self.head_map[...])
        self.branch[...] = jnp.zeros_like(self.branch)
        self.mask[...] = allowed_mask(self.seg_col, self.seg_row)
        kv.wait()
        self.raw[:, self.query_cols :] = mm(self.normed[...], self.kv_buf[...].reshape(model, 2 * self.key_cols))

    def step(self, t):
        slot = lax.rem(t, 2)

        @pl.when(t + 1 < self.count)
        def _():
            for c in self.fetch(t + 1, 1 - slot):
                c.start()

        for c in self.fetch(t, slot):
            c.wait()
        cosine, sine = self.tables[0], self.tables[1]

        @pl.when(lax.rem(t, self.per_key) == 0)
        def _():
            shift = pl.multiple_of(t // self.per_key * HEAD_DIM, HEAD_DIM)
            key = head_norm(self.raw[:, pl.ds(self.query_cols + shift, HEAD_DIM)], self.gains[2:3, :])
            self.k_rot[...] = rope(key, cosine, sine).astype(BF16)
            self.v_low[...] = self.raw[:, pl.ds(self.query_cols + self.key_cols + shift, HEAD_DIM)].astype(BF16)

        at = pl.ds(pl.multiple_of(t * self.cols, self.cols), self.cols)
        query_raw = mm(self.normed[...], self.w_buf[slot].reshape(self.normed.shape[1], self.cols))
        self.raw[:, at] = query_raw
        mask = self.mask[...] > 0.0
        k_rot, v_low = self.k_rot[...], self.v_low[...]
        outs = []
        for h in range(self.cols // HEAD_DIM):
            query = head_norm(query_raw[:, h * HEAD_DIM : (h + 1) * HEAD_DIM], self.gains[1:2, :])
            q_rot = rope(query, cosine, sine).astype(BF16)
            scores = mm(q_rot, k_rot, 1, 1) * (1.0 / math.sqrt(HEAD_DIM))
            raised = jnp.where(mask, jnp.exp(scores), 0.0)
            probs = (raised / jnp.sum(raised, 1, keepdims=True)).astype(BF16)
            outs.append(mm(probs, v_low).astype(BF16))
        out = jnp.concatenate(outs, 1)
        self.attended[:, at] = out
        self.branch[...] += mm(out, self.o_buf[slot].reshape(self.cols, self.normed.shape[1]))


def head_norm(raw, gain):
    return raw * lax.rsqrt(jnp.mean(raw * raw, 1, keepdims=True) + EPS) * gain


def allowed_mask(seg_col, seg_row):
    length = seg_col.shape[0]
    row = lax.broadcasted_iota(jnp.int32, (length, length), 0)
    col = lax.broadcasted_iota(jnp.int32, (length, length), 1)
    same = seg_col[...] == seg_row[...]
    return jnp.where(jnp.logical_and(same, col <= row), 1.0, 0.0)


def gather_attention_kernel(nz, plan, columns, *refs):
    shards, inputs = refs[:4], refs[4:9]
    gathered, outs = refs[9:13], refs[13:19]
    scratch = refs[19:]
    z, e = place()
    greet(z, e, nz)
    w = Gather(nz, shards[:3], gathered[:3], *scratch[:3])
    g = Gather(nz, shards[3:], gathered[3:], *scratch[3:6])
    hidden, head_map, tables, seg_col, seg_row = inputs
    a = Attention(columns, hidden, *gathered[:3], head_map, tables, seg_col, seg_row, *outs, *scratch[6:])
    first, steps = w.steps(), g.steps()
    for step in first[:-2]:
        step()
    steps[0]()
    first[-2]()
    steps[1]()
    first[-1]()
    for j in range(nz):
        w.shared_near(j)
        w.shared_far(j)
    w.kept()
    a.prepare()
    run_beside(a.count, a.step, steps[2:], plan)
    for j in range(nz):
        g.shared_near(j)
        g.shared_far(j)
    for j in range(nz):
        w.drain(j, True)
        g.drain(j)


def gather_with_attention(w_mixed, w_out, small, rows, columns, hidden, head_map, tables, segments, collective_id):
    nz, width = lax.axis_size("dp"), lax.axis_size("expert")
    length, model = hidden.shape
    shards = [a.reshape((4, a.shape[0] // 4) + a.shape[1:]) for a in (w_mixed, w_out, small, rows)]
    cols = 4 * HEAD_DIM
    mixed, query_cols = w_mixed.shape[1], w_out.shape[0] * nz * width
    owners = cols // w_out.shape[0]
    vmem = pl.BlockSpec(memory_space=pltpu.VMEM)
    hbm = pl.BlockSpec(memory_space=pl.ANY)
    lead = (nz, width) + shards[0].shape[:2]
    outs = pl.pallas_call(
        functools.partial(gather_attention_kernel, nz, [0, 0, 2, 1, 1, 1, 2, 2], columns),
        out_shape=[jax.ShapeDtypeStruct((nz, width) + s.shape, s.dtype) for s in shards]
        + [
            jax.ShapeDtypeStruct((length, mixed), F32),
            jax.ShapeDtypeStruct((length, model), BF16),
            jax.ShapeDtypeStruct((length, query_cols), BF16),
            jax.ShapeDtypeStruct((length, model), F32),
            jax.ShapeDtypeStruct((8, model), F32),
            jax.ShapeDtypeStruct((8, HEAD_DIM), F32),
        ],
        in_specs=[vmem] * 9,
        out_specs=[hbm] * 4 + [vmem] * 6,
        scratch_shapes=gather_scratch(nz, 3)
        + gather_scratch(nz, 1)
        + [
            pltpu.VMEM((2,) + lead + (cols,), BF16),
            pltpu.VMEM((2, owners) + shards[1].shape, BF16),
            pltpu.VMEM(lead + (mixed - query_cols,), BF16),
            pltpu.VMEM((nz, width) + shards[2].shape, BF16),
            pltpu.VMEM((length, length), F32),
            pltpu.VMEM((length, HEAD_DIM), BF16),
            pltpu.VMEM((length, HEAD_DIM), BF16),
            pltpu.SemaphoreType.DMA((3, 2)),
        ],
        compiler_params=pltpu.CompilerParams(
            collective_id=collective_id, has_side_effects=True, vmem_limit_bytes=VMEM_LIMIT
        ),
        name="gather_attention",
    )(*shards, hidden, head_map, tables, segments[:, None], segments[None, :])
    whole = [o.reshape((-1, o.shape[-1])) for o in outs[:4]]
    return whole + list(outs[4:])


class ExpertGrads:
    TILE = 256

    def __init__(self, rows, down, act, gate_pre, up_pre, grad_gate, grad_up, grad_down,
                 tile, gate_buf, up_buf, gate_stage, up_stage, sems):
        self.rows, self.down, self.act, self.gate_pre, self.up_pre = rows, down, act, gate_pre, up_pre
        self.grad_gate, self.grad_up, self.grad_down = grad_gate, grad_up, grad_down
        self.tile, self.gate_buf, self.up_buf = tile, gate_buf, up_buf
        self.gate_stage, self.up_stage, self.sems = gate_stage, up_stage, sems
        self.half = rows.shape[1] // self.TILE
        self.count = 2 * self.half

    def at(self, t):
        return pl.ds(pl.multiple_of(lax.rem(t, self.half) * self.TILE, self.TILE), self.TILE)

    def each(self, t, act):
        slot = lax.rem(t, 2)
        for source, here in ((self.rows, t < self.half), (self.down, t >= self.half)):
            @pl.when(here)
            def _():
                act(pltpu.make_async_copy(source.at[:, self.at(t)], self.tile.at[slot], self.sems.at[0, slot]))

    def hidden(self, source, buf, k):
        return pltpu.make_async_copy(source, buf, self.sems.at[1, k])

    def put(self, t, act):
        for out, here in ((self.grad_gate, t < self.half), (self.grad_down, t >= self.half)):
            @pl.when(here)
            def _():
                act(pltpu.make_async_copy(self.gate_stage, out.at[self.at(t), :], self.sems.at[2, 0]))

    def put_up(self, t):
        return pltpu.make_async_copy(self.up_stage, self.grad_up.at[self.at(t), :], self.sems.at[2, 1])

    def prepare(self):
        self.hidden(self.gate_pre, self.gate_buf, 0).start()
        self.hidden(self.up_pre, self.up_buf, 1).start()
        self.each(jnp.int32(0), lambda c: c.start())

    def step(self, t):
        slot = lax.rem(t, 2)

        @pl.when(t + 1 < self.count)
        def _():
            self.each(t + 1, lambda c: c.start())

        @pl.when(t == 0)
        def _():
            self.hidden(self.gate_pre, self.gate_buf, 0).wait()
            self.hidden(self.up_pre, self.up_buf, 1).wait()

        @pl.when(t == self.half)
        def _():
            copy = self.hidden(self.act, self.gate_buf, 0)
            copy.start()
            copy.wait()

        self.each(t, lambda c: c.wait())

        @pl.when(t > 0)
        def _():
            self.put(t - 1, lambda c: c.wait())

        self.gate_stage[...] = mm(self.tile[slot], self.gate_buf[...], 0, 0)
        self.put(t, lambda c: c.start())

        @pl.when(t < self.half)
        def _():
            @pl.when(t > 0)
            def _():
                self.put_up(t - 1).wait()

            self.up_stage[...] = mm(self.tile[slot], self.up_buf[...], 0, 0)
            self.put_up(t).start()

    def end(self):
        self.put(jnp.int32(self.count - 1), lambda c: c.wait())
        self.put_up(jnp.int32(self.half - 1)).wait()


def scatter_grads_kernel(nz, plan, count, *refs):
    terms, inputs = refs[:count], refs[count : count + 5]
    totals, outs = refs[count + 5 : 2 * count + 5], refs[2 * count + 5 : 2 * count + 8]
    scratch = refs[2 * count + 8 :]
    groups = [scratch[k * count : (k + 1) * count] for k in range(Scatter.BUFFERS)]
    rest = scratch[Scatter.BUFFERS * count :]
    z, e = place()
    greet(z, e, nz)
    s = Scatter(nz, terms, totals, *groups, *rest[:3])
    w = ExpertGrads(*inputs, *outs, *rest[3:])
    s.begin()
    w.prepare()
    run_beside(w.count, w.step, s.steps(), plan)
    w.end()
    for j in range(nz):
        s.drain(j)


def scatter_with_grads(arrays, rows, down, act, gate_pre, up_pre, collective_id):
    nz, width = lax.axis_size("dp"), lax.axis_size("expert")
    count, devices = len(arrays), nz * width
    terms = [a.reshape(nz, width, 4, a.shape[0] // (4 * devices), a.shape[1]) for a in arrays]
    shapes = [t.shape[3:] for t in terms]
    picked, model = rows.shape
    ff = act.shape[1]
    tile = ExpertGrads.TILE
    vmem = pl.BlockSpec(memory_space=pltpu.VMEM)
    hbm = pl.BlockSpec(memory_space=pl.ANY)
    plan = [3, 1, 0, 0, 0, 0, 3, 0, 0, 0, 0, 2] + [0] * 16
    outs = pl.pallas_call(
        functools.partial(scatter_grads_kernel, nz, plan, count),
        out_shape=[jax.ShapeDtypeStruct((4,) + s, F32) for s in shapes] + [jax.ShapeDtypeStruct((model, ff), F32)] * 3,
        in_specs=[hbm] * (count + 5),
        out_specs=[vmem] * count + [hbm] * 3,
        scratch_shapes=scatter_buffers(nz, width, [(s, a.dtype) for s, a in zip(shapes, arrays)])
        + [
            pltpu.VMEM((2, picked, tile), BF16),
            pltpu.VMEM((picked, ff), BF16),
            pltpu.VMEM((picked, ff), BF16),
            pltpu.VMEM((tile, ff), F32),
            pltpu.VMEM((tile, ff), F32),
            pltpu.SemaphoreType.DMA((3, 2)),
        ],
        compiler_params=pltpu.CompilerParams(
            collective_id=collective_id, has_side_effects=True, vmem_limit_bytes=VMEM_LIMIT
        ),
        name="scatter_grads",
    )(*terms, rows, down, act, gate_pre, up_pre)
    return [o.reshape(4 * s[0], s[1]) for o, s in zip(outs, shapes)] + list(outs[count:])


def pack_columns(columns, rows, lanes, dtype):
    parts = [c.astype(dtype) for c in columns]
    used = sum(c.shape[1] for c in parts)
    return jnp.concatenate(parts + [jnp.zeros((rows, lanes - used), dtype)], 1)


def per_device_gather(
    hidden_in,
    segment_ids,
    expert_ids,
    attn_gain,
    query_gain,
    key_gain,
    w_query,
    w_key,
    w_value,
    w_output,
    mlp_gain,
    w_router,
    w_gate,
    w_up,
    w_down,
    out_grad,
):
    devices = lax.axis_size(("dp", "expert"))
    me = lax.axis_index(("dp", "expert"))
    length, choices = expert_ids.shape
    width = hidden_in.shape[1]
    experts_total = devices
    capacity = 5 * length * choices // (4 * experts_total)
    query_cols, key_cols = w_query.shape[1], w_key.shape[1]
    rows = w_query.shape[0]
    head_rows = query_gain.shape[0]

    column = lambda v: jnp.pad(v, (0, rows - v.shape[0]))[:, None]
    lanes = 128 * pl.cdiv(experts_total + 4, 128)
    small = pack_columns(
        [w_router, column(attn_gain), column(mlp_gain), column(query_gain), column(key_gain)], rows, lanes, BF16
    )
    w_mixed = jnp.concatenate([w_query, w_key, w_value], 1)

    cosine_table, sine_table = rope_tables(jnp.arange(length) % TOK_DEV, HEAD_DIM)
    cosine, sine = cosine_table[:, 0], sine_table[:, 0]
    tables = jnp.stack([jnp.concatenate([cosine, cosine], 1), jnp.concatenate([-sine, sine], 1)])
    lane = jnp.arange(HEAD_DIM)
    head_map = (jnp.arange(width)[:, None] == (lane // head_rows * rows + lane % head_rows)[None, :]).astype(BF16)
    columns = (experts_total, experts_total + 2, experts_total + 3, experts_total + 1)
    w_mixed, w_out, small, all_grads, mixed, normed_attn, attended, branch, wide_gains, head_gains = gather_with_attention(
        w_mixed, w_output, small, out_grad, columns, hidden_in, head_map, tables, segment_ids, 3
    )
    router = small[:, :experts_total]
    attn_gain, mlp_gain = wide_gains[0], wide_gains[3]
    head_gains = head_gains[1:3]
    plain_in = hidden_in.astype(F32)
    inv_attn = rms_scale(plain_in)
    residual = plain_in + branch

    inv_mlp = rms_scale(residual)
    normed_mlp = (residual * inv_mlp * mlp_gain).astype(BF16)
    logits = jnp.dot(normed_mlp, router, preferred_element_type=F32)
    chosen = jnp.any(expert_ids[:, :, None] == jnp.arange(experts_total)[None, None, :], 1)
    raised = jnp.where(chosen, jnp.exp(logits), 0.0)
    gate = raised / jnp.sum(raised, -1, keepdims=True)
    position = jnp.arange(length)
    not_after = (position[None, :] <= position[:, None]).astype(BF16)
    rank = jnp.dot(not_after, chosen.astype(BF16), preferred_element_type=F32) - 1.0
    rank = jnp.where(chosen, rank, -1.0)
    gate_high = lax.reduce_precision(gate, 8, 7)
    table = pack_columns([gate_high, gate - gate_high, rank], length, 128 * pl.cdiv(3 * experts_total, 128), BF16)

    y_terms, r_terms, gate_terms, rows_in, down_in, act, gate_pre_grad, up_pre_grad = gather_with_experts(
        normed_mlp, table, all_grads, w_gate[0], w_up[0], w_down[0], capacity, 2
    )
    is_me = (jnp.arange(experts_total) == me).astype(F32)
    gate_terms = (gate_terms * is_me[None, :, None]).reshape(devices * experts_total, length)
    row_grad_sum, gate_grad, grad_w_gate, grad_w_up, grad_w_down = scatter_with_grads(
        [r_terms.reshape(devices * length, width), gate_terms], rows_in, down_in, act, gate_pre_grad, up_pre_grad, 4
    )
    grad_w_gate, grad_w_up, grad_w_down = grad_w_gate[None], grad_w_up[None], grad_w_down.T[None]

    gate_grad = gate_grad.T
    sel_grad = gate * (gate_grad - jnp.sum(gate * gate_grad, -1, keepdims=True))
    logit_grad = jnp.where(chosen, sel_grad, 0.0).astype(BF16)
    grad_w_router = jnp.dot(logit_grad.T, normed_mlp, preferred_element_type=F32)
    normed_mlp_grad = row_grad_sum + jnp.dot(logit_grad, router.T, preferred_element_type=F32)
    grad_mlp_gain = jnp.sum(normed_mlp_grad * residual * inv_mlp, 0)
    residual_grad = out_grad.astype(F32) + norm_grad(normed_mlp_grad, residual, inv_mlp, mlp_gain)

    branch_grad = residual_grad.astype(BF16)
    mixed_out, gain_grads, normed_attn_grad, grad_w_output, grad_w_mixed = scatter_with_attention(
        y_terms.reshape(devices * length, width), branch_grad, w_out, mixed, tables, head_gains, segment_ids,
        normed_attn, attended, w_mixed, 5,
    )
    block_out = residual + mixed_out
    grad_attn_gain = jnp.sum(normed_attn_grad * plain_in * inv_attn, 0)
    grad_in = residual_grad + norm_grad(normed_attn_grad, plain_in, inv_attn, attn_gain)

    head_rows_grad = jnp.dot(gain_grads, head_map.T.astype(F32), precision=lax.Precision.HIGHEST)
    small_rows = jnp.concatenate([grad_w_router, grad_attn_gain[None], grad_mlp_gain[None], head_rows_grad], 0)
    small_grads = jnp.pad(small_rows, ((0, lanes - small_rows.shape[0]), (0, 0))).T
    share_mixed, share_w_output, share_small = scatter_sum([grad_w_mixed, grad_w_output, small_grads], 6)
    return (
        block_out,
        grad_in,
        share_small[:, experts_total],
        share_small[:head_rows, experts_total + 2],
        share_small[:head_rows, experts_total + 3],
        share_mixed[:, :query_cols],
        share_mixed[:, query_cols : query_cols + key_cols],
        share_mixed[:, query_cols + key_cols :],
        share_w_output,
        share_small[:, experts_total + 1],
        share_small[:, :experts_total],
        grad_w_gate,
        grad_w_up,
        grad_w_down,
    )


def per_device(*arguments):
    expert_ids, w_gate = arguments[2], arguments[12]
    devices, width = lax.axis_size(("dp", "expert")), lax.axis_size("expert")
    length, choices = expert_ids.shape
    capacity = 5 * length * choices // (4 * devices)
    dense = devices <= 4 * choices and w_gate.shape[0] == 1 and width == 8
    if dense and capacity % 16 == 0 and devices % 4 == 0:
        return per_device_gather(*arguments)
    return per_device_exchange(*arguments)


def solution(mesh):
    in_specs = (
        P(("dp", "expert"), None),
        P(("dp", "expert")),
        P(("dp", "expert"), None),
        P(("dp", "expert")),
        P(("dp", "expert")),
        P(("dp", "expert")),
        P(("dp", "expert"), None),
        P(("dp", "expert"), None),
        P(("dp", "expert"), None),
        P(("dp", "expert"), None),
        P(("dp", "expert")),
        P(("dp", "expert"), None),
        P(("dp", "expert"), None, None),
        P(("dp", "expert"), None, None),
        P(("dp", "expert"), None, None),
        P(("dp", "expert"), None),
    )
    out_specs = (
        P(("dp", "expert"), None),
        P(("dp", "expert"), None),
        P(("dp", "expert")),
        P(("dp", "expert")),
        P(("dp", "expert")),
        P(("dp", "expert"), None),
        P(("dp", "expert"), None),
        P(("dp", "expert"), None),
        P(("dp", "expert"), None),
        P(("dp", "expert")),
        P(("dp", "expert"), None),
        P(("dp", "expert"), None, None),
        P(("dp", "expert"), None, None),
        P(("dp", "expert"), None, None),
    )
    return jax.shard_map(
        per_device, mesh=mesh, in_specs=in_specs, out_specs=out_specs, check_vma=False
    )
```
